32 devices in a mesh: gx: 2 (over x), gy: 1, gz: 16 (over z, y, core).
Axes of the slice: x: 2, y: 2, z: 4, core: 2. Of those that a mesh axis runs over, the one named last changes fastest.
Arguments:
- volume: bfloat16 [32, 64, 8, 256], P(None, 'gx', 'gy', 'gz'), may hold values from -6 to 6
- weight_a: bfloat16 [3, 3, 3, 32, 64], replicated, may hold values from -0.21875 to 0.21875
- bias_a: float32 [64], replicated, may hold values from -3 to 3
- weight_b: bfloat16 [3, 3, 3, 64, 128], replicated, may hold values from -0.15625 to 0.15625
- bias_b: float32 [128], replicated, may hold values from -3 to 3
- cotangent: bfloat16 [128, 32, 4, 128], P(None, ('gx', 'gz'), 'gy'), may hold values from -24 to 24
Outputs:
- features: bfloat16 [128, 32, 4, 128], P(None, ('gx', 'gz'), 'gy')
- grad_input: bfloat16 [32, 64, 8, 256], P(None, 'gx', 'gy', 'gz')
- grad_weight_a: float32 [3, 3, 3, 32, 64], replicated
- grad_bias_a: float32 [64], replicated
- grad_weight_b: float32 [3, 3, 3, 64, 128], replicated
- grad_bias_b: float32 [128], replicated
The draws below stay inside these ranges and needn't reach their ends.
All inputs are finite; a program needn't handle non-finite values.
Results may differ from the reference program's by a relative error of at most 0.012.
Values may be sent and summed in bfloat16 or wider, within the bound.
A program may use at most 128 MiB of HBM per device.

```python
import math
import jax
import jax.numpy as jnp
from jax import lax

C1 = 32
C2 = 64
C3 = 128
NX = 64
NY = 8
NZ = 256


def level_of(key, dims, shards, least, top_value):
    def one(axis_at, blocks):
        steps = jax.random.uniform(jax.random.fold_in(jax.random.fold_in(key, 6), axis_at), (blocks,), jnp.float32, least / len(shards), top_value / len(shards))
        return jnp.repeat(jnp.exp(steps), dims[axis_at] // blocks).reshape((-1,) + (1,) * (len(dims) - axis_at - 1))

    level = one(*shards[0])
    for cut in shards[1:]:
        level = level * one(*cut)
    return level


def centred(own_key, shape, deviation, limit, cuts=(), dtype=jnp.bfloat16):
    entries = deviation * jax.random.normal(own_key, shape, jnp.float32)
    if cuts:
        entries = entries * level_of(own_key, shape, cuts, -0.22, 0.18)
    return jnp.clip(entries, -limit, limit).astype(dtype)


def setup_inputs(seed: int = 0) -> dict:
    seeds = jax.random.split(jax.random.key(seed), 7)
    return {
        "volume": centred(seeds[0], (C1, NX, NY, NZ), 1.0, 6.0, ((1, 2), (3, 16))),
        "weight_a": centred(seeds[1], (3, 3, 3, C1, C2), (27 * C1) ** -0.5, 0.21875),
        "bias_a": centred(seeds[2], (C2,), 0.5, 3.0, (), jnp.float32),
        "weight_b": centred(seeds[3], (3, 3, 3, C2, C3), (27 * C2) ** -0.5, 0.15625),
        "bias_b": centred(seeds[4], (C3,), 0.5, 3.0, (), jnp.float32),
        "cotangent": centred(seeds[5], (C3, NX // 2, NY // 2, NZ // 2), 4.0, 24.0, ((1, 32),)),
    }


def activate(value):
    return value * jax.nn.sigmoid(value)

def slope_of(value):
    sigma = jax.nn.sigmoid(value)
    return sigma + value * sigma * (1.0 - sigma)

def conv_valid(padded, weight):
    result = lax.conv_general_dilated(padded[None], weight, (1, 1, 1), 'VALID', dimension_numbers=('NCDHW', 'DHWIO', 'NCDHW'), preferred_element_type=jnp.float32)
    return result[0]

def flipped(weight):
    return jnp.transpose(weight[::-1, ::-1, ::-1], (0, 1, 2, 4, 3))

def pad_all(field):
    return jnp.pad(field, ((0, 0), (1, 1), (1, 1), (1, 1)))

def average_pool(field):
    shape = field.shape
    split = field.reshape(shape[0], shape[1] // 2, 2, shape[2] // 2, 2, shape[3] // 2, 2)
    return lax.optimization_barrier(jnp.sum(split, axis=(2, 4, 6))) * 0.125

def spread_back(field):
    shape = field.shape
    larger = jnp.broadcast_to(field[:, :, None, :, None, :, None], (shape[0], shape[1], 2, shape[2], 2, shape[3], 2))
    return larger.reshape(shape[0], 2 * shape[1], 2 * shape[2], 2 * shape[3])

def weight_terms(padded, grad):
    width_in = padded.shape[0]
    width_out = grad.shape[0]
    extent = grad.shape[1:]
    flattened = grad.reshape(width_out, extent[0] * extent[1] * extent[2])
    products = []
    for first in range(3):
        for second in range(3):
            for third in range(3):
                window = padded[:, first:first + extent[0], second:second + extent[1], third:third + extent[2]]
                window = window.reshape(width_in, extent[0] * extent[1] * extent[2])
                products.append(lax.dot_general(window, flattened, (((1,), (1,)), ((), ())), preferred_element_type=jnp.float32))
    return jnp.stack(products).reshape(3, 3, 3, width_in, width_out)

def reference(volume, weight_a, bias_a, weight_b, bias_b, cotangent):
    scale_a = 1.0 / math.sqrt(NX * NY * NZ)
    scale_b = 1.0 / math.sqrt(NX * NY * NZ // 8)
    padded_a = pad_all(volume)
    before_a = conv_valid(padded_a, weight_a) + bias_a[:, None, None, None]
    pooled = average_pool(activate(before_a)).astype(jnp.bfloat16)
    padded_b = pad_all(pooled)
    before_b = conv_valid(padded_b, weight_b) + bias_b[:, None, None, None]
    features = activate(before_b).astype(jnp.bfloat16)
    grad_b = (cotangent.astype(jnp.float32) * slope_of(before_b)).astype(jnp.bfloat16)
    grad_weight_b = weight_terms(padded_b, grad_b) * scale_b
    grad_bias_b = lax.optimization_barrier(jnp.sum(grad_b.astype(jnp.float32), axis=(1, 2, 3))) * scale_b
    grad_pooled = conv_valid(pad_all(grad_b), flipped(weight_b)).astype(jnp.bfloat16)
    grad_a = (spread_back(grad_pooled.astype(jnp.float32)) * 0.125 * slope_of(before_a)).astype(jnp.bfloat16)
    grad_weight_a = weight_terms(padded_a, grad_a) * scale_a
    grad_bias_a = lax.optimization_barrier(jnp.sum(grad_a.astype(jnp.float32), axis=(1, 2, 3))) * scale_a
    grad_input = conv_valid(pad_all(grad_a), flipped(weight_a)).astype(jnp.bfloat16)
    return (features, grad_input, grad_weight_a, grad_bias_a, grad_weight_b, grad_bias_b)
```

```python
import functools
import math

import jax
import jax.numpy as jnp
from jax import lax
from jax.experimental import pallas as pl
from jax.experimental.pallas import tpu as pltpu
from jax.sharding import PartitionSpec as P

LINE = ("gx", "gz")
MESH = pl.DeviceIdType.MESH


def shared(block, axis, dim, width):
    count = lax.axis_size(axis)
    if count == 1:
        edge = jnp.zeros_like(lax.slice_in_dim(block, 0, width, axis=dim))
        return edge, edge
    forward = [(i, i + 1) for i in range(count - 1)]
    backward = [(target, source) for source, target in forward]
    last = block.shape[dim]
    low = lax.ppermute(lax.slice_in_dim(block, last - width, last, axis=dim), axis, forward)
    high = lax.ppermute(lax.slice_in_dim(block, 0, width, axis=dim), axis, backward)
    return low, high


def widened(flat, planes, rows, depth):
    low, high = shared(flat, LINE, 1, rows * depth)
    if lax.axis_size("gy") == 1:
        gap = jnp.zeros((flat.shape[0], depth), flat.dtype)
        pieces = [gap, low, gap]
        for plane in range(planes):
            pieces += [gap, flat[:, plane * rows * depth : (plane + 1) * rows * depth], gap]
        return jnp.concatenate(pieces + [gap, high, gap], axis=1)
    whole = jnp.concatenate([low, flat, high], axis=1)
    whole = whole.reshape(flat.shape[0], planes + 2, rows, depth)
    low, high = shared(whole, "gy", 2, 1)
    return jnp.concatenate([low, whole, high], axis=2).reshape(flat.shape[0], -1)


def slope_of(value):
    sigma = jax.nn.sigmoid(value)
    return sigma + value * sigma * (1.0 - sigma)


def put_windows(wide_ref, windows, planes, rows, depth):
    wide = wide_ref[...]
    width, extent = wide.shape
    place = lax.broadcasted_iota(jnp.int32, (width, extent), 1) % depth
    loose = wide.astype(jnp.float32)
    before = jnp.where(place == 0, 0.0, pltpu.roll(loose, 1, 1)).astype(jnp.bfloat16)
    after = jnp.where(place == depth - 1, 0.0, pltpu.roll(loose, extent - 1, 1)).astype(jnp.bfloat16)
    size = rows * depth
    for third, moved in enumerate((before, wide, after)):
        for first in range(3):
            for second in range(3):
                at = (first * 9 + second * 3 + third) * width
                for plane in range(planes):
                    begin = ((plane + first) * (rows + 2) + second) * depth
                    windows[at : at + width, plane * size : (plane + 1) * size] = moved[
                        :, begin : begin + size
                    ]


def dot_rows(left, right):
    return lax.dot_general(
        left, right, (((1,), (1,)), ((), ())), preferred_element_type=jnp.float32
    )


def forward_a_kernel(dims, wide_ref, weight_ref, bias_ref, pool_ref, before_ref, pooled_ref, windows):
    planes, rows, depth = dims
    put_windows(wide_ref, windows, *dims)
    before = jnp.dot(weight_ref[...], windows[...], preferred_element_type=jnp.float32)
    before = before + bias_ref[...]
    before_ref[...] = before
    active = before * jax.nn.sigmoid(before)
    size = rows * depth
    for row in range(rows // 2):
        parts = [
            active[:, plane * size + (2 * row + j) * depth : plane * size + (2 * row + j + 1) * depth]
            for plane in range(planes)
            for j in range(2)
        ]
        summed = sum(parts[1:], parts[0])
        paired = jnp.dot(
            summed, pool_ref[...], precision=lax.Precision.HIGHEST, preferred_element_type=jnp.float32
        )
        pooled_ref[:, row * depth // 2 : (row + 1) * depth // 2] = (paired * 0.125).astype(jnp.bfloat16)


def middle_kernel(dims, wide_ref, weight_ref, bias_ref, cot_ref, feat_ref, grad_ref, wb_ref, bb_ref, windows):
    put_windows(wide_ref, windows, *dims)
    before = jnp.dot(weight_ref[...], windows[...], preferred_element_type=jnp.float32)
    before = before + bias_ref[...]
    feat_ref[...] = (before * jax.nn.sigmoid(before)).astype(jnp.bfloat16)
    grad = (cot_ref[...].astype(jnp.float32) * slope_of(before)).astype(jnp.bfloat16)
    grad_ref[...] = grad
    wb_ref[...] = dot_rows(windows[...], grad)
    bb_ref[...] = dot_rows(jnp.ones((8, grad.shape[1]), jnp.bfloat16), grad)


def backward_b_kernel(dims, fine, wide_ref, weight_ref, before_ref, spread_ref, grad_ref, windows):
    put_windows(wide_ref, windows, *dims)
    pooled = jnp.dot(weight_ref[...], windows[...], preferred_element_type=jnp.float32)
    pooled = pooled.astype(jnp.bfloat16)
    planes, rows, depth = fine
    size = rows * depth
    for row in range(rows // 2):
        part = pooled[:, row * depth // 2 : (row + 1) * depth // 2]
        spread = jnp.dot(part, spread_ref[...], preferred_element_type=jnp.float32) * 0.125
        for plane in range(planes):
            for j in range(2):
                begin = plane * size + (2 * row + j) * depth
                slope = slope_of(before_ref[:, begin : begin + depth])
                grad_ref[:, begin : begin + depth] = (spread * slope).astype(jnp.bfloat16)


def weight_a_kernel(dims, wide_ref, grad_ref, wa_ref, ba_ref, windows):
    put_windows(wide_ref, windows, *dims)
    grad = grad_ref[...]
    wa_ref[...] = dot_rows(windows[...], grad)
    ba_ref[...] = dot_rows(jnp.ones((8, grad.shape[1]), jnp.bfloat16), grad)


def backward_a_kernel(dims, wide_ref, weight_ref, out_ref, windows):
    put_windows(wide_ref, windows, *dims)
    out = jnp.dot(weight_ref[...], windows[...], preferred_element_type=jnp.float32)
    out_ref[...] = out.astype(jnp.bfloat16)


def local_kernel(body, outs, windows, flops, *operands):
    moved = sum(x.size * x.dtype.itemsize for x in operands)
    return pl.pallas_call(
        body,
        out_shape=[jax.ShapeDtypeStruct(shape, dtype) for shape, dtype in outs],
        in_specs=[pl.BlockSpec(memory_space=pltpu.VMEM)] * len(operands),
        out_specs=[pl.BlockSpec(memory_space=pltpu.VMEM)] * len(outs),
        scratch_shapes=[pltpu.VMEM(windows, jnp.bfloat16)],
        compiler_params=pltpu.CompilerParams(vmem_limit_bytes=48 * 2**20),
        cost_estimate=pl.CostEstimate(flops=flops, bytes_accessed=moved, transcendentals=0),
    )(*operands)


def partner_of(axis, bit):
    me = lax.axis_index(axis)
    mine = (me // bit) % 2
    return me + bit * (1 - 2 * mine), mine


def sum_kernel(steps, halvings, rows, scales, wa_ref, ba_ref, wb_ref, bb_ref, *rest):
    out_wa, out_ba, out_wb, out_bb, acc, gathered, *scratch = rest
    half, width = wa_ref.shape[0] // 2, wa_ref.shape[1]
    top = wb_ref.shape[0]
    count = len(steps)
    sends = scratch[:count]
    recvs = scratch[count : 2 * count]
    sem_send, sem_recv = scratch[2 * count :]
    partners = [partner_of(axis, bit) for axis, bit in steps]
    barrier = pltpu.get_barrier_semaphore()
    for (axis, _), (partner, _) in zip(steps, partners):
        pl.semaphore_signal(barrier, inc=1, device_id={axis: partner}, device_id_type=MESH)
    acc[:top] = wb_ref[...]
    acc[top : top + half, :width] = wa_ref[:half]
    acc[top : top + half, width:] = wa_ref[half:]
    acc[top + half :] = jnp.zeros((rows - top - half, 128), jnp.float32)
    acc[top + half : top + half + 8, :width] = ba_ref[...]
    acc[top + half + 8 : top + half + 16] = bb_ref[...]
    pl.semaphore_wait(barrier, count)
    offset = 0
    size = rows
    kept = []
    for at, ((axis, _), (partner, mine)) in enumerate(zip(steps, partners)):
        source = acc
        if at < halvings:
            size = size // 2
            away = pl.multiple_of(offset + (1 - mine) * size, 16)
            offset = pl.multiple_of(offset + mine * size, 16)
        else:
            away = offset
        sends[at][...] = source[pl.ds(away, size)].astype(jnp.bfloat16)
        copy = pltpu.make_async_remote_copy(
            src_ref=sends[at],
            dst_ref=recvs[at],
            send_sem=sem_send.at[at],
            recv_sem=sem_recv.at[at],
            device_id={axis: partner},
            device_id_type=MESH,
        )
        copy.start()
        copy.wait()
        if at < halvings:
            acc[pl.ds(offset, size)] = source[pl.ds(offset, size)] + recvs[at][...].astype(jnp.float32)
            kept.append((offset, size))
        else:
            acc[pl.ds(offset, size)] = sends[at][...].astype(jnp.float32) + recvs[at][...].astype(jnp.float32)
    gathered[pl.ds(offset, size)] = acc[pl.ds(offset, size)].astype(jnp.bfloat16)
    for back in range(halvings):
        at = halvings - 1 - back
        begin, extent = kept[at]
        (axis, _), (partner, _) = steps[at], partners[at]
        here = gathered.at[pl.ds(begin, extent)]
        copy = pltpu.make_async_remote_copy(
            src_ref=here,
            dst_ref=here,
            send_sem=sem_send.at[count + back],
            recv_sem=sem_recv.at[count + back],
            device_id={axis: partner},
            device_id_type=MESH,
        )
        copy.start()
        copy.wait()
    scale_a, scale_b = scales
    total = gathered[...].astype(jnp.float32)
    out_wb[...] = total[:top] * scale_b
    out_wa[:half] = total[top : top + half, :width] * scale_a
    out_wa[half:] = total[top : top + half, width:] * scale_a
    out_ba[...] = total[top + half : top + half + 1, :width] * scale_a
    out_bb[...] = total[top + half + 8 : top + half + 9] * scale_b


def summed_grads(wa, ba, wb, bb, scales):
    used = wb.shape[0] + wa.shape[0] // 2 + 16
    rows = used + -used % 128
    cut = {
        axis: [2**i for i in range(lax.axis_size(axis).bit_length() - 1)] for axis in ("gz", "gx", "gy")
    }
    steps = [("gz", bit) for bit in cut["gz"][:1]]
    steps += [("gx", bit) for bit in cut["gx"]] + [("gy", bit) for bit in cut["gy"]]
    steps += [("gz", bit) for bit in cut["gz"][1:]]
    halvings = 0
    sizes = []
    size = rows
    for _ in steps:
        if len(sizes) == halvings and size % 32 == 0:
            size //= 2
            halvings += 1
        sizes.append(size)
    buffers = [pltpu.VMEM((s, 128), jnp.bfloat16) for s in sizes]
    total = len(steps) + halvings
    shapes = [wa.shape, (1, ba.shape[1]), wb.shape, (1, bb.shape[1])]
    return pl.pallas_call(
        functools.partial(sum_kernel, steps, halvings, rows, scales),
        out_shape=[jax.ShapeDtypeStruct(shape, jnp.float32) for shape in shapes],
        in_specs=[pl.BlockSpec(memory_space=pltpu.VMEM)] * 4,
        out_specs=[pl.BlockSpec(memory_space=pltpu.VMEM)] * 4,
        scratch_shapes=[
            pltpu.VMEM((rows, 128), jnp.float32),
            pltpu.VMEM((rows, 128), jnp.bfloat16),
            *buffers,
            *buffers,
            pltpu.SemaphoreType.DMA((total,)),
            pltpu.SemaphoreType.DMA((total,)),
        ],
        compiler_params=pltpu.CompilerParams(collective_id=0, has_side_effects=True),
    )(wa, ba, wb, bb)


def line_ends(axis_sizes):
    across, count = axis_sizes
    total = across * count
    line = lax.axis_index("gx") * count + lax.axis_index("gz")
    after, before = (line + 1) % total, (line + total - 1) % total
    ids = [{"gx": at // count, "gz": at % count} for at in (after, before)]
    return line, total, ids


class Halo:
    def __init__(self, wide, dims, where, sems, at):
        planes, rows, depth = dims
        self.line, self.total, ids = where
        size, stride = rows * depth, (rows + 2) * depth
        spot = lambda plane: wide.at[:, plane * stride + depth : plane * stride + depth + size]
        send, recv = sems
        self.up, self.down = [
            pltpu.make_async_remote_copy(
                src_ref=spot(source),
                dst_ref=spot(target),
                send_sem=send.at[at + i],
                recv_sem=recv.at[at + i],
                device_id=ids[i],
                device_id_type=MESH,
            )
            for i, (source, target) in enumerate(((planes, 0), (1, planes + 1)))
        ]

    def start(self):
        pl.when(self.line < self.total - 1)(self.up.start)
        pl.when(self.line > 0)(self.down.start)

    def wait(self):
        @pl.when(self.line < self.total - 1)
        def _():
            self.up.wait_send()
            self.down.wait_recv()

        @pl.when(self.line > 0)
        def _():
            self.down.wait_send()
            self.up.wait_recv()


class Summing:
    def __init__(self, steps, sizes, acc, gathered, sends, recvs, sems):
        self.steps, self.sizes = steps, sizes
        self.acc, self.gathered, self.sends, self.recvs = acc, gathered, sends, recvs
        self.sems = sems
        self.partners = [partner_of(axis, bit) for axis, bit in steps]
        rows = [acc.shape[0]] + list(sizes)
        self.halvings = sum(a != b for a, b in zip(rows, sizes))
        self.stages = len(steps) + self.halvings
        self.offset = 0
        self.kept = []
        self.flying = None

    def copy(self, stage, source, target, step):
        send, recv = self.sems
        self.flying = pltpu.make_async_remote_copy(
            src_ref=source,
            dst_ref=target,
            send_sem=send.at[stage],
            recv_sem=recv.at[stage],
            device_id={self.steps[step][0]: self.partners[step][0]},
            device_id_type=MESH,
        )
        self.flying.start()

    def start(self, stage):
        if stage < len(self.steps):
            size = self.sizes[stage]
            away = self.offset
            if stage < self.halvings:
                mine = self.partners[stage][1]
                away = pl.multiple_of(self.offset + (1 - mine) * size, 16)
                self.offset = pl.multiple_of(self.offset + mine * size, 16)
                self.kept.append((self.offset, size))
            self.sends[stage][...] = self.acc[pl.ds(away, size)].astype(jnp.bfloat16)
            self.copy(stage, self.sends[stage], self.recvs[stage], stage)
        else:
            step = self.halvings - 1 - (stage - len(self.steps))
            begin, size = self.kept[step]
            here = self.gathered.at[pl.ds(begin, size)]
            self.copy(stage, here, here, step)

    def finish(self, stage):
        self.flying.wait()
        if stage >= len(self.steps):
            return
        here = pl.ds(self.offset, self.sizes[stage])
        came = self.recvs[stage][...].astype(jnp.float32)
        own = self.acc[here] if stage < self.halvings else self.sends[stage][...].astype(jnp.float32)
        total = own + came
        if stage == len(self.steps) - 1:
            self.gathered[here] = total.astype(jnp.bfloat16)
        else:
            self.acc[here] = total


def place(wide, flat, dims):
    planes, rows, depth = dims
    size, stride = rows * depth, (rows + 2) * depth
    for plane in range(planes):
        begin = (plane + 1) * stride + depth
        wide[:, begin : begin + size] = flat[:, plane * size : (plane + 1) * size]


def whole_kernel(setting, *refs):
    fine, coarse, sizes_line, steps, cuts_a, cuts_b, scales = setting
    slab, w_a, b_a, pool, w_b, b_b, cot, v_b, spread, v_a = refs[:10]
    features, grad_slab, out_wa, out_ba, out_wb, out_bb = refs[10:16]
    wide_a, wide_b, wide_gb, wide_ga, win_a, win_b, win_gb, win_ga = refs[16:24]
    before_a, pooled, grad_b, grad_a, acc_a, acc_b, all_a, all_b = refs[24:32]
    count = len(steps)
    send_a, recv_a, send_b, recv_b = [refs[32 + i * count : 32 + (i + 1) * count] for i in range(4)]
    sems = refs[32 + 4 * count :]
    where = line_ends(sizes_line)
    line, total, ids = where
    barrier = pltpu.get_barrier_semaphore()
    for wide in (wide_a, wide_b, wide_gb, wide_ga):
        wide[...] = jnp.zeros_like(wide)
    place(wide_a, slab, fine)
    for axis, bit in steps:
        partner, _ = partner_of(axis, bit)
        pl.semaphore_signal(barrier, inc=1, device_id={axis: partner}, device_id_type=MESH)
    for device in ids:
        pl.semaphore_signal(barrier, inc=1, device_id=device, device_id_type=MESH)
    pl.semaphore_wait(barrier, count + 2)
    halos = [
        Halo(wide, dims, where, sems[:2], 2 * i)
        for i, (wide, dims) in enumerate(
            ((wide_a, fine), (wide_b, coarse), (wide_gb, coarse), (wide_ga, fine))
        )
    ]
    sum_a = Summing(steps, cuts_a, acc_a, all_a, send_a, recv_a, sems[2:4])
    sum_b = Summing(steps, cuts_b, acc_b, all_b, send_b, recv_b, sems[4:6])

    halos[0].start()
    halos[0].wait()
    forward_a_kernel(fine, wide_a, w_a, b_a, pool, before_a, pooled, win_a)
    place(wide_b, pooled, coarse)
    halos[1].start()
    halos[1].wait()
    top_b = out_wb.shape[0]
    middle_kernel(
        coarse, wide_b, w_b, b_b, cot, features, grad_b, acc_b.at[:top_b], acc_b.at[top_b : top_b + 8], win_b
    )
    place(wide_gb, grad_b, coarse)
    halos[2].start()
    acc_b[top_b + 8 :] = jnp.zeros((acc_b.shape[0] - top_b - 8, acc_b.shape[1]), jnp.float32)
    sum_b.start(0)
    halos[2].wait()
    backward_b_kernel(coarse, fine, wide_gb, v_b, before_a, spread, grad_a, win_gb)
    place(wide_ga, grad_a, fine)
    halos[3].start()
    sum_b.finish(0)
    sum_b.start(1)
    grad = grad_a[...]
    half, width = out_wa.shape[0] // 2, out_wa.shape[1]
    acc_a[:half, :width] = dot_rows(win_a[:half], grad)
    acc_a[:half, width:] = dot_rows(win_a[half:], grad)
    acc_a[half:] = jnp.zeros((acc_a.shape[0] - half, acc_a.shape[1]), jnp.float32)
    acc_a[half : half + 8, :width] = dot_rows(jnp.ones((8, grad.shape[1]), jnp.bfloat16), grad)
    sum_b.finish(1)
    sum_b.start(2)
    sum_a.start(0)
    halos[3].wait()
    backward_a_kernel(fine, wide_ga, v_a, grad_slab, win_ga)
    for stage in range(max(sum_a.stages, sum_b.stages - 2)):
        if stage + 2 < sum_b.stages:
            sum_b.finish(stage + 2)
            if stage + 3 < sum_b.stages:
                sum_b.start(stage + 3)
        if stage < sum_a.stages:
            sum_a.finish(stage)
            if stage + 1 < sum_a.stages:
                sum_a.start(stage + 1)
    scale_a, scale_b = scales
    out_wb[...] = all_b[:top_b].astype(jnp.float32) * scale_b
    out_bb[...] = all_b[top_b : top_b + 16].astype(jnp.float32)[:1] * scale_b
    out_wa[:half] = all_a[:half, :width].astype(jnp.float32) * scale_a
    out_wa[half:] = all_a[:half, width:].astype(jnp.float32) * scale_a
    out_ba[...] = all_a[half : half + 16, :width].astype(jnp.float32)[:1] * scale_a


def stage_sizes(rows, steps):
    sizes = []
    for _ in steps:
        halve = rows % 32 == 0 and len(sizes) < 3
        rows = rows // 2 if halve else rows
        sizes.append(rows)
    return sizes


def all_steps():
    cut = {
        axis: [2**i for i in range(lax.axis_size(axis).bit_length() - 1)] for axis in ("gz", "gx", "gy")
    }
    steps = [("gz", bit) for bit in cut["gz"][:1]]
    steps += [("gx", bit) for bit in cut["gx"]] + [("gy", bit) for bit in cut["gy"]]
    return steps + [("gz", bit) for bit in cut["gz"][1:]]


def between_exchanges(fine, coarse, scales, slab, weight_a, bias_a, weight_b, bias_b, cot, pool):
    f32, bf16 = jnp.float32, jnp.bfloat16
    c1, cells = slab.shape
    c2, c3 = weight_b.shape[3:]
    fewer = cells // 8
    steps = all_steps()
    rows_a = 27 * c1 // 2 + 16
    rows_a += -rows_a % 128
    rows_b = 27 * c2 + 16
    rows_b += -rows_b % 128
    cuts_a, cuts_b = stage_sizes(rows_a, steps), stage_sizes(rows_b, steps)
    extent = lambda dims: (dims[0] + 2) * (dims[1] + 2) * dims[2]
    setting = (fine, coarse, (lax.axis_size("gx"), lax.axis_size("gz")), steps, cuts_a, cuts_b, scales)
    buffers = [pltpu.VMEM((n, 128), bf16) for cuts in (cuts_a, cuts_a, cuts_b, cuts_b) for n in cuts]
    outs = [
        ((c3, fewer), bf16),
        ((c1, cells), bf16),
        ((27 * c1, c2), f32),
        ((1, c2), f32),
        ((27 * c2, c3), f32),
        ((1, c3), f32),
    ]
    operands = (
        slab,
        outward(weight_a),
        bias_a[:, None],
        pool,
        outward(weight_b),
        bias_b[:, None],
        cot,
        inward(weight_b),
        pool.T.astype(bf16),
        inward(weight_a),
    )
    most = 2 * len(steps)
    return pl.pallas_call(
        functools.partial(whole_kernel, setting),
        out_shape=[jax.ShapeDtypeStruct(shape, dtype) for shape, dtype in outs],
        in_specs=[pl.BlockSpec(memory_space=pltpu.VMEM)] * len(operands),
        out_specs=[pl.BlockSpec(memory_space=pltpu.VMEM)] * len(outs),
        scratch_shapes=[
            pltpu.VMEM((c1, extent(fine)), bf16),
            pltpu.VMEM((c2, extent(coarse)), bf16),
            pltpu.VMEM((c3, extent(coarse)), bf16),
            pltpu.VMEM((c2, extent(fine)), bf16),
            pltpu.VMEM((27 * c1, cells), bf16),
            pltpu.VMEM((27 * c2, fewer), bf16),
            pltpu.VMEM((27 * c3, fewer), bf16),
            pltpu.VMEM((27 * c2, cells), bf16),
            pltpu.VMEM((c2, cells), f32),
            pltpu.VMEM((c2, fewer), bf16),
            pltpu.VMEM((c3, fewer), bf16),
            pltpu.VMEM((c2, cells), bf16),
            pltpu.VMEM((rows_a, 128), f32),
            pltpu.VMEM((rows_b, 128), f32),
            pltpu.VMEM((rows_a, 128), bf16),
            pltpu.VMEM((rows_b, 128), bf16),
            *buffers,
            pltpu.SemaphoreType.DMA((8,)),
            pltpu.SemaphoreType.DMA((8,)),
            *[pltpu.SemaphoreType.DMA((most,))] * 4,
        ],
        compiler_params=pltpu.CompilerParams(
            collective_id=1, has_side_effects=True, vmem_limit_bytes=60 * 2**20
        ),
    )(*operands)


def outward(weight):
    return weight.reshape(-1, weight.shape[-1]).T


def inward(weight):
    taps = weight[::-1, ::-1, ::-1].reshape(27, *weight.shape[3:])
    return jnp.transpose(taps, (1, 0, 2)).reshape(weight.shape[3], -1)


def lanes_of(shape):
    return lax.broadcasted_iota(jnp.int32, shape, len(shape) - 1)


def rows_of(shape):
    return lax.broadcasted_iota(jnp.int32, shape, 0)


def ones_where(mask):
    return jnp.where(mask, 1.0, 0.0).astype(jnp.bfloat16)


def dot(left, right):
    return jnp.dot(left, right, preferred_element_type=jnp.float32)


def by_parts(rank_bits, mask):
    place = {}
    for at, (axis, bit) in enumerate(rank_bits):
        if mask >> at & 1:
            me = place.get(axis, lax.axis_index(axis))
            place[axis] = me + bit * (1 - 2 * ((lax.axis_index(axis) // bit) % 2))
    return place


def own_rank(rank_bits, mask=0):
    total = 0
    for at, (axis, bit) in enumerate(rank_bits):
        mine = (lax.axis_index(axis) // bit) % 2
        total = total + ((1 - mine) if mask >> at & 1 else mine) * 2**at
    return total


def remote(source, target, sems, at, device):
    return pltpu.make_async_remote_copy(
        src_ref=source,
        dst_ref=target,
        send_sem=sems[0].at[at],
        recv_sem=sems[1].at[at],
        device_id=device,
        device_id_type=MESH,
    )


class Reduction:
    def __init__(self, groups, acc, summed, sends, recvs, sems):
        self.groups, self.acc, self.summed = groups, acc, summed
        self.sends, self.recvs, self.sems = sends, recvs, sems
        self.offset, self.size = 0, acc.shape[0]
        self.kept = []
        self.flying = []
        self.used = 0
        self.stage = 0
        self.stages = 2 * len(groups) - 1

    def fly(self, source, target, device):
        copy = remote(source, target, self.sems, self.used, device)
        self.used += 1
        copy.start()
        self.flying.append(copy)

    def start(self):
        last = len(self.groups) - 1
        at = self.stage
        if at < last:
            bits = self.groups[at]
            members = 2 ** len(bits)
            part = self.size // members
            send, recv = self.sends[at], self.recvs[at]
            send[...] = self.acc[pl.ds(self.offset, self.size)].astype(jnp.bfloat16)
            for mask in range(1, members):
                begin = pl.multiple_of(own_rank(bits, mask) * part, 16)
                self.fly(send.at[pl.ds(begin, part)], recv.at[mask - 1], by_parts(bits, mask))
            self.kept.append((self.offset, self.size))
            self.offset = pl.multiple_of(self.offset + own_rank(bits) * part, 16)
            self.size = part
        elif at == last:
            bits = self.groups[at]
            recv = self.recvs[at]
            mine = own_rank(bits)
            recv[mine] = self.acc[pl.ds(self.offset, self.size)].astype(jnp.bfloat16)
            for mask in range(1, 2 ** len(bits)):
                self.fly(recv.at[mine], recv.at[mine], by_parts(bits, mask))
        else:
            bits = self.groups[2 * last - at]
            here = self.summed.at[pl.ds(self.offset, self.size)]
            for mask in range(1, 2 ** len(bits)):
                self.fly(here, here, by_parts(bits, mask))
            self.offset, self.size = self.kept.pop()

    def finish(self):
        last = len(self.groups) - 1
        at = self.stage
        for copy in self.flying:
            copy.wait()
        self.flying = []
        self.stage += 1
        if at > last:
            return
        recv = self.recvs[at]
        if at < last:
            here = pl.ds(self.offset, self.size)
            total = self.acc[here]
            for i in range(recv.shape[0]):
                total = total + recv[i].astype(jnp.float32)
            self.acc[here] = total
        else:
            total = recv[0].astype(jnp.float32)
            for i in range(1, recv.shape[0]):
                total = total + recv[i].astype(jnp.float32)
            self.summed[pl.ds(self.offset, self.size)] = total.astype(jnp.bfloat16)


class Border:
    def __init__(self, first, last, edge, inbox, sems, at):
        me, count = lax.axis_index("gz"), lax.axis_size("gz")
        side = 1 - lax.axis_index("gx")
        self.inner, self.outer = me > 0, me < count - 1
        up, down = (me + 1) % count, (me + count - 1) % count
        low, high, beside, beside_low, beside_high = inbox
        self.always = remote(edge, beside, sems, at + 2, {"gx": side})
        self.up = [
            remote(last, low, sems, at, {"gz": up}),
            remote(edge, beside_low, sems, at + 3, {"gx": side, "gz": up}),
        ]
        self.down = [
            remote(first, high, sems, at + 1, {"gz": down}),
            remote(edge, beside_high, sems, at + 4, {"gx": side, "gz": down}),
        ]

    def start(self):
        @pl.when(self.outer)
        def _():
            for copy in self.up:
                copy.start()

        @pl.when(self.inner)
        def _():
            for copy in self.down:
                copy.start()

        self.always.start()

    def wait(self):
        self.always.wait()

        @pl.when(self.outer)
        def _():
            for copy in self.up:
                copy.wait_send()
            for copy in self.down:
                copy.wait_recv()

        @pl.when(self.inner)
        def _():
            for copy in self.down:
                copy.wait_send()
            for copy in self.up:
                copy.wait_recv()


def gathered_edge(tiles, extent):
    shape = tiles[0].shape
    lane = lanes_of(shape)
    high = lax.axis_index("gx") == 0
    edge = jnp.where(high, extent - 1, 0)
    at_edge = lane % extent == edge
    total = None
    for i, tile in enumerate(tiles):
        kept = jnp.where(at_edge, tile, 0.0)
        kept = pltpu.roll(kept, i, 1) if i else kept
        total = kept if total is None else total + kept
    back = pltpu.roll(total, 128 - (extent - 1), 1)
    return jnp.where(high, back, total)


def rolled(value, by):
    by = by % 128
    return pltpu.roll(value, by, 1) if by else value


def beside(tile, edges, extent):
    low_edge, high_edge, at = edges
    lane = lanes_of(tile.shape)
    before = jnp.where(lane % extent == 0, rolled(low_edge, -at), rolled(tile, 1))
    after = jnp.where(lane % extent == extent - 1, rolled(high_edge, extent - 1 - at), rolled(tile, -1))
    return before, after


def sided(edge):
    high = lax.axis_index("gx") == 0
    return jnp.where(high, 0.0, edge), jnp.where(high, edge, 0.0)


def moved_rows(pair, stride):
    lane = lanes_of(pair[0].shape)
    down = [rolled(tile, stride) for tile in pair]
    up = [rolled(tile, -stride) for tile in pair]
    low = lane < stride
    high = lane < 128 - stride
    before = (jnp.where(low, 0.0, down[0]), jnp.where(low, down[0], down[1]))
    after = (jnp.where(high, up[0], up[1]), jnp.where(high, up[1], 0.0))
    return before, after


def moved_half(tile, stride):
    lane = lanes_of(tile.shape) % 64
    before = jnp.where(lane < stride, 0.0, rolled(tile, stride))
    after = jnp.where(lane < 64 - stride, rolled(tile, -stride), 0.0)
    return before, after


def inbox_values(inbox):
    low, high, across, across_low, across_high = [ref[...].astype(jnp.float32) for ref in inbox]
    return low, high, sided(across), sided(across_low), sided(across_high)


def fine_planes(read, inbox, planes):
    low, high, across, across_low, across_high = inbox_values(inbox)
    for p in range(planes + 2):
        if p == 0:
            pair, edge, at = (low[:, :128], low[:, 128:]), across_low, 2 * (planes - 1)
        elif p == planes + 1:
            pair, edge, at = (high[:, :128], high[:, 128:]), across_high, 0
        else:
            pair, edge, at = read(p - 1), across, 2 * (p - 1)
        sides = [beside(tile, (*edge, at + g), 32) for g, tile in enumerate(pair)]
        yield p, ((sides[0][0], sides[1][0]), pair, (sides[0][1], sides[1][1]))


def coarse_tiles(field, inbox, tiles):
    low, high, across, across_low, across_high = inbox_values(inbox)
    half = lanes_of(low.shape) < 64
    for t in range(tiles):
        tile = field[:, t * 128 : (t + 1) * 128].astype(jnp.float32)
        sides = list(beside(tile, (*across, t), 16))
        if t == 0:
            sides_low = beside(low, (*across_low, tiles - 1), 16)
            tile = jnp.where(half, low, tile)
            sides = [jnp.where(half, a, b) for a, b in zip(sides_low, sides)]
        if t == tiles - 1:
            sides_high = beside(high, (*across_high, 0), 16)
            tile = jnp.where(half, tile, high)
            sides = [jnp.where(half, b, a) for a, b in zip(sides_high, sides)]
        yield t, (sides[0], tile, sides[1])


def column(row, size):
    wide = jnp.broadcast_to(row, (size, size))
    eye = rows_of((size, size)) == lanes_of((size, size))
    return jnp.sum(jnp.where(eye, wide, 0.0), axis=1, keepdims=True)


def joined_thirds(terms, tiles):
    half = None
    low = [rolled(terms(0, t), 64) for t in range(tiles)]
    high = [rolled(terms(2, t), 64) for t in range(tiles)]
    out = []
    for t in range(tiles):
        if half is None:
            half = lanes_of(low[0].shape) < 64
        before, after = low[max(t - 1, 0)], high[min(t + 1, tiles - 1)]
        out.append(terms(1, t) + jnp.where(half, before + high[t], low[t] + after))
    return out


def block_kernel(setting, *refs):
    groups, scale_a = setting
    volume, w_a, b_a, w_b, b_b, cot = refs[:6]
    features, grad_in, out_wa, out_ba, sum_b = refs[6:11]
    (
        stage, own_a, windows_a, sums_a, slope_a, halves, pooled, windows_b, sums_b,
        cot_sent, cot_came, cot_here, grad_b, lines_b, sums_gb, grads_a, lines_a, sums_ga,
        feat_sent, feat_came, mat_a, mat_b, mat_ga, mat_gb, near, far, acc_a, acc_b, sum_a,
    ) = refs[11:40]
    rest = list(refs[40:])
    inboxes = [[rest.pop(0) for _ in range(5)] for _ in range(4)]
    edges = [rest.pop(0) for _ in range(4)]
    count = len(groups)
    send_a = [rest.pop(0) for _ in range(count - 1)]
    recv_a = [rest.pop(0) for _ in range(count)]
    send_b = [rest.pop(0) for _ in range(count - 1)]
    recv_b = [rest.pop(0) for _ in range(count)]
    sems_halo, sems_cot, sems_feat, sems_a, sems_b = [(rest.pop(0), rest.pop(0)) for _ in range(5)]
    f32, bf16 = jnp.float32, jnp.bfloat16
    c1, rows, planes, width = volume.shape
    c2, c3 = w_a.shape[2], w_b.shape[2]
    tiles = planes // 4 + 1
    me, members = lax.axis_index("gz"), lax.axis_size("gz")
    whole = [bit for group in groups for bit in group]
    line = [bit for bit in whole if bit[0] == "gz"]

    for inbox in inboxes:
        for box in inbox:
            box[...] = jnp.zeros_like(box)
    barrier = pltpu.get_barrier_semaphore()
    for mask in range(1, 2 ** len(whole)):
        pl.semaphore_signal(barrier, inc=1, device_id=by_parts(whole, mask), device_id_type=MESH)

    for g in range(2):
        for i in range(4):
            part = volume[:, 4 * g + i].astype(f32).reshape(c1 * planes, width)
            stage[:, width * i : width * (i + 1)] = part
        for z in range(planes):
            tile = stage[pl.ds(z, c1, stride=planes), :]
            own_a[:, z * 256 + g * 128 : z * 256 + (g + 1) * 128] = tile.astype(bf16)

    def read_a(z):
        return tuple(own_a[:, z * 256 + g * 128 : z * 256 + (g + 1) * 128].astype(f32) for g in range(2))

    edges[0][...] = gathered_edge([tile for z in range(planes) for tile in read_a(z)], 32).astype(bf16)
    r, l = rows_of(far.shape), lanes_of(far.shape)
    far[...] = ones_where(((r >> 3) & 3 == l >> 7) & (((r >> 5) << 3) + (r & 7) == l & 127))
    cot_sent[...] = dot_rows(far[...], cot[...]).astype(bf16)
    pl.semaphore_wait(barrier, 2 ** len(whole) - 1)

    border_a = Border(own_a.at[:, :256], own_a.at[:, (planes - 1) * 256 :], edges[0], inboxes[0], sems_halo, 0)
    border_a.start()

    def exchange(sent, came, sems):
        flying = []
        size = sent.shape[0] // members
        for mask in range(1, members):
            begin = pl.multiple_of(own_rank(line, mask) * size, 16)
            copy = remote(
                sent.at[pl.ds(begin, size)],
                came.at[pl.ds(pl.multiple_of(me * size, 16), size)],
                sems,
                mask - 1,
                by_parts(line, mask),
            )
            copy.start()
            flying.append(copy)
        here = pl.ds(pl.multiple_of(me * size, 16), size)
        came[here] = sent[here]
        return flying

    cot_flying = exchange(cot_sent, cot_came, sems_cot)

    eye = ones_where(rows_of((c2, c2)) == lanes_of((c2, c2)))
    eye_b = ones_where(rows_of((c3, c3)) == lanes_of((c3, c3)))
    for kz in range(3):
        block = w_a[:].reshape(9, 3, c1, c2)[:, kz].reshape(9 * c1, c2)
        mat_a[kz * c2 : (kz + 1) * c2] = dot_rows(eye, block).astype(bf16)
        block = w_b[:].reshape(9, 3, c2, c3)[:, kz].reshape(9 * c2, c3)
        mat_b[kz * c3 : (kz + 1) * c3] = dot_rows(eye_b, block).astype(bf16)
        for ky in range(3):
            for kx in range(3):
                tap = ((2 - kx) * 3 + 2 - ky) * 3 + 2 - kz
                at = kz * 3 + ky
                mat_ga[at * c1 : (at + 1) * c1, kx * c2 : (kx + 1) * c2] = w_a[tap]
                mat_gb[at * c2 : (at + 1) * c2, kx * c3 : (kx + 1) * c3] = w_b[tap]
    col_a, col_b = column(b_a[...], c2), column(b_b[...], c3)
    r, l = rows_of(near.shape), lanes_of(near.shape)
    near[...] = ones_where(
        ((r & 7) + 1 == l >> 6) & ((r >> 3) & 3 == (l >> 4) & 3) & (r >> 5 == l & 15)
    )
    r, l = rows_of((512, 128)), lanes_of((512, 128))
    pool = ones_where(
        (r >> 8 == l >> 6) & ((r >> 6) & 3 == (l >> 4) & 3) & ((r & 31) >> 1 == l & 15)
    )
    halves[...] = jnp.zeros_like(halves)
    for kz in range(3):
        for p in range(planes + 2):
            if not 0 <= p + kz - 2 < planes:
                grads_a[kz * c2 : (kz + 1) * c2, p * 256 : (p + 1) * 256] = jnp.zeros((c2, 256), bf16)
    acc_a[...] = jnp.zeros_like(acc_a)
    border_a.wait()

    for p, thirds in fine_planes(read_a, inboxes[0], planes):
        for kx, pair in enumerate(thirds):
            before, after = moved_rows(pair, 32)
            for ky, (first, second) in enumerate((before, pair, after)):
                at = (kx * 3 + ky) * c1
                windows_a[at : at + c1, p * 256 : p * 256 + 128] = first.astype(bf16)
                windows_a[at : at + c1, p * 256 + 128 : (p + 1) * 256] = second.astype(bf16)
    step = 3 * 256
    for begin in range(0, windows_a.shape[1], step):
        sums_a[:, begin : begin + step] = dot(mat_a[...], windows_a[:, begin : begin + step])
    for z in range(planes):
        value = (
            sums_a[:c2, z * 256 : (z + 1) * 256]
            + sums_a[c2 : 2 * c2, (z + 1) * 256 : (z + 2) * 256]
            + sums_a[2 * c2 :, (z + 2) * 256 : (z + 3) * 256]
            + col_a
        )
        sigma = jax.nn.sigmoid(value)
        active = value * sigma
        slope_a[:, z * 256 : (z + 1) * 256] = (sigma + active * (1.0 - sigma)) * 0.125
        if z % 2:
            active = active + kept
            pz = z // 2 + 1
            upper = active.astype(bf16)
            lower = (active - upper.astype(f32)).astype(bf16)
            at, lane = pz // 2 * c2, pz % 2 * 256
            halves[at : at + c2, lane : lane + 256] = upper
            halves[tiles * c2 + at : tiles * c2 + at + c2, lane : lane + 256] = lower
        else:
            kept = active
    both = dot(halves[...], pool)
    both = (both[: tiles * c2] + both[tiles * c2 :]) * 0.125
    for t in range(tiles):
        pooled[:, t * 128 : (t + 1) * 128] = both[t * c2 : (t + 1) * c2].astype(bf16)

    def coarse_edge(field):
        return gathered_edge([field[:, t * 128 : (t + 1) * 128].astype(f32) for t in range(tiles)], 16)

    edges[1][...] = coarse_edge(pooled).astype(bf16)
    last = (tiles - 1) * 128
    border_b = Border(pooled.at[:, :128], pooled.at[:, last:], edges[1], inboxes[1], sems_halo, 5)
    border_b.start()
    for copy in cot_flying:
        copy.wait()
    came = jnp.transpose(cot_came[...].astype(f32)).astype(bf16)
    cot_here[...] = dot(came, near[...])
    border_b.wait()

    for t, thirds in coarse_tiles(pooled, inboxes[1], tiles):
        for kx, tile in enumerate(thirds):
            before, after = moved_half(tile, 16)
            for ky, value in enumerate((before, tile, after)):
                at = (kx * 3 + ky) * c2
                windows_b[at : at + c2, t * 128 : (t + 1) * 128] = value.astype(bf16)
    sums_b[...] = dot(mat_b[...], windows_b[...])
    joined = joined_thirds(lambda k, t: sums_b[k * c3 : (k + 1) * c3, t * 128 : (t + 1) * 128], tiles)
    feats = []
    for t, value in enumerate(joined):
        value = value + col_b
        sigma = jax.nn.sigmoid(value)
        active = value * sigma
        feats.append(active.astype(bf16))
        slope = sigma + active * (1.0 - sigma)
        grad = cot_here[:, t * 128 : (t + 1) * 128] * slope
        grad_b[c3 : 2 * c3, t * 128 : (t + 1) * 128] = grad.astype(bf16)
    own_gb = grad_b.at[c3 : 2 * c3]
    edges[2][...] = coarse_edge(own_gb).astype(bf16)
    border_gb = Border(own_gb.at[:, :128], own_gb.at[:, last:], edges[2], inboxes[2], sems_halo, 10)
    border_gb.start()

    half = lanes_of((c3, 128)) < 64
    turned = [rolled(own_gb[:, t * 128 : (t + 1) * 128].astype(f32), 64) for t in range(tiles)]
    zero = jnp.zeros_like(turned[0])
    for t in range(tiles):
        later = turned[t + 1] if t + 1 < tiles else zero
        earlier = turned[t - 1] if t else zero
        here = slice(t * 128, (t + 1) * 128)
        grad_b[:c3, here] = jnp.where(half, turned[t], later).astype(bf16)
        grad_b[2 * c3 :, here] = jnp.where(half, earlier, turned[t]).astype(bf16)
    terms = dot_rows(windows_b[...], grad_b[...])
    for at in range(9):
        for kz in range(3):
            tap = at * 3 + kz
            acc_b[tap * c2 : (tap + 1) * c2] = terms[at * c2 : (at + 1) * c2, kz * c3 : (kz + 1) * c3]
    top = 27 * c2
    acc_b[top:] = jnp.zeros((acc_b.shape[0] - top, c3), f32)
    acc_b[top : top + 8] = dot_rows(jnp.ones((8, tiles * 128), bf16), own_gb[...])
    total_b = Reduction(groups, acc_b, sum_b, send_b, recv_b, sems_b)
    total_b.start()
    feat_sent[...] = dot_rows(near[...], jnp.concatenate(feats, axis=1)).astype(bf16)
    feat_flying = exchange(feat_sent, feat_came, sems_feat)
    border_gb.wait()

    for t, thirds in coarse_tiles(own_gb, inboxes[2], tiles):
        for kx, tile in enumerate(thirds):
            lines_b[kx * c3 : (kx + 1) * c3, t * 128 : (t + 1) * 128] = tile.astype(bf16)
    sums_gb[...] = dot(mat_gb[...], lines_b[...])
    total_b.finish()
    total_b.start()
    by_row = [
        joined_thirds(
            lambda k, t: sums_gb[(k * 3 + ky) * c2 : (k * 3 + ky + 1) * c2, t * 128 : (t + 1) * 128], tiles
        )
        for ky in range(3)
    ]
    small = []
    for t in range(tiles):
        value = by_row[1][t] + moved_half(by_row[0][t], 16)[0] + moved_half(by_row[2][t], 16)[1]
        small.append(value.astype(bf16))
    spread = dot_rows(jnp.concatenate(small, axis=0), pool)
    for z in range(planes):
        pz = z // 2 + 1
        large = spread[pz // 2 * c2 : (pz // 2 + 1) * c2, pz % 2 * 256 : (pz % 2 + 1) * 256]
        grad = (large * slope_a[:, z * 256 : (z + 1) * 256]).astype(bf16)
        for kz in range(3):
            grads_a[kz * c2 : (kz + 1) * c2, (z + kz) * 256 : (z + kz + 1) * 256] = grad

    own_ga = grads_a.at[c2 : 2 * c2]

    def read_ga(z):
        return tuple(
            own_ga[:, (z + 1) * 256 + g * 128 : (z + 1) * 256 + (g + 1) * 128].astype(f32) for g in range(2)
        )

    edges[3][...] = gathered_edge([tile for z in range(planes) for tile in read_ga(z)], 32).astype(bf16)
    border_ga = Border(
        own_ga.at[:, 256:512], own_ga.at[:, planes * 256 : (planes + 1) * 256], edges[3], inboxes[3], sems_halo, 15
    )
    border_ga.start()

    terms = dot_rows(windows_a[...], grads_a[...])
    deep = 9 * c1
    acc_a[:deep] = terms[:, : 2 * c2]
    acc_a[deep : deep + deep // 2, :c2] = terms[: deep // 2, 2 * c2 :]
    acc_a[deep : deep + deep // 2, c2:] = terms[deep // 2 :, 2 * c2 :]
    top_a = deep + deep // 2
    acc_a[top_a : top_a + 8, :c2] = dot_rows(jnp.ones((8, planes * 256), bf16), own_ga[:, 256 : (planes + 1) * 256])
    total_a = Reduction(groups, acc_a, sum_a, send_a, recv_a, sems_a)
    total_a.start()
    total_b.finish()
    total_b.start()
    border_ga.wait()

    for p, thirds in fine_planes(read_ga, inboxes[3], planes):
        for kx, pair in enumerate(thirds):
            for g, tile in enumerate(pair):
                at = p * 256 + g * 128
                lines_a[kx * c2 : (kx + 1) * c2, at : at + 128] = tile.astype(bf16)
    total_a.finish()
    total_a.start()
    for begin in range(0, lines_a.shape[1], step):
        sums_ga[:, begin : begin + step] = dot(mat_ga[...], lines_a[:, begin : begin + step])
    total_b.finish()
    total_b.start()
    for copy in feat_flying:
        copy.wait()
    came = jnp.transpose(feat_came[...].astype(f32)).astype(bf16)
    features[...] = dot(came, far[...]).astype(bf16)
    total_a.finish()
    total_a.start()
    results = []
    for z in range(planes):
        by_row = []
        for ky in range(3):
            value = None
            for kz in range(3):
                at = (kz * 3 + ky) * c1
                term = sums_ga[at : at + c1, (z + kz) * 256 : (z + kz + 1) * 256]
                value = term if value is None else value + term
            by_row.append((value[:, :128], value[:, 128:]))
        before, after = moved_rows(by_row[0], 32)[0], moved_rows(by_row[2], 32)[1]
        results.append([by_row[1][g] + before[g] + after[g] for g in range(2)])
    for g in range(2):
        for z in range(planes):
            stage[pl.ds(z, c1, stride=planes), :] = results[z][g]
        for i in range(4):
            part = stage[:, width * i : width * (i + 1)].astype(bf16)
            grad_in[:, 4 * g + i] = part.reshape(c1, planes, width)

    while total_b.stage < total_b.stages or total_a.stage < total_a.stages:
        for total in (total_b, total_a):
            if total.stage < total.stages:
                total.finish()
                if total.stage < total.stages:
                    total.start()
    for at in range(9):
        here = slice(at * c1, (at + 1) * c1)
        pair = sum_a[here].astype(f32) * scale_a
        low = at * c1 - (0 if at * c1 < deep // 2 else deep // 2)
        out_wa[at * 3] = pair[:, :c2]
        out_wa[at * 3 + 1] = pair[:, c2:]
    last_rows = sum_a[deep : deep + deep // 2].astype(f32) * scale_a
    thirds = jnp.concatenate([last_rows[:, :c2], last_rows[:, c2:]], axis=0)
    for at in range(9):
        out_wa[at * 3 + 2] = thirds[at * c1 : (at + 1) * c1]
    out_ba[...] = sum_a[top_a : top_a + 16].astype(f32)[:1, :c2] * scale_a


def all_groups():
    cut = {axis: [2**i for i in range(lax.axis_size(axis).bit_length() - 1)] for axis in ("gz", "gx")}
    line = [("gz", bit) for bit in cut["gz"]]
    return [line[:1], [("gx", bit) for bit in cut["gx"]] + line[1:2], line[2:]]


def on_blocks(volume, weight_a, bias_a, weight_b, bias_b, cotangent, scales):
    f32, bf16 = jnp.float32, jnp.bfloat16
    c1, width, rows, planes = volume.shape
    c2, c3 = weight_b.shape[3:]
    members = lax.axis_size("gz")
    groups = all_groups()
    tiles = planes // 4 + 1
    long, short = (planes + 2) * 256, tiles * 128
    cells = planes * 256
    rows_a, rows_b = 512, 27 * c2 + 64
    fewer = cells // 8

    def buffers(total):
        sends, recvs = [], []
        size = total
        for group in groups[:-1]:
            n = 2 ** len(group)
            sends.append(pltpu.VMEM((size, 128), bf16))
            size //= n
            recvs.append(pltpu.VMEM((n - 1, size, 128), bf16))
        recvs.append(pltpu.VMEM((2 ** len(groups[-1]), size, 128), bf16))
        return sends + recvs

    inboxes = []
    for channels, plane in ((c1, 256), (c2, 128), (c3, 128), (c2, 256)):
        inboxes += [pltpu.VMEM((channels, plane), bf16)] * 2 + [pltpu.VMEM((channels, 128), bf16)] * 3
    count = 2 * sum(2 ** len(group) - 1 for group in groups[:-1]) + 2 ** len(groups[-1]) - 1
    outs = [
        ((c3, fewer), bf16),
        ((c1, rows, planes, width), bf16),
        ((27, c1, c2), f32),
        ((1, c2), f32),
        ((rows_b, c3), bf16),
    ]
    operands = (
        jnp.transpose(volume, (0, 2, 3, 1)),
        weight_a.reshape(27, c1, c2),
        bias_a[None],
        weight_b.reshape(27, c2, c3),
        bias_b[None],
        cotangent.reshape(c3, fewer),
    )
    features, grad_in, sum_wa, sum_ba, sum_b = pl.pallas_call(
        functools.partial(block_kernel, (groups, scales[0])),
        out_shape=[jax.ShapeDtypeStruct(shape, dtype) for shape, dtype in outs],
        in_specs=[pl.BlockSpec(memory_space=pltpu.VMEM)] * len(operands),
        out_specs=[pl.BlockSpec(memory_space=pltpu.VMEM)] * len(outs),
        scratch_shapes=[
            pltpu.VMEM((c1 * planes, 128), f32),
            pltpu.VMEM((c1, cells), bf16),
            pltpu.VMEM((9 * c1, long), bf16),
            pltpu.VMEM((3 * c2, long), f32),
            pltpu.VMEM((c2, cells), f32),
            pltpu.VMEM((2 * tiles * c2, 512), bf16),
            pltpu.VMEM((c2, short), bf16),
            pltpu.VMEM((9 * c2, short), bf16),
            pltpu.VMEM((3 * c3, short), f32),
            pltpu.VMEM((fewer, c3), bf16),
            pltpu.VMEM((fewer, c3), bf16),
            pltpu.VMEM((c3, short), f32),
            pltpu.VMEM((3 * c3, short), bf16),
            pltpu.VMEM((3 * c3, short), bf16),
            pltpu.VMEM((9 * c2, short), f32),
            pltpu.VMEM((3 * c2, long), bf16),
            pltpu.VMEM((3 * c2, long), bf16),
            pltpu.VMEM((9 * c1, long), f32),
            pltpu.VMEM((fewer, c3), bf16),
            pltpu.VMEM((fewer, c3), bf16),
            pltpu.VMEM((3 * c2, 9 * c1), bf16),
            pltpu.VMEM((3 * c3, 9 * c2), bf16),
            pltpu.VMEM((9 * c1, 3 * c2), bf16),
            pltpu.VMEM((9 * c2, 3 * c3), bf16),
            pltpu.VMEM((fewer, short), bf16),
            pltpu.VMEM((fewer, fewer), bf16),
            pltpu.VMEM((rows_a, 128), f32),
            pltpu.VMEM((rows_b, 128), f32),
            pltpu.VMEM((rows_a, 128), bf16),
            *inboxes,
            *[pltpu.VMEM((channels, 128), bf16) for channels in (c1, c2, c3, c2)],
            *buffers(rows_a),
            *buffers(rows_b),
            *[pltpu.SemaphoreType.DMA((20,))] * 2,
            *[pltpu.SemaphoreType.DMA((members - 1,))] * 4,
            *[pltpu.SemaphoreType.DMA((count,))] * 4,
        ],
        compiler_params=pltpu.CompilerParams(
            collective_id=2, has_side_effects=True, vmem_limit_bytes=60 * 2**20
        ),
    )(*operands)
    total_b = sum_b[: 27 * c2 + 1].astype(f32) * scales[1]
    return (
        features.reshape(cotangent.shape),
        jnp.transpose(grad_in, (0, 3, 1, 2)),
        sum_wa.reshape(weight_a.shape),
        sum_ba.reshape(c2),
        total_b[: 27 * c2].reshape(weight_b.shape),
        total_b[27 * c2],
    )


def fits_blocks(volume, weight_b):
    c1, width, rows, planes = volume.shape
    sizes = {axis: lax.axis_size(axis) for axis in ("gx", "gy", "gz")}
    return (
        sizes == {"gx": 2, "gy": 1, "gz": planes}
        and (width, rows, planes) == (32, 8, 16)
        and (c1, *weight_b.shape[3:]) == (32, 64, 128)
    )


def on_device(volume, weight_a, bias_a, weight_b, bias_b, cotangent):
    f32, bf16 = jnp.float32, jnp.bfloat16
    count = lax.axis_size("gz")
    devices_all = lax.axis_size("gx") * lax.axis_size("gy") * count
    c1, nx, rows, nz = volume.shape
    cells = nx * rows * nz
    scale_a = 1.0 / math.sqrt(cells * devices_all)
    scale_b = 1.0 / math.sqrt(cells * devices_all // 8)
    c2, c3 = weight_b.shape[3:]
    if fits_blocks(volume, weight_b):
        return on_blocks(volume, weight_a, bias_a, weight_b, bias_b, cotangent, (scale_a, scale_b))
    planes, depth = nx // count, nz * count
    fine = (planes, rows, depth)
    coarse = (planes // 2, rows // 2, depth // 2)
    fewer = cells // 8
    pool = (jnp.arange(depth)[:, None] // 2 == jnp.arange(depth // 2)[None]).astype(f32)
    work_a = 2 * 27 * c1 * c2 * cells
    work_b = 2 * 27 * c2 * c3 * fewer

    slab = lax.all_to_all(volume, "gz", split_axis=1, concat_axis=3, tiled=True).reshape(c1, cells)
    if lax.axis_size("gy") == 1:
        features, grad_slab, sum_wa, sum_ba, sum_wb, sum_bb = between_exchanges(
            fine,
            coarse,
            (scale_a, scale_b),
            slab,
            weight_a,
            bias_a,
            weight_b,
            bias_b,
            cotangent.reshape(c3, fewer),
            pool,
        )
    else:
        wide_a = widened(slab, *fine)
        before_a, pooled = local_kernel(
            functools.partial(forward_a_kernel, fine),
            [((c2, cells), f32), ((c2, fewer), bf16)],
            (27 * c1, cells),
            work_a,
            wide_a,
            outward(weight_a),
            bias_a[:, None],
            pool,
        )
        wide_b = widened(pooled, *coarse)
        features, grad_b, part_wb, part_bb = local_kernel(
            functools.partial(middle_kernel, coarse),
            [((c3, fewer), bf16), ((c3, fewer), bf16), ((27 * c2, c3), f32), ((8, c3), f32)],
            (27 * c2, fewer),
            2 * work_b,
            wide_b,
            outward(weight_b),
            bias_b[:, None],
            cotangent.reshape(c3, fewer),
        )
        (grad_a,) = local_kernel(
            functools.partial(backward_b_kernel, coarse, fine),
            [((c2, cells), bf16)],
            (27 * c3, fewer),
            work_b,
            widened(grad_b, *coarse),
            inward(weight_b),
            before_a,
            pool.T.astype(bf16),
        )
        part_wa, part_ba = local_kernel(
            functools.partial(weight_a_kernel, fine),
            [((27 * c1, c2), f32), ((8, c2), f32)],
            (27 * c1, cells),
            work_a,
            wide_a,
            grad_a,
        )
        (grad_slab,) = local_kernel(
            functools.partial(backward_a_kernel, fine),
            [((c1, cells), bf16)],
            (27 * c2, cells),
            work_a,
            widened(grad_a, *fine),
            inward(weight_a),
        )
        sum_wa, sum_ba, sum_wb, sum_bb = summed_grads(
            part_wa, part_ba, part_wb, part_bb, (scale_a, scale_b)
        )
    grad_input = lax.all_to_all(
        grad_slab.reshape(c1, planes, rows, depth), "gz", split_axis=3, concat_axis=1, tiled=True
    )
    return (
        features.reshape(cotangent.shape),
        grad_input,
        sum_wa.reshape(weight_a.shape),
        sum_ba.reshape(c2),
        sum_wb.reshape(weight_b.shape),
        sum_bb.reshape(c3),
    )


def solution(mesh):
    return jax.shard_map(
        on_device,
        mesh=mesh,
        in_specs=(P(None, "gx", "gy", "gz"), P(), P(), P(), P(), P(None, ("gx", "gz"), "gy", None)),
        out_specs=(
            P(None, ("gx", "gz"), "gy", None),
            P(None, "gx", "gy", "gz"),
            P(),
            P(),
            P(),
            P(),
        ),
        check_vma=False,
    )
```

```python
import functools
import math

import jax
import jax.numpy as jnp
from jax import lax
from jax.experimental import pallas as pl
from jax.experimental.pallas import tpu as pltpu
from jax.sharding import PartitionSpec as P

LINE = ("gx", "gz")
MESH = pl.DeviceIdType.MESH


def shared(block, axis, dim, width):
    count = lax.axis_size(axis)
    if count == 1:
        edge = jnp.zeros_like(lax.slice_in_dim(block, 0, width, axis=dim))
        return edge, edge
    forward = [(i, i + 1) for i in range(count - 1)]
    backward = [(target, source) for source, target in forward]
    last = block.shape[dim]
    low = lax.ppermute(lax.slice_in_dim(block, last - width, last, axis=dim), axis, forward)
    high = lax.ppermute(lax.slice_in_dim(block, 0, width, axis=dim), axis, backward)
    return low, high


def widened(flat, planes, rows, depth):
    low, high = shared(flat, LINE, 1, rows * depth)
    if lax.axis_size("gy") == 1:
        gap = jnp.zeros((flat.shape[0], depth), flat.dtype)
        pieces = [gap, low, gap]
        for plane in range(planes):
            pieces += [gap, flat[:, plane * rows * depth : (plane + 1) * rows * depth], gap]
        return jnp.concatenate(pieces + [gap, high, gap], axis=1)
    whole = jnp.concatenate([low, flat, high], axis=1)
    whole = whole.reshape(flat.shape[0], planes + 2, rows, depth)
    low, high = shared(whole, "gy", 2, 1)
    return jnp.concatenate([low, whole, high], axis=2).reshape(flat.shape[0], -1)


def slope_of(value):
    sigma = jax.nn.sigmoid(value)
    return sigma + value * sigma * (1.0 - sigma)


def put_windows(wide_ref, windows, planes, rows, depth):
    wide = wide_ref[...]
    width, extent = wide.shape
    place = lax.broadcasted_iota(jnp.int32, (width, extent), 1) % depth
    loose = wide.astype(jnp.float32)
    before = jnp.where(place == 0, 0.0, pltpu.roll(loose, 1, 1)).astype(jnp.bfloat16)
    after = jnp.where(place == depth - 1, 0.0, pltpu.roll(loose, extent - 1, 1)).astype(jnp.bfloat16)
    size = rows * depth
    for third, moved in enumerate((before, wide, after)):
        for first in range(3):
            for second in range(3):
                at = (first * 9 + second * 3 + third) * width
                for plane in range(planes):
                    begin = ((plane + first) * (rows + 2) + second) * depth
                    windows[at : at + width, plane * size : (plane + 1) * size] = moved[
                        :, begin : begin + size
                    ]


def dot_rows(left, right):
    return lax.dot_general(
        left, right, (((1,), (1,)), ((), ())), preferred_element_type=jnp.float32
    )


def forward_a_kernel(dims, wide_ref, weight_ref, bias_ref, pool_ref, before_ref, pooled_ref, windows):
    planes, rows, depth = dims
    put_windows(wide_ref, windows, *dims)
    before = jnp.dot(weight_ref[...], windows[...], preferred_element_type=jnp.float32)
    before = before + bias_ref[...]
    before_ref[...] = before
    active = before * jax.nn.sigmoid(before)
    size = rows * depth
    for row in range(rows // 2):
        parts = [
            active[:, plane * size + (2 * row + j) * depth : plane * size + (2 * row + j + 1) * depth]
            for plane in range(planes)
            for j in range(2)
        ]
        summed = sum(parts[1:], parts[0])
        paired = jnp.dot(
            summed, pool_ref[...], precision=lax.Precision.HIGHEST, preferred_element_type=jnp.float32
        )
        pooled_ref[:, row * depth // 2 : (row + 1) * depth // 2] = (paired * 0.125).astype(jnp.bfloat16)


def middle_kernel(dims, wide_ref, weight_ref, bias_ref, cot_ref, feat_ref, grad_ref, wb_ref, bb_ref, windows):
    put_windows(wide_ref, windows, *dims)
    before = jnp.dot(weight_ref[...], windows[...], preferred_element_type=jnp.float32)
    before = before + bias_ref[...]
    feat_ref[...] = (before * jax.nn.sigmoid(before)).astype(jnp.bfloat16)
    grad = (cot_ref[...].astype(jnp.float32) * slope_of(before)).astype(jnp.bfloat16)
    grad_ref[...] = grad
    wb_ref[...] = dot_rows(windows[...], grad)
    bb_ref[...] = dot_rows(jnp.ones((8, grad.shape[1]), jnp.bfloat16), grad)


def backward_b_kernel(dims, fine, wide_ref, weight_ref, before_ref, spread_ref, grad_ref, windows):
    put_windows(wide_ref, windows, *dims)
    pooled = jnp.dot(weight_ref[...], windows[...], preferred_element_type=jnp.float32)
    pooled = pooled.astype(jnp.bfloat16)
    planes, rows, depth = fine
    size = rows * depth
    for row in range(rows // 2):
        part = pooled[:, row * depth // 2 : (row + 1) * depth // 2]
        spread = jnp.dot(part, spread_ref[...], preferred_element_type=jnp.float32) * 0.125
        for plane in range(planes):
            for j in range(2):
                begin = plane * size + (2 * row + j) * depth
                slope = slope_of(before_ref[:, begin : begin + depth])
                grad_ref[:, begin : begin + depth] = (spread * slope).astype(jnp.bfloat16)


def weight_a_kernel(dims, wide_ref, grad_ref, wa_ref, ba_ref, windows):
    put_windows(wide_ref, windows, *dims)
    grad = grad_ref[...]
    wa_ref[...] = dot_rows(windows[...], grad)
    ba_ref[...] = dot_rows(jnp.ones((8, grad.shape[1]), jnp.bfloat16), grad)


def backward_a_kernel(dims, wide_ref, weight_ref, out_ref, windows):
    put_windows(wide_ref, windows, *dims)
    out = jnp.dot(weight_ref[...], windows[...], preferred_element_type=jnp.float32)
    out_ref[...] = out.astype(jnp.bfloat16)


def local_kernel(body, outs, windows, flops, *operands):
    moved = sum(x.size * x.dtype.itemsize for x in operands)
    return pl.pallas_call(
        body,
        out_shape=[jax.ShapeDtypeStruct(shape, dtype) for shape, dtype in outs],
        in_specs=[pl.BlockSpec(memory_space=pltpu.VMEM)] * len(operands),
        out_specs=[pl.BlockSpec(memory_space=pltpu.VMEM)] * len(outs),
        scratch_shapes=[pltpu.VMEM(windows, jnp.bfloat16)],
        compiler_params=pltpu.CompilerParams(vmem_limit_bytes=48 * 2**20),
        cost_estimate=pl.CostEstimate(flops=flops, bytes_accessed=moved, transcendentals=0),
    )(*operands)


def partner_of(axis, bit):
    me = lax.axis_index(axis)
    mine = (me // bit) % 2
    return me + bit * (1 - 2 * mine), mine


def sum_kernel(steps, halvings, rows, scales, wa_ref, ba_ref, wb_ref, bb_ref, *rest):
    out_wa, out_ba, out_wb, out_bb, acc, gathered, *scratch = rest
    half, width = wa_ref.shape[0] // 2, wa_ref.shape[1]
    top = wb_ref.shape[0]
    count = len(steps)
    sends = scratch[:count]
    recvs = scratch[count : 2 * count]
    sem_send, sem_recv = scratch[2 * count :]
    partners = [partner_of(axis, bit) for axis, bit in steps]
    barrier = pltpu.get_barrier_semaphore()
    for (axis, _), (partner, _) in zip(steps, partners):
        pl.semaphore_signal(barrier, inc=1, device_id={axis: partner}, device_id_type=MESH)
    acc[:top] = wb_ref[...]
    acc[top : top + half, :width] = wa_ref[:half]
    acc[top : top + half, width:] = wa_ref[half:]
    acc[top + half :] = jnp.zeros((rows - top - half, 128), jnp.float32)
    acc[top + half : top + half + 8, :width] = ba_ref[...]
    acc[top + half + 8 : top + half + 16] = bb_ref[...]
    pl.semaphore_wait(barrier, count)
    offset = 0
    size = rows
    kept = []
    for at, ((axis, _), (partner, mine)) in enumerate(zip(steps, partners)):
        source = acc
        if at < halvings:
            size = size // 2
            away = pl.multiple_of(offset + (1 - mine) * size, 16)
            offset = pl.multiple_of(offset + mine * size, 16)
        else:
            away = offset
        sends[at][...] = source[pl.ds(away, size)].astype(jnp.bfloat16)
        copy = pltpu.make_async_remote_copy(
            src_ref=sends[at],
            dst_ref=recvs[at],
            send_sem=sem_send.at[at],
            recv_sem=sem_recv.at[at],
            device_id={axis: partner},
            device_id_type=MESH,
        )
        copy.start()
        copy.wait()
        if at < halvings:
            acc[pl.ds(offset, size)] = source[pl.ds(offset, size)] + recvs[at][...].astype(jnp.float32)
            kept.append((offset, size))
        else:
            acc[pl.ds(offset, size)] = sends[at][...].astype(jnp.float32) + recvs[at][...].astype(jnp.float32)
    gathered[pl.ds(offset, size)] = acc[pl.ds(offset, size)].astype(jnp.bfloat16)
    for back in range(halvings):
        at = halvings - 1 - back
        begin, extent = kept[at]
        (axis, _), (partner, _) = steps[at], partners[at]
        here = gathered.at[pl.ds(begin, extent)]
        copy = pltpu.make_async_remote_copy(
            src_ref=here,
            dst_ref=here,
            send_sem=sem_send.at[count + back],
            recv_sem=sem_recv.at[count + back],
            device_id={axis: partner},
            device_id_type=MESH,
        )
        copy.start()
        copy.wait()
    scale_a, scale_b = scales
    total = gathered[...].astype(jnp.float32)
    out_wb[...] = total[:top] * scale_b
    out_wa[:half] = total[top : top + half, :width] * scale_a
    out_wa[half:] = total[top : top + half, width:] * scale_a
    out_ba[...] = total[top + half : top + half + 1, :width] * scale_a
    out_bb[...] = total[top + half + 8 : top + half + 9] * scale_b


def summed_grads(wa, ba, wb, bb, scales):
    used = wb.shape[0] + wa.shape[0] // 2 + 16
    rows = used + -used % 128
    cut = {
        axis: [2**i for i in range(lax.axis_size(axis).bit_length() - 1)] for axis in ("gz", "gx", "gy")
    }
    steps = [("gz", bit) for bit in cut["gz"][:1]]
    steps += [("gx", bit) for bit in cut["gx"]] + [("gy", bit) for bit in cut["gy"]]
    steps += [("gz", bit) for bit in cut["gz"][1:]]
    halvings = 0
    sizes = []
    size = rows
    for _ in steps:
        if len(sizes) == halvings and size % 32 == 0:
            size //= 2
            halvings += 1
        sizes.append(size)
    buffers = [pltpu.VMEM((s, 128), jnp.bfloat16) for s in sizes]
    total = len(steps) + halvings
    shapes = [wa.shape, (1, ba.shape[1]), wb.shape, (1, bb.shape[1])]
    return pl.pallas_call(
        functools.partial(sum_kernel, steps, halvings, rows, scales),
        out_shape=[jax.ShapeDtypeStruct(shape, jnp.float32) for shape in shapes],
        in_specs=[pl.BlockSpec(memory_space=pltpu.VMEM)] * 4,
        out_specs=[pl.BlockSpec(memory_space=pltpu.VMEM)] * 4,
        scratch_shapes=[
            pltpu.VMEM((rows, 128), jnp.float32),
            pltpu.VMEM((rows, 128), jnp.bfloat16),
            *buffers,
            *buffers,
            pltpu.SemaphoreType.DMA((total,)),
            pltpu.SemaphoreType.DMA((total,)),
        ],
        compiler_params=pltpu.CompilerParams(collective_id=0, has_side_effects=True),
    )(wa, ba, wb, bb)


def line_ends(axis_sizes):
    across, count = axis_sizes
    total = across * count
    line = lax.axis_index("gx") * count + lax.axis_index("gz")
    after, before = (line + 1) % total, (line + total - 1) % total
    ids = [{"gx": at // count, "gz": at % count} for at in (after, before)]
    return line, total, ids


class Halo:
    def __init__(self, wide, dims, where, sems, at):
        planes, rows, depth = dims
        self.line, self.total, ids = where
        size, stride = rows * depth, (rows + 2) * depth
        spot = lambda plane: wide.at[:, plane * stride + depth : plane * stride + depth + size]
        send, recv = sems
        self.up, self.down = [
            pltpu.make_async_remote_copy(
                src_ref=spot(source),
                dst_ref=spot(target),
                send_sem=send.at[at + i],
                recv_sem=recv.at[at + i],
                device_id=ids[i],
                device_id_type=MESH,
            )
            for i, (source, target) in enumerate(((planes, 0), (1, planes + 1)))
        ]

    def start(self):
        pl.when(self.line < self.total - 1)(self.up.start)
        pl.when(self.line > 0)(self.down.start)

    def wait(self):
        @pl.when(self.line < self.total - 1)
        def _():
            self.up.wait_send()
            self.down.wait_recv()

        @pl.when(self.line > 0)
        def _():
            self.down.wait_send()
            self.up.wait_recv()


class Summing:
    def __init__(self, steps, sizes, acc, gathered, sends, recvs, sems):
        self.steps, self.sizes = steps, sizes
        self.acc, self.gathered, self.sends, self.recvs = acc, gathered, sends, recvs
        self.sems = sems
        self.partners = [partner_of(axis, bit) for axis, bit in steps]
        rows = [acc.shape[0]] + list(sizes)
        self.halvings = sum(a != b for a, b in zip(rows, sizes))
        self.stages = len(steps) + self.halvings
        self.offset = 0
        self.kept = []
        self.flying = None

    def copy(self, stage, source, target, step):
        send, recv = self.sems
        self.flying = pltpu.make_async_remote_copy(
            src_ref=source,
            dst_ref=target,
            send_sem=send.at[stage],
            recv_sem=recv.at[stage],
            device_id={self.steps[step][0]: self.partners[step][0]},
            device_id_type=MESH,
        )
        self.flying.start()

    def start(self, stage):
        if stage < len(self.steps):
            size = self.sizes[stage]
            away = self.offset
            if stage < self.halvings:
                mine = self.partners[stage][1]
                away = pl.multiple_of(self.offset + (1 - mine) * size, 16)
                self.offset = pl.multiple_of(self.offset + mine * size, 16)
                self.kept.append((self.offset, size))
            self.sends[stage][...] = self.acc[pl.ds(away, size)].astype(jnp.bfloat16)
            self.copy(stage, self.sends[stage], self.recvs[stage], stage)
        else:
            step = self.halvings - 1 - (stage - len(self.steps))
            begin, size = self.kept[step]
            here = self.gathered.at[pl.ds(begin, size)]
            self.copy(stage, here, here, step)

    def finish(self, stage):
        self.flying.wait()
        if stage >= len(self.steps):
            return
        here = pl.ds(self.offset, self.sizes[stage])
        came = self.recvs[stage][...].astype(jnp.float32)
        own = self.acc[here] if stage < self.halvings else self.sends[stage][...].astype(jnp.float32)
        total = own + came
        if stage == len(self.steps) - 1:
            self.gathered[here] = total.astype(jnp.bfloat16)
        else:
            self.acc[here] = total


def place(wide, flat, dims):
    planes, rows, depth = dims
    size, stride = rows * depth, (rows + 2) * depth
    for plane in range(planes):
        begin = (plane + 1) * stride + depth
        wide[:, begin : begin + size] = flat[:, plane * size : (plane + 1) * size]


def whole_kernel(setting, *refs):
    fine, coarse, sizes_line, steps, cuts_a, cuts_b, scales = setting
    slab, w_a, b_a, pool, w_b, b_b, cot, v_b, spread, v_a = refs[:10]
    features, grad_slab, out_wa, out_ba, out_wb, out_bb = refs[10:16]
    wide_a, wide_b, wide_gb, wide_ga, win_a, win_b, win_gb, win_ga = refs[16:24]
    before_a, pooled, grad_b, grad_a, acc_a, acc_b, all_a, all_b = refs[24:32]
    count = len(steps)
    send_a, recv_a, send_b, recv_b = [refs[32 + i * count : 32 + (i + 1) * count] for i in range(4)]
    sems = refs[32 + 4 * count :]
    where = line_ends(sizes_line)
    line, total, ids = where
    barrier = pltpu.get_barrier_semaphore()
    for wide in (wide_a, wide_b, wide_gb, wide_ga):
        wide[...] = jnp.zeros_like(wide)
    place(wide_a, slab, fine)
    for axis, bit in steps:
        partner, _ = partner_of(axis, bit)
        pl.semaphore_signal(barrier, inc=1, device_id={axis: partner}, device_id_type=MESH)
    for device in ids:
        pl.semaphore_signal(barrier, inc=1, device_id=device, device_id_type=MESH)
    pl.semaphore_wait(barrier, count + 2)
    halos = [
        Halo(wide, dims, where, sems[:2], 2 * i)
        for i, (wide, dims) in enumerate(
            ((wide_a, fine), (wide_b, coarse), (wide_gb, coarse), (wide_ga, fine))
        )
    ]
    sum_a = Summing(steps, cuts_a, acc_a, all_a, send_a, recv_a, sems[2:4])
    sum_b = Summing(steps, cuts_b, acc_b, all_b, send_b, recv_b, sems[4:6])

    halos[0].start()
    halos[0].wait()
    forward_a_kernel(fine, wide_a, w_a, b_a, pool, before_a, pooled, win_a)
    place(wide_b, pooled, coarse)
    halos[1].start()
    halos[1].wait()
    top_b = out_wb.shape[0]
    middle_kernel(
        coarse, wide_b, w_b, b_b, cot, features, grad_b, acc_b.at[:top_b], acc_b.at[top_b : top_b + 8], win_b
    )
    place(wide_gb, grad_b, coarse)
    halos[2].start()
    acc_b[top_b + 8 :] = jnp.zeros((acc_b.shape[0] - top_b - 8, acc_b.shape[1]), jnp.float32)
    sum_b.start(0)
    halos[2].wait()
    backward_b_kernel(coarse, fine, wide_gb, v_b, before_a, spread, grad_a, win_gb)
    place(wide_ga, grad_a, fine)
    halos[3].start()
    sum_b.finish(0)
    sum_b.start(1)
    grad = grad_a[...]
    half, width = out_wa.shape[0] // 2, out_wa.shape[1]
    acc_a[:half, :width] = dot_rows(win_a[:half], grad)
    acc_a[:half, width:] = dot_rows(win_a[half:], grad)
    acc_a[half:] = jnp.zeros((acc_a.shape[0] - half, acc_a.shape[1]), jnp.float32)
    acc_a[half : half + 8, :width] = dot_rows(jnp.ones((8, grad.shape[1]), jnp.bfloat16), grad)
    sum_b.finish(1)
    sum_b.start(2)
    sum_a.start(0)
    halos[3].wait()
    backward_a_kernel(fine, wide_ga, v_a, grad_slab, win_ga)
    for stage in range(max(sum_a.stages, sum_b.stages - 2)):
        if stage + 2 < sum_b.stages:
            sum_b.finish(stage + 2)
            if stage + 3 < sum_b.stages:
                sum_b.start(stage + 3)
        if stage < sum_a.stages:
            sum_a.finish(stage)
            if stage + 1 < sum_a.stages:
                sum_a.start(stage + 1)
    scale_a, scale_b = scales
    out_wb[...] = all_b[:top_b].astype(jnp.float32) * scale_b
    out_bb[...] = all_b[top_b : top_b + 16].astype(jnp.float32)[:1] * scale_b
    out_wa[:half] = all_a[:half, :width].astype(jnp.float32) * scale_a
    out_wa[half:] = all_a[:half, width:].astype(jnp.float32) * scale_a
    out_ba[...] = all_a[half : half + 16, :width].astype(jnp.float32)[:1] * scale_a


def stage_sizes(rows, steps):
    sizes = []
    for _ in steps:
        halve = rows % 32 == 0 and len(sizes) < 3
        rows = rows // 2 if halve else rows
        sizes.append(rows)
    return sizes


def all_steps():
    cut = {
        axis: [2**i for i in range(lax.axis_size(axis).bit_length() - 1)] for axis in ("gz", "gx", "gy")
    }
    steps = [("gz", bit) for bit in cut["gz"][:1]]
    steps += [("gx", bit) for bit in cut["gx"]] + [("gy", bit) for bit in cut["gy"]]
    return steps + [("gz", bit) for bit in cut["gz"][1:]]


def between_exchanges(fine, coarse, scales, slab, weight_a, bias_a, weight_b, bias_b, cot, pool):
    f32, bf16 = jnp.float32, jnp.bfloat16
    c1, cells = slab.shape
    c2, c3 = weight_b.shape[3:]
    fewer = cells // 8
    steps = all_steps()
    rows_a = 27 * c1 // 2 + 16
    rows_a += -rows_a % 128
    rows_b = 27 * c2 + 16
    rows_b += -rows_b % 128
    cuts_a, cuts_b = stage_sizes(rows_a, steps), stage_sizes(rows_b, steps)
    extent = lambda dims: (dims[0] + 2) * (dims[1] + 2) * dims[2]
    setting = (fine, coarse, (lax.axis_size("gx"), lax.axis_size("gz")), steps, cuts_a, cuts_b, scales)
    buffers = [pltpu.VMEM((n, 128), bf16) for cuts in (cuts_a, cuts_a, cuts_b, cuts_b) for n in cuts]
    outs = [
        ((c3, fewer), bf16),
        ((c1, cells), bf16),
        ((27 * c1, c2), f32),
        ((1, c2), f32),
        ((27 * c2, c3), f32),
        ((1, c3), f32),
    ]
    operands = (
        slab,
        outward(weight_a),
        bias_a[:, None],
        pool,
        outward(weight_b),
        bias_b[:, None],
        cot,
        inward(weight_b),
        pool.T.astype(bf16),
        inward(weight_a),
    )
    most = 2 * len(steps)
    return pl.pallas_call(
        functools.partial(whole_kernel, setting),
        out_shape=[jax.ShapeDtypeStruct(shape, dtype) for shape, dtype in outs],
        in_specs=[pl.BlockSpec(memory_space=pltpu.VMEM)] * len(operands),
        out_specs=[pl.BlockSpec(memory_space=pltpu.VMEM)] * len(outs),
        scratch_shapes=[
            pltpu.VMEM((c1, extent(fine)), bf16),
            pltpu.VMEM((c2, extent(coarse)), bf16),
            pltpu.VMEM((c3, extent(coarse)), bf16),
            pltpu.VMEM((c2, extent(fine)), bf16),
            pltpu.VMEM((27 * c1, cells), bf16),
            pltpu.VMEM((27 * c2, fewer), bf16),
            pltpu.VMEM((27 * c3, fewer), bf16),
            pltpu.VMEM((27 * c2, cells), bf16),
            pltpu.VMEM((c2, cells), f32),
            pltpu.VMEM((c2, fewer), bf16),
            pltpu.VMEM((c3, fewer), bf16),
            pltpu.VMEM((c2, cells), bf16),
            pltpu.VMEM((rows_a, 128), f32),
            pltpu.VMEM((rows_b, 128), f32),
            pltpu.VMEM((rows_a, 128), bf16),
            pltpu.VMEM((rows_b, 128), bf16),
            *buffers,
            pltpu.SemaphoreType.DMA((8,)),
            pltpu.SemaphoreType.DMA((8,)),
            *[pltpu.SemaphoreType.DMA((most,))] * 4,
        ],
        compiler_params=pltpu.CompilerParams(
            collective_id=1, has_side_effects=True, vmem_limit_bytes=60 * 2**20
        ),
    )(*operands)


def outward(weight):
    return weight.reshape(-1, weight.shape[-1]).T


def inward(weight):
    taps = weight[::-1, ::-1, ::-1].reshape(27, *weight.shape[3:])
    return jnp.transpose(taps, (1, 0, 2)).reshape(weight.shape[3], -1)


def lanes_of(shape):
    return lax.broadcasted_iota(jnp.int32, shape, len(shape) - 1)


def rows_of(shape):
    return lax.broadcasted_iota(jnp.int32, shape, 0)


def ones_where(mask):
    return jnp.where(mask, 1.0, 0.0).astype(jnp.bfloat16)


def dot(left, right):
    return jnp.dot(left, right, preferred_element_type=jnp.float32)


def by_parts(rank_bits, mask):
    place = {}
    for at, (axis, bit) in enumerate(rank_bits):
        if mask >> at & 1:
            me = place.get(axis, lax.axis_index(axis))
            place[axis] = me + bit * (1 - 2 * ((lax.axis_index(axis) // bit) % 2))
    return place


def own_rank(rank_bits, mask=0):
    total = 0
    for at, (axis, bit) in enumerate(rank_bits):
        mine = (lax.axis_index(axis) // bit) % 2
        total = total + ((1 - mine) if mask >> at & 1 else mine) * 2**at
    return total


def remote(source, target, sems, at, device):
    return pltpu.make_async_remote_copy(
        src_ref=source,
        dst_ref=target,
        send_sem=sems[0].at[at],
        recv_sem=sems[1].at[at],
        device_id=device,
        device_id_type=MESH,
    )


class Reduction:
    def __init__(self, groups, exchanged, acc, summed, sends, recvs, sems):
        self.groups, self.exchanged, self.acc, self.summed = groups, exchanged, acc, summed
        self.sends, self.recvs, self.sems = sends, recvs, sems
        self.offset, self.size = 0, acc.shape[0]
        self.kept = []
        self.flying = []
        self.used = 0
        self.stage = 0
        self.stages = 2 * len(groups) - (1 if exchanged else 0)

    def fly(self, source, target, device):
        copy = remote(source, target, self.sems, self.used, device)
        self.used += 1
        copy.start()
        self.flying.append(copy)

    def start(self):
        at = self.stage
        count = len(self.groups)
        if self.exchanged and at == count - 1:
            bits = self.groups[at]
            recv = self.recvs[at]
            mine = own_rank(bits)
            recv[mine] = self.acc[pl.ds(self.offset, self.size)].astype(jnp.bfloat16)
            for mask in range(1, 2 ** len(bits)):
                self.fly(recv.at[mine], recv.at[mine], by_parts(bits, mask))
        elif at < count:
            bits = self.groups[at]
            members = 2 ** len(bits)
            part = self.size // members
            send, recv = self.sends[at], self.recvs[at]
            send[...] = self.acc[pl.ds(self.offset, self.size)].astype(jnp.bfloat16)
            for mask in range(1, members):
                begin = pl.multiple_of(own_rank(bits, mask) * part, 16)
                self.fly(send.at[pl.ds(begin, part)], recv.at[mask - 1], by_parts(bits, mask))
            self.kept.append((self.offset, self.size))
            self.offset = pl.multiple_of(self.offset + own_rank(bits) * part, 16)
            self.size = part
        else:
            bits = self.groups[len(self.kept) - 1]
            here = self.summed.at[pl.ds(self.offset, self.size)]
            for mask in range(1, 2 ** len(bits)):
                self.fly(here, here, by_parts(bits, mask))
            self.offset, self.size = self.kept.pop()

    def finish(self):
        at = self.stage
        count = len(self.groups)
        for copy in self.flying:
            copy.wait()
        self.flying = []
        self.stage += 1
        if at >= count:
            return
        recv = self.recvs[at]
        here = pl.ds(self.offset, self.size)
        if self.exchanged and at == count - 1:
            total = recv[0].astype(jnp.float32)
            for i in range(1, recv.shape[0]):
                total = total + recv[i].astype(jnp.float32)
        else:
            total = self.acc[here]
            for i in range(recv.shape[0]):
                total = total + recv[i].astype(jnp.float32)
        if at == count - 1:
            self.summed[here] = total.astype(jnp.bfloat16)
        else:
            self.acc[here] = total

    def step(self):
        self.finish()
        if self.stage < self.stages:
            self.start()


class Border:
    def __init__(self, first, last, edge, inbox, sems, at):
        me, count = lax.axis_index("gz"), lax.axis_size("gz")
        side = 1 - lax.axis_index("gx")
        self.inner, self.outer = me > 0, me < count - 1
        up, down = (me + 1) % count, (me + count - 1) % count
        low, high, beside, beside_low, beside_high = inbox
        self.always = remote(edge, beside, sems, at + 2, {"gx": side})
        self.up = [
            remote(last, low, sems, at, {"gz": up}),
            remote(edge, beside_low, sems, at + 3, {"gx": side, "gz": up}),
        ]
        self.down = [
            remote(first, high, sems, at + 1, {"gz": down}),
            remote(edge, beside_high, sems, at + 4, {"gx": side, "gz": down}),
        ]

    def start(self):
        @pl.when(self.outer)
        def _():
            for copy in self.up:
                copy.start()

        @pl.when(self.inner)
        def _():
            for copy in self.down:
                copy.start()

        self.always.start()

    def wait(self):
        self.always.wait()

        @pl.when(self.outer)
        def _():
            for copy in self.up:
                copy.wait_send()
            for copy in self.down:
                copy.wait_recv()

        @pl.when(self.inner)
        def _():
            for copy in self.down:
                copy.wait_send()
            for copy in self.up:
                copy.wait_recv()


def gathered_edge(tiles, extent):
    shape = tiles[0].shape
    lane = lanes_of(shape)
    high = lax.axis_index("gx") == 0
    edge = jnp.where(high, extent - 1, 0)
    at_edge = lane & (extent - 1) == edge
    total = None
    for i, tile in enumerate(tiles):
        kept = jnp.where(at_edge, tile, 0.0)
        kept = pltpu.roll(kept, i, 1) if i else kept
        total = kept if total is None else total + kept
    back = pltpu.roll(total, 128 - (extent - 1), 1)
    return jnp.where(high, back, total)


def rolled(value, by):
    by = by % 128
    return pltpu.roll(value, by, 1) if by else value


def beside(tile, edges, extent):
    low_edge, high_edge, at = edges
    lane = lanes_of(tile.shape)
    before = jnp.where(lane & (extent - 1) == 0, rolled(low_edge, -at), rolled(tile, 1))
    after = jnp.where(lane & (extent - 1) == extent - 1, rolled(high_edge, extent - 1 - at), rolled(tile, -1))
    return before, after


def sided(edge):
    high = lax.axis_index("gx") == 0
    return jnp.where(high, 0.0, edge), jnp.where(high, edge, 0.0)


def moved_rows(pair, stride):
    lane = lanes_of(pair[0].shape)
    down = [rolled(tile, stride) for tile in pair]
    up = [rolled(tile, -stride) for tile in pair]
    low = lane < stride
    high = lane < 128 - stride
    before = (jnp.where(low, 0.0, down[0]), jnp.where(low, down[0], down[1]))
    after = (jnp.where(high, up[0], up[1]), jnp.where(high, up[1], 0.0))
    return before, after


def moved_half(tile, stride):
    lane = lanes_of(tile.shape) & 63
    before = jnp.where(lane < stride, 0.0, rolled(tile, stride))
    after = jnp.where(lane < 64 - stride, rolled(tile, -stride), 0.0)
    return before, after


def inbox_values(inbox):
    low, high, across, across_low, across_high = [ref[...].astype(jnp.float32) for ref in inbox]
    return low, high, sided(across), sided(across_low), sided(across_high)


def fine_planes(read, inbox, planes):
    low, high, across, across_low, across_high = inbox_values(inbox)
    for p in range(planes + 2):
        if p == 0:
            pair, edge, at = (low[:, :128], low[:, 128:]), across_low, 2 * (planes - 1)
        elif p == planes + 1:
            pair, edge, at = (high[:, :128], high[:, 128:]), across_high, 0
        else:
            pair, edge, at = read(p - 1), across, 2 * (p - 1)
        sides = [beside(tile, (*edge, at + g), 32) for g, tile in enumerate(pair)]
        yield p, ((sides[0][0], sides[1][0]), pair, (sides[0][1], sides[1][1]))


def coarse_tiles(field, inbox, tiles):
    low, high, across, across_low, across_high = inbox_values(inbox)
    half = lanes_of(low.shape) < 64
    for t in range(tiles):
        tile = field[:, t * 128 : (t + 1) * 128].astype(jnp.float32)
        sides = list(beside(tile, (*across, t), 16))
        if t == 0:
            sides_low = beside(low, (*across_low, tiles - 1), 16)
            tile = jnp.where(half, low, tile)
            sides = [jnp.where(half, a, b) for a, b in zip(sides_low, sides)]
        if t == tiles - 1:
            sides_high = beside(high, (*across_high, 0), 16)
            tile = jnp.where(half, tile, high)
            sides = [jnp.where(half, b, a) for a, b in zip(sides_high, sides)]
        yield t, (sides[0], tile, sides[1])


def column(row, size):
    wide = jnp.broadcast_to(row, (size, size))
    eye = rows_of((size, size)) == lanes_of((size, size))
    return jnp.sum(jnp.where(eye, wide, 0.0), axis=1, keepdims=True)


def joined_thirds(terms, tiles):
    half = None
    low = [rolled(terms(0, t), 64) for t in range(tiles)]
    high = [rolled(terms(2, t), 64) for t in range(tiles)]
    out = []
    for t in range(tiles):
        if half is None:
            half = lanes_of(low[0].shape) < 64
        before, after = low[max(t - 1, 0)], high[min(t + 1, tiles - 1)]
        out.append(terms(1, t) + jnp.where(half, before + high[t], low[t] + after))
    return out


def block_kernel(groups, *refs):
    inputs, outputs = refs[:6], refs[6:10]
    volume, w_a, b_a, w_b, b_b, cot = refs[10:16]
    (
        stage, own_a, windows_a, sums_a, slope_a, halves, pooled, windows_b, sums_b,
        cot_sent, cot_came, cot_here, grad_b, lines_b, sums_gb, grads_a, lines_a, sums_ga,
        feat_sent, feat_came, mat_a, mat_b, mat_ga, mat_gb, near, far, acc_a, acc_b,
        features, grad_in, sum_a, sum_b,
    ) = refs[16:48]
    rest = list(refs[48:])
    inboxes = [[rest.pop(0) for _ in range(5)] for _ in range(4)]
    edges = [rest.pop(0) for _ in range(4)]
    count = len(groups)
    send_a, recv_a = [rest.pop(0)], [rest.pop(0)]
    send_b = [rest.pop(0) for _ in range(count - 1)]
    recv_b = [rest.pop(0) for _ in range(count)]
    sems_halo, sems_cot, sems_feat, sems_a, sems_b = [(rest.pop(0), rest.pop(0)) for _ in range(5)]
    sems_in, sems_out = rest
    f32, bf16 = jnp.float32, jnp.bfloat16
    c1, rows, planes, width = volume.shape
    c2, c3 = w_a.shape[2], w_b.shape[2]
    tiles = planes // 4 + 1
    me, members = lax.axis_index("gz"), lax.axis_size("gz")
    whole = [bit for group in groups for bit in group]
    line = [bit for bit in whole if bit[0] == "gz"]

    barrier = pltpu.get_barrier_semaphore()
    for mask in range(1, 2 ** len(whole)):
        pl.semaphore_signal(barrier, inc=1, device_id=by_parts(whole, mask), device_id_type=MESH)
    loads = [
        pltpu.make_async_copy(source, target, sems_in.at[at])
        for at, (source, target) in enumerate(zip(inputs, refs[10:16]))
    ]
    for at in (0, 5, 1, 3, 2, 4):
        loads[at].start()

    @pl.when(me == 0)
    def _():
        for inbox in inboxes:
            for box in (inbox[0], inbox[3]):
                box[...] = jnp.zeros_like(box)

    @pl.when(me == members - 1)
    def _():
        for inbox in inboxes:
            for box in (inbox[1], inbox[4]):
                box[...] = jnp.zeros_like(box)

    loads[0].wait()
    for g in range(2):
        for i in range(4):
            part = volume[:, 4 * g + i].astype(f32).reshape(c1 * planes, width)
            stage[:, width * i : width * (i + 1)] = part
        for z in range(planes):
            tile = stage[pl.ds(z, c1, stride=planes), :]
            own_a[:, z * 256 + g * 128 : z * 256 + (g + 1) * 128] = tile.astype(bf16)

    def read_a(z):
        return tuple(own_a[:, z * 256 + g * 128 : z * 256 + (g + 1) * 128].astype(f32) for g in range(2))

    edges[0][...] = gathered_edge([tile for z in range(planes) for tile in read_a(z)], 32).astype(bf16)
    pl.semaphore_wait(barrier, 2 ** len(whole) - 1)

    border_a = Border(own_a.at[:, :256], own_a.at[:, (planes - 1) * 256 :], edges[0], inboxes[0], sems_halo, 0)
    border_a.start()

    def exchange(sent, came, sems):
        flying = []
        size = sent.shape[0] // members
        for mask in range(1, members):
            begin = pl.multiple_of(own_rank(line, mask) * size, 16)
            copy = remote(
                sent.at[pl.ds(begin, size)],
                came.at[pl.ds(pl.multiple_of(me * size, 16), size)],
                sems,
                mask - 1,
                by_parts(line, mask),
            )
            copy.start()
            flying.append(copy)
        here = pl.ds(pl.multiple_of(me * size, 16), size)
        came[here] = sent[here]
        return flying

    r, l = rows_of(far.shape), lanes_of(far.shape)
    far[...] = ones_where(((r >> 3) & 3 == l >> 7) & (((r >> 5) << 3) + (r & 7) == l & 127))
    loads[5].wait()
    half_rows = rows // 2
    stage[...] = cot[...].astype(f32)
    spaced = [stage[pl.ds(y, c3, stride=half_rows), :].astype(bf16) for y in range(half_rows)]
    cot_sent[...] = dot_rows(far[...], jnp.concatenate(spaced, axis=1)).astype(bf16)
    cot_flying = exchange(cot_sent, cot_came, sems_cot)
    for load in loads[1:5]:
        load.wait()

    eye = ones_where(rows_of((c2, c2)) == lanes_of((c2, c2)))
    eye_b = ones_where(rows_of((c3, c3)) == lanes_of((c3, c3)))
    for kz in range(3):
        block = w_a[:].reshape(9, 3, c1, c2)[:, kz].reshape(9 * c1, c2)
        mat_a[kz * c2 : (kz + 1) * c2] = dot_rows(eye, block).astype(bf16)
        block = w_b[:].reshape(9, 3, c2, c3)[:, kz].reshape(9 * c2, c3)
        mat_b[kz * c3 : (kz + 1) * c3] = dot_rows(eye_b, block).astype(bf16)
        for ky in range(3):
            for kx in range(3):
                tap = ((2 - kx) * 3 + 2 - ky) * 3 + 2 - kz
                at = kz * 3 + ky
                mat_ga[at * c1 : (at + 1) * c1, kx * c2 : (kx + 1) * c2] = w_a[tap]
                mat_gb[at * c2 : (at + 1) * c2, kx * c3 : (kx + 1) * c3] = w_b[tap]
    col_a, col_b = column(b_a[...], c2), column(b_b[...], c3)
    r, l = rows_of(near.shape), lanes_of(near.shape)
    near[...] = ones_where(
        ((r & 7) + 1 == l >> 6) & ((r >> 3) & 3 == (l >> 4) & 3) & (r >> 5 == l & 15)
    )
    r, l = rows_of((512, 128)), lanes_of((512, 128))
    pool = ones_where(
        (r >> 8 == l >> 6) & ((r >> 6) & 3 == (l >> 4) & 3) & ((r & 31) >> 1 == l & 15)
    )
    halves[...] = jnp.zeros_like(halves)
    for kz in range(3):
        for p in range(planes + 2):
            if not 0 <= p + kz - 2 < planes:
                grads_a[kz * c2 : (kz + 1) * c2, p * 256 : (p + 1) * 256] = jnp.zeros((c2, 256), bf16)
    acc_a[...] = jnp.zeros_like(acc_a)
    border_a.wait()

    for p, thirds in fine_planes(read_a, inboxes[0], planes):
        for kx, pair in enumerate(thirds):
            before, after = moved_rows(pair, 32)
            for ky, (first, second) in enumerate((before, pair, after)):
                at = (kx * 3 + ky) * c1
                windows_a[at : at + c1, p * 256 : p * 256 + 128] = first.astype(bf16)
                windows_a[at : at + c1, p * 256 + 128 : (p + 1) * 256] = second.astype(bf16)
    step = 2 * 256
    for begin in range(0, windows_a.shape[1], step):
        sums_a[:, begin : begin + step] = dot(mat_a[...], windows_a[:, begin : begin + step])
    for z in range(planes):
        value = (
            sums_a[:c2, z * 256 : (z + 1) * 256]
            + sums_a[c2 : 2 * c2, (z + 1) * 256 : (z + 2) * 256]
            + sums_a[2 * c2 :, (z + 2) * 256 : (z + 3) * 256]
            + col_a
        )
        sigma = jax.nn.sigmoid(value)
        active = value * sigma
        slope_a[:, z * 256 : (z + 1) * 256] = (sigma + active * (1.0 - sigma)) * 0.125
        if z % 2:
            active = active + kept
            pz = z // 2 + 1
            upper = active.astype(bf16)
            lower = (active - upper.astype(f32)).astype(bf16)
            at, lane = pz // 2 * c2, pz % 2 * 256
            halves[at : at + c2, lane : lane + 256] = upper
            halves[tiles * c2 + at : tiles * c2 + at + c2, lane : lane + 256] = lower
        else:
            kept = active
    both = dot(halves[...], pool)
    both = (both[: tiles * c2] + both[tiles * c2 :]) * 0.125
    for t in range(tiles):
        pooled[:, t * 128 : (t + 1) * 128] = both[t * c2 : (t + 1) * c2].astype(bf16)

    def coarse_edge(field):
        return gathered_edge([field[:, t * 128 : (t + 1) * 128].astype(f32) for t in range(tiles)], 16)

    edges[1][...] = coarse_edge(pooled).astype(bf16)
    last = (tiles - 1) * 128
    border_b = Border(pooled.at[:, :128], pooled.at[:, last:], edges[1], inboxes[1], sems_halo, 5)
    border_b.start()
    for copy in cot_flying:
        copy.wait()
    came = jnp.transpose(cot_came[...].astype(f32)).astype(bf16)
    cot_here[...] = dot(came, near[...])
    border_b.wait()

    for t, thirds in coarse_tiles(pooled, inboxes[1], tiles):
        for kx, tile in enumerate(thirds):
            before, after = moved_half(tile, 16)
            for ky, value in enumerate((before, tile, after)):
                at = (kx * 3 + ky) * c2
                windows_b[at : at + c2, t * 128 : (t + 1) * 128] = value.astype(bf16)
    sums_b[...] = dot(mat_b[...], windows_b[...])
    joined = joined_thirds(lambda k, t: sums_b[k * c3 : (k + 1) * c3, t * 128 : (t + 1) * 128], tiles)
    feats = []
    for t, value in enumerate(joined):
        value = value + col_b
        sigma = jax.nn.sigmoid(value)
        active = value * sigma
        feats.append(active.astype(bf16))
        slope = sigma + active * (1.0 - sigma)
        grad = cot_here[:, t * 128 : (t + 1) * 128] * slope
        grad_b[c3 : 2 * c3, t * 128 : (t + 1) * 128] = grad.astype(bf16)
    own_gb = grad_b.at[c3 : 2 * c3]
    edges[2][...] = coarse_edge(own_gb).astype(bf16)
    border_gb = Border(own_gb.at[:, :128], own_gb.at[:, last:], edges[2], inboxes[2], sems_halo, 10)
    border_gb.start()

    half = lanes_of((c3, 128)) < 64
    turned = [rolled(own_gb[:, t * 128 : (t + 1) * 128].astype(f32), 64) for t in range(tiles)]
    zero = jnp.zeros_like(turned[0])
    for t in range(tiles):
        later = turned[t + 1] if t + 1 < tiles else zero
        earlier = turned[t - 1] if t else zero
        here = slice(t * 128, (t + 1) * 128)
        grad_b[:c3, here] = jnp.where(half, turned[t], later).astype(bf16)
        grad_b[2 * c3 :, here] = jnp.where(half, earlier, turned[t]).astype(bf16)
    terms = dot_rows(windows_b[...], grad_b[...])
    for at in range(9):
        for kz in range(3):
            tap = at * 3 + kz
            acc_b[tap * c2 : (tap + 1) * c2] = terms[at * c2 : (at + 1) * c2, kz * c3 : (kz + 1) * c3]
    top = 27 * c2
    acc_b[top:] = jnp.zeros((acc_b.shape[0] - top, c3), f32)
    acc_b[top : top + 8] = dot_rows(jnp.ones((8, tiles * 128), bf16), own_gb[...])
    total_b = Reduction(groups, True, acc_b, sum_b, send_b, recv_b, sems_b)
    total_b.start()
    feat_sent[...] = dot_rows(near[...], jnp.concatenate(feats, axis=1)).astype(bf16)
    feat_flying = exchange(feat_sent, feat_came, sems_feat)
    total_b.step()
    border_gb.wait()

    for t, thirds in coarse_tiles(own_gb, inboxes[2], tiles):
        for kx, tile in enumerate(thirds):
            lines_b[kx * c3 : (kx + 1) * c3, t * 128 : (t + 1) * 128] = tile.astype(bf16)
    sums_gb[...] = dot(mat_gb[...], lines_b[...])
    by_row = [
        joined_thirds(
            lambda k, t: sums_gb[(k * 3 + ky) * c2 : (k * 3 + ky + 1) * c2, t * 128 : (t + 1) * 128], tiles
        )
        for ky in range(3)
    ]
    small = []
    for t in range(tiles):
        value = by_row[1][t] + moved_half(by_row[0][t], 16)[0] + moved_half(by_row[2][t], 16)[1]
        small.append(value.astype(bf16))
    spread = dot_rows(jnp.concatenate(small, axis=0), pool)
    for z in range(planes):
        pz = z // 2 + 1
        large = spread[pz // 2 * c2 : (pz // 2 + 1) * c2, pz % 2 * 256 : (pz % 2 + 1) * 256]
        grad = (large * slope_a[:, z * 256 : (z + 1) * 256]).astype(bf16)
        for kz in range(3):
            grads_a[kz * c2 : (kz + 1) * c2, (z + kz) * 256 : (z + kz + 1) * 256] = grad

    own_ga = grads_a.at[c2 : 2 * c2]

    def read_ga(z):
        return tuple(
            own_ga[:, (z + 1) * 256 + g * 128 : (z + 1) * 256 + (g + 1) * 128].astype(f32) for g in range(2)
        )

    edges[3][...] = gathered_edge([tile for z in range(planes) for tile in read_ga(z)], 32).astype(bf16)
    border_ga = Border(
        own_ga.at[:, 256:512], own_ga.at[:, planes * 256 : (planes + 1) * 256], edges[3], inboxes[3], sems_halo, 15
    )
    border_ga.start()
    total_b.step()

    terms = dot_rows(windows_a[...], grads_a[...])
    deep = 9 * c1
    acc_a[:deep] = terms[:, : 2 * c2]
    acc_a[deep : deep + deep // 2, :c2] = terms[: deep // 2, 2 * c2 :]
    acc_a[deep : deep + deep // 2, c2:] = terms[deep // 2 :, 2 * c2 :]
    top_a = deep + deep // 2
    acc_a[top_a : top_a + 8, :c2] = dot_rows(jnp.ones((8, planes * 256), bf16), own_ga[:, 256 : (planes + 1) * 256])
    total_a = Reduction([whole], False, acc_a, sum_a, send_a, recv_a, sems_a)
    total_a.start()
    border_ga.wait()

    for p, thirds in fine_planes(read_ga, inboxes[3], planes):
        for kx, pair in enumerate(thirds):
            for g, tile in enumerate(pair):
                at = p * 256 + g * 128
                lines_a[kx * c2 : (kx + 1) * c2, at : at + 128] = tile.astype(bf16)
    for begin in range(0, lines_a.shape[1], step):
        sums_ga[:, begin : begin + step] = dot(mat_ga[...], lines_a[:, begin : begin + step])
    total_a.step()
    total_b.step()
    for copy in feat_flying:
        copy.wait()
    came = jnp.transpose(feat_came[...].astype(f32)).astype(bf16)
    ours = dot(came, far[...])
    for y in range(half_rows):
        stage[pl.ds(y, c3, stride=half_rows), :] = ours[:, y * 128 : (y + 1) * 128]
    features[...] = stage[...].astype(bf16)
    stores = [
        pltpu.make_async_copy(source, target, sems_out.at[at])
        for at, (source, target) in enumerate(zip((features, grad_in, sum_a, sum_b), outputs))
    ]
    stores[0].start()
    results = []
    for z in range(planes):
        by_row = []
        for ky in range(3):
            value = None
            for kz in range(3):
                at = (kz * 3 + ky) * c1
                term = sums_ga[at : at + c1, (z + kz) * 256 : (z + kz + 1) * 256]
                value = term if value is None else value + term
            by_row.append((value[:, :128], value[:, 128:]))
        before, after = moved_rows(by_row[0], 32)[0], moved_rows(by_row[2], 32)[1]
        results.append([by_row[1][g] + before[g] + after[g] for g in range(2)])
    for g in range(2):
        for z in range(planes):
            stage[pl.ds(z, c1, stride=planes), :] = results[z][g]
        for i in range(4):
            part = stage[:, width * i : width * (i + 1)].astype(bf16)
            grad_in[:, 4 * g + i] = part.reshape(c1, planes, width)

    stores[1].start()
    total_a.finish()
    stores[2].start()
    while total_b.stage < total_b.stages:
        total_b.step()
    stores[3].start()
    for store in stores:
        store.wait()


def last_kernel(scales, *refs):
    feat, grad, sum_a, sum_b, out_feat, out_grad, out_wa, out_ba, out_wb, out_bb = refs[:10]
    kept_feat, kept_grad, kept_a, kept_b, wa, ba, wb, bb, sems_in, sems_out = refs[10:]
    f32 = jnp.float32
    scale_a, scale_b = scales
    inputs = (sum_b, grad, sum_a, feat)
    kept = (kept_b, kept_grad, kept_a, kept_feat)
    loads = [
        pltpu.make_async_copy(source, target, sems_in.at[at])
        for at, (source, target) in enumerate(zip(inputs, kept))
    ]
    for load in loads:
        load.start()
    places = ((wb, out_wb), (kept_grad, out_grad), (wa, out_wa), (kept_feat, out_feat), (ba, out_ba), (bb, out_bb))
    stores = [
        pltpu.make_async_copy(source, target, sems_out.at[at]) for at, (source, target) in enumerate(places)
    ]
    loads[0].wait()
    top = wb.shape[0]
    wb[...] = kept_b[:top].astype(f32) * scale_b
    stores[0].start()
    bb[...] = kept_b[top : top + 16].astype(f32)[:1] * scale_b
    stores[5].start()
    loads[1].wait()
    stores[1].start()
    loads[2].wait()
    c1, c2 = wa.shape[1:]
    deep = 9 * c1
    pairs = kept_a[:deep].astype(f32) * scale_a
    tail = kept_a[deep : deep + deep // 2].astype(f32) * scale_a
    thirds = jnp.concatenate([tail[:, :c2], tail[:, c2:]], axis=0)
    for at in range(9):
        here = slice(at * c1, (at + 1) * c1)
        wa[at * 3] = pairs[here, :c2]
        wa[at * 3 + 1] = pairs[here, c2:]
        wa[at * 3 + 2] = thirds[here]
    stores[2].start()
    top_a = deep + deep // 2
    ba[...] = kept_a[top_a : top_a + 16].astype(f32)[:1, :c2] * scale_a
    stores[4].start()
    loads[3].wait()
    stores[3].start()
    for store in stores:
        store.wait()


def all_groups():
    cut = {axis: [2**i for i in range(lax.axis_size(axis).bit_length() - 1)] for axis in ("gz", "gx")}
    line = [("gz", bit) for bit in cut["gz"]]
    return [line[:1], [("gx", bit) for bit in cut["gx"]] + line[1:2], line[2:]]


def on_blocks(volume, weight_a, bias_a, weight_b, bias_b, cotangent, scales):
    f32, bf16 = jnp.float32, jnp.bfloat16
    c1, width, rows, planes = volume.shape
    c2, c3 = weight_b.shape[3:]
    members = lax.axis_size("gz")
    groups = all_groups()
    tiles = planes // 4 + 1
    long, short = (planes + 2) * 256, tiles * 128
    cells = planes * 256
    rows_a, rows_b = 512, 27 * c2 + 64
    fewer = cells // 8

    def buffers(total, groups, exchanged):
        sends, recvs = [], []
        size = total
        for at, group in enumerate(groups):
            n = 2 ** len(group)
            if exchanged and at == len(groups) - 1:
                recvs.append(pltpu.VMEM((n, size, 128), bf16))
                continue
            sends.append(pltpu.VMEM((size, 128), bf16))
            size //= n
            recvs.append(pltpu.VMEM((n - 1, size, 128), bf16))
        return sends + recvs

    inboxes = []
    for channels, plane in ((c1, 256), (c2, 128), (c3, 128), (c2, 256)):
        inboxes += [pltpu.VMEM((channels, plane), bf16)] * 2 + [pltpu.VMEM((channels, 128), bf16)] * 3
    whole = sum(groups, [])
    count_a = 2 * (2 ** len(whole) - 1)
    count_b = 2 * sum(2 ** len(group) - 1 for group in groups[:-1]) + 2 ** len(groups[-1]) - 1
    passed = [
        ((c3 * rows // 2, 128), bf16),
        ((c1, rows, planes, width), bf16),
        ((rows_a, 128), bf16),
        ((rows_b, 128), bf16),
    ]
    operands = (
        jnp.transpose(volume, (0, 2, 3, 1)),
        weight_a.reshape(27, c1, c2),
        bias_a[None],
        weight_b.reshape(27, c2, c3),
        bias_b[None],
        cotangent.reshape(c3 * rows // 2, 128),
    )
    anywhere = pl.BlockSpec(memory_space=pl.ANY)
    middle = pl.pallas_call(
        functools.partial(block_kernel, groups),
        out_shape=[jax.ShapeDtypeStruct(shape, dtype) for shape, dtype in passed],
        in_specs=[anywhere] * len(operands),
        out_specs=[anywhere] * len(passed),
        scratch_shapes=[
            *[pltpu.VMEM(x.shape, x.dtype) for x in operands],
            pltpu.VMEM((c1 * planes, 128), f32),
            pltpu.VMEM((c1, cells), bf16),
            pltpu.VMEM((9 * c1, long), bf16),
            pltpu.VMEM((3 * c2, long), f32),
            pltpu.VMEM((c2, cells), f32),
            pltpu.VMEM((2 * tiles * c2, 512), bf16),
            pltpu.VMEM((c2, short), bf16),
            pltpu.VMEM((9 * c2, short), bf16),
            pltpu.VMEM((3 * c3, short), f32),
            pltpu.VMEM((fewer, c3), bf16),
            pltpu.VMEM((fewer, c3), bf16),
            pltpu.VMEM((c3, short), f32),
            pltpu.VMEM((3 * c3, short), bf16),
            pltpu.VMEM((3 * c3, short), bf16),
            pltpu.VMEM((9 * c2, short), f32),
            pltpu.VMEM((3 * c2, long), bf16),
            pltpu.VMEM((3 * c2, long), bf16),
            pltpu.VMEM((9 * c1, long), f32),
            pltpu.VMEM((fewer, c3), bf16),
            pltpu.VMEM((fewer, c3), bf16),
            pltpu.VMEM((3 * c2, 9 * c1), bf16),
            pltpu.VMEM((3 * c3, 9 * c2), bf16),
            pltpu.VMEM((9 * c1, 3 * c2), bf16),
            pltpu.VMEM((9 * c2, 3 * c3), bf16),
            pltpu.VMEM((fewer, short), bf16),
            pltpu.VMEM((fewer, fewer), bf16),
            pltpu.VMEM((rows_a, 128), f32),
            pltpu.VMEM((rows_b, 128), f32),
            *[pltpu.VMEM(shape, dtype) for shape, dtype in passed],
            *inboxes,
            *[pltpu.VMEM((channels, 128), bf16) for channels in (c1, c2, c3, c2)],
            *buffers(rows_a, [whole], False),
            *buffers(rows_b, groups, True),
            *[pltpu.SemaphoreType.DMA((20,))] * 2,
            *[pltpu.SemaphoreType.DMA((members - 1,))] * 4,
            *[pltpu.SemaphoreType.DMA((count_a,))] * 2,
            *[pltpu.SemaphoreType.DMA((count_b,))] * 2,
            pltpu.SemaphoreType.DMA((len(operands),)),
            pltpu.SemaphoreType.DMA((len(passed),)),
        ],
        compiler_params=pltpu.CompilerParams(
            collective_id=2, has_side_effects=True, vmem_limit_bytes=60 * 2**20
        ),
    )(*operands)
    outs = [
        *passed[:2],
        ((27, c1, c2), f32),
        ((1, c2), f32),
        ((27 * c2, c3), f32),
        ((1, c3), f32),
    ]
    features, grad_in, sum_wa, sum_ba, sum_wb, sum_bb = pl.pallas_call(
        functools.partial(last_kernel, scales),
        out_shape=[jax.ShapeDtypeStruct(shape, dtype) for shape, dtype in outs],
        in_specs=[anywhere] * len(passed),
        out_specs=[anywhere] * len(outs),
        scratch_shapes=[
            *[pltpu.VMEM(shape, dtype) for shape, dtype in passed + outs[2:]],
            pltpu.SemaphoreType.DMA((len(passed),)),
            pltpu.SemaphoreType.DMA((len(outs),)),
        ],
    )(*middle)
    return (
        features.reshape(cotangent.shape),
        jnp.transpose(grad_in, (0, 3, 1, 2)),
        sum_wa.reshape(weight_a.shape),
        sum_ba.reshape(c2),
        sum_wb.reshape(weight_b.shape),
        sum_bb.reshape(c3),
    )


def fits_blocks(volume, weight_b):
    c1, width, rows, planes = volume.shape
    sizes = {axis: lax.axis_size(axis) for axis in ("gx", "gy", "gz")}
    return (
        sizes == {"gx": 2, "gy": 1, "gz": planes}
        and (width, rows, planes) == (32, 8, 16)
        and (c1, *weight_b.shape[3:]) == (32, 64, 128)
    )


def on_device(volume, weight_a, bias_a, weight_b, bias_b, cotangent):
    f32, bf16 = jnp.float32, jnp.bfloat16
    count = lax.axis_size("gz")
    devices_all = lax.axis_size("gx") * lax.axis_size("gy") * count
    c1, nx, rows, nz = volume.shape
    cells = nx * rows * nz
    scale_a = 1.0 / math.sqrt(cells * devices_all)
    scale_b = 1.0 / math.sqrt(cells * devices_all // 8)
    c2, c3 = weight_b.shape[3:]
    if fits_blocks(volume, weight_b):
        return on_blocks(volume, weight_a, bias_a, weight_b, bias_b, cotangent, (scale_a, scale_b))
    planes, depth = nx // count, nz * count
    fine = (planes, rows, depth)
    coarse = (planes // 2, rows // 2, depth // 2)
    fewer = cells // 8
    pool = (jnp.arange(depth)[:, None] // 2 == jnp.arange(depth // 2)[None]).astype(f32)
    work_a = 2 * 27 * c1 * c2 * cells
    work_b = 2 * 27 * c2 * c3 * fewer

    slab = lax.all_to_all(volume, "gz", split_axis=1, concat_axis=3, tiled=True).reshape(c1, cells)
    if lax.axis_size("gy") == 1:
        features, grad_slab, sum_wa, sum_ba, sum_wb, sum_bb = between_exchanges(
            fine,
            coarse,
            (scale_a, scale_b),
            slab,
            weight_a,
            bias_a,
            weight_b,
            bias_b,
            cotangent.reshape(c3, fewer),
            pool,
        )
    else:
        wide_a = widened(slab, *fine)
        before_a, pooled = local_kernel(
            functools.partial(forward_a_kernel, fine),
            [((c2, cells), f32), ((c2, fewer), bf16)],
            (27 * c1, cells),
            work_a,
            wide_a,
            outward(weight_a),
            bias_a[:, None],
            pool,
        )
        wide_b = widened(pooled, *coarse)
        features, grad_b, part_wb, part_bb = local_kernel(
            functools.partial(middle_kernel, coarse),
            [((c3, fewer), bf16), ((c3, fewer), bf16), ((27 * c2, c3), f32), ((8, c3), f32)],
            (27 * c2, fewer),
            2 * work_b,
            wide_b,
            outward(weight_b),
            bias_b[:, None],
            cotangent.reshape(c3, fewer),
        )
        (grad_a,) = local_kernel(
            functools.partial(backward_b_kernel, coarse, fine),
            [((c2, cells), bf16)],
            (27 * c3, fewer),
            work_b,
            widened(grad_b, *coarse),
            inward(weight_b),
            before_a,
            pool.T.astype(bf16),
        )
        part_wa, part_ba = local_kernel(
            functools.partial(weight_a_kernel, fine),
            [((27 * c1, c2), f32), ((8, c2), f32)],
            (27 * c1, cells),
            work_a,
            wide_a,
            grad_a,
        )
        (grad_slab,) = local_kernel(
            functools.partial(backward_a_kernel, fine),
            [((c1, cells), bf16)],
            (27 * c2, cells),
            work_a,
            widened(grad_a, *fine),
            inward(weight_a),
        )
        sum_wa, sum_ba, sum_wb, sum_bb = summed_grads(
            part_wa, part_ba, part_wb, part_bb, (scale_a, scale_b)
        )
    grad_input = lax.all_to_all(
        grad_slab.reshape(c1, planes, rows, depth), "gz", split_axis=3, concat_axis=1, tiled=True
    )
    return (
        features.reshape(cotangent.shape),
        grad_input,
        sum_wa.reshape(weight_a.shape),
        sum_ba.reshape(c2),
        sum_wb.reshape(weight_b.shape),
        sum_bb.reshape(c3),
    )


def solution(mesh):
    return jax.shard_map(
        on_device,
        mesh=mesh,
        in_specs=(P(None, "gx", "gy", "gz"), P(), P(), P(), P(), P(None, ("gx", "gz"), "gy", None)),
        out_specs=(
            P(None, ("gx", "gz"), "gy", None),
            P(None, "gx", "gy", "gz"),
            P(),
            P(),
            P(),
            P(),
        ),
        check_vma=False,
    )
```

```python
import functools
import math

import jax
import jax.numpy as jnp
from jax import lax
from jax.experimental import pallas as pl
from jax.experimental.pallas import tpu as pltpu
from jax.sharding import PartitionSpec as P

LINE = ("gx", "gz")
MESH = pl.DeviceIdType.MESH


def shared(block, axis, dim, width):
    count = lax.axis_size(axis)
    if count == 1:
        edge = jnp.zeros_like(lax.slice_in_dim(block, 0, width, axis=dim))
        return edge, edge
    forward = [(i, i + 1) for i in range(count - 1)]
    backward = [(target, source) for source, target in forward]
    last = block.shape[dim]
    low = lax.ppermute(lax.slice_in_dim(block, last - width, last, axis=dim), axis, forward)
    high = lax.ppermute(lax.slice_in_dim(block, 0, width, axis=dim), axis, backward)
    return low, high


def widened(flat, planes, rows, depth):
    low, high = shared(flat, LINE, 1, rows * depth)
    if lax.axis_size("gy") == 1:
        gap = jnp.zeros((flat.shape[0], depth), flat.dtype)
        pieces = [gap, low, gap]
        for plane in range(planes):
            pieces += [gap, flat[:, plane * rows * depth : (plane + 1) * rows * depth], gap]
        return jnp.concatenate(pieces + [gap, high, gap], axis=1)
    whole = jnp.concatenate([low, flat, high], axis=1)
    whole = whole.reshape(flat.shape[0], planes + 2, rows, depth)
    low, high = shared(whole, "gy", 2, 1)
    return jnp.concatenate([low, whole, high], axis=2).reshape(flat.shape[0], -1)


def slope_of(value):
    sigma = jax.nn.sigmoid(value)
    return sigma + value * sigma * (1.0 - sigma)


def put_windows(wide_ref, windows, planes, rows, depth):
    wide = wide_ref[...]
    width, extent = wide.shape
    place = lax.broadcasted_iota(jnp.int32, (width, extent), 1) % depth
    loose = wide.astype(jnp.float32)
    before = jnp.where(place == 0, 0.0, pltpu.roll(loose, 1, 1)).astype(jnp.bfloat16)
    after = jnp.where(place == depth - 1, 0.0, pltpu.roll(loose, extent - 1, 1)).astype(jnp.bfloat16)
    size = rows * depth
    for third, moved in enumerate((before, wide, after)):
        for first in range(3):
            for second in range(3):
                at = (first * 9 + second * 3 + third) * width
                for plane in range(planes):
                    begin = ((plane + first) * (rows + 2) + second) * depth
                    windows[at : at + width, plane * size : (plane + 1) * size] = moved[
                        :, begin : begin + size
                    ]


def dot_rows(left, right):
    return lax.dot_general(
        left, right, (((1,), (1,)), ((), ())), preferred_element_type=jnp.float32
    )


def forward_a_kernel(dims, wide_ref, weight_ref, bias_ref, pool_ref, before_ref, pooled_ref, windows):
    planes, rows, depth = dims
    put_windows(wide_ref, windows, *dims)
    before = jnp.dot(weight_ref[...], windows[...], preferred_element_type=jnp.float32)
    before = before + bias_ref[...]
    before_ref[...] = before
    active = before * jax.nn.sigmoid(before)
    size = rows * depth
    for row in range(rows // 2):
        parts = [
            active[:, plane * size + (2 * row + j) * depth : plane * size + (2 * row + j + 1) * depth]
            for plane in range(planes)
            for j in range(2)
        ]
        summed = sum(parts[1:], parts[0])
        paired = jnp.dot(
            summed, pool_ref[...], precision=lax.Precision.HIGHEST, preferred_element_type=jnp.float32
        )
        pooled_ref[:, row * depth // 2 : (row + 1) * depth // 2] = (paired * 0.125).astype(jnp.bfloat16)


def middle_kernel(dims, wide_ref, weight_ref, bias_ref, cot_ref, feat_ref, grad_ref, wb_ref, bb_ref, windows):
    put_windows(wide_ref, windows, *dims)
    before = jnp.dot(weight_ref[...], windows[...], preferred_element_type=jnp.float32)
    before = before + bias_ref[...]
    feat_ref[...] = (before * jax.nn.sigmoid(before)).astype(jnp.bfloat16)
    grad = (cot_ref[...].astype(jnp.float32) * slope_of(before)).astype(jnp.bfloat16)
    grad_ref[...] = grad
    wb_ref[...] = dot_rows(windows[...], grad)
    bb_ref[...] = dot_rows(jnp.ones((8, grad.shape[1]), jnp.bfloat16), grad)


def backward_b_kernel(dims, fine, wide_ref, weight_ref, before_ref, spread_ref, grad_ref, windows):
    put_windows(wide_ref, windows, *dims)
    pooled = jnp.dot(weight_ref[...], windows[...], preferred_element_type=jnp.float32)
    pooled = pooled.astype(jnp.bfloat16)
    planes, rows, depth = fine
    size = rows * depth
    for row in range(rows // 2):
        part = pooled[:, row * depth // 2 : (row + 1) * depth // 2]
        spread = jnp.dot(part, spread_ref[...], preferred_element_type=jnp.float32) * 0.125
        for plane in range(planes):
            for j in range(2):
                begin = plane * size + (2 * row + j) * depth
                slope = slope_of(before_ref[:, begin : begin + depth])
                grad_ref[:, begin : begin + depth] = (spread * slope).astype(jnp.bfloat16)


def weight_a_kernel(dims, wide_ref, grad_ref, wa_ref, ba_ref, windows):
    put_windows(wide_ref, windows, *dims)
    grad = grad_ref[...]
    wa_ref[...] = dot_rows(windows[...], grad)
    ba_ref[...] = dot_rows(jnp.ones((8, grad.shape[1]), jnp.bfloat16), grad)


def backward_a_kernel(dims, wide_ref, weight_ref, out_ref, windows):
    put_windows(wide_ref, windows, *dims)
    out = jnp.dot(weight_ref[...], windows[...], preferred_element_type=jnp.float32)
    out_ref[...] = out.astype(jnp.bfloat16)


def local_kernel(body, outs, windows, flops, *operands):
    moved = sum(x.size * x.dtype.itemsize for x in operands)
    return pl.pallas_call(
        body,
        out_shape=[jax.ShapeDtypeStruct(shape, dtype) for shape, dtype in outs],
        in_specs=[pl.BlockSpec(memory_space=pltpu.VMEM)] * len(operands),
        out_specs=[pl.BlockSpec(memory_space=pltpu.VMEM)] * len(outs),
        scratch_shapes=[pltpu.VMEM(windows, jnp.bfloat16)],
        compiler_params=pltpu.CompilerParams(vmem_limit_bytes=48 * 2**20),
        cost_estimate=pl.CostEstimate(flops=flops, bytes_accessed=moved, transcendentals=0),
    )(*operands)


def partner_of(axis, bit):
    me = lax.axis_index(axis)
    mine = (me // bit) % 2
    return me + bit * (1 - 2 * mine), mine


def sum_kernel(steps, halvings, rows, scales, wa_ref, ba_ref, wb_ref, bb_ref, *rest):
    out_wa, out_ba, out_wb, out_bb, acc, gathered, *scratch = rest
    half, width = wa_ref.shape[0] // 2, wa_ref.shape[1]
    top = wb_ref.shape[0]
    count = len(steps)
    sends = scratch[:count]
    recvs = scratch[count : 2 * count]
    sem_send, sem_recv = scratch[2 * count :]
    partners = [partner_of(axis, bit) for axis, bit in steps]
    barrier = pltpu.get_barrier_semaphore()
    for (axis, _), (partner, _) in zip(steps, partners):
        pl.semaphore_signal(barrier, inc=1, device_id={axis: partner}, device_id_type=MESH)
    acc[:top] = wb_ref[...]
    acc[top : top + half, :width] = wa_ref[:half]
    acc[top : top + half, width:] = wa_ref[half:]
    acc[top + half :] = jnp.zeros((rows - top - half, 128), jnp.float32)
    acc[top + half : top + half + 8, :width] = ba_ref[...]
    acc[top + half + 8 : top + half + 16] = bb_ref[...]
    pl.semaphore_wait(barrier, count)
    offset = 0
    size = rows
    kept = []
    for at, ((axis, _), (partner, mine)) in enumerate(zip(steps, partners)):
        source = acc
        if at < halvings:
            size = size // 2
            away = pl.multiple_of(offset + (1 - mine) * size, 16)
            offset = pl.multiple_of(offset + mine * size, 16)
        else:
            away = offset
        sends[at][...] = source[pl.ds(away, size)].astype(jnp.bfloat16)
        copy = pltpu.make_async_remote_copy(
            src_ref=sends[at],
            dst_ref=recvs[at],
            send_sem=sem_send.at[at],
            recv_sem=sem_recv.at[at],
            device_id={axis: partner},
            device_id_type=MESH,
        )
        copy.start()
        copy.wait()
        if at < halvings:
            acc[pl.ds(offset, size)] = source[pl.ds(offset, size)] + recvs[at][...].astype(jnp.float32)
            kept.append((offset, size))
        else:
            acc[pl.ds(offset, size)] = sends[at][...].astype(jnp.float32) + recvs[at][...].astype(jnp.float32)
    gathered[pl.ds(offset, size)] = acc[pl.ds(offset, size)].astype(jnp.bfloat16)
    for back in range(halvings):
        at = halvings - 1 - back
        begin, extent = kept[at]
        (axis, _), (partner, _) = steps[at], partners[at]
        here = gathered.at[pl.ds(begin, extent)]
        copy = pltpu.make_async_remote_copy(
            src_ref=here,
            dst_ref=here,
            send_sem=sem_send.at[count + back],
            recv_sem=sem_recv.at[count + back],
            device_id={axis: partner},
            device_id_type=MESH,
        )
        copy.start()
        copy.wait()
    scale_a, scale_b = scales
    total = gathered[...].astype(jnp.float32)
    out_wb[...] = total[:top] * scale_b
    out_wa[:half] = total[top : top + half, :width] * scale_a
    out_wa[half:] = total[top : top + half, width:] * scale_a
    out_ba[...] = total[top + half : top + half + 1, :width] * scale_a
    out_bb[...] = total[top + half + 8 : top + half + 9] * scale_b


def summed_grads(wa, ba, wb, bb, scales):
    used = wb.shape[0] + wa.shape[0] // 2 + 16
    rows = used + -used % 128
    cut = {
        axis: [2**i for i in range(lax.axis_size(axis).bit_length() - 1)] for axis in ("gz", "gx", "gy")
    }
    steps = [("gz", bit) for bit in cut["gz"][:1]]
    steps += [("gx", bit) for bit in cut["gx"]] + [("gy", bit) for bit in cut["gy"]]
    steps += [("gz", bit) for bit in cut["gz"][1:]]
    halvings = 0
    sizes = []
    size = rows
    for _ in steps:
        if len(sizes) == halvings and size % 32 == 0:
            size //= 2
            halvings += 1
        sizes.append(size)
    buffers = [pltpu.VMEM((s, 128), jnp.bfloat16) for s in sizes]
    total = len(steps) + halvings
    shapes = [wa.shape, (1, ba.shape[1]), wb.shape, (1, bb.shape[1])]
    return pl.pallas_call(
        functools.partial(sum_kernel, steps, halvings, rows, scales),
        out_shape=[jax.ShapeDtypeStruct(shape, jnp.float32) for shape in shapes],
        in_specs=[pl.BlockSpec(memory_space=pltpu.VMEM)] * 4,
        out_specs=[pl.BlockSpec(memory_space=pltpu.VMEM)] * 4,
        scratch_shapes=[
            pltpu.VMEM((rows, 128), jnp.float32),
            pltpu.VMEM((rows, 128), jnp.bfloat16),
            *buffers,
            *buffers,
            pltpu.SemaphoreType.DMA((total,)),
            pltpu.SemaphoreType.DMA((total,)),
        ],
        compiler_params=pltpu.CompilerParams(collective_id=0, has_side_effects=True),
    )(wa, ba, wb, bb)


def line_ends(axis_sizes):
    across, count = axis_sizes
    total = across * count
    line = lax.axis_index("gx") * count + lax.axis_index("gz")
    after, before = (line + 1) % total, (line + total - 1) % total
    ids = [{"gx": at // count, "gz": at % count} for at in (after, before)]
    return line, total, ids


class Halo:
    def __init__(self, wide, dims, where, sems, at):
        planes, rows, depth = dims
        self.line, self.total, ids = where
        size, stride = rows * depth, (rows + 2) * depth
        spot = lambda plane: wide.at[:, plane * stride + depth : plane * stride + depth + size]
        send, recv = sems
        self.up, self.down = [
            pltpu.make_async_remote_copy(
                src_ref=spot(source),
                dst_ref=spot(target),
                send_sem=send.at[at + i],
                recv_sem=recv.at[at + i],
                device_id=ids[i],
                device_id_type=MESH,
            )
            for i, (source, target) in enumerate(((planes, 0), (1, planes + 1)))
        ]

    def start(self):
        pl.when(self.line < self.total - 1)(self.up.start)
        pl.when(self.line > 0)(self.down.start)

    def wait(self):
        @pl.when(self.line < self.total - 1)
        def _():
            self.up.wait_send()
            self.down.wait_recv()

        @pl.when(self.line > 0)
        def _():
            self.down.wait_send()
            self.up.wait_recv()


class Summing:
    def __init__(self, steps, sizes, acc, gathered, sends, recvs, sems):
        self.steps, self.sizes = steps, sizes
        self.acc, self.gathered, self.sends, self.recvs = acc, gathered, sends, recvs
        self.sems = sems
        self.partners = [partner_of(axis, bit) for axis, bit in steps]
        rows = [acc.shape[0]] + list(sizes)
        self.halvings = sum(a != b for a, b in zip(rows, sizes))
        self.stages = len(steps) + self.halvings
        self.offset = 0
        self.kept = []
        self.flying = None

    def copy(self, stage, source, target, step):
        send, recv = self.sems
        self.flying = pltpu.make_async_remote_copy(
            src_ref=source,
            dst_ref=target,
            send_sem=send.at[stage],
            recv_sem=recv.at[stage],
            device_id={self.steps[step][0]: self.partners[step][0]},
            device_id_type=MESH,
        )
        self.flying.start()

    def start(self, stage):
        if stage < len(self.steps):
            size = self.sizes[stage]
            away = self.offset
            if stage < self.halvings:
                mine = self.partners[stage][1]
                away = pl.multiple_of(self.offset + (1 - mine) * size, 16)
                self.offset = pl.multiple_of(self.offset + mine * size, 16)
                self.kept.append((self.offset, size))
            self.sends[stage][...] = self.acc[pl.ds(away, size)].astype(jnp.bfloat16)
            self.copy(stage, self.sends[stage], self.recvs[stage], stage)
        else:
            step = self.halvings - 1 - (stage - len(self.steps))
            begin, size = self.kept[step]
            here = self.gathered.at[pl.ds(begin, size)]
            self.copy(stage, here, here, step)

    def finish(self, stage):
        self.flying.wait()
        if stage >= len(self.steps):
            return
        here = pl.ds(self.offset, self.sizes[stage])
        came = self.recvs[stage][...].astype(jnp.float32)
        own = self.acc[here] if stage < self.halvings else self.sends[stage][...].astype(jnp.float32)
        total = own + came
        if stage == len(self.steps) - 1:
            self.gathered[here] = total.astype(jnp.bfloat16)
        else:
            self.acc[here] = total


def place(wide, flat, dims):
    planes, rows, depth = dims
    size, stride = rows * depth, (rows + 2) * depth
    for plane in range(planes):
        begin = (plane + 1) * stride + depth
        wide[:, begin : begin + size] = flat[:, plane * size : (plane + 1) * size]


def whole_kernel(setting, *refs):
    fine, coarse, sizes_line, steps, cuts_a, cuts_b, scales = setting
    slab, w_a, b_a, pool, w_b, b_b, cot, v_b, spread, v_a = refs[:10]
    features, grad_slab, out_wa, out_ba, out_wb, out_bb = refs[10:16]
    wide_a, wide_b, wide_gb, wide_ga, win_a, win_b, win_gb, win_ga = refs[16:24]
    before_a, pooled, grad_b, grad_a, acc_a, acc_b, all_a, all_b = refs[24:32]
    count = len(steps)
    send_a, recv_a, send_b, recv_b = [refs[32 + i * count : 32 + (i + 1) * count] for i in range(4)]
    sems = refs[32 + 4 * count :]
    where = line_ends(sizes_line)
    line, total, ids = where
    barrier = pltpu.get_barrier_semaphore()
    for wide in (wide_a, wide_b, wide_gb, wide_ga):
        wide[...] = jnp.zeros_like(wide)
    place(wide_a, slab, fine)
    for axis, bit in steps:
        partner, _ = partner_of(axis, bit)
        pl.semaphore_signal(barrier, inc=1, device_id={axis: partner}, device_id_type=MESH)
    for device in ids:
        pl.semaphore_signal(barrier, inc=1, device_id=device, device_id_type=MESH)
    pl.semaphore_wait(barrier, count + 2)
    halos = [
        Halo(wide, dims, where, sems[:2], 2 * i)
        for i, (wide, dims) in enumerate(
            ((wide_a, fine), (wide_b, coarse), (wide_gb, coarse), (wide_ga, fine))
        )
    ]
    sum_a = Summing(steps, cuts_a, acc_a, all_a, send_a, recv_a, sems[2:4])
    sum_b = Summing(steps, cuts_b, acc_b, all_b, send_b, recv_b, sems[4:6])

    halos[0].start()
    halos[0].wait()
    forward_a_kernel(fine, wide_a, w_a, b_a, pool, before_a, pooled, win_a)
    place(wide_b, pooled, coarse)
    halos[1].start()
    halos[1].wait()
    top_b = out_wb.shape[0]
    middle_kernel(
        coarse, wide_b, w_b, b_b, cot, features, grad_b, acc_b.at[:top_b], acc_b.at[top_b : top_b + 8], win_b
    )
    place(wide_gb, grad_b, coarse)
    halos[2].start()
    acc_b[top_b + 8 :] = jnp.zeros((acc_b.shape[0] - top_b - 8, acc_b.shape[1]), jnp.float32)
    sum_b.start(0)
    halos[2].wait()
    backward_b_kernel(coarse, fine, wide_gb, v_b, before_a, spread, grad_a, win_gb)
    place(wide_ga, grad_a, fine)
    halos[3].start()
    sum_b.finish(0)
    sum_b.start(1)
    grad = grad_a[...]
    half, width = out_wa.shape[0] // 2, out_wa.shape[1]
    acc_a[:half, :width] = dot_rows(win_a[:half], grad)
    acc_a[:half, width:] = dot_rows(win_a[half:], grad)
    acc_a[half:] = jnp.zeros((acc_a.shape[0] - half, acc_a.shape[1]), jnp.float32)
    acc_a[half : half + 8, :width] = dot_rows(jnp.ones((8, grad.shape[1]), jnp.bfloat16), grad)
    sum_b.finish(1)
    sum_b.start(2)
    sum_a.start(0)
    halos[3].wait()
    backward_a_kernel(fine, wide_ga, v_a, grad_slab, win_ga)
    for stage in range(max(sum_a.stages, sum_b.stages - 2)):
        if stage + 2 < sum_b.stages:
            sum_b.finish(stage + 2)
            if stage + 3 < sum_b.stages:
                sum_b.start(stage + 3)
        if stage < sum_a.stages:
            sum_a.finish(stage)
            if stage + 1 < sum_a.stages:
                sum_a.start(stage + 1)
    scale_a, scale_b = scales
    out_wb[...] = all_b[:top_b].astype(jnp.float32) * scale_b
    out_bb[...] = all_b[top_b : top_b + 16].astype(jnp.float32)[:1] * scale_b
    out_wa[:half] = all_a[:half, :width].astype(jnp.float32) * scale_a
    out_wa[half:] = all_a[:half, width:].astype(jnp.float32) * scale_a
    out_ba[...] = all_a[half : half + 16, :width].astype(jnp.float32)[:1] * scale_a


def stage_sizes(rows, steps):
    sizes = []
    for _ in steps:
        halve = rows % 32 == 0 and len(sizes) < 3
        rows = rows // 2 if halve else rows
        sizes.append(rows)
    return sizes


def all_steps():
    cut = {
        axis: [2**i for i in range(lax.axis_size(axis).bit_length() - 1)] for axis in ("gz", "gx", "gy")
    }
    steps = [("gz", bit) for bit in cut["gz"][:1]]
    steps += [("gx", bit) for bit in cut["gx"]] + [("gy", bit) for bit in cut["gy"]]
    return steps + [("gz", bit) for bit in cut["gz"][1:]]


def between_exchanges(fine, coarse, scales, slab, weight_a, bias_a, weight_b, bias_b, cot, pool):
    f32, bf16 = jnp.float32, jnp.bfloat16
    c1, cells = slab.shape
    c2, c3 = weight_b.shape[3:]
    fewer = cells // 8
    steps = all_steps()
    rows_a = 27 * c1 // 2 + 16
    rows_a += -rows_a % 128
    rows_b = 27 * c2 + 16
    rows_b += -rows_b % 128
    cuts_a, cuts_b = stage_sizes(rows_a, steps), stage_sizes(rows_b, steps)
    extent = lambda dims: (dims[0] + 2) * (dims[1] + 2) * dims[2]
    setting = (fine, coarse, (lax.axis_size("gx"), lax.axis_size("gz")), steps, cuts_a, cuts_b, scales)
    buffers = [pltpu.VMEM((n, 128), bf16) for cuts in (cuts_a, cuts_a, cuts_b, cuts_b) for n in cuts]
    outs = [
        ((c3, fewer), bf16),
        ((c1, cells), bf16),
        ((27 * c1, c2), f32),
        ((1, c2), f32),
        ((27 * c2, c3), f32),
        ((1, c3), f32),
    ]
    operands = (
        slab,
        outward(weight_a),
        bias_a[:, None],
        pool,
        outward(weight_b),
        bias_b[:, None],
        cot,
        inward(weight_b),
        pool.T.astype(bf16),
        inward(weight_a),
    )
    most = 2 * len(steps)
    return pl.pallas_call(
        functools.partial(whole_kernel, setting),
        out_shape=[jax.ShapeDtypeStruct(shape, dtype) for shape, dtype in outs],
        in_specs=[pl.BlockSpec(memory_space=pltpu.VMEM)] * len(operands),
        out_specs=[pl.BlockSpec(memory_space=pltpu.VMEM)] * len(outs),
        scratch_shapes=[
            pltpu.VMEM((c1, extent(fine)), bf16),
            pltpu.VMEM((c2, extent(coarse)), bf16),
            pltpu.VMEM((c3, extent(coarse)), bf16),
            pltpu.VMEM((c2, extent(fine)), bf16),
            pltpu.VMEM((27 * c1, cells), bf16),
            pltpu.VMEM((27 * c2, fewer), bf16),
            pltpu.VMEM((27 * c3, fewer), bf16),
            pltpu.VMEM((27 * c2, cells), bf16),
            pltpu.VMEM((c2, cells), f32),
            pltpu.VMEM((c2, fewer), bf16),
            pltpu.VMEM((c3, fewer), bf16),
            pltpu.VMEM((c2, cells), bf16),
            pltpu.VMEM((rows_a, 128), f32),
            pltpu.VMEM((rows_b, 128), f32),
            pltpu.VMEM((rows_a, 128), bf16),
            pltpu.VMEM((rows_b, 128), bf16),
            *buffers,
            pltpu.SemaphoreType.DMA((8,)),
            pltpu.SemaphoreType.DMA((8,)),
            *[pltpu.SemaphoreType.DMA((most,))] * 4,
        ],
        compiler_params=pltpu.CompilerParams(
            collective_id=1, has_side_effects=True, vmem_limit_bytes=60 * 2**20
        ),
    )(*operands)


def outward(weight):
    return weight.reshape(-1, weight.shape[-1]).T


def inward(weight):
    taps = weight[::-1, ::-1, ::-1].reshape(27, *weight.shape[3:])
    return jnp.transpose(taps, (1, 0, 2)).reshape(weight.shape[3], -1)


def lanes_of(shape):
    return lax.broadcasted_iota(jnp.int32, shape, len(shape) - 1)


def rows_of(shape):
    return lax.broadcasted_iota(jnp.int32, shape, 0)


def ones_where(mask):
    return jnp.where(mask, 1.0, 0.0).astype(jnp.bfloat16)


def dot(left, right):
    return jnp.dot(left, right, preferred_element_type=jnp.float32)


def by_parts(rank_bits, mask):
    place = {}
    for at, (axis, bit) in enumerate(rank_bits):
        if mask >> at & 1:
            me = place.get(axis, lax.axis_index(axis))
            place[axis] = me + bit * (1 - 2 * ((lax.axis_index(axis) // bit) % 2))
    return place


def own_rank(rank_bits, mask=0):
    total = 0
    for at, (axis, bit) in enumerate(rank_bits):
        mine = (lax.axis_index(axis) // bit) % 2
        total = total + ((1 - mine) if mask >> at & 1 else mine) * 2**at
    return total


def remote(source, target, sems, at, device):
    return pltpu.make_async_remote_copy(
        src_ref=source,
        dst_ref=target,
        send_sem=sems[0].at[at],
        recv_sem=sems[1].at[at],
        device_id=device,
        device_id_type=MESH,
    )


class Reduction:
    def __init__(self, groups, exchanged, acc, summed, sends, recvs, sems):
        self.groups, self.exchanged, self.acc, self.summed = groups, exchanged, acc, summed
        self.sends, self.recvs, self.sems = sends, recvs, sems
        self.offset, self.size = 0, acc.shape[0]
        self.kept = []
        self.flying = []
        self.used = 0
        self.stage = 0
        self.stages = 2 * len(groups) - (1 if exchanged else 0)

    def fly(self, source, target, device):
        copy = remote(source, target, self.sems, self.used, device)
        self.used += 1
        copy.start()
        self.flying.append(copy)

    def start(self):
        at = self.stage
        count = len(self.groups)
        if self.exchanged and at == count - 1:
            bits = self.groups[at]
            recv = self.recvs[at]
            mine = own_rank(bits)
            recv[mine] = self.acc[pl.ds(self.offset, self.size)].astype(jnp.bfloat16)
            for mask in range(1, 2 ** len(bits)):
                self.fly(recv.at[mine], recv.at[mine], by_parts(bits, mask))
        elif at < count:
            bits = self.groups[at]
            members = 2 ** len(bits)
            part = self.size // members
            send, recv = self.sends[at], self.recvs[at]
            send[...] = self.acc[pl.ds(self.offset, self.size)].astype(jnp.bfloat16)
            for mask in range(1, members):
                begin = pl.multiple_of(own_rank(bits, mask) * part, 8)
                self.fly(send.at[pl.ds(begin, part)], recv.at[mask - 1], by_parts(bits, mask))
            self.kept.append((self.offset, self.size))
            self.offset = pl.multiple_of(self.offset + own_rank(bits) * part, 8)
            self.size = part
        else:
            bits = self.groups[len(self.kept) - 1]
            here = self.summed.at[pl.ds(self.offset, self.size)]
            for mask in range(1, 2 ** len(bits)):
                self.fly(here, here, by_parts(bits, mask))
            self.offset, self.size = self.kept.pop()

    def finish(self):
        at = self.stage
        count = len(self.groups)
        for copy in self.flying:
            copy.wait()
        self.flying = []
        self.stage += 1
        if at >= count:
            return
        recv = self.recvs[at]
        here = pl.ds(self.offset, self.size)
        if self.exchanged and at == count - 1:
            total = recv[0].astype(jnp.float32)
            for i in range(1, recv.shape[0]):
                total = total + recv[i].astype(jnp.float32)
        else:
            total = self.acc[here]
            for i in range(recv.shape[0]):
                total = total + recv[i].astype(jnp.float32)
        if at == count - 1:
            self.summed[here] = total.astype(jnp.bfloat16)
        else:
            self.acc[here] = total

    def step(self):
        self.finish()
        if self.stage < self.stages:
            self.start()


class Border:
    def __init__(self, first, last, edge, inbox, sems, at):
        me, count = lax.axis_index("gz"), lax.axis_size("gz")
        side = 1 - lax.axis_index("gx")
        self.inner, self.outer = me > 0, me < count - 1
        up, down = (me + 1) % count, (me + count - 1) % count
        low, high, beside, beside_low, beside_high = inbox
        self.always = remote(edge, beside, sems, at + 2, {"gx": side})
        self.up = [
            remote(last, low, sems, at, {"gz": up}),
            remote(edge, beside_low, sems, at + 3, {"gx": side, "gz": up}),
        ]
        self.down = [
            remote(first, high, sems, at + 1, {"gz": down}),
            remote(edge, beside_high, sems, at + 4, {"gx": side, "gz": down}),
        ]

    def start(self):
        @pl.when(self.outer)
        def _():
            for copy in self.up:
                copy.start()

        @pl.when(self.inner)
        def _():
            for copy in self.down:
                copy.start()

        self.always.start()

    def wait(self):
        self.always.wait()

        @pl.when(self.outer)
        def _():
            for copy in self.up:
                copy.wait_send()
            for copy in self.down:
                copy.wait_recv()

        @pl.when(self.inner)
        def _():
            for copy in self.down:
                copy.wait_send()
            for copy in self.up:
                copy.wait_recv()


def gathered_edge(tiles, extent, slots):
    shape = tiles[0].shape
    lane = lanes_of(shape)
    high = lax.axis_index("gx") == 0
    edge = jnp.where(high, extent - 1, 0)
    at_edge = lane & (extent - 1) == edge
    total = None
    for i, tile in enumerate(tiles):
        kept = rolled(jnp.where(at_edge, tile, 0.0), i % slots)
        total = kept if total is None else total + kept
    back = pltpu.roll(total, 128 - (extent - 1), 1)
    return jnp.where(high, back, total)


def rolled(value, by):
    by = by % 128
    return pltpu.roll(value, by, 1) if by else value


def quarters(edge):
    size = edge.shape[0] // 4
    return sum(rolled(edge[q * size : (q + 1) * size], 4 * q) for q in range(4))


def spread_edge(edge, by, packed):
    if not packed:
        return rolled(edge, by)
    return jnp.concatenate([rolled(edge, by - 4 * q) for q in range(4)], axis=0)


def halved(tile, low):
    size = tile.shape[0] // 2
    lane = lanes_of((size, 128))
    upper, lower = tile[:size], rolled(tile[size:], 64)
    return jnp.where(lane < 64, upper, lower) if low else jnp.where(lane < 64, lower, upper)


def beside(tile, edges, extent, packed):
    low_edge, high_edge, at = edges
    lane = lanes_of(tile.shape) & (extent - 1)
    before = jnp.where(lane == 0, spread_edge(low_edge, -at, packed), rolled(tile, 1))
    after = jnp.where(lane == extent - 1, spread_edge(high_edge, extent - 1 - at, packed), rolled(tile, -1))
    return before, after


def sided(edge):
    high = lax.axis_index("gx") == 0
    zero = jnp.zeros_like(edge)
    return jnp.where(high, zero, edge), jnp.where(high, edge, zero)


def moved_rows(pair, stride):
    lane = lanes_of(pair[0].shape)
    down = [rolled(tile, stride) for tile in pair]
    up = [rolled(tile, -stride) for tile in pair]
    low = lane < stride
    high = lane < 128 - stride
    zero = jnp.zeros_like(pair[0])
    before = (jnp.where(low, zero, down[0]), jnp.where(low, down[0], down[1]))
    after = (jnp.where(high, up[0], up[1]), jnp.where(high, up[1], zero))
    return before, after


def moved_half(tile, stride):
    lane = lanes_of(tile.shape) & 63
    zero = jnp.zeros_like(tile)
    before = jnp.where(lane < stride, zero, rolled(tile, stride))
    after = jnp.where(lane < 64 - stride, rolled(tile, -stride), zero)
    return before, after


def inbox_values(inbox):
    low, high, across, across_low, across_high = [ref[...] for ref in inbox]
    return low, high, sided(across), sided(across_low), sided(across_high)


def fine_planes(read, inbox, planes):
    low, high, across, across_low, across_high = inbox_values(inbox)
    for p in range(planes + 2):
        if p == 0:
            pair, edge, at = (low[:, :128], low[:, 128:]), across_low, 2 * (planes - 1)
        elif p == planes + 1:
            pair, edge, at = (high[:, :128], high[:, 128:]), across_high, 0
        else:
            pair, edge, at = read(p - 1), across, 2 * (p - 1)
        sides = [beside(tile, (*edge, at + g), 32, False) for g, tile in enumerate(pair)]
        yield p, ((sides[0][0], sides[1][0]), pair, (sides[0][1], sides[1][1]))


def coarse_tiles(field, inbox, tiles):
    low, high, across, across_low, across_high = inbox_values(inbox)
    low = jnp.concatenate([low, rolled(low, 64)], axis=0)
    high = jnp.concatenate([high, rolled(high, 64)], axis=0)
    half = lanes_of(low.shape) < 64
    for t in range(tiles):
        tile = field[:, t * 128 : (t + 1) * 128]
        sides = list(beside(tile, (*across, t % 4), 16, True))
        if t == 0:
            sides_low = beside(low, (*across_low, (tiles - 1) % 4), 16, True)
            tile = jnp.where(half, low, tile)
            sides = [jnp.where(half, a, b) for a, b in zip(sides_low, sides)]
        if t == tiles - 1:
            sides_high = beside(high, (*across_high, 0), 16, True)
            tile = jnp.where(half, tile, high)
            sides = [jnp.where(half, b, a) for a, b in zip(sides_high, sides)]
        yield t, (sides[0], tile, sides[1])


def column(row, size):
    wide = jnp.broadcast_to(row, (size, size))
    eye = rows_of((size, size)) == lanes_of((size, size))
    return jnp.sum(jnp.where(eye, wide, 0.0), axis=1, keepdims=True)


def joined_thirds(terms, tiles):
    half = None
    low = [rolled(terms(0, t), 64) for t in range(tiles)]
    high = [rolled(terms(2, t), 64) for t in range(tiles)]
    out = []
    for t in range(tiles):
        if half is None:
            half = lanes_of(low[0].shape) < 64
        before, after = low[max(t - 1, 0)], high[min(t + 1, tiles - 1)]
        out.append(terms(1, t) + jnp.where(half, before + high[t], low[t] + after))
    return out


def block_kernel(setting, *refs):
    groups, groups_a, cuts = setting
    inputs, outputs = refs[:6], refs[6:10]
    volume, w_a, b_a, w_b, b_b, cot = refs[10:16]
    (
        stage, own_a, windows_a, sums_a, slope_a, halves, pooled, windows_b, sums_b,
        cot_sent, cot_came, cot_here, grad_b, lines_b, sums_gb, grads_a, lines_a, sums_ga,
        feat_sent, feat_came, mat_a, mat_b, mat_ga, mat_gb, near, far, acc_a, acc_b,
        features, grad_in, sum_a, sum_b,
    ) = refs[16:48]
    rest = list(refs[48:])
    inboxes = [[rest.pop(0) for _ in range(5)] for _ in range(4)]
    edges = [rest.pop(0) for _ in range(4)]
    ends_b, ends_gb = [[rest.pop(0), rest.pop(0)] for _ in range(2)]
    count = len(groups)
    takes = lambda n: [rest.pop(0) for _ in range(n)]
    send_a, recv_a = takes(1), takes(2)
    send_b, recv_b, send_c, recv_c = [takes(count) for _ in range(4)]
    sems_halo, sems_cot, sems_feat, sems_a, sems_b, sems_c = [takes(2) for _ in range(6)]
    sems_in, sems_out = rest
    f32, bf16 = jnp.float32, jnp.bfloat16
    c1, rows, planes, width = volume.shape
    c2, c3 = w_a.shape[2], w_b.shape[2]
    tiles = planes // 4 + 1
    me, members = lax.axis_index("gz"), lax.axis_size("gz")
    whole = [bit for group in groups for bit in group]
    line = [bit for bit in whole if bit[0] == "gz"]

    barrier = pltpu.get_barrier_semaphore()
    for mask in range(1, 2 ** len(whole)):
        pl.semaphore_signal(barrier, inc=1, device_id=by_parts(whole, mask), device_id_type=MESH)
    loads = [
        pltpu.make_async_copy(source, target, sems_in.at[at])
        for at, (source, target) in enumerate(zip(inputs, refs[10:16]))
    ]
    parts = 4
    share = c1 // parts
    loads_v = [
        pltpu.make_async_copy(
            inputs[0].at[i * share : (i + 1) * share],
            volume.at[i * share : (i + 1) * share],
            sems_in.at[6 + i],
        )
        for i in range(parts)
    ]
    for load in loads_v:
        load.start()
    for at in (5, 1, 3, 2, 4):
        loads[at].start()

    @pl.when(me == 0)
    def _():
        for inbox in inboxes:
            for box in (inbox[0], inbox[3]):
                box[...] = jnp.zeros_like(box)

    @pl.when(me == members - 1)
    def _():
        for inbox in inboxes:
            for box in (inbox[1], inbox[4]):
                box[...] = jnp.zeros_like(box)

    for load in loads_v:
        load.wait()
    for g in range(2):
        for i in range(4):
            part = volume[:, 4 * g + i].astype(f32).reshape(c1 * planes, width)
            stage[:, width * i : width * (i + 1)] = part
        for z in range(planes):
            tile = stage[pl.ds(z, c1, stride=planes), :]
            own_a[:, z * 256 + g * 128 : z * 256 + (g + 1) * 128] = tile.astype(bf16)

    def read_a(z):
        return tuple(own_a[:, z * 256 + g * 128 : z * 256 + (g + 1) * 128] for g in range(2))

    edges[0][...] = gathered_edge([tile.astype(f32) for z in range(planes) for tile in read_a(z)], 32, 32).astype(bf16)
    pl.semaphore_wait(barrier, 2 ** len(whole) - 1)

    border_a = Border(own_a.at[:, :256], own_a.at[:, (planes - 1) * 256 :], edges[0], inboxes[0], sems_halo, 0)
    border_a.start()

    def exchange(sent, came, sems):
        flying = []
        size = sent.shape[0] // members
        for mask in range(1, members):
            begin = pl.multiple_of(own_rank(line, mask) * size, 16)
            copy = remote(
                sent.at[pl.ds(begin, size)],
                came.at[pl.ds(pl.multiple_of(me * size, 16), size)],
                sems,
                mask - 1,
                by_parts(line, mask),
            )
            copy.start()
            flying.append(copy)
        here = pl.ds(pl.multiple_of(me * size, 16), size)
        came[here] = sent[here]
        return flying

    r, l = rows_of(far.shape), lanes_of(far.shape)
    far[...] = ones_where(((r >> 3) & 3 == l >> 7) & (((r >> 5) << 3) + (r & 7) == l & 127))
    loads[5].wait()
    half_rows = rows // 2
    stage[...] = cot[...].astype(f32)
    spaced = [stage[pl.ds(y, c3, stride=half_rows), :].astype(bf16) for y in range(half_rows)]
    cot_sent[...] = dot_rows(far[...], jnp.concatenate(spaced, axis=1)).astype(bf16)
    cot_flying = exchange(cot_sent, cot_came, sems_cot)
    for load in loads[1:5]:
        load.wait()

    eye = ones_where(rows_of((c2, c2)) == lanes_of((c2, c2)))
    eye_b = ones_where(rows_of((c3, c3)) == lanes_of((c3, c3)))
    for kz in range(3):
        block = w_a[:].reshape(9, 3, c1, c2)[:, kz].reshape(9 * c1, c2)
        mat_a[kz * c2 : (kz + 1) * c2] = dot_rows(eye, block).astype(bf16)
        block = w_b[:].reshape(9, 3, c2, c3)[:, kz].reshape(9 * c2, c3)
        mat_b[kz * c3 : (kz + 1) * c3] = dot_rows(eye_b, block).astype(bf16)
        for ky in range(3):
            for kx in range(3):
                tap = ((2 - kx) * 3 + 2 - ky) * 3 + 2 - kz
                at = kz * 3 + ky
                mat_ga[at * c1 : (at + 1) * c1, kx * c2 : (kx + 1) * c2] = w_a[tap]
                mat_gb[at * c2 : (at + 1) * c2, kx * c3 : (kx + 1) * c3] = w_b[tap]
    col_a, col_b = column(b_a[...], c2), column(b_b[...], c3)
    r, l = rows_of(near.shape), lanes_of(near.shape)
    near[...] = ones_where(
        ((r & 7) + 1 == l >> 6) & ((r >> 3) & 3 == (l >> 4) & 3) & (r >> 5 == l & 15)
    )
    r, l = rows_of((512, 128)), lanes_of((512, 128))
    pool = ones_where(
        (r >> 8 == l >> 6) & ((r >> 6) & 3 == (l >> 4) & 3) & ((r & 31) >> 1 == l & 15)
    )
    halves[...] = jnp.zeros_like(halves)
    for kz in range(3):
        for p in range(planes + 2):
            if not 0 <= p + kz - 2 < planes:
                grads_a[kz * c2 : (kz + 1) * c2, p * 256 : (p + 1) * 256] = jnp.zeros((c2, 256), bf16)
    acc_a[...] = jnp.zeros_like(acc_a)
    border_a.wait()

    step = 2 * 256
    for p, thirds in fine_planes(read_a, inboxes[0], planes):
        for kx, pair in enumerate(thirds):
            before, after = moved_rows(pair, 32)
            for ky, (first, second) in enumerate((before, pair, after)):
                at = (kx * 3 + ky) * c1
                windows_a[at : at + c1, p * 256 : p * 256 + 128] = first.astype(bf16)
                windows_a[at : at + c1, p * 256 + 128 : (p + 1) * 256] = second.astype(bf16)
        if p % 2:
            here = slice((p - 1) * 256, (p + 1) * 256)
            sums_a[:, here] = dot(mat_a[...], windows_a[:, here])
    for z in range(planes):
        value = (
            sums_a[:c2, z * 256 : (z + 1) * 256]
            + sums_a[c2 : 2 * c2, (z + 1) * 256 : (z + 2) * 256]
            + sums_a[2 * c2 :, (z + 2) * 256 : (z + 3) * 256]
            + col_a
        )
        sigma = jax.nn.sigmoid(value)
        active = value * sigma
        slope_a[:, z * 256 : (z + 1) * 256] = (sigma + active * (1.0 - sigma)) * 0.125
        if z % 2:
            active = active + kept
            pz = z // 2 + 1
            upper = active.astype(bf16)
            lower = (active - upper.astype(f32)).astype(bf16)
            at, lane = pz // 2 * c2, pz % 2 * 256
            halves[at : at + c2, lane : lane + 256] = upper
            halves[tiles * c2 + at : tiles * c2 + at + c2, lane : lane + 256] = lower
        else:
            kept = active
    both = dot(halves[...], pool)
    both = (both[: tiles * c2] + both[tiles * c2 :]) * 0.125
    for t in range(tiles):
        pooled[:, t * 128 : (t + 1) * 128] = both[t * c2 : (t + 1) * c2].astype(bf16)

    def coarse_border(field, edge, ends, inbox, at):
        parts = [field[:, t * 128 : (t + 1) * 128].astype(f32) for t in range(tiles)]
        edge[...] = quarters(gathered_edge(parts, 16, 4)).astype(bf16)
        ends[0][...] = halved(parts[0], False).astype(bf16)
        ends[1][...] = halved(parts[-1], True).astype(bf16)
        return Border(ends[0], ends[1], edge, inbox, sems_halo, at)

    border_b = coarse_border(pooled, edges[1], ends_b, inboxes[1], 5)
    border_b.start()
    for copy in cot_flying:
        copy.wait()
    came = jnp.transpose(cot_came[...].astype(f32)).astype(bf16)
    cot_here[...] = dot(came, near[...])
    border_b.wait()

    for t, thirds in coarse_tiles(pooled, inboxes[1], tiles):
        for kx, tile in enumerate(thirds):
            before, after = moved_half(tile, 16)
            for ky, value in enumerate((before, tile, after)):
                at = (kx * 3 + ky) * c2
                windows_b[at : at + c2, t * 128 : (t + 1) * 128] = value.astype(bf16)
    sums_b[...] = dot(mat_b[...], windows_b[...])
    joined = joined_thirds(lambda k, t: sums_b[k * c3 : (k + 1) * c3, t * 128 : (t + 1) * 128], tiles)
    feats = []
    for t, value in enumerate(joined):
        value = value + col_b
        sigma = jax.nn.sigmoid(value)
        active = value * sigma
        feats.append(active.astype(bf16))
        slope = sigma + active * (1.0 - sigma)
        grad = cot_here[:, t * 128 : (t + 1) * 128] * slope
        grad_b[c3 : 2 * c3, t * 128 : (t + 1) * 128] = grad.astype(bf16)
    own_gb = grad_b.at[c3 : 2 * c3]
    border_gb = coarse_border(own_gb, edges[2], ends_gb, inboxes[2], 10)
    border_gb.start()

    half = lanes_of((c3, 128)) < 64
    turned = [rolled(own_gb[:, t * 128 : (t + 1) * 128].astype(f32), 64) for t in range(tiles)]
    zero = jnp.zeros_like(turned[0])
    for t in range(tiles):
        later = turned[t + 1] if t + 1 < tiles else zero
        earlier = turned[t - 1] if t else zero
        here = slice(t * 128, (t + 1) * 128)
        grad_b[:c3, here] = jnp.where(half, turned[t], later).astype(bf16)
        grad_b[2 * c3 :, here] = jnp.where(half, earlier, turned[t]).astype(bf16)
    top = 27 * c2

    def sum_terms(first, last):
        terms = dot_rows(windows_b[first * c2 : last * c2], grad_b[...])
        for at in range(first, last):
            for kz in range(3):
                tap = at * 3 + kz
                acc_b[tap * c2 : (tap + 1) * c2] = terms[
                    (at - first) * c2 : (at - first + 1) * c2, kz * c3 : (kz + 1) * c3
                ]

    cut = cuts[0]
    early = -(-cut // (3 * c2))
    sum_terms(0, early)
    total_b = Reduction(groups, False, acc_b.at[:cut], sum_b.at[:cut], send_b, recv_b, sems_b)
    total_b.start()
    sum_terms(early, 9)
    acc_b[top:] = jnp.zeros((acc_b.shape[0] - top, c3), f32)
    acc_b[top : top + 8] = dot_rows(jnp.ones((8, tiles * 128), bf16), own_gb[...])
    total_c = Reduction(groups, False, acc_b.at[cut:], sum_b.at[cut:], send_c, recv_c, sems_c)
    total_c.start()
    feat_sent[...] = dot_rows(near[...], jnp.concatenate(feats, axis=1)).astype(bf16)
    feat_flying = exchange(feat_sent, feat_came, sems_feat)
    total_b.step()
    total_c.step()
    border_gb.wait()

    for t, thirds in coarse_tiles(own_gb, inboxes[2], tiles):
        for kx, tile in enumerate(thirds):
            lines_b[kx * c3 : (kx + 1) * c3, t * 128 : (t + 1) * 128] = tile.astype(bf16)
    sums_gb[...] = dot(mat_gb[...], lines_b[...])
    by_row = [
        joined_thirds(
            lambda k, t: sums_gb[(k * 3 + ky) * c2 : (k * 3 + ky + 1) * c2, t * 128 : (t + 1) * 128], tiles
        )
        for ky in range(3)
    ]
    small = []
    for t in range(tiles):
        value = by_row[1][t] + moved_half(by_row[0][t], 16)[0] + moved_half(by_row[2][t], 16)[1]
        small.append(value.astype(bf16))
    spread = dot_rows(jnp.concatenate(small, axis=0), pool)
    for z in range(planes):
        pz = z // 2 + 1
        large = spread[pz // 2 * c2 : (pz // 2 + 1) * c2, pz % 2 * 256 : (pz % 2 + 1) * 256]
        grad = (large * slope_a[:, z * 256 : (z + 1) * 256]).astype(bf16)
        for kz in range(3):
            grads_a[kz * c2 : (kz + 1) * c2, (z + kz) * 256 : (z + kz + 1) * 256] = grad

    own_ga = grads_a.at[c2 : 2 * c2]

    def read_ga(z):
        return tuple(
            own_ga[:, (z + 1) * 256 + g * 128 : (z + 1) * 256 + (g + 1) * 128] for g in range(2)
        )

    edges[3][...] = gathered_edge([tile.astype(f32) for z in range(planes) for tile in read_ga(z)], 32, 32).astype(bf16)
    border_ga = Border(
        own_ga.at[:, 256:512], own_ga.at[:, planes * 256 : (planes + 1) * 256], edges[3], inboxes[3], sems_halo, 15
    )
    border_ga.start()

    terms = dot_rows(windows_a[...], grads_a[...])
    deep = 9 * c1
    acc_a[:deep] = terms[:, : 2 * c2]
    acc_a[deep : deep + deep // 2, :c2] = terms[: deep // 2, 2 * c2 :]
    acc_a[deep : deep + deep // 2, c2:] = terms[deep // 2 :, 2 * c2 :]
    top_a = deep + deep // 2
    acc_a[top_a : top_a + 8, :c2] = dot_rows(jnp.ones((8, planes * 256), bf16), own_ga[:, 256 : (planes + 1) * 256])
    total_a = Reduction(groups_a, True, acc_a, sum_a, send_a, recv_a, sems_a)
    total_a.start()
    total_b.step()
    total_c.step()
    border_ga.wait()

    for p, thirds in fine_planes(read_ga, inboxes[3], planes):
        for kx, pair in enumerate(thirds):
            for g, tile in enumerate(pair):
                at = p * 256 + g * 128
                lines_a[kx * c2 : (kx + 1) * c2, at : at + 128] = tile.astype(bf16)
    for begin in range(0, lines_a.shape[1], step):
        sums_ga[:, begin : begin + step] = dot(mat_ga[...], lines_a[:, begin : begin + step])
    total_a.step()
    total_b.step()
    total_c.step()
    for copy in feat_flying:
        copy.wait()
    came = jnp.transpose(feat_came[...].astype(f32)).astype(bf16)
    ours = dot(came, far[...])
    for y in range(half_rows):
        stage[pl.ds(y, c3, stride=half_rows), :] = ours[:, y * 128 : (y + 1) * 128]
    features[...] = stage[...].astype(bf16)
    stores = [
        pltpu.make_async_copy(source, target, sems_out.at[at])
        for at, (source, target) in enumerate(zip((features, grad_in, sum_a, sum_b), outputs))
    ]
    stores[0].start()
    results = []
    for z in range(planes):
        by_row = []
        for ky in range(3):
            value = None
            for kz in range(3):
                at = (kz * 3 + ky) * c1
                term = sums_ga[at : at + c1, (z + kz) * 256 : (z + kz + 1) * 256]
                value = term if value is None else value + term
            by_row.append((value[:, :128], value[:, 128:]))
        before, after = moved_rows(by_row[0], 32)[0], moved_rows(by_row[2], 32)[1]
        results.append([by_row[1][g] + before[g] + after[g] for g in range(2)])
    for g in range(2):
        for z in range(planes):
            stage[pl.ds(z, c1, stride=planes), :] = results[z][g]
        for i in range(4):
            part = stage[:, width * i : width * (i + 1)].astype(bf16)
            grad_in[:, 4 * g + i] = part.reshape(c1, planes, width)

    stores[1].start()
    while min(total.stage - total.stages for total in (total_a, total_b, total_c)) < 0:
        for total in (total_b, total_c, total_a):
            if total.stage < total.stages:
                total.step()
    stores[2].start()
    stores[3].start()
    for store in stores:
        store.wait()


def last_kernel(scales, *refs):
    feat, grad, sum_a, sum_b, out_feat, out_grad, out_wa, out_ba, out_wb, out_bb = refs[:10]
    kept_feat, kept_grad, kept_a, kept_b, wa, ba, wb, bb, sems_in, sems_out = refs[10:]
    f32 = jnp.float32
    scale_a, scale_b = scales
    inputs = (sum_b, grad, sum_a, feat)
    kept = (kept_b, kept_grad, kept_a, kept_feat)
    loads = [
        pltpu.make_async_copy(source, target, sems_in.at[at])
        for at, (source, target) in enumerate(zip(inputs, kept))
    ]
    for load in loads:
        load.start()
    places = ((wb, out_wb), (kept_grad, out_grad), (wa, out_wa), (kept_feat, out_feat), (ba, out_ba), (bb, out_bb))
    stores = [
        pltpu.make_async_copy(source, target, sems_out.at[at]) for at, (source, target) in enumerate(places)
    ]
    loads[0].wait()
    top = wb.shape[0]
    wb[...] = kept_b[:top].astype(f32) * scale_b
    stores[0].start()
    bb[...] = kept_b[top : top + 16].astype(f32)[:1] * scale_b
    stores[5].start()
    loads[1].wait()
    stores[1].start()
    loads[2].wait()
    c1, c2 = wa.shape[1:]
    deep = 9 * c1
    pairs = kept_a[:deep].astype(f32) * scale_a
    tail = kept_a[deep : deep + deep // 2].astype(f32) * scale_a
    thirds = jnp.concatenate([tail[:, :c2], tail[:, c2:]], axis=0)
    for at in range(9):
        here = slice(at * c1, (at + 1) * c1)
        wa[at * 3] = pairs[here, :c2]
        wa[at * 3 + 1] = pairs[here, c2:]
        wa[at * 3 + 2] = thirds[here]
    stores[2].start()
    top_a = deep + deep // 2
    ba[...] = kept_a[top_a : top_a + 16].astype(f32)[:1, :c2] * scale_a
    stores[4].start()
    loads[3].wait()
    stores[3].start()
    for store in stores:
        store.wait()


def all_groups():
    cut = {axis: [2**i for i in range(lax.axis_size(axis).bit_length() - 1)] for axis in ("gz", "gx")}
    line = [("gz", bit) for bit in cut["gz"]]
    return [line[:1], [("gx", bit) for bit in cut["gx"]] + line[1:2], line[2:]]


def on_blocks(volume, weight_a, bias_a, weight_b, bias_b, cotangent, scales):
    f32, bf16 = jnp.float32, jnp.bfloat16
    c1, width, rows, planes = volume.shape
    c2, c3 = weight_b.shape[3:]
    members = lax.axis_size("gz")
    groups = all_groups()
    tiles = planes // 4 + 1
    long, short = (planes + 2) * 256, tiles * 128
    cells = planes * 256
    rows_a, rows_b = 512, 27 * c2 + 64
    fewer = cells // 8

    def buffers(total, groups, exchanged):
        sends, recvs = [], []
        size = total
        for at, group in enumerate(groups):
            n = 2 ** len(group)
            if exchanged and at == len(groups) - 1:
                recvs.append(pltpu.VMEM((n, size, 128), bf16))
                continue
            sends.append(pltpu.VMEM((size, 128), bf16))
            size //= n
            recvs.append(pltpu.VMEM((n - 1, size, 128), bf16))
        return sends + recvs

    inboxes = []
    for size, plane, edge in ((c1, 256, c1), (c2 // 2, 128, c2 // 4), (c3 // 2, 128, c3 // 4), (c2, 256, c2)):
        inboxes += [pltpu.VMEM((size, plane), bf16)] * 2 + [pltpu.VMEM((edge, 128), bf16)] * 3
    groups_a = [groups[0] + groups[1], groups[2]]
    count_a = 2 * (2 ** len(groups_a[0]) - 1) + 2 ** len(groups_a[1]) - 1
    count_b = 2 * sum(2 ** len(group) - 1 for group in groups)
    cuts = (1024, rows_b - 1024)
    passed = [
        ((c3 * rows // 2, 128), bf16),
        ((c1, rows, planes, width), bf16),
        ((rows_a, 128), bf16),
        ((rows_b, 128), bf16),
    ]
    operands = (
        jnp.transpose(volume, (0, 2, 3, 1)),
        weight_a.reshape(27, c1, c2),
        bias_a[None],
        weight_b.reshape(27, c2, c3),
        bias_b[None],
        cotangent.reshape(c3 * rows // 2, 128),
    )
    anywhere = pl.BlockSpec(memory_space=pl.ANY)
    middle = pl.pallas_call(
        functools.partial(block_kernel, (groups, groups_a, cuts)),
        out_shape=[jax.ShapeDtypeStruct(shape, dtype) for shape, dtype in passed],
        in_specs=[anywhere] * len(operands),
        out_specs=[anywhere] * len(passed),
        scratch_shapes=[
            *[pltpu.VMEM(x.shape, x.dtype) for x in operands],
            pltpu.VMEM((c1 * planes, 128), f32),
            pltpu.VMEM((c1, cells), bf16),
            pltpu.VMEM((9 * c1, long), bf16),
            pltpu.VMEM((3 * c2, long), f32),
            pltpu.VMEM((c2, cells), f32),
            pltpu.VMEM((2 * tiles * c2, 512), bf16),
            pltpu.VMEM((c2, short), bf16),
            pltpu.VMEM((9 * c2, short), bf16),
            pltpu.VMEM((3 * c3, short), f32),
            pltpu.VMEM((fewer, c3), bf16),
            pltpu.VMEM((fewer, c3), bf16),
            pltpu.VMEM((c3, short), f32),
            pltpu.VMEM((3 * c3, short), bf16),
            pltpu.VMEM((3 * c3, short), bf16),
            pltpu.VMEM((9 * c2, short), f32),
            pltpu.VMEM((3 * c2, long), bf16),
            pltpu.VMEM((3 * c2, long), bf16),
            pltpu.VMEM((9 * c1, long), f32),
            pltpu.VMEM((fewer, c3), bf16),
            pltpu.VMEM((fewer, c3), bf16),
            pltpu.VMEM((3 * c2, 9 * c1), bf16),
            pltpu.VMEM((3 * c3, 9 * c2), bf16),
            pltpu.VMEM((9 * c1, 3 * c2), bf16),
            pltpu.VMEM((9 * c2, 3 * c3), bf16),
            pltpu.VMEM((fewer, short), bf16),
            pltpu.VMEM((fewer, fewer), bf16),
            pltpu.VMEM((rows_a, 128), f32),
            pltpu.VMEM((rows_b, 128), f32),
            *[pltpu.VMEM(shape, dtype) for shape, dtype in passed],
            *inboxes,
            *[pltpu.VMEM((size, 128), bf16) for size in (c1, c2 // 4, c3 // 4, c2)],
            *[pltpu.VMEM((size // 2, 128), bf16) for size in (c2, c2, c3, c3)],
            *buffers(rows_a, groups_a, True),
            *buffers(cuts[0], groups, False),
            *buffers(cuts[1], groups, False),
            *[pltpu.SemaphoreType.DMA((20,))] * 2,
            *[pltpu.SemaphoreType.DMA((members - 1,))] * 4,
            *[pltpu.SemaphoreType.DMA((count_a,))] * 2,
            *[pltpu.SemaphoreType.DMA((count_b,))] * 4,
            pltpu.SemaphoreType.DMA((len(operands) + 4,)),
            pltpu.SemaphoreType.DMA((len(passed),)),
        ],
        compiler_params=pltpu.CompilerParams(
            collective_id=2, has_side_effects=True, vmem_limit_bytes=60 * 2**20
        ),
    )(*operands)
    outs = [
        *passed[:2],
        ((27, c1, c2), f32),
        ((1, c2), f32),
        ((27 * c2, c3), f32),
        ((1, c3), f32),
    ]
    features, grad_in, sum_wa, sum_ba, sum_wb, sum_bb = pl.pallas_call(
        functools.partial(last_kernel, scales),
        out_shape=[jax.ShapeDtypeStruct(shape, dtype) for shape, dtype in outs],
        in_specs=[anywhere] * len(passed),
        out_specs=[anywhere] * len(outs),
        scratch_shapes=[
            *[pltpu.VMEM(shape, dtype) for shape, dtype in passed + outs[2:]],
            pltpu.SemaphoreType.DMA((len(passed),)),
            pltpu.SemaphoreType.DMA((len(outs),)),
        ],
    )(*middle)
    return (
        features.reshape(cotangent.shape),
        jnp.transpose(grad_in, (0, 3, 1, 2)),
        sum_wa.reshape(weight_a.shape),
        sum_ba.reshape(c2),
        sum_wb.reshape(weight_b.shape),
        sum_bb.reshape(c3),
    )


def fits_blocks(volume, weight_b):
    c1, width, rows, planes = volume.shape
    sizes = {axis: lax.axis_size(axis) for axis in ("gx", "gy", "gz")}
    return (
        sizes == {"gx": 2, "gy": 1, "gz": planes}
        and (width, rows, planes) == (32, 8, 16)
        and (c1, *weight_b.shape[3:]) == (32, 64, 128)
    )


def on_device(volume, weight_a, bias_a, weight_b, bias_b, cotangent):
    f32, bf16 = jnp.float32, jnp.bfloat16
    count = lax.axis_size("gz")
    devices_all = lax.axis_size("gx") * lax.axis_size("gy") * count
    c1, nx, rows, nz = volume.shape
    cells = nx * rows * nz
    scale_a = 1.0 / math.sqrt(cells * devices_all)
    scale_b = 1.0 / math.sqrt(cells * devices_all // 8)
    c2, c3 = weight_b.shape[3:]
    if fits_blocks(volume, weight_b):
        return on_blocks(volume, weight_a, bias_a, weight_b, bias_b, cotangent, (scale_a, scale_b))
    planes, depth = nx // count, nz * count
    fine = (planes, rows, depth)
    coarse = (planes // 2, rows // 2, depth // 2)
    fewer = cells // 8
    pool = (jnp.arange(depth)[:, None] // 2 == jnp.arange(depth // 2)[None]).astype(f32)
    work_a = 2 * 27 * c1 * c2 * cells
    work_b = 2 * 27 * c2 * c3 * fewer

    slab = lax.all_to_all(volume, "gz", split_axis=1, concat_axis=3, tiled=True).reshape(c1, cells)
    if lax.axis_size("gy") == 1:
        features, grad_slab, sum_wa, sum_ba, sum_wb, sum_bb = between_exchanges(
            fine,
            coarse,
            (scale_a, scale_b),
            slab,
            weight_a,
            bias_a,
            weight_b,
            bias_b,
            cotangent.reshape(c3, fewer),
            pool,
        )
    else:
        wide_a = widened(slab, *fine)
        before_a, pooled = local_kernel(
            functools.partial(forward_a_kernel, fine),
            [((c2, cells), f32), ((c2, fewer), bf16)],
            (27 * c1, cells),
            work_a,
            wide_a,
            outward(weight_a),
            bias_a[:, None],
            pool,
        )
        wide_b = widened(pooled, *coarse)
        features, grad_b, part_wb, part_bb = local_kernel(
            functools.partial(middle_kernel, coarse),
            [((c3, fewer), bf16), ((c3, fewer), bf16), ((27 * c2, c3), f32), ((8, c3), f32)],
            (27 * c2, fewer),
            2 * work_b,
            wide_b,
            outward(weight_b),
            bias_b[:, None],
            cotangent.reshape(c3, fewer),
        )
        (grad_a,) = local_kernel(
            functools.partial(backward_b_kernel, coarse, fine),
            [((c2, cells), bf16)],
            (27 * c3, fewer),
            work_b,
            widened(grad_b, *coarse),
            inward(weight_b),
            before_a,
            pool.T.astype(bf16),
        )
        part_wa, part_ba = local_kernel(
            functools.partial(weight_a_kernel, fine),
            [((27 * c1, c2), f32), ((8, c2), f32)],
            (27 * c1, cells),
            work_a,
            wide_a,
            grad_a,
        )
        (grad_slab,) = local_kernel(
            functools.partial(backward_a_kernel, fine),
            [((c1, cells), bf16)],
            (27 * c2, cells),
            work_a,
            widened(grad_a, *fine),
            inward(weight_a),
        )
        sum_wa, sum_ba, sum_wb, sum_bb = summed_grads(
            part_wa, part_ba, part_wb, part_bb, (scale_a, scale_b)
        )
    grad_input = lax.all_to_all(
        grad_slab.reshape(c1, planes, rows, depth), "gz", split_axis=3, concat_axis=1, tiled=True
    )
    return (
        features.reshape(cotangent.shape),
        grad_input,
        sum_wa.reshape(weight_a.shape),
        sum_ba.reshape(c2),
        sum_wb.reshape(weight_b.shape),
        sum_bb.reshape(c3),
    )


def solution(mesh):
    return jax.shard_map(
        on_device,
        mesh=mesh,
        in_specs=(P(None, "gx", "gy", "gz"), P(), P(), P(), P(), P(None, ("gx", "gz"), "gy", None)),
        out_specs=(
            P(None, ("gx", "gz"), "gy", None),
            P(None, "gx", "gy", "gz"),
            P(),
            P(),
            P(),
            P(),
        ),
        check_vma=False,
    )
```

```python
import functools
import math

import jax
import jax.numpy as jnp
from jax import lax
from jax.experimental import pallas as pl
from jax.experimental.pallas import tpu as pltpu
from jax.sharding import PartitionSpec as P

LINE = ("gx", "gz")
MESH = pl.DeviceIdType.MESH


def shared(block, axis, dim, width):
    count = lax.axis_size(axis)
    if count == 1:
        edge = jnp.zeros_like(lax.slice_in_dim(block, 0, width, axis=dim))
        return edge, edge
    forward = [(i, i + 1) for i in range(count - 1)]
    backward = [(target, source) for source, target in forward]
    last = block.shape[dim]
    low = lax.ppermute(lax.slice_in_dim(block, last - width, last, axis=dim), axis, forward)
    high = lax.ppermute(lax.slice_in_dim(block, 0, width, axis=dim), axis, backward)
    return low, high


def widened(flat, planes, rows, depth):
    low, high = shared(flat, LINE, 1, rows * depth)
    if lax.axis_size("gy") == 1:
        gap = jnp.zeros((flat.shape[0], depth), flat.dtype)
        pieces = [gap, low, gap]
        for plane in range(planes):
            pieces += [gap, flat[:, plane * rows * depth : (plane + 1) * rows * depth], gap]
        return jnp.concatenate(pieces + [gap, high, gap], axis=1)
    whole = jnp.concatenate([low, flat, high], axis=1)
    whole = whole.reshape(flat.shape[0], planes + 2, rows, depth)
    low, high = shared(whole, "gy", 2, 1)
    return jnp.concatenate([low, whole, high], axis=2).reshape(flat.shape[0], -1)


def slope_of(value):
    sigma = jax.nn.sigmoid(value)
    return sigma + value * sigma * (1.0 - sigma)


def put_windows(wide_ref, windows, planes, rows, depth):
    wide = wide_ref[...]
    width, extent = wide.shape
    place = lax.broadcasted_iota(jnp.int32, (width, extent), 1) % depth
    loose = wide.astype(jnp.float32)
    before = jnp.where(place == 0, 0.0, pltpu.roll(loose, 1, 1)).astype(jnp.bfloat16)
    after = jnp.where(place == depth - 1, 0.0, pltpu.roll(loose, extent - 1, 1)).astype(jnp.bfloat16)
    size = rows * depth
    for third, moved in enumerate((before, wide, after)):
        for first in range(3):
            for second in range(3):
                at = (first * 9 + second * 3 + third) * width
                for plane in range(planes):
                    begin = ((plane + first) * (rows + 2) + second) * depth
                    windows[at : at + width, plane * size : (plane + 1) * size] = moved[
                        :, begin : begin + size
                    ]


def dot_rows(left, right):
    return lax.dot_general(
        left, right, (((1,), (1,)), ((), ())), preferred_element_type=jnp.float32
    )


def forward_a_kernel(dims, wide_ref, weight_ref, bias_ref, pool_ref, before_ref, pooled_ref, windows):
    planes, rows, depth = dims
    put_windows(wide_ref, windows, *dims)
    before = jnp.dot(weight_ref[...], windows[...], preferred_element_type=jnp.float32)
    before = before + bias_ref[...]
    before_ref[...] = before
    active = before * jax.nn.sigmoid(before)
    size = rows * depth
    for row in range(rows // 2):
        parts = [
            active[:, plane * size + (2 * row + j) * depth : plane * size + (2 * row + j + 1) * depth]
            for plane in range(planes)
            for j in range(2)
        ]
        summed = sum(parts[1:], parts[0])
        paired = jnp.dot(
            summed, pool_ref[...], precision=lax.Precision.HIGHEST, preferred_element_type=jnp.float32
        )
        pooled_ref[:, row * depth // 2 : (row + 1) * depth // 2] = (paired * 0.125).astype(jnp.bfloat16)


def middle_kernel(dims, wide_ref, weight_ref, bias_ref, cot_ref, feat_ref, grad_ref, wb_ref, bb_ref, windows):
    put_windows(wide_ref, windows, *dims)
    before = jnp.dot(weight_ref[...], windows[...], preferred_element_type=jnp.float32)
    before = before + bias_ref[...]
    feat_ref[...] = (before * jax.nn.sigmoid(before)).astype(jnp.bfloat16)
    grad = (cot_ref[...].astype(jnp.float32) * slope_of(before)).astype(jnp.bfloat16)
    grad_ref[...] = grad
    wb_ref[...] = dot_rows(windows[...], grad)
    bb_ref[...] = dot_rows(jnp.ones((8, grad.shape[1]), jnp.bfloat16), grad)


def backward_b_kernel(dims, fine, wide_ref, weight_ref, before_ref, spread_ref, grad_ref, windows):
    put_windows(wide_ref, windows, *dims)
    pooled = jnp.dot(weight_ref[...], windows[...], preferred_element_type=jnp.float32)
    pooled = pooled.astype(jnp.bfloat16)
    planes, rows, depth = fine
    size = rows * depth
    for row in range(rows // 2):
        part = pooled[:, row * depth // 2 : (row + 1) * depth // 2]
        spread = jnp.dot(part, spread_ref[...], preferred_element_type=jnp.float32) * 0.125
        for plane in range(planes):
            for j in range(2):
                begin = plane * size + (2 * row + j) * depth
                slope = slope_of(before_ref[:, begin : begin + depth])
                grad_ref[:, begin : begin + depth] = (spread * slope).astype(jnp.bfloat16)


def weight_a_kernel(dims, wide_ref, grad_ref, wa_ref, ba_ref, windows):
    put_windows(wide_ref, windows, *dims)
    grad = grad_ref[...]
    wa_ref[...] = dot_rows(windows[...], grad)
    ba_ref[...] = dot_rows(jnp.ones((8, grad.shape[1]), jnp.bfloat16), grad)


def backward_a_kernel(dims, wide_ref, weight_ref, out_ref, windows):
    put_windows(wide_ref, windows, *dims)
    out = jnp.dot(weight_ref[...], windows[...], preferred_element_type=jnp.float32)
    out_ref[...] = out.astype(jnp.bfloat16)


def local_kernel(body, outs, windows, flops, *operands):
    moved = sum(x.size * x.dtype.itemsize for x in operands)
    return pl.pallas_call(
        body,
        out_shape=[jax.ShapeDtypeStruct(shape, dtype) for shape, dtype in outs],
        in_specs=[pl.BlockSpec(memory_space=pltpu.VMEM)] * len(operands),
        out_specs=[pl.BlockSpec(memory_space=pltpu.VMEM)] * len(outs),
        scratch_shapes=[pltpu.VMEM(windows, jnp.bfloat16)],
        compiler_params=pltpu.CompilerParams(vmem_limit_bytes=48 * 2**20),
        cost_estimate=pl.CostEstimate(flops=flops, bytes_accessed=moved, transcendentals=0),
    )(*operands)


def partner_of(axis, bit):
    me = lax.axis_index(axis)
    mine = (me // bit) % 2
    return me + bit * (1 - 2 * mine), mine


def sum_kernel(steps, halvings, rows, scales, wa_ref, ba_ref, wb_ref, bb_ref, *rest):
    out_wa, out_ba, out_wb, out_bb, acc, gathered, *scratch = rest
    half, width = wa_ref.shape[0] // 2, wa_ref.shape[1]
    top = wb_ref.shape[0]
    count = len(steps)
    sends = scratch[:count]
    recvs = scratch[count : 2 * count]
    sem_send, sem_recv = scratch[2 * count :]
    partners = [partner_of(axis, bit) for axis, bit in steps]
    barrier = pltpu.get_barrier_semaphore()
    for (axis, _), (partner, _) in zip(steps, partners):
        pl.semaphore_signal(barrier, inc=1, device_id={axis: partner}, device_id_type=MESH)
    acc[:top] = wb_ref[...]
    acc[top : top + half, :width] = wa_ref[:half]
    acc[top : top + half, width:] = wa_ref[half:]
    acc[top + half :] = jnp.zeros((rows - top - half, 128), jnp.float32)
    acc[top + half : top + half + 8, :width] = ba_ref[...]
    acc[top + half + 8 : top + half + 16] = bb_ref[...]
    pl.semaphore_wait(barrier, count)
    offset = 0
    size = rows
    kept = []
    for at, ((axis, _), (partner, mine)) in enumerate(zip(steps, partners)):
        source = acc
        if at < halvings:
            size = size // 2
            away = pl.multiple_of(offset + (1 - mine) * size, 16)
            offset = pl.multiple_of(offset + mine * size, 16)
        else:
            away = offset
        sends[at][...] = source[pl.ds(away, size)].astype(jnp.bfloat16)
        copy = pltpu.make_async_remote_copy(
            src_ref=sends[at],
            dst_ref=recvs[at],
            send_sem=sem_send.at[at],
            recv_sem=sem_recv.at[at],
            device_id={axis: partner},
            device_id_type=MESH,
        )
        copy.start()
        copy.wait()
        if at < halvings:
            acc[pl.ds(offset, size)] = source[pl.ds(offset, size)] + recvs[at][...].astype(jnp.float32)
            kept.append((offset, size))
        else:
            acc[pl.ds(offset, size)] = sends[at][...].astype(jnp.float32) + recvs[at][...].astype(jnp.float32)
    gathered[pl.ds(offset, size)] = acc[pl.ds(offset, size)].astype(jnp.bfloat16)
    for back in range(halvings):
        at = halvings - 1 - back
        begin, extent = kept[at]
        (axis, _), (partner, _) = steps[at], partners[at]
        here = gathered.at[pl.ds(begin, extent)]
        copy = pltpu.make_async_remote_copy(
            src_ref=here,
            dst_ref=here,
            send_sem=sem_send.at[count + back],
            recv_sem=sem_recv.at[count + back],
            device_id={axis: partner},
            device_id_type=MESH,
        )
        copy.start()
        copy.wait()
    scale_a, scale_b = scales
    total = gathered[...].astype(jnp.float32)
    out_wb[...] = total[:top] * scale_b
    out_wa[:half] = total[top : top + half, :width] * scale_a
    out_wa[half:] = total[top : top + half, width:] * scale_a
    out_ba[...] = total[top + half : top + half + 1, :width] * scale_a
    out_bb[...] = total[top + half + 8 : top + half + 9] * scale_b


def summed_grads(wa, ba, wb, bb, scales):
    used = wb.shape[0] + wa.shape[0] // 2 + 16
    rows = used + -used % 128
    cut = {
        axis: [2**i for i in range(lax.axis_size(axis).bit_length() - 1)] for axis in ("gz", "gx", "gy")
    }
    steps = [("gz", bit) for bit in cut["gz"][:1]]
    steps += [("gx", bit) for bit in cut["gx"]] + [("gy", bit) for bit in cut["gy"]]
    steps += [("gz", bit) for bit in cut["gz"][1:]]
    halvings = 0
    sizes = []
    size = rows
    for _ in steps:
        if len(sizes) == halvings and size % 32 == 0:
            size //= 2
            halvings += 1
        sizes.append(size)
    buffers = [pltpu.VMEM((s, 128), jnp.bfloat16) for s in sizes]
    total = len(steps) + halvings
    shapes = [wa.shape, (1, ba.shape[1]), wb.shape, (1, bb.shape[1])]
    return pl.pallas_call(
        functools.partial(sum_kernel, steps, halvings, rows, scales),
        out_shape=[jax.ShapeDtypeStruct(shape, jnp.float32) for shape in shapes],
        in_specs=[pl.BlockSpec(memory_space=pltpu.VMEM)] * 4,
        out_specs=[pl.BlockSpec(memory_space=pltpu.VMEM)] * 4,
        scratch_shapes=[
            pltpu.VMEM((rows, 128), jnp.float32),
            pltpu.VMEM((rows, 128), jnp.bfloat16),
            *buffers,
            *buffers,
            pltpu.SemaphoreType.DMA((total,)),
            pltpu.SemaphoreType.DMA((total,)),
        ],
        compiler_params=pltpu.CompilerParams(collective_id=0, has_side_effects=True),
    )(wa, ba, wb, bb)


def line_ends(axis_sizes):
    across, count = axis_sizes
    total = across * count
    line = lax.axis_index("gx") * count + lax.axis_index("gz")
    after, before = (line + 1) % total, (line + total - 1) % total
    ids = [{"gx": at // count, "gz": at % count} for at in (after, before)]
    return line, total, ids


class Halo:
    def __init__(self, wide, dims, where, sems, at):
        planes, rows, depth = dims
        self.line, self.total, ids = where
        size, stride = rows * depth, (rows + 2) * depth
        spot = lambda plane: wide.at[:, plane * stride + depth : plane * stride + depth + size]
        send, recv = sems
        self.up, self.down = [
            pltpu.make_async_remote_copy(
                src_ref=spot(source),
                dst_ref=spot(target),
                send_sem=send.at[at + i],
                recv_sem=recv.at[at + i],
                device_id=ids[i],
                device_id_type=MESH,
            )
            for i, (source, target) in enumerate(((planes, 0), (1, planes + 1)))
        ]

    def start(self):
        pl.when(self.line < self.total - 1)(self.up.start)
        pl.when(self.line > 0)(self.down.start)

    def wait(self):
        @pl.when(self.line < self.total - 1)
        def _():
            self.up.wait_send()
            self.down.wait_recv()

        @pl.when(self.line > 0)
        def _():
            self.down.wait_send()
            self.up.wait_recv()


class Summing:
    def __init__(self, steps, sizes, acc, gathered, sends, recvs, sems):
        self.steps, self.sizes = steps, sizes
        self.acc, self.gathered, self.sends, self.recvs = acc, gathered, sends, recvs
        self.sems = sems
        self.partners = [partner_of(axis, bit) for axis, bit in steps]
        rows = [acc.shape[0]] + list(sizes)
        self.halvings = sum(a != b for a, b in zip(rows, sizes))
        self.stages = len(steps) + self.halvings
        self.offset = 0
        self.kept = []
        self.flying = None

    def copy(self, stage, source, target, step):
        send, recv = self.sems
        self.flying = pltpu.make_async_remote_copy(
            src_ref=source,
            dst_ref=target,
            send_sem=send.at[stage],
            recv_sem=recv.at[stage],
            device_id={self.steps[step][0]: self.partners[step][0]},
            device_id_type=MESH,
        )
        self.flying.start()

    def start(self, stage):
        if stage < len(self.steps):
            size = self.sizes[stage]
            away = self.offset
            if stage < self.halvings:
                mine = self.partners[stage][1]
                away = pl.multiple_of(self.offset + (1 - mine) * size, 16)
                self.offset = pl.multiple_of(self.offset + mine * size, 16)
                self.kept.append((self.offset, size))
            self.sends[stage][...] = self.acc[pl.ds(away, size)].astype(jnp.bfloat16)
            self.copy(stage, self.sends[stage], self.recvs[stage], stage)
        else:
            step = self.halvings - 1 - (stage - len(self.steps))
            begin, size = self.kept[step]
            here = self.gathered.at[pl.ds(begin, size)]
            self.copy(stage, here, here, step)

    def finish(self, stage):
        self.flying.wait()
        if stage >= len(self.steps):
            return
        here = pl.ds(self.offset, self.sizes[stage])
        came = self.recvs[stage][...].astype(jnp.float32)
        own = self.acc[here] if stage < self.halvings else self.sends[stage][...].astype(jnp.float32)
        total = own + came
        if stage == len(self.steps) - 1:
            self.gathered[here] = total.astype(jnp.bfloat16)
        else:
            self.acc[here] = total


def place(wide, flat, dims):
    planes, rows, depth = dims
    size, stride = rows * depth, (rows + 2) * depth
    for plane in range(planes):
        begin = (plane + 1) * stride + depth
        wide[:, begin : begin + size] = flat[:, plane * size : (plane + 1) * size]


def whole_kernel(setting, *refs):
    fine, coarse, sizes_line, steps, cuts_a, cuts_b, scales = setting
    slab, w_a, b_a, pool, w_b, b_b, cot, v_b, spread, v_a = refs[:10]
    features, grad_slab, out_wa, out_ba, out_wb, out_bb = refs[10:16]
    wide_a, wide_b, wide_gb, wide_ga, win_a, win_b, win_gb, win_ga = refs[16:24]
    before_a, pooled, grad_b, grad_a, acc_a, acc_b, all_a, all_b = refs[24:32]
    count = len(steps)
    send_a, recv_a, send_b, recv_b = [refs[32 + i * count : 32 + (i + 1) * count] for i in range(4)]
    sems = refs[32 + 4 * count :]
    where = line_ends(sizes_line)
    line, total, ids = where
    barrier = pltpu.get_barrier_semaphore()
    for wide in (wide_a, wide_b, wide_gb, wide_ga):
        wide[...] = jnp.zeros_like(wide)
    place(wide_a, slab, fine)
    for axis, bit in steps:
        partner, _ = partner_of(axis, bit)
        pl.semaphore_signal(barrier, inc=1, device_id={axis: partner}, device_id_type=MESH)
    for device in ids:
        pl.semaphore_signal(barrier, inc=1, device_id=device, device_id_type=MESH)
    pl.semaphore_wait(barrier, count + 2)
    halos = [
        Halo(wide, dims, where, sems[:2], 2 * i)
        for i, (wide, dims) in enumerate(
            ((wide_a, fine), (wide_b, coarse), (wide_gb, coarse), (wide_ga, fine))
        )
    ]
    sum_a = Summing(steps, cuts_a, acc_a, all_a, send_a, recv_a, sems[2:4])
    sum_b = Summing(steps, cuts_b, acc_b, all_b, send_b, recv_b, sems[4:6])

    halos[0].start()
    halos[0].wait()
    forward_a_kernel(fine, wide_a, w_a, b_a, pool, before_a, pooled, win_a)
    place(wide_b, pooled, coarse)
    halos[1].start()
    halos[1].wait()
    top_b = out_wb.shape[0]
    middle_kernel(
        coarse, wide_b, w_b, b_b, cot, features, grad_b, acc_b.at[:top_b], acc_b.at[top_b : top_b + 8], win_b
    )
    place(wide_gb, grad_b, coarse)
    halos[2].start()
    acc_b[top_b + 8 :] = jnp.zeros((acc_b.shape[0] - top_b - 8, acc_b.shape[1]), jnp.float32)
    sum_b.start(0)
    halos[2].wait()
    backward_b_kernel(coarse, fine, wide_gb, v_b, before_a, spread, grad_a, win_gb)
    place(wide_ga, grad_a, fine)
    halos[3].start()
    sum_b.finish(0)
    sum_b.start(1)
    grad = grad_a[...]
    half, width = out_wa.shape[0] // 2, out_wa.shape[1]
    acc_a[:half, :width] = dot_rows(win_a[:half], grad)
    acc_a[:half, width:] = dot_rows(win_a[half:], grad)
    acc_a[half:] = jnp.zeros((acc_a.shape[0] - half, acc_a.shape[1]), jnp.float32)
    acc_a[half : half + 8, :width] = dot_rows(jnp.ones((8, grad.shape[1]), jnp.bfloat16), grad)
    sum_b.finish(1)
    sum_b.start(2)
    sum_a.start(0)
    halos[3].wait()
    backward_a_kernel(fine, wide_ga, v_a, grad_slab, win_ga)
    for stage in range(max(sum_a.stages, sum_b.stages - 2)):
        if stage + 2 < sum_b.stages:
            sum_b.finish(stage + 2)
            if stage + 3 < sum_b.stages:
                sum_b.start(stage + 3)
        if stage < sum_a.stages:
            sum_a.finish(stage)
            if stage + 1 < sum_a.stages:
                sum_a.start(stage + 1)
    scale_a, scale_b = scales
    out_wb[...] = all_b[:top_b].astype(jnp.float32) * scale_b
    out_bb[...] = all_b[top_b : top_b + 16].astype(jnp.float32)[:1] * scale_b
    out_wa[:half] = all_a[:half, :width].astype(jnp.float32) * scale_a
    out_wa[half:] = all_a[:half, width:].astype(jnp.float32) * scale_a
    out_ba[...] = all_a[half : half + 16, :width].astype(jnp.float32)[:1] * scale_a


def stage_sizes(rows, steps):
    sizes = []
    for _ in steps:
        halve = rows % 32 == 0 and len(sizes) < 3
        rows = rows // 2 if halve else rows
        sizes.append(rows)
    return sizes


def all_steps():
    cut = {
        axis: [2**i for i in range(lax.axis_size(axis).bit_length() - 1)] for axis in ("gz", "gx", "gy")
    }
    steps = [("gz", bit) for bit in cut["gz"][:1]]
    steps += [("gx", bit) for bit in cut["gx"]] + [("gy", bit) for bit in cut["gy"]]
    return steps + [("gz", bit) for bit in cut["gz"][1:]]


def between_exchanges(fine, coarse, scales, slab, weight_a, bias_a, weight_b, bias_b, cot, pool):
    f32, bf16 = jnp.float32, jnp.bfloat16
    c1, cells = slab.shape
    c2, c3 = weight_b.shape[3:]
    fewer = cells // 8
    steps = all_steps()
    rows_a = 27 * c1 // 2 + 16
    rows_a += -rows_a % 128
    rows_b = 27 * c2 + 16
    rows_b += -rows_b % 128
    cuts_a, cuts_b = stage_sizes(rows_a, steps), stage_sizes(rows_b, steps)
    extent = lambda dims: (dims[0] + 2) * (dims[1] + 2) * dims[2]
    setting = (fine, coarse, (lax.axis_size("gx"), lax.axis_size("gz")), steps, cuts_a, cuts_b, scales)
    buffers = [pltpu.VMEM((n, 128), bf16) for cuts in (cuts_a, cuts_a, cuts_b, cuts_b) for n in cuts]
    outs = [
        ((c3, fewer), bf16),
        ((c1, cells), bf16),
        ((27 * c1, c2), f32),
        ((1, c2), f32),
        ((27 * c2, c3), f32),
        ((1, c3), f32),
    ]
    operands = (
        slab,
        outward(weight_a),
        bias_a[:, None],
        pool,
        outward(weight_b),
        bias_b[:, None],
        cot,
        inward(weight_b),
        pool.T.astype(bf16),
        inward(weight_a),
    )
    most = 2 * len(steps)
    return pl.pallas_call(
        functools.partial(whole_kernel, setting),
        out_shape=[jax.ShapeDtypeStruct(shape, dtype) for shape, dtype in outs],
        in_specs=[pl.BlockSpec(memory_space=pltpu.VMEM)] * len(operands),
        out_specs=[pl.BlockSpec(memory_space=pltpu.VMEM)] * len(outs),
        scratch_shapes=[
            pltpu.VMEM((c1, extent(fine)), bf16),
            pltpu.VMEM((c2, extent(coarse)), bf16),
            pltpu.VMEM((c3, extent(coarse)), bf16),
            pltpu.VMEM((c2, extent(fine)), bf16),
            pltpu.VMEM((27 * c1, cells), bf16),
            pltpu.VMEM((27 * c2, fewer), bf16),
            pltpu.VMEM((27 * c3, fewer), bf16),
            pltpu.VMEM((27 * c2, cells), bf16),
            pltpu.VMEM((c2, cells), f32),
            pltpu.VMEM((c2, fewer), bf16),
            pltpu.VMEM((c3, fewer), bf16),
            pltpu.VMEM((c2, cells), bf16),
            pltpu.VMEM((rows_a, 128), f32),
            pltpu.VMEM((rows_b, 128), f32),
            pltpu.VMEM((rows_a, 128), bf16),
            pltpu.VMEM((rows_b, 128), bf16),
            *buffers,
            pltpu.SemaphoreType.DMA((8,)),
            pltpu.SemaphoreType.DMA((8,)),
            *[pltpu.SemaphoreType.DMA((most,))] * 4,
        ],
        compiler_params=pltpu.CompilerParams(
            collective_id=1, has_side_effects=True, vmem_limit_bytes=60 * 2**20
        ),
    )(*operands)


def outward(weight):
    return weight.reshape(-1, weight.shape[-1]).T


def inward(weight):
    taps = weight[::-1, ::-1, ::-1].reshape(27, *weight.shape[3:])
    return jnp.transpose(taps, (1, 0, 2)).reshape(weight.shape[3], -1)


def lanes_of(shape):
    return lax.broadcasted_iota(jnp.int32, shape, len(shape) - 1)


def rows_of(shape):
    return lax.broadcasted_iota(jnp.int32, shape, 0)


def ones_where(mask):
    return jnp.where(mask, 1.0, 0.0).astype(jnp.bfloat16)


def dot(left, right):
    return jnp.dot(left, right, preferred_element_type=jnp.float32)


def by_parts(rank_bits, mask):
    place = {}
    for at, (axis, bit) in enumerate(rank_bits):
        if mask >> at & 1:
            me = place.get(axis, lax.axis_index(axis))
            place[axis] = me + bit * (1 - 2 * ((lax.axis_index(axis) // bit) % 2))
    return place


def own_rank(rank_bits, mask=0):
    total = 0
    for at, (axis, bit) in enumerate(rank_bits):
        mine = (lax.axis_index(axis) // bit) % 2
        total = total + ((1 - mine) if mask >> at & 1 else mine) * 2**at
    return total


def remote(source, target, sems, at, device, sent_at=None):
    return pltpu.make_async_remote_copy(
        src_ref=source,
        dst_ref=target,
        send_sem=sems[0].at[at if sent_at is None else sent_at],
        recv_sem=sems[1].at[at],
        device_id=device,
        device_id_type=MESH,
    )


def flipped_bits(bits, mask):
    return tuple(bit for at, bit in enumerate(bits) if mask >> at & 1)


class Reduction:
    def __init__(self, groups, exchanged, acc, summed, sends, recvs, sems):
        self.groups, self.exchanged, self.acc, self.summed = groups, exchanged, acc, summed
        self.sends, self.recvs, self.sems = sends, recvs, sems
        self.offset, self.size = 0, acc.shape[0]
        self.parts = []
        self.all = None
        self.stage = 0
        bits = sum(groups[:-1] if exchanged else groups, [])
        self.levels = [level for level in reversed(all_groups()) if level[0] in bits]
        self.stages = len(groups) + len(self.levels)
        self.used = len(groups)
        self.places = {}
        self.sent = 0

    def fly(self, source, target, device):
        remote(source, target, self.sems, self.stage, device).start()

    def piece(self, flipped, level, mask, arrived):
        key = (flipped, level, mask) if level + 1 < len(self.levels) else level
        if key not in self.places:
            self.places[key] = self.used
            self.used += 1
        whose = flipped + flipped_bits(self.levels[level], mask) if arrived else flipped
        offset = 0
        for bits, part in self.parts:
            turned = sum(1 << at for at, bit in enumerate(bits) if bit in whose)
            offset = offset + own_rank(bits, turned) * part
        here = self.summed.at[pl.ds(pl.multiple_of(offset, 8), self.size)]
        device = by_parts(self.levels[level], mask)
        return remote(here, here, self.sems, self.places[key], device, len(self.groups))

    def pieces(self, count, at):
        here = self.summed.at[: count * self.size]
        return remote(here, here, self.sems, at, by_parts(self.levels[-1], 1), len(self.groups))

    def pass_on(self, flipped, first):
        for level in range(first, len(self.levels)):
            for mask in range(1, 2 ** len(self.levels[level])):
                self.piece(flipped, level, mask, False).start()
                self.sent += 1

    def start(self):
        at = self.stage
        count = len(self.groups)
        if at > count:
            return
        if at == count:
            self.known = [()]
            self.pass_on((), 0)
        elif self.exchanged and at == count - 1:
            bits = self.groups[at]
            recv = self.recvs[at]
            mine = own_rank(bits)
            recv[mine] = self.acc[pl.ds(self.offset, self.size)].astype(jnp.bfloat16)
            for mask in range(1, 2 ** len(bits)):
                self.fly(recv.at[mine], recv.at[mine], by_parts(bits, mask))
            rest = recv.at[: recv.shape[0] - 1]
            self.all = remote(rest, rest, self.sems, at, by_parts(bits, 1))
        else:
            bits = self.groups[at]
            members = 2 ** len(bits)
            part = self.size // members
            send, recv = self.sends[at], self.recvs[at]
            send[...] = self.acc[pl.ds(self.offset, self.size)].astype(jnp.bfloat16)
            for mask in range(1, members):
                begin = pl.multiple_of(own_rank(bits, mask) * part, 8)
                self.fly(send.at[pl.ds(begin, part)], recv.at[mask - 1], by_parts(bits, mask))
            self.all = remote(recv, recv, self.sems, at, by_parts(bits, 1))
            self.parts.append((bits, part))
            self.offset = pl.multiple_of(self.offset + own_rank(bits) * part, 8)
            self.size = part

    def finish(self):
        at = self.stage
        count = len(self.groups)
        self.stage += 1
        if at >= count:
            level = at - count
            if level + 1 == len(self.levels):
                self.pieces(len(self.known) * (2 ** len(self.levels[level]) - 1), self.places[level]).wait_recv()
                self.pieces(self.sent, 0).wait_send()
                return
            came = []
            for flipped in self.known:
                for mask in range(1, 2 ** len(self.levels[level])):
                    self.piece(flipped, level, mask, True).wait_recv()
                    whose = flipped + flipped_bits(self.levels[level], mask)
                    self.pass_on(whose, level + 1)
                    came.append(whose)
            self.known = self.known + came
            return
        self.all.wait()
        recv = self.recvs[at]
        here = pl.ds(self.offset, self.size)
        if self.exchanged and at == count - 1:
            total = recv[0].astype(jnp.float32)
            for i in range(1, recv.shape[0]):
                total = total + recv[i].astype(jnp.float32)
        else:
            total = self.acc[here]
            for i in range(recv.shape[0]):
                total = total + recv[i].astype(jnp.float32)
        if at == count - 1:
            self.summed[here] = total.astype(jnp.bfloat16)
        else:
            self.acc[here] = total

    def step(self):
        self.finish()
        if self.stage < self.stages:
            self.start()


class Border:
    def __init__(self, first, last, edge, inbox, sems, at):
        me, count = lax.axis_index("gz"), lax.axis_size("gz")
        side = 1 - lax.axis_index("gx")
        self.inner, self.outer = me > 0, me < count - 1
        up, down = (me + 1) % count, (me + count - 1) % count
        low, high, beside, beside_low, beside_high = inbox
        self.always = remote(edge, beside, sems, at + 2, {"gx": side})
        self.up = [
            remote(last, low, sems, at, {"gz": up}),
            remote(edge, beside_low, sems, at + 3, {"gx": side, "gz": up}),
        ]
        self.down = [
            remote(first, high, sems, at + 1, {"gz": down}),
            remote(edge, beside_high, sems, at + 4, {"gx": side, "gz": down}),
        ]

    def start(self):
        @pl.when(self.outer)
        def _():
            for copy in self.up:
                copy.start()

        @pl.when(self.inner)
        def _():
            for copy in self.down:
                copy.start()

        self.always.start()

    def wait(self):
        self.always.wait()

        @pl.when(self.outer)
        def _():
            for copy in self.up:
                copy.wait_send()
            for copy in self.down:
                copy.wait_recv()

        @pl.when(self.inner)
        def _():
            for copy in self.down:
                copy.wait_send()
            for copy in self.up:
                copy.wait_recv()


def gathered_edge(tiles, extent, slots):
    shape = tiles[0].shape
    lane = lanes_of(shape)
    high = lax.axis_index("gx") == 0
    edge = jnp.where(high, extent - 1, 0)
    at_edge = lane & (extent - 1) == edge
    total = None
    for i, tile in enumerate(tiles):
        kept = rolled(jnp.where(at_edge, tile, 0.0), i % slots)
        total = kept if total is None else total + kept
    back = pltpu.roll(total, 128 - (extent - 1), 1)
    return jnp.where(high, back, total)


def rolled(value, by):
    by = by % 128
    return pltpu.roll(value, by, 1) if by else value


def quarters(edge):
    size = edge.shape[0] // 4
    return sum(rolled(edge[q * size : (q + 1) * size], 4 * q) for q in range(4))


def spread_edge(edge, by, packed):
    if not packed:
        return rolled(edge, by)
    return jnp.concatenate([rolled(edge, by - 4 * q) for q in range(4)], axis=0)


def halved(tile, low):
    size = tile.shape[0] // 2
    lane = lanes_of((size, 128))
    upper, lower = tile[:size], rolled(tile[size:], 64)
    return jnp.where(lane < 64, upper, lower) if low else jnp.where(lane < 64, lower, upper)


def beside(tile, edges, extent, packed):
    low_edge, high_edge, at = edges
    lane = lanes_of(tile.shape) & (extent - 1)
    before = jnp.where(lane == 0, spread_edge(low_edge, -at, packed), rolled(tile, 1))
    after = jnp.where(lane == extent - 1, spread_edge(high_edge, extent - 1 - at, packed), rolled(tile, -1))
    return before, after


def sided(edge):
    high = lax.axis_index("gx") == 0
    zero = jnp.zeros_like(edge)
    return jnp.where(high, zero, edge), jnp.where(high, edge, zero)


def moved_rows(pair, stride):
    lane = lanes_of(pair[0].shape)
    down = [rolled(tile, stride) for tile in pair]
    up = [rolled(tile, -stride) for tile in pair]
    low = lane < stride
    high = lane < 128 - stride
    zero = jnp.zeros_like(pair[0])
    before = (jnp.where(low, zero, down[0]), jnp.where(low, down[0], down[1]))
    after = (jnp.where(high, up[0], up[1]), jnp.where(high, up[1], zero))
    return before, after


def moved_half(tile, stride):
    lane = lanes_of(tile.shape) & 63
    zero = jnp.zeros_like(tile)
    before = jnp.where(lane < stride, zero, rolled(tile, stride))
    after = jnp.where(lane < 64 - stride, rolled(tile, -stride), zero)
    return before, after


def inbox_values(inbox):
    low, high, across, across_low, across_high = [ref[...] for ref in inbox]
    return low, high, sided(across), sided(across_low), sided(across_high)


def fine_planes(read, inbox, planes):
    low, high, across, across_low, across_high = inbox_values(inbox)
    for p in range(planes + 2):
        if p == 0:
            pair, edge, at = (low[:, :128], low[:, 128:]), across_low, 2 * (planes - 1)
        elif p == planes + 1:
            pair, edge, at = (high[:, :128], high[:, 128:]), across_high, 0
        else:
            pair, edge, at = read(p - 1), across, 2 * (p - 1)
        sides = [beside(tile, (*edge, at + g), 32, False) for g, tile in enumerate(pair)]
        yield p, ((sides[0][0], sides[1][0]), pair, (sides[0][1], sides[1][1]))


def coarse_tiles(field, inbox, tiles):
    low, high, across, across_low, across_high = inbox_values(inbox)
    low = jnp.concatenate([low, rolled(low, 64)], axis=0)
    high = jnp.concatenate([high, rolled(high, 64)], axis=0)
    half = lanes_of(low.shape) < 64
    for t in range(tiles):
        tile = field[:, t * 128 : (t + 1) * 128]
        sides = list(beside(tile, (*across, t % 4), 16, True))
        if t == 0:
            sides_low = beside(low, (*across_low, (tiles - 1) % 4), 16, True)
            tile = jnp.where(half, low, tile)
            sides = [jnp.where(half, a, b) for a, b in zip(sides_low, sides)]
        if t == tiles - 1:
            sides_high = beside(high, (*across_high, 0), 16, True)
            tile = jnp.where(half, tile, high)
            sides = [jnp.where(half, b, a) for a, b in zip(sides_high, sides)]
        yield t, (sides[0], tile, sides[1])


def column(row, size):
    wide = jnp.broadcast_to(row, (size, size))
    eye = rows_of((size, size)) == lanes_of((size, size))
    return jnp.sum(jnp.where(eye, wide, 0.0), axis=1, keepdims=True)


def joined_thirds(terms, tiles):
    half = None
    low = [rolled(terms(0, t), 64) for t in range(tiles)]
    high = [rolled(terms(2, t), 64) for t in range(tiles)]
    out = []
    for t in range(tiles):
        if half is None:
            half = lanes_of(low[0].shape) < 64
        before, after = low[max(t - 1, 0)], high[min(t + 1, tiles - 1)]
        out.append(terms(1, t) + jnp.where(half, before + high[t], low[t] + after))
    return out


def block_kernel(setting, *refs):
    groups, groups_a, cuts = setting
    inputs = refs[:6]
    features, grad_in, sum_a, sum_b = refs[6:10]
    volume, w_a, b_a, w_b, b_b, cot = refs[10:16]
    (
        stage, own_a, windows_a, sums_a, slope_a, halves, pooled, windows_b, sums_b,
        cot_sent, cot_came, cot_here, grad_b, lines_b, sums_gb, grads_a, lines_a, sums_ga,
        feat_sent, feat_came, mat_a, mat_b, mat_ga, mat_gb, near, far, acc_a, acc_b,
    ) = refs[16:44]
    rest = list(refs[44:])
    inboxes = [[rest.pop(0) for _ in range(5)] for _ in range(4)]
    edges = [rest.pop(0) for _ in range(4)]
    ends_b, ends_gb = [[rest.pop(0), rest.pop(0)] for _ in range(2)]
    count = len(groups)
    takes = lambda n: [rest.pop(0) for _ in range(n)]
    send_a, recv_a = takes(1), takes(2)
    send_b, recv_b, send_c, recv_c = [takes(count) for _ in range(4)]
    sems_halo, sems_cot, sems_feat, sems_a, sems_b, sems_c = [takes(2) for _ in range(6)]
    (sems_in,) = rest
    f32, bf16 = jnp.float32, jnp.bfloat16
    c1, rows, planes, width = volume.shape
    c2, c3 = w_a.shape[2], w_b.shape[2]
    tiles = planes // 4 + 1
    me, members = lax.axis_index("gz"), lax.axis_size("gz")
    whole = [bit for group in groups for bit in group]
    line = [bit for bit in whole if bit[0] == "gz"]

    barrier = pltpu.get_barrier_semaphore()
    for mask in range(1, 2 ** len(whole)):
        pl.semaphore_signal(barrier, inc=1, device_id=by_parts(whole, mask), device_id_type=MESH)
    loads = {
        at: pltpu.make_async_copy(inputs[at], refs[10 + at], sems_in.at[at]) for at in range(1, len(inputs))
    }
    parts = 4
    share = c1 // parts
    loads_v = [
        pltpu.make_async_copy(
            inputs[0].at[i * share : (i + 1) * share],
            volume.at[i * share : (i + 1) * share],
            sems_in.at[0],
        )
        for i in range(parts)
    ]
    for load in loads_v:
        load.start()
    for at in (5, 1, 3, 2, 4):
        loads[at].start()

    @pl.when(me == 0)
    def _():
        for inbox in inboxes:
            for box in (inbox[0], inbox[3]):
                box[...] = jnp.zeros_like(box)

    @pl.when(me == members - 1)
    def _():
        for inbox in inboxes:
            for box in (inbox[1], inbox[4]):
                box[...] = jnp.zeros_like(box)

    pltpu.make_async_copy(inputs[0], volume, sems_in.at[0]).wait()
    for g in range(2):
        for i in range(4):
            part = volume[:, 4 * g + i].astype(f32).reshape(c1 * planes, width)
            stage[:, width * i : width * (i + 1)] = part
        for z in range(planes):
            tile = stage[pl.ds(z, c1, stride=planes), :]
            own_a[:, z * 256 + g * 128 : z * 256 + (g + 1) * 128] = tile.astype(bf16)

    def read_a(z):
        return tuple(own_a[:, z * 256 + g * 128 : z * 256 + (g + 1) * 128] for g in range(2))

    edges[0][...] = gathered_edge([tile.astype(f32) for z in range(planes) for tile in read_a(z)], 32, 32).astype(bf16)
    pl.semaphore_wait(barrier, 2 ** len(whole) - 1)

    border_a = Border(own_a.at[:, :256], own_a.at[:, (planes - 1) * 256 :], edges[0], inboxes[0], sems_halo, 0)
    border_a.start()

    def exchange(sent, came, sems):
        size = sent.shape[0] // members
        for mask in range(1, members):
            begin = pl.multiple_of(own_rank(line, mask) * size, 16)
            remote(
                sent.at[pl.ds(begin, size)],
                came.at[pl.ds(pl.multiple_of(me * size, 16), size)],
                sems,
                0,
                by_parts(line, mask),
            ).start()
        here = pl.ds(pl.multiple_of(me * size, 16), size)
        came[here] = sent[here]
        most = (members - 1) * size
        return remote(sent.at[:most], came.at[:most], sems, 0, by_parts(line, 1))

    r, l = rows_of(far.shape), lanes_of(far.shape)
    far[...] = ones_where(((r >> 3) & 3 == l >> 7) & (((r >> 5) << 3) + (r & 7) == l & 127))
    loads[5].wait()
    half_rows = rows // 2
    stage[...] = cot[...].astype(f32)
    spaced = [stage[pl.ds(y, c3, stride=half_rows), :].astype(bf16) for y in range(half_rows)]
    cot_sent[...] = dot_rows(far[...], jnp.concatenate(spaced, axis=1)).astype(bf16)
    cot_flying = exchange(cot_sent, cot_came, sems_cot)
    for at in range(1, 5):
        loads[at].wait()

    eye = ones_where(rows_of((c2, c2)) == lanes_of((c2, c2)))
    eye_b = ones_where(rows_of((c3, c3)) == lanes_of((c3, c3)))
    for kz in range(3):
        block = w_a[:].reshape(9, 3, c1, c2)[:, kz].reshape(9 * c1, c2)
        mat_a[kz * c2 : (kz + 1) * c2] = dot_rows(eye, block).astype(bf16)
        block = w_b[:].reshape(9, 3, c2, c3)[:, kz].reshape(9 * c2, c3)
        mat_b[kz * c3 : (kz + 1) * c3] = dot_rows(eye_b, block).astype(bf16)
        for ky in range(3):
            for kx in range(3):
                tap = ((2 - kx) * 3 + 2 - ky) * 3 + 2 - kz
                at = kz * 3 + ky
                mat_ga[at * c1 : (at + 1) * c1, kx * c2 : (kx + 1) * c2] = w_a[tap]
                mat_gb[at * c2 : (at + 1) * c2, kx * c3 : (kx + 1) * c3] = w_b[tap]
    col_a, col_b = column(b_a[...], c2), column(b_b[...], c3)
    r, l = rows_of(near.shape), lanes_of(near.shape)
    near[...] = ones_where(
        ((r & 7) + 1 == l >> 6) & ((r >> 3) & 3 == (l >> 4) & 3) & (r >> 5 == l & 15)
    )
    r, l = rows_of((512, 128)), lanes_of((512, 128))
    pool = ones_where(
        (r >> 8 == l >> 6) & ((r >> 6) & 3 == (l >> 4) & 3) & ((r & 31) >> 1 == l & 15)
    )
    halves[...] = jnp.zeros_like(halves)
    for kz in range(3):
        for p in range(planes + 2):
            if not 0 <= p + kz - 2 < planes:
                grads_a[kz * c2 : (kz + 1) * c2, p * 256 : (p + 1) * 256] = jnp.zeros((c2, 256), bf16)
    acc_a[...] = jnp.zeros_like(acc_a)
    border_a.wait()

    step = 2 * 256
    for p, thirds in fine_planes(read_a, inboxes[0], planes):
        for kx, pair in enumerate(thirds):
            before, after = moved_rows(pair, 32)
            for ky, (first, second) in enumerate((before, pair, after)):
                at = (kx * 3 + ky) * c1
                windows_a[at : at + c1, p * 256 : p * 256 + 128] = first.astype(bf16)
                windows_a[at : at + c1, p * 256 + 128 : (p + 1) * 256] = second.astype(bf16)
        if p % 2:
            here = slice((p - 1) * 256, (p + 1) * 256)
            sums_a[:, here] = dot(mat_a[...], windows_a[:, here])
    for z in range(planes):
        value = (
            sums_a[:c2, z * 256 : (z + 1) * 256]
            + sums_a[c2 : 2 * c2, (z + 1) * 256 : (z + 2) * 256]
            + sums_a[2 * c2 :, (z + 2) * 256 : (z + 3) * 256]
            + col_a
        )
        sigma = jax.nn.sigmoid(value)
        active = value * sigma
        slope_a[:, z * 256 : (z + 1) * 256] = (sigma + active * (1.0 - sigma)) * 0.125
        if z % 2:
            active = active + kept
            pz = z // 2 + 1
            upper = active.astype(bf16)
            lower = (active - upper.astype(f32)).astype(bf16)
            at, lane = pz // 2 * c2, pz % 2 * 256
            halves[at : at + c2, lane : lane + 256] = upper
            halves[tiles * c2 + at : tiles * c2 + at + c2, lane : lane + 256] = lower
        else:
            kept = active
    both = dot(halves[...], pool)
    both = (both[: tiles * c2] + both[tiles * c2 :]) * 0.125
    for t in range(tiles):
        pooled[:, t * 128 : (t + 1) * 128] = both[t * c2 : (t + 1) * c2].astype(bf16)

    def coarse_border(field, edge, ends, inbox, at):
        parts = [field[:, t * 128 : (t + 1) * 128].astype(f32) for t in range(tiles)]
        edge[...] = quarters(gathered_edge(parts, 16, 4)).astype(bf16)
        ends[0][...] = halved(parts[0], False).astype(bf16)
        ends[1][...] = halved(parts[-1], True).astype(bf16)
        return Border(ends[0], ends[1], edge, inbox, sems_halo, at)

    border_b = coarse_border(pooled, edges[1], ends_b, inboxes[1], 5)
    border_b.start()
    cot_flying.wait()
    came = jnp.transpose(cot_came[...].astype(f32)).astype(bf16)
    cot_here[...] = dot(came, near[...])
    border_b.wait()

    for t, thirds in coarse_tiles(pooled, inboxes[1], tiles):
        for kx, tile in enumerate(thirds):
            before, after = moved_half(tile, 16)
            for ky, value in enumerate((before, tile, after)):
                at = (kx * 3 + ky) * c2
                windows_b[at : at + c2, t * 128 : (t + 1) * 128] = value.astype(bf16)
    sums_b[...] = dot(mat_b[...], windows_b[...])
    joined = joined_thirds(lambda k, t: sums_b[k * c3 : (k + 1) * c3, t * 128 : (t + 1) * 128], tiles)
    feats = []
    for t, value in enumerate(joined):
        value = value + col_b
        sigma = jax.nn.sigmoid(value)
        active = value * sigma
        feats.append(active.astype(bf16))
        slope = sigma + active * (1.0 - sigma)
        grad = cot_here[:, t * 128 : (t + 1) * 128] * slope
        grad_b[c3 : 2 * c3, t * 128 : (t + 1) * 128] = grad.astype(bf16)
    own_gb = grad_b.at[c3 : 2 * c3]
    border_gb = coarse_border(own_gb, edges[2], ends_gb, inboxes[2], 10)
    border_gb.start()

    half = lanes_of((c3, 128)) < 64
    turned = [rolled(own_gb[:, t * 128 : (t + 1) * 128].astype(f32), 64) for t in range(tiles)]
    zero = jnp.zeros_like(turned[0])
    for t in range(tiles):
        later = turned[t + 1] if t + 1 < tiles else zero
        earlier = turned[t - 1] if t else zero
        here = slice(t * 128, (t + 1) * 128)
        grad_b[:c3, here] = jnp.where(half, turned[t], later).astype(bf16)
        grad_b[2 * c3 :, here] = jnp.where(half, earlier, turned[t]).astype(bf16)
    top = 27 * c2

    def sum_terms(first, last):
        terms = dot_rows(windows_b[first * c2 : last * c2], grad_b[...])
        for at in range(first, last):
            for kz in range(3):
                tap = at * 3 + kz
                acc_b[tap * c2 : (tap + 1) * c2] = terms[
                    (at - first) * c2 : (at - first + 1) * c2, kz * c3 : (kz + 1) * c3
                ]

    cut = cuts[0]
    early = -(-cut // (3 * c2))
    sum_terms(0, early)
    total_b = Reduction(groups, False, acc_b.at[:cut], sum_b.at[:cut], send_b, recv_b, sems_b)
    total_b.start()
    sum_terms(early, 9)
    acc_b[top:] = jnp.zeros((acc_b.shape[0] - top, c3), f32)
    acc_b[top : top + 8] = dot_rows(jnp.ones((8, tiles * 128), bf16), own_gb[...])
    total_c = Reduction(groups, False, acc_b.at[cut:], sum_b.at[cut:], send_c, recv_c, sems_c)
    total_c.start()
    feat_sent[...] = dot_rows(near[...], jnp.concatenate(feats, axis=1)).astype(bf16)
    feat_flying = exchange(feat_sent, feat_came, sems_feat)
    total_b.step()
    total_c.step()
    border_gb.wait()

    for t, thirds in coarse_tiles(own_gb, inboxes[2], tiles):
        for kx, tile in enumerate(thirds):
            lines_b[kx * c3 : (kx + 1) * c3, t * 128 : (t + 1) * 128] = tile.astype(bf16)
    sums_gb[...] = dot(mat_gb[...], lines_b[...])
    by_row = [
        joined_thirds(
            lambda k, t: sums_gb[(k * 3 + ky) * c2 : (k * 3 + ky + 1) * c2, t * 128 : (t + 1) * 128], tiles
        )
        for ky in range(3)
    ]
    small = []
    for t in range(tiles):
        value = by_row[1][t] + moved_half(by_row[0][t], 16)[0] + moved_half(by_row[2][t], 16)[1]
        small.append(value.astype(bf16))
    spread = dot_rows(jnp.concatenate(small, axis=0), pool)
    for z in range(planes):
        pz = z // 2 + 1
        large = spread[pz // 2 * c2 : (pz // 2 + 1) * c2, pz % 2 * 256 : (pz % 2 + 1) * 256]
        grad = (large * slope_a[:, z * 256 : (z + 1) * 256]).astype(bf16)
        for kz in range(3):
            grads_a[kz * c2 : (kz + 1) * c2, (z + kz) * 256 : (z + kz + 1) * 256] = grad

    own_ga = grads_a.at[c2 : 2 * c2]

    def read_ga(z):
        return tuple(
            own_ga[:, (z + 1) * 256 + g * 128 : (z + 1) * 256 + (g + 1) * 128] for g in range(2)
        )

    edges[3][...] = gathered_edge([tile.astype(f32) for z in range(planes) for tile in read_ga(z)], 32, 32).astype(bf16)
    border_ga = Border(
        own_ga.at[:, 256:512], own_ga.at[:, planes * 256 : (planes + 1) * 256], edges[3], inboxes[3], sems_halo, 15
    )
    border_ga.start()

    terms = dot_rows(windows_a[...], grads_a[...])
    deep = 9 * c1
    acc_a[:deep] = terms[:, : 2 * c2]
    acc_a[deep : deep + deep // 2, :c2] = terms[: deep // 2, 2 * c2 :]
    acc_a[deep : deep + deep // 2, c2:] = terms[deep // 2 :, 2 * c2 :]
    top_a = deep + deep // 2
    acc_a[top_a : top_a + 8, :c2] = dot_rows(jnp.ones((8, planes * 256), bf16), own_ga[:, 256 : (planes + 1) * 256])
    total_a = Reduction(groups_a, True, acc_a, sum_a, send_a, recv_a, sems_a)
    total_a.start()
    total_b.step()
    total_c.step()
    border_ga.wait()

    for p, thirds in fine_planes(read_ga, inboxes[3], planes):
        for kx, pair in enumerate(thirds):
            for g, tile in enumerate(pair):
                at = p * 256 + g * 128
                lines_a[kx * c2 : (kx + 1) * c2, at : at + 128] = tile.astype(bf16)
    for begin in range(0, lines_a.shape[1], step):
        sums_ga[:, begin : begin + step] = dot(mat_ga[...], lines_a[:, begin : begin + step])
    total_a.step()
    total_b.step()
    total_c.step()
    feat_flying.wait()
    came = jnp.transpose(feat_came[...].astype(f32)).astype(bf16)
    ours = dot(came, far[...])
    for y in range(half_rows):
        stage[pl.ds(y, c3, stride=half_rows), :] = ours[:, y * 128 : (y + 1) * 128]
    features[...] = stage[...].astype(bf16)
    results = []
    for z in range(planes):
        by_row = []
        for ky in range(3):
            value = None
            for kz in range(3):
                at = (kz * 3 + ky) * c1
                term = sums_ga[at : at + c1, (z + kz) * 256 : (z + kz + 1) * 256]
                value = term if value is None else value + term
            by_row.append((value[:, :128], value[:, 128:]))
        before, after = moved_rows(by_row[0], 32)[0], moved_rows(by_row[2], 32)[1]
        results.append([by_row[1][g] + before[g] + after[g] for g in range(2)])
    for g in range(2):
        for z in range(planes):
            stage[pl.ds(z, c1, stride=planes), :] = results[z][g]
        for i in range(4):
            part = stage[:, width * i : width * (i + 1)].astype(bf16)
            grad_in[:, 4 * g + i] = part.reshape(c1, planes, width)

    while min(total.stage - total.stages for total in (total_a, total_b, total_c)) < 0:
        for total in (total_b, total_c, total_a):
            if total.stage < total.stages:
                total.step()


def last_kernel(scales, *refs):
    feat, grad, sum_a, sum_b, out_feat, out_grad, out_wa, out_ba, out_wb, out_bb = refs[:10]
    wa, ba, wb, bb, sems_out = refs[10:]
    f32 = jnp.float32
    scale_a, scale_b = scales
    places = ((grad, out_grad), (feat, out_feat), (wb, out_wb), (bb, out_bb), (wa, out_wa), (ba, out_ba))
    stores = [
        pltpu.make_async_copy(source, target, sems_out.at[at]) for at, (source, target) in enumerate(places)
    ]
    stores[0].start()
    stores[1].start()
    top = wb.shape[0]
    wb[...] = sum_b[:top].astype(f32) * scale_b
    stores[2].start()
    bb[...] = sum_b[top : top + 16].astype(f32)[:1] * scale_b
    stores[3].start()
    c1, c2 = wa.shape[1:]
    deep = 9 * c1
    pairs = sum_a[:deep].astype(f32) * scale_a
    tail = sum_a[deep : deep + deep // 2].astype(f32) * scale_a
    thirds = jnp.concatenate([tail[:, :c2], tail[:, c2:]], axis=0)
    for at in range(9):
        here = slice(at * c1, (at + 1) * c1)
        wa[at * 3] = pairs[here, :c2]
        wa[at * 3 + 1] = pairs[here, c2:]
        wa[at * 3 + 2] = thirds[here]
    stores[4].start()
    top_a = deep + deep // 2
    ba[...] = sum_a[top_a : top_a + 16].astype(f32)[:1, :c2] * scale_a
    stores[5].start()
    for store in stores:
        store.wait()


def all_groups():
    cut = {axis: [2**i for i in range(lax.axis_size(axis).bit_length() - 1)] for axis in ("gz", "gx")}
    line = [("gz", bit) for bit in cut["gz"]]
    return [line[:1], [("gx", bit) for bit in cut["gx"]] + line[1:2], line[2:]]


def on_blocks(volume, weight_a, bias_a, weight_b, bias_b, cotangent, scales):
    f32, bf16 = jnp.float32, jnp.bfloat16
    c1, width, rows, planes = volume.shape
    c2, c3 = weight_b.shape[3:]
    members = lax.axis_size("gz")
    groups = all_groups()
    tiles = planes // 4 + 1
    long, short = (planes + 2) * 256, tiles * 128
    cells = planes * 256
    rows_a, rows_b = 512, 27 * c2 + 64
    fewer = cells // 8

    def buffers(total, groups, exchanged):
        sends, recvs = [], []
        size = total
        for at, group in enumerate(groups):
            n = 2 ** len(group)
            if exchanged and at == len(groups) - 1:
                recvs.append(pltpu.VMEM((n, size, 128), bf16))
                continue
            sends.append(pltpu.VMEM((size, 128), bf16))
            size //= n
            recvs.append(pltpu.VMEM((n - 1, size, 128), bf16))
        return sends + recvs

    inboxes = []
    for size, plane, edge in ((c1, 256, c1), (c2 // 2, 128, c2 // 4), (c3 // 2, 128, c3 // 4), (c2, 256, c2)):
        inboxes += [pltpu.VMEM((size, plane), bf16)] * 2 + [pltpu.VMEM((edge, 128), bf16)] * 3
    groups_a = [groups[0] + groups[1], groups[2]]
    by_level = [2 ** len(group) for group in groups]
    count_a = len(groups_a) + by_level[1]
    count_b = len(groups) + by_level[2] * by_level[1]
    cuts = (1024, rows_b - 1024)
    passed = [
        ((c3 * rows // 2, 128), bf16),
        ((c1, rows, planes, width), bf16),
        ((rows_a, 128), bf16),
        ((rows_b, 128), bf16),
    ]
    operands = (
        jnp.transpose(volume, (0, 2, 3, 1)),
        weight_a.reshape(27, c1, c2),
        bias_a[None],
        weight_b.reshape(27, c2, c3),
        bias_b[None],
        cotangent.reshape(c3 * rows // 2, 128),
    )
    anywhere, inside = pl.BlockSpec(memory_space=pl.ANY), pl.BlockSpec(memory_space=pltpu.VMEM)
    middle = pl.pallas_call(
        functools.partial(block_kernel, (groups, groups_a, cuts)),
        out_shape=[pltpu.VMEM(shape, dtype) for shape, dtype in passed],
        in_specs=[anywhere] * len(operands),
        out_specs=[inside] * len(passed),
        scratch_shapes=[
            *[pltpu.VMEM(x.shape, x.dtype) for x in operands],
            pltpu.VMEM((c1 * planes, 128), f32),
            pltpu.VMEM((c1, cells), bf16),
            pltpu.VMEM((9 * c1, long), bf16),
            pltpu.VMEM((3 * c2, long), f32),
            pltpu.VMEM((c2, cells), f32),
            pltpu.VMEM((2 * tiles * c2, 512), bf16),
            pltpu.VMEM((c2, short), bf16),
            pltpu.VMEM((9 * c2, short), bf16),
            pltpu.VMEM((3 * c3, short), f32),
            pltpu.VMEM((fewer, c3), bf16),
            pltpu.VMEM((fewer, c3), bf16),
            pltpu.VMEM((c3, short), f32),
            pltpu.VMEM((3 * c3, short), bf16),
            pltpu.VMEM((3 * c3, short), bf16),
            pltpu.VMEM((9 * c2, short), f32),
            pltpu.VMEM((3 * c2, long), bf16),
            pltpu.VMEM((3 * c2, long), bf16),
            pltpu.VMEM((9 * c1, long), f32),
            pltpu.VMEM((fewer, c3), bf16),
            pltpu.VMEM((fewer, c3), bf16),
            pltpu.VMEM((3 * c2, 9 * c1), bf16),
            pltpu.VMEM((3 * c3, 9 * c2), bf16),
            pltpu.VMEM((9 * c1, 3 * c2), bf16),
            pltpu.VMEM((9 * c2, 3 * c3), bf16),
            pltpu.VMEM((fewer, short), bf16),
            pltpu.VMEM((fewer, fewer), bf16),
            pltpu.VMEM((rows_a, 128), f32),
            pltpu.VMEM((rows_b, 128), f32),
            *inboxes,
            *[pltpu.VMEM((size, 128), bf16) for size in (c1, c2 // 4, c3 // 4, c2)],
            *[pltpu.VMEM((size // 2, 128), bf16) for size in (c2, c2, c3, c3)],
            *buffers(rows_a, groups_a, True),
            *buffers(cuts[0], groups, False),
            *buffers(cuts[1], groups, False),
            *[pltpu.SemaphoreType.DMA((20,))] * 2,
            *[pltpu.SemaphoreType.DMA((1,))] * 4,
            *[pltpu.SemaphoreType.DMA((n,)) for n in (len(groups_a) + 1, count_a)],
            *[pltpu.SemaphoreType.DMA((n,)) for n in (len(groups) + 1, count_b)] * 2,
            pltpu.SemaphoreType.DMA((len(operands),)),
        ],
        compiler_params=pltpu.CompilerParams(
            collective_id=2, has_side_effects=True, vmem_limit_bytes=60 * 2**20
        ),
    )(*operands)
    outs = [
        *passed[:2],
        ((27, c1, c2), f32),
        ((1, c2), f32),
        ((27 * c2, c3), f32),
        ((1, c3), f32),
    ]
    features, grad_in, sum_wa, sum_ba, sum_wb, sum_bb = pl.pallas_call(
        functools.partial(last_kernel, scales),
        out_shape=[jax.ShapeDtypeStruct(shape, dtype) for shape, dtype in outs],
        in_specs=[inside] * len(passed),
        out_specs=[anywhere] * len(outs),
        scratch_shapes=[
            *[pltpu.VMEM(shape, dtype) for shape, dtype in outs[2:]],
            pltpu.SemaphoreType.DMA((len(outs),)),
        ],
    )(*[pltpu.with_memory_space_constraint(x, pltpu.VMEM) for x in middle])
    return (
        features.reshape(cotangent.shape),
        jnp.transpose(grad_in, (0, 3, 1, 2)),
        sum_wa.reshape(weight_a.shape),
        sum_ba.reshape(c2),
        sum_wb.reshape(weight_b.shape),
        sum_bb.reshape(c3),
    )


def fits_blocks(volume, weight_b):
    c1, width, rows, planes = volume.shape
    sizes = {axis: lax.axis_size(axis) for axis in ("gx", "gy", "gz")}
    return (
        sizes == {"gx": 2, "gy": 1, "gz": planes}
        and (width, rows, planes) == (32, 8, 16)
        and (c1, *weight_b.shape[3:]) == (32, 64, 128)
    )


def on_device(volume, weight_a, bias_a, weight_b, bias_b, cotangent):
    f32, bf16 = jnp.float32, jnp.bfloat16
    count = lax.axis_size("gz")
    devices_all = lax.axis_size("gx") * lax.axis_size("gy") * count
    c1, nx, rows, nz = volume.shape
    cells = nx * rows * nz
    scale_a = 1.0 / math.sqrt(cells * devices_all)
    scale_b = 1.0 / math.sqrt(cells * devices_all // 8)
    c2, c3 = weight_b.shape[3:]
    if fits_blocks(volume, weight_b):
        return on_blocks(volume, weight_a, bias_a, weight_b, bias_b, cotangent, (scale_a, scale_b))
    planes, depth = nx // count, nz * count
    fine = (planes, rows, depth)
    coarse = (planes // 2, rows // 2, depth // 2)
    fewer = cells // 8
    pool = (jnp.arange(depth)[:, None] // 2 == jnp.arange(depth // 2)[None]).astype(f32)
    work_a = 2 * 27 * c1 * c2 * cells
    work_b = 2 * 27 * c2 * c3 * fewer

    slab = lax.all_to_all(volume, "gz", split_axis=1, concat_axis=3, tiled=True).reshape(c1, cells)
    if lax.axis_size("gy") == 1:
        features, grad_slab, sum_wa, sum_ba, sum_wb, sum_bb = between_exchanges(
            fine,
            coarse,
            (scale_a, scale_b),
            slab,
            weight_a,
            bias_a,
            weight_b,
            bias_b,
            cotangent.reshape(c3, fewer),
            pool,
        )
    else:
        wide_a = widened(slab, *fine)
        before_a, pooled = local_kernel(
            functools.partial(forward_a_kernel, fine),
            [((c2, cells), f32), ((c2, fewer), bf16)],
            (27 * c1, cells),
            work_a,
            wide_a,
            outward(weight_a),
            bias_a[:, None],
            pool,
        )
        wide_b = widened(pooled, *coarse)
        features, grad_b, part_wb, part_bb = local_kernel(
            functools.partial(middle_kernel, coarse),
            [((c3, fewer), bf16), ((c3, fewer), bf16), ((27 * c2, c3), f32), ((8, c3), f32)],
            (27 * c2, fewer),
            2 * work_b,
            wide_b,
            outward(weight_b),
            bias_b[:, None],
            cotangent.reshape(c3, fewer),
        )
        (grad_a,) = local_kernel(
            functools.partial(backward_b_kernel, coarse, fine),
            [((c2, cells), bf16)],
            (27 * c3, fewer),
            work_b,
            widened(grad_b, *coarse),
            inward(weight_b),
            before_a,
            pool.T.astype(bf16),
        )
        part_wa, part_ba = local_kernel(
            functools.partial(weight_a_kernel, fine),
            [((27 * c1, c2), f32), ((8, c2), f32)],
            (27 * c1, cells),
            work_a,
            wide_a,
            grad_a,
        )
        (grad_slab,) = local_kernel(
            functools.partial(backward_a_kernel, fine),
            [((c1, cells), bf16)],
            (27 * c2, cells),
            work_a,
            widened(grad_a, *fine),
            inward(weight_a),
        )
        sum_wa, sum_ba, sum_wb, sum_bb = summed_grads(
            part_wa, part_ba, part_wb, part_bb, (scale_a, scale_b)
        )
    grad_input = lax.all_to_all(
        grad_slab.reshape(c1, planes, rows, depth), "gz", split_axis=3, concat_axis=1, tiled=True
    )
    return (
        features.reshape(cotangent.shape),
        grad_input,
        sum_wa.reshape(weight_a.shape),
        sum_ba.reshape(c2),
        sum_wb.reshape(weight_b.shape),
        sum_bb.reshape(c3),
    )


def solution(mesh):
    return jax.shard_map(
        on_device,
        mesh=mesh,
        in_specs=(P(None, "gx", "gy", "gz"), P(), P(), P(), P(), P(None, ("gx", "gz"), "gy", None)),
        out_specs=(
            P(None, ("gx", "gz"), "gy", None),
            P(None, "gx", "gy", "gz"),
            P(),
            P(),
            P(),
            P(),
        ),
        check_vma=False,
    )
```

```python
import functools
import math

import jax
import jax.numpy as jnp
from jax import lax
from jax.experimental import pallas as pl
from jax.experimental.pallas import tpu as pltpu
from jax.sharding import PartitionSpec as P

LINE = ("gx", "gz")
MESH = pl.DeviceIdType.MESH


def shared(block, axis, dim, width):
    count = lax.axis_size(axis)
    if count == 1:
        edge = jnp.zeros_like(lax.slice_in_dim(block, 0, width, axis=dim))
        return edge, edge
    forward = [(i, i + 1) for i in range(count - 1)]
    backward = [(target, source) for source, target in forward]
    last = block.shape[dim]
    low = lax.ppermute(lax.slice_in_dim(block, last - width, last, axis=dim), axis, forward)
    high = lax.ppermute(lax.slice_in_dim(block, 0, width, axis=dim), axis, backward)
    return low, high


def widened(flat, planes, rows, depth):
    low, high = shared(flat, LINE, 1, rows * depth)
    if lax.axis_size("gy") == 1:
        gap = jnp.zeros((flat.shape[0], depth), flat.dtype)
        pieces = [gap, low, gap]
        for plane in range(planes):
            pieces += [gap, flat[:, plane * rows * depth : (plane + 1) * rows * depth], gap]
        return jnp.concatenate(pieces + [gap, high, gap], axis=1)
    whole = jnp.concatenate([low, flat, high], axis=1)
    whole = whole.reshape(flat.shape[0], planes + 2, rows, depth)
    low, high = shared(whole, "gy", 2, 1)
    return jnp.concatenate([low, whole, high], axis=2).reshape(flat.shape[0], -1)


def slope_of(value):
    sigma = jax.nn.sigmoid(value)
    return sigma + value * sigma * (1.0 - sigma)


def put_windows(wide_ref, windows, planes, rows, depth):
    wide = wide_ref[...]
    width, extent = wide.shape
    place = lax.broadcasted_iota(jnp.int32, (width, extent), 1) % depth
    loose = wide.astype(jnp.float32)
    before = jnp.where(place == 0, 0.0, pltpu.roll(loose, 1, 1)).astype(jnp.bfloat16)
    after = jnp.where(place == depth - 1, 0.0, pltpu.roll(loose, extent - 1, 1)).astype(jnp.bfloat16)
    size = rows * depth
    for third, moved in enumerate((before, wide, after)):
        for first in range(3):
            for second in range(3):
                at = (first * 9 + second * 3 + third) * width
                for plane in range(planes):
                    begin = ((plane + first) * (rows + 2) + second) * depth
                    windows[at : at + width, plane * size : (plane + 1) * size] = moved[
                        :, begin : begin + size
                    ]


def dot_rows(left, right):
    return lax.dot_general(
        left, right, (((1,), (1,)), ((), ())), preferred_element_type=jnp.float32
    )


def forward_a_kernel(dims, wide_ref, weight_ref, bias_ref, pool_ref, before_ref, pooled_ref, windows):
    planes, rows, depth = dims
    put_windows(wide_ref, windows, *dims)
    before = jnp.dot(weight_ref[...], windows[...], preferred_element_type=jnp.float32)
    before = before + bias_ref[...]
    before_ref[...] = before
    active = before * jax.nn.sigmoid(before)
    size = rows * depth
    for row in range(rows // 2):
        parts = [
            active[:, plane * size + (2 * row + j) * depth : plane * size + (2 * row + j + 1) * depth]
            for plane in range(planes)
            for j in range(2)
        ]
        summed = sum(parts[1:], parts[0])
        paired = jnp.dot(
            summed, pool_ref[...], precision=lax.Precision.HIGHEST, preferred_element_type=jnp.float32
        )
        pooled_ref[:, row * depth // 2 : (row + 1) * depth // 2] = (paired * 0.125).astype(jnp.bfloat16)


def middle_kernel(dims, wide_ref, weight_ref, bias_ref, cot_ref, feat_ref, grad_ref, wb_ref, bb_ref, windows):
    put_windows(wide_ref, windows, *dims)
    before = jnp.dot(weight_ref[...], windows[...], preferred_element_type=jnp.float32)
    before = before + bias_ref[...]
    feat_ref[...] = (before * jax.nn.sigmoid(before)).astype(jnp.bfloat16)
    grad = (cot_ref[...].astype(jnp.float32) * slope_of(before)).astype(jnp.bfloat16)
    grad_ref[...] = grad
    wb_ref[...] = dot_rows(windows[...], grad)
    bb_ref[...] = dot_rows(jnp.ones((8, grad.shape[1]), jnp.bfloat16), grad)


def backward_b_kernel(dims, fine, wide_ref, weight_ref, before_ref, spread_ref, grad_ref, windows):
    put_windows(wide_ref, windows, *dims)
    pooled = jnp.dot(weight_ref[...], windows[...], preferred_element_type=jnp.float32)
    pooled = pooled.astype(jnp.bfloat16)
    planes, rows, depth = fine
    size = rows * depth
    for row in range(rows // 2):
        part = pooled[:, row * depth // 2 : (row + 1) * depth // 2]
        spread = jnp.dot(part, spread_ref[...], preferred_element_type=jnp.float32) * 0.125
        for plane in range(planes):
            for j in range(2):
                begin = plane * size + (2 * row + j) * depth
                slope = slope_of(before_ref[:, begin : begin + depth])
                grad_ref[:, begin : begin + depth] = (spread * slope).astype(jnp.bfloat16)


def weight_a_kernel(dims, wide_ref, grad_ref, wa_ref, ba_ref, windows):
    put_windows(wide_ref, windows, *dims)
    grad = grad_ref[...]
    wa_ref[...] = dot_rows(windows[...], grad)
    ba_ref[...] = dot_rows(jnp.ones((8, grad.shape[1]), jnp.bfloat16), grad)


def backward_a_kernel(dims, wide_ref, weight_ref, out_ref, windows):
    put_windows(wide_ref, windows, *dims)
    out = jnp.dot(weight_ref[...], windows[...], preferred_element_type=jnp.float32)
    out_ref[...] = out.astype(jnp.bfloat16)


def local_kernel(body, outs, windows, flops, *operands):
    moved = sum(x.size * x.dtype.itemsize for x in operands)
    return pl.pallas_call(
        body,
        out_shape=[jax.ShapeDtypeStruct(shape, dtype) for shape, dtype in outs],
        in_specs=[pl.BlockSpec(memory_space=pltpu.VMEM)] * len(operands),
        out_specs=[pl.BlockSpec(memory_space=pltpu.VMEM)] * len(outs),
        scratch_shapes=[pltpu.VMEM(windows, jnp.bfloat16)],
        compiler_params=pltpu.CompilerParams(vmem_limit_bytes=48 * 2**20),
        cost_estimate=pl.CostEstimate(flops=flops, bytes_accessed=moved, transcendentals=0),
    )(*operands)


def partner_of(axis, bit):
    me = lax.axis_index(axis)
    mine = (me // bit) % 2
    return me + bit * (1 - 2 * mine), mine


def sum_kernel(steps, halvings, rows, scales, wa_ref, ba_ref, wb_ref, bb_ref, *rest):
    out_wa, out_ba, out_wb, out_bb, acc, gathered, *scratch = rest
    half, width = wa_ref.shape[0] // 2, wa_ref.shape[1]
    top = wb_ref.shape[0]
    count = len(steps)
    sends = scratch[:count]
    recvs = scratch[count : 2 * count]
    sem_send, sem_recv = scratch[2 * count :]
    partners = [partner_of(axis, bit) for axis, bit in steps]
    barrier = pltpu.get_barrier_semaphore()
    for (axis, _), (partner, _) in zip(steps, partners):
        pl.semaphore_signal(barrier, inc=1, device_id={axis: partner}, device_id_type=MESH)
    acc[:top] = wb_ref[...]
    acc[top : top + half, :width] = wa_ref[:half]
    acc[top : top + half, width:] = wa_ref[half:]
    acc[top + half :] = jnp.zeros((rows - top - half, 128), jnp.float32)
    acc[top + half : top + half + 8, :width] = ba_ref[...]
    acc[top + half + 8 : top + half + 16] = bb_ref[...]
    pl.semaphore_wait(barrier, count)
    offset = 0
    size = rows
    kept = []
    for at, ((axis, _), (partner, mine)) in enumerate(zip(steps, partners)):
        source = acc
        if at < halvings:
            size = size // 2
            away = pl.multiple_of(offset + (1 - mine) * size, 16)
            offset = pl.multiple_of(offset + mine * size, 16)
        else:
            away = offset
        sends[at][...] = source[pl.ds(away, size)].astype(jnp.bfloat16)
        copy = pltpu.make_async_remote_copy(
            src_ref=sends[at],
            dst_ref=recvs[at],
            send_sem=sem_send.at[at],
            recv_sem=sem_recv.at[at],
            device_id={axis: partner},
            device_id_type=MESH,
        )
        copy.start()
        copy.wait()
        if at < halvings:
            acc[pl.ds(offset, size)] = source[pl.ds(offset, size)] + recvs[at][...].astype(jnp.float32)
            kept.append((offset, size))
        else:
            acc[pl.ds(offset, size)] = sends[at][...].astype(jnp.float32) + recvs[at][...].astype(jnp.float32)
    gathered[pl.ds(offset, size)] = acc[pl.ds(offset, size)].astype(jnp.bfloat16)
    for back in range(halvings):
        at = halvings - 1 - back
        begin, extent = kept[at]
        (axis, _), (partner, _) = steps[at], partners[at]
        here = gathered.at[pl.ds(begin, extent)]
        copy = pltpu.make_async_remote_copy(
            src_ref=here,
            dst_ref=here,
            send_sem=sem_send.at[count + back],
            recv_sem=sem_recv.at[count + back],
            device_id={axis: partner},
            device_id_type=MESH,
        )
        copy.start()
        copy.wait()
    scale_a, scale_b = scales
    total = gathered[...].astype(jnp.float32)
    out_wb[...] = total[:top] * scale_b
    out_wa[:half] = total[top : top + half, :width] * scale_a
    out_wa[half:] = total[top : top + half, width:] * scale_a
    out_ba[...] = total[top + half : top + half + 1, :width] * scale_a
    out_bb[...] = total[top + half + 8 : top + half + 9] * scale_b


def summed_grads(wa, ba, wb, bb, scales):
    used = wb.shape[0] + wa.shape[0] // 2 + 16
    rows = used + -used % 128
    cut = {
        axis: [2**i for i in range(lax.axis_size(axis).bit_length() - 1)] for axis in ("gz", "gx", "gy")
    }
    steps = [("gz", bit) for bit in cut["gz"][:1]]
    steps += [("gx", bit) for bit in cut["gx"]] + [("gy", bit) for bit in cut["gy"]]
    steps += [("gz", bit) for bit in cut["gz"][1:]]
    halvings = 0
    sizes = []
    size = rows
    for _ in steps:
        if len(sizes) == halvings and size % 32 == 0:
            size //= 2
            halvings += 1
        sizes.append(size)
    buffers = [pltpu.VMEM((s, 128), jnp.bfloat16) for s in sizes]
    total = len(steps) + halvings
    shapes = [wa.shape, (1, ba.shape[1]), wb.shape, (1, bb.shape[1])]
    return pl.pallas_call(
        functools.partial(sum_kernel, steps, halvings, rows, scales),
        out_shape=[jax.ShapeDtypeStruct(shape, jnp.float32) for shape in shapes],
        in_specs=[pl.BlockSpec(memory_space=pltpu.VMEM)] * 4,
        out_specs=[pl.BlockSpec(memory_space=pltpu.VMEM)] * 4,
        scratch_shapes=[
            pltpu.VMEM((rows, 128), jnp.float32),
            pltpu.VMEM((rows, 128), jnp.bfloat16),
            *buffers,
            *buffers,
            pltpu.SemaphoreType.DMA((total,)),
            pltpu.SemaphoreType.DMA((total,)),
        ],
        compiler_params=pltpu.CompilerParams(collective_id=0, has_side_effects=True),
    )(wa, ba, wb, bb)


def line_ends(axis_sizes):
    across, count = axis_sizes
    total = across * count
    line = lax.axis_index("gx") * count + lax.axis_index("gz")
    after, before = (line + 1) % total, (line + total - 1) % total
    ids = [{"gx": at // count, "gz": at % count} for at in (after, before)]
    return line, total, ids


class Halo:
    def __init__(self, wide, dims, where, sems, at):
        planes, rows, depth = dims
        self.line, self.total, ids = where
        size, stride = rows * depth, (rows + 2) * depth
        spot = lambda plane: wide.at[:, plane * stride + depth : plane * stride + depth + size]
        send, recv = sems
        self.up, self.down = [
            pltpu.make_async_remote_copy(
                src_ref=spot(source),
                dst_ref=spot(target),
                send_sem=send.at[at + i],
                recv_sem=recv.at[at + i],
                device_id=ids[i],
                device_id_type=MESH,
            )
            for i, (source, target) in enumerate(((planes, 0), (1, planes + 1)))
        ]

    def start(self):
        pl.when(self.line < self.total - 1)(self.up.start)
        pl.when(self.line > 0)(self.down.start)

    def wait(self):
        @pl.when(self.line < self.total - 1)
        def _():
            self.up.wait_send()
            self.down.wait_recv()

        @pl.when(self.line > 0)
        def _():
            self.down.wait_send()
            self.up.wait_recv()


class Summing:
    def __init__(self, steps, sizes, acc, gathered, sends, recvs, sems):
        self.steps, self.sizes = steps, sizes
        self.acc, self.gathered, self.sends, self.recvs = acc, gathered, sends, recvs
        self.sems = sems
        self.partners = [partner_of(axis, bit) for axis, bit in steps]
        rows = [acc.shape[0]] + list(sizes)
        self.halvings = sum(a != b for a, b in zip(rows, sizes))
        self.stages = len(steps) + self.halvings
        self.offset = 0
        self.kept = []
        self.flying = None

    def copy(self, stage, source, target, step):
        send, recv = self.sems
        self.flying = pltpu.make_async_remote_copy(
            src_ref=source,
            dst_ref=target,
            send_sem=send.at[stage],
            recv_sem=recv.at[stage],
            device_id={self.steps[step][0]: self.partners[step][0]},
            device_id_type=MESH,
        )
        self.flying.start()

    def start(self, stage):
        if stage < len(self.steps):
            size = self.sizes[stage]
            away = self.offset
            if stage < self.halvings:
                mine = self.partners[stage][1]
                away = pl.multiple_of(self.offset + (1 - mine) * size, 16)
                self.offset = pl.multiple_of(self.offset + mine * size, 16)
                self.kept.append((self.offset, size))
            self.sends[stage][...] = self.acc[pl.ds(away, size)].astype(jnp.bfloat16)
            self.copy(stage, self.sends[stage], self.recvs[stage], stage)
        else:
            step = self.halvings - 1 - (stage - len(self.steps))
            begin, size = self.kept[step]
            here = self.gathered.at[pl.ds(begin, size)]
            self.copy(stage, here, here, step)

    def finish(self, stage):
        self.flying.wait()
        if stage >= len(self.steps):
            return
        here = pl.ds(self.offset, self.sizes[stage])
        came = self.recvs[stage][...].astype(jnp.float32)
        own = self.acc[here] if stage < self.halvings else self.sends[stage][...].astype(jnp.float32)
        total = own + came
        if stage == len(self.steps) - 1:
            self.gathered[here] = total.astype(jnp.bfloat16)
        else:
            self.acc[here] = total


def place(wide, flat, dims):
    planes, rows, depth = dims
    size, stride = rows * depth, (rows + 2) * depth
    for plane in range(planes):
        begin = (plane + 1) * stride + depth
        wide[:, begin : begin + size] = flat[:, plane * size : (plane + 1) * size]


def whole_kernel(setting, *refs):
    fine, coarse, sizes_line, steps, cuts_a, cuts_b, scales = setting
    slab, w_a, b_a, pool, w_b, b_b, cot, v_b, spread, v_a = refs[:10]
    features, grad_slab, out_wa, out_ba, out_wb, out_bb = refs[10:16]
    wide_a, wide_b, wide_gb, wide_ga, win_a, win_b, win_gb, win_ga = refs[16:24]
    before_a, pooled, grad_b, grad_a, acc_a, acc_b, all_a, all_b = refs[24:32]
    count = len(steps)
    send_a, recv_a, send_b, recv_b = [refs[32 + i * count : 32 + (i + 1) * count] for i in range(4)]
    sems = refs[32 + 4 * count :]
    where = line_ends(sizes_line)
    line, total, ids = where
    barrier = pltpu.get_barrier_semaphore()
    for wide in (wide_a, wide_b, wide_gb, wide_ga):
        wide[...] = jnp.zeros_like(wide)
    place(wide_a, slab, fine)
    for axis, bit in steps:
        partner, _ = partner_of(axis, bit)
        pl.semaphore_signal(barrier, inc=1, device_id={axis: partner}, device_id_type=MESH)
    for device in ids:
        pl.semaphore_signal(barrier, inc=1, device_id=device, device_id_type=MESH)
    pl.semaphore_wait(barrier, count + 2)
    halos = [
        Halo(wide, dims, where, sems[:2], 2 * i)
        for i, (wide, dims) in enumerate(
            ((wide_a, fine), (wide_b, coarse), (wide_gb, coarse), (wide_ga, fine))
        )
    ]
    sum_a = Summing(steps, cuts_a, acc_a, all_a, send_a, recv_a, sems[2:4])
    sum_b = Summing(steps, cuts_b, acc_b, all_b, send_b, recv_b, sems[4:6])

    halos[0].start()
    halos[0].wait()
    forward_a_kernel(fine, wide_a, w_a, b_a, pool, before_a, pooled, win_a)
    place(wide_b, pooled, coarse)
    halos[1].start()
    halos[1].wait()
    top_b = out_wb.shape[0]
    middle_kernel(
        coarse, wide_b, w_b, b_b, cot, features, grad_b, acc_b.at[:top_b], acc_b.at[top_b : top_b + 8], win_b
    )
    place(wide_gb, grad_b, coarse)
    halos[2].start()
    acc_b[top_b + 8 :] = jnp.zeros((acc_b.shape[0] - top_b - 8, acc_b.shape[1]), jnp.float32)
    sum_b.start(0)
    halos[2].wait()
    backward_b_kernel(coarse, fine, wide_gb, v_b, before_a, spread, grad_a, win_gb)
    place(wide_ga, grad_a, fine)
    halos[3].start()
    sum_b.finish(0)
    sum_b.start(1)
    grad = grad_a[...]
    half, width = out_wa.shape[0] // 2, out_wa.shape[1]
    acc_a[:half, :width] = dot_rows(win_a[:half], grad)
    acc_a[:half, width:] = dot_rows(win_a[half:], grad)
    acc_a[half:] = jnp.zeros((acc_a.shape[0] - half, acc_a.shape[1]), jnp.float32)
    acc_a[half : half + 8, :width] = dot_rows(jnp.ones((8, grad.shape[1]), jnp.bfloat16), grad)
    sum_b.finish(1)
    sum_b.start(2)
    sum_a.start(0)
    halos[3].wait()
    backward_a_kernel(fine, wide_ga, v_a, grad_slab, win_ga)
    for stage in range(max(sum_a.stages, sum_b.stages - 2)):
        if stage + 2 < sum_b.stages:
            sum_b.finish(stage + 2)
            if stage + 3 < sum_b.stages:
                sum_b.start(stage + 3)
        if stage < sum_a.stages:
            sum_a.finish(stage)
            if stage + 1 < sum_a.stages:
                sum_a.start(stage + 1)
    scale_a, scale_b = scales
    out_wb[...] = all_b[:top_b].astype(jnp.float32) * scale_b
    out_bb[...] = all_b[top_b : top_b + 16].astype(jnp.float32)[:1] * scale_b
    out_wa[:half] = all_a[:half, :width].astype(jnp.float32) * scale_a
    out_wa[half:] = all_a[:half, width:].astype(jnp.float32) * scale_a
    out_ba[...] = all_a[half : half + 16, :width].astype(jnp.float32)[:1] * scale_a


def stage_sizes(rows, steps):
    sizes = []
    for _ in steps:
        halve = rows % 32 == 0 and len(sizes) < 3
        rows = rows // 2 if halve else rows
        sizes.append(rows)
    return sizes


def all_steps():
    cut = {
        axis: [2**i for i in range(lax.axis_size(axis).bit_length() - 1)] for axis in ("gz", "gx", "gy")
    }
    steps = [("gz", bit) for bit in cut["gz"][:1]]
    steps += [("gx", bit) for bit in cut["gx"]] + [("gy", bit) for bit in cut["gy"]]
    return steps + [("gz", bit) for bit in cut["gz"][1:]]


def between_exchanges(fine, coarse, scales, slab, weight_a, bias_a, weight_b, bias_b, cot, pool):
    f32, bf16 = jnp.float32, jnp.bfloat16
    c1, cells = slab.shape
    c2, c3 = weight_b.shape[3:]
    fewer = cells // 8
    steps = all_steps()
    rows_a = 27 * c1 // 2 + 16
    rows_a += -rows_a % 128
    rows_b = 27 * c2 + 16
    rows_b += -rows_b % 128
    cuts_a, cuts_b = stage_sizes(rows_a, steps), stage_sizes(rows_b, steps)
    extent = lambda dims: (dims[0] + 2) * (dims[1] + 2) * dims[2]
    setting = (fine, coarse, (lax.axis_size("gx"), lax.axis_size("gz")), steps, cuts_a, cuts_b, scales)
    buffers = [pltpu.VMEM((n, 128), bf16) for cuts in (cuts_a, cuts_a, cuts_b, cuts_b) for n in cuts]
    outs = [
        ((c3, fewer), bf16),
        ((c1, cells), bf16),
        ((27 * c1, c2), f32),
        ((1, c2), f32),
        ((27 * c2, c3), f32),
        ((1, c3), f32),
    ]
    operands = (
        slab,
        outward(weight_a),
        bias_a[:, None],
        pool,
        outward(weight_b),
        bias_b[:, None],
        cot,
        inward(weight_b),
        pool.T.astype(bf16),
        inward(weight_a),
    )
    most = 2 * len(steps)
    return pl.pallas_call(
        functools.partial(whole_kernel, setting),
        out_shape=[jax.ShapeDtypeStruct(shape, dtype) for shape, dtype in outs],
        in_specs=[pl.BlockSpec(memory_space=pltpu.VMEM)] * len(operands),
        out_specs=[pl.BlockSpec(memory_space=pltpu.VMEM)] * len(outs),
        scratch_shapes=[
            pltpu.VMEM((c1, extent(fine)), bf16),
            pltpu.VMEM((c2, extent(coarse)), bf16),
            pltpu.VMEM((c3, extent(coarse)), bf16),
            pltpu.VMEM((c2, extent(fine)), bf16),
            pltpu.VMEM((27 * c1, cells), bf16),
            pltpu.VMEM((27 * c2, fewer), bf16),
            pltpu.VMEM((27 * c3, fewer), bf16),
            pltpu.VMEM((27 * c2, cells), bf16),
            pltpu.VMEM((c2, cells), f32),
            pltpu.VMEM((c2, fewer), bf16),
            pltpu.VMEM((c3, fewer), bf16),
            pltpu.VMEM((c2, cells), bf16),
            pltpu.VMEM((rows_a, 128), f32),
            pltpu.VMEM((rows_b, 128), f32),
            pltpu.VMEM((rows_a, 128), bf16),
            pltpu.VMEM((rows_b, 128), bf16),
            *buffers,
            pltpu.SemaphoreType.DMA((8,)),
            pltpu.SemaphoreType.DMA((8,)),
            *[pltpu.SemaphoreType.DMA((most,))] * 4,
        ],
        compiler_params=pltpu.CompilerParams(
            collective_id=1, has_side_effects=True, vmem_limit_bytes=60 * 2**20
        ),
    )(*operands)


def outward(weight):
    return weight.reshape(-1, weight.shape[-1]).T


def inward(weight):
    taps = weight[::-1, ::-1, ::-1].reshape(27, *weight.shape[3:])
    return jnp.transpose(taps, (1, 0, 2)).reshape(weight.shape[3], -1)


def lanes_of(shape):
    return lax.broadcasted_iota(jnp.int32, shape, len(shape) - 1)


def rows_of(shape):
    return lax.broadcasted_iota(jnp.int32, shape, 0)


def ones_where(mask):
    return jnp.where(mask, 1.0, 0.0).astype(jnp.bfloat16)


def dot(left, right):
    return jnp.dot(left, right, preferred_element_type=jnp.float32)


def by_parts(rank_bits, mask):
    place = {}
    for at, (axis, bit) in enumerate(rank_bits):
        if mask >> at & 1:
            me = place.get(axis, lax.axis_index(axis))
            place[axis] = me + bit * (1 - 2 * ((lax.axis_index(axis) // bit) % 2))
    return place


def own_rank(rank_bits, mask=0):
    total = 0
    for at, (axis, bit) in enumerate(rank_bits):
        mine = (lax.axis_index(axis) // bit) % 2
        total = total + ((1 - mine) if mask >> at & 1 else mine) * 2**at
    return total


def remote(source, target, sems, at, device, sent_at=None):
    return pltpu.make_async_remote_copy(
        src_ref=source,
        dst_ref=target,
        send_sem=sems[0].at[at if sent_at is None else sent_at],
        recv_sem=sems[1].at[at],
        device_id=device,
        device_id_type=MESH,
    )


def flipped_bits(bits, mask):
    return tuple(bit for at, bit in enumerate(bits) if mask >> at & 1)


class Reduction:
    def __init__(self, groups, exchanged, acc, summed, sends, recvs, sems):
        self.groups, self.exchanged, self.acc, self.summed = groups, exchanged, acc, summed
        self.sends, self.recvs, self.sems = sends, recvs, sems
        self.offset, self.size = 0, acc.shape[0]
        self.parts = []
        self.all = None
        self.stage = 0
        bits = sum(groups[:-1] if exchanged else groups, [])
        self.levels = [level for level in reversed(all_groups()) if level[0] in bits]
        self.stages = len(groups) + len(self.levels)
        self.used = len(groups)
        self.places = {}
        self.sent = 0

    def fly(self, source, target, device):
        remote(source, target, self.sems, self.stage, device).start()

    def piece(self, flipped, level, mask, arrived):
        key = (flipped, level, mask) if level + 1 < len(self.levels) else level
        if key not in self.places:
            self.places[key] = self.used
            self.used += 1
        whose = flipped + flipped_bits(self.levels[level], mask) if arrived else flipped
        offset = 0
        for bits, part in self.parts:
            turned = sum(1 << at for at, bit in enumerate(bits) if bit in whose)
            offset = offset + own_rank(bits, turned) * part
        here = self.summed.at[pl.ds(pl.multiple_of(offset, 8), self.size)]
        device = by_parts(self.levels[level], mask)
        return remote(here, here, self.sems, self.places[key], device, len(self.groups))

    def pieces(self, count, at):
        here = self.summed.at[: count * self.size]
        return remote(here, here, self.sems, at, by_parts(self.levels[-1], 1), len(self.groups))

    def pass_on(self, flipped, first):
        for level in range(first, len(self.levels)):
            for mask in range(1, 2 ** len(self.levels[level])):
                self.piece(flipped, level, mask, False).start()
                self.sent += 1

    def start(self):
        at = self.stage
        count = len(self.groups)
        if at > count:
            return
        if at == count:
            self.known = [()]
            self.pass_on((), 0)
        elif self.exchanged and at == count - 1:
            bits = self.groups[at]
            recv = self.recvs[at]
            mine = own_rank(bits)
            recv[mine] = self.acc[pl.ds(self.offset, self.size)].astype(jnp.bfloat16)
            for mask in range(1, 2 ** len(bits)):
                self.fly(recv.at[mine], recv.at[mine], by_parts(bits, mask))
            rest = recv.at[: recv.shape[0] - 1]
            self.all = remote(rest, rest, self.sems, at, by_parts(bits, 1))
        else:
            bits = self.groups[at]
            members = 2 ** len(bits)
            part = self.size // members
            send, recv = self.sends[at], self.recvs[at]
            send[...] = self.acc[pl.ds(self.offset, self.size)].astype(jnp.bfloat16)
            for mask in range(1, members):
                begin = pl.multiple_of(own_rank(bits, mask) * part, 8)
                self.fly(send.at[pl.ds(begin, part)], recv.at[mask - 1], by_parts(bits, mask))
            self.all = remote(recv, recv, self.sems, at, by_parts(bits, 1))
            self.parts.append((bits, part))
            self.offset = pl.multiple_of(self.offset + own_rank(bits) * part, 8)
            self.size = part

    def finish(self):
        at = self.stage
        count = len(self.groups)
        self.stage += 1
        if at >= count:
            level = at - count
            if level + 1 == len(self.levels):
                self.pieces(len(self.known) * (2 ** len(self.levels[level]) - 1), self.places[level]).wait_recv()
                self.pieces(self.sent, 0).wait_send()
                return
            came = []
            for flipped in self.known:
                for mask in range(1, 2 ** len(self.levels[level])):
                    self.piece(flipped, level, mask, True).wait_recv()
                    whose = flipped + flipped_bits(self.levels[level], mask)
                    self.pass_on(whose, level + 1)
                    came.append(whose)
            self.known = self.known + came
            return
        self.all.wait()
        recv = self.recvs[at]
        here = pl.ds(self.offset, self.size)
        if self.exchanged and at == count - 1:
            total = recv[0].astype(jnp.float32)
            for i in range(1, recv.shape[0]):
                total = total + recv[i].astype(jnp.float32)
        else:
            total = self.acc[here]
            for i in range(recv.shape[0]):
                total = total + recv[i].astype(jnp.float32)
        if at == count - 1:
            self.summed[here] = total.astype(jnp.bfloat16)
        else:
            self.acc[here] = total

    def step(self):
        self.finish()
        if self.stage < self.stages:
            self.start()


class Border:
    def __init__(self, first, last, edge, inbox, sems, at):
        me, count = lax.axis_index("gz"), lax.axis_size("gz")
        side = 1 - lax.axis_index("gx")
        self.inner, self.outer = me > 0, me < count - 1
        up, down = (me + 1) % count, (me + count - 1) % count
        low, high, beside, beside_low, beside_high = inbox
        self.always = remote(edge, beside, sems, at + 2, {"gx": side})
        self.up = [
            remote(last, low, sems, at, {"gz": up}),
            remote(edge, beside_low, sems, at + 3, {"gx": side, "gz": up}),
        ]
        self.down = [
            remote(first, high, sems, at + 1, {"gz": down}),
            remote(edge, beside_high, sems, at + 4, {"gx": side, "gz": down}),
        ]

    def start(self):
        @pl.when(self.outer)
        def _():
            for copy in self.up:
                copy.start()

        @pl.when(self.inner)
        def _():
            for copy in self.down:
                copy.start()

        self.always.start()

    def wait(self):
        self.always.wait()

        @pl.when(self.outer)
        def _():
            for copy in self.up:
                copy.wait_send()
            for copy in self.down:
                copy.wait_recv()

        @pl.when(self.inner)
        def _():
            for copy in self.down:
                copy.wait_send()
            for copy in self.up:
                copy.wait_recv()


def gathered_edge(tiles, extent, slots):
    shape = tiles[0].shape
    lane = lanes_of(shape)
    high = lax.axis_index("gx") == 0
    edge = jnp.where(high, extent - 1, 0)
    at_edge = lane & (extent - 1) == edge
    total = None
    for i, tile in enumerate(tiles):
        kept = rolled(jnp.where(at_edge, tile, 0.0), i % slots)
        total = kept if total is None else total + kept
    back = pltpu.roll(total, 128 - (extent - 1), 1)
    return jnp.where(high, back, total)


def rolled(value, by):
    by = by % 128
    return pltpu.roll(value, by, 1) if by else value


def quarters(edge):
    size = edge.shape[0] // 4
    return sum(rolled(edge[q * size : (q + 1) * size], 4 * q) for q in range(4))


def spread_edge(edge, by, packed):
    if not packed:
        return rolled(edge, by)
    return jnp.concatenate([rolled(edge, by - 4 * q) for q in range(4)], axis=0)


def halved(tile, low):
    size = tile.shape[0] // 2
    lane = lanes_of((size, 128))
    upper, lower = tile[:size], rolled(tile[size:], 64)
    return jnp.where(lane < 64, upper, lower) if low else jnp.where(lane < 64, lower, upper)


def beside(tile, edges, extent, packed):
    low_edge, high_edge, at = edges
    lane = lanes_of(tile.shape) & (extent - 1)
    before = jnp.where(lane == 0, spread_edge(low_edge, -at, packed), rolled(tile, 1))
    after = jnp.where(lane == extent - 1, spread_edge(high_edge, extent - 1 - at, packed), rolled(tile, -1))
    return before, after


def sided(edge):
    high = lax.axis_index("gx") == 0
    zero = jnp.zeros_like(edge)
    return jnp.where(high, zero, edge), jnp.where(high, edge, zero)


def moved_rows(pair, stride):
    lane = lanes_of(pair[0].shape)
    down = [rolled(tile, stride) for tile in pair]
    up = [rolled(tile, -stride) for tile in pair]
    low = lane < stride
    high = lane < 128 - stride
    zero = jnp.zeros_like(pair[0])
    before = (jnp.where(low, zero, down[0]), jnp.where(low, down[0], down[1]))
    after = (jnp.where(high, up[0], up[1]), jnp.where(high, up[1], zero))
    return before, after


def put_rows(windows, pair, begin, plane, size):
    before, after = moved_rows(pair, 32)
    for ky, tiles in enumerate((before, pair, after)):
        for g, tile in enumerate(tiles):
            lane = plane * 256 + g * 128
            windows[begin + ky * size : begin + (ky + 1) * size, lane : lane + 128] = tile


def moved_half(tile, stride):
    lane = lanes_of(tile.shape) & 63
    zero = jnp.zeros_like(tile)
    before = jnp.where(lane < stride, zero, rolled(tile, stride))
    after = jnp.where(lane < 64 - stride, rolled(tile, -stride), zero)
    return before, after


def inbox_values(inbox):
    low, high, across, across_low, across_high = [ref[...] for ref in inbox]
    return low, high, sided(across), sided(across_low), sided(across_high)


def fine_planes(read, inbox, planes):
    low, high, across, across_low, across_high = inbox_values(inbox)
    for p in range(planes + 2):
        if p == 0:
            pair, edge, at = (low[:, :128], low[:, 128:]), across_low, 2 * (planes - 1)
        elif p == planes + 1:
            pair, edge, at = (high[:, :128], high[:, 128:]), across_high, 0
        else:
            pair, edge, at = read(p - 1), across, 2 * (p - 1)
        sides = [beside(tile, (*edge, at + g), 32, False) for g, tile in enumerate(pair)]
        yield p, ((sides[0][0], sides[1][0]), pair, (sides[0][1], sides[1][1]))


def coarse_tiles(field, inbox, tiles):
    low, high, across, across_low, across_high = inbox_values(inbox)
    low = jnp.concatenate([low, rolled(low, 64)], axis=0)
    high = jnp.concatenate([high, rolled(high, 64)], axis=0)
    half = lanes_of(low.shape) < 64
    for t in range(tiles):
        tile = field[:, t * 128 : (t + 1) * 128]
        sides = list(beside(tile, (*across, t % 4), 16, True))
        if t == 0:
            sides_low = beside(low, (*across_low, (tiles - 1) % 4), 16, True)
            tile = jnp.where(half, low, tile)
            sides = [jnp.where(half, a, b) for a, b in zip(sides_low, sides)]
        if t == tiles - 1:
            sides_high = beside(high, (*across_high, 0), 16, True)
            tile = jnp.where(half, tile, high)
            sides = [jnp.where(half, b, a) for a, b in zip(sides_high, sides)]
        yield t, (sides[0], tile, sides[1])


def column(row, size):
    wide = jnp.broadcast_to(row, (size, size))
    eye = rows_of((size, size)) == lanes_of((size, size))
    return jnp.sum(jnp.where(eye, wide, 0.0), axis=1, keepdims=True)


def joined_thirds(terms, tiles):
    half = None
    low = [rolled(terms(0, t), 64) for t in range(tiles)]
    high = [rolled(terms(2, t), 64) for t in range(tiles)]
    out = []
    for t in range(tiles):
        if half is None:
            half = lanes_of(low[0].shape) < 64
        before, after = low[max(t - 1, 0)], high[min(t + 1, tiles - 1)]
        out.append(terms(1, t) + jnp.where(half, before + high[t], low[t] + after))
    return out


def block_kernel(setting, *refs):
    groups, groups_a, cuts = setting
    inputs = refs[:6]
    features, grad_in, sum_a, sum_b = refs[6:10]
    volume, w_a, b_a, w_b, b_b, cot = refs[10:16]
    (
        stage, own_a, windows_a, sums_a, slope_a, halves, pooled, windows_b, sums_b,
        cot_sent, cot_came, cot_here, grad_b, lines_b, sums_gb, grads_a, lines_a, sums_ga,
        feat_sent, feat_came, mat_a, mat_b, mat_ga, mat_gb, near, far, acc_a, acc_b,
    ) = refs[16:44]
    rest = list(refs[44:])
    inboxes = [[rest.pop(0) for _ in range(5)] for _ in range(4)]
    edges = [rest.pop(0) for _ in range(4)]
    ends_b, ends_gb = [[rest.pop(0), rest.pop(0)] for _ in range(2)]
    count = len(groups)
    takes = lambda n: [rest.pop(0) for _ in range(n)]
    send_a, recv_a = takes(1), takes(2)
    send_b, recv_b, send_c, recv_c = [takes(count) for _ in range(4)]
    sems_halo, sems_cot, sems_feat, sems_a, sems_b, sems_c = [takes(2) for _ in range(6)]
    (sems_in,) = rest
    f32, bf16 = jnp.float32, jnp.bfloat16
    c1, rows, planes, width = volume.shape
    c2, c3 = w_a.shape[2], w_b.shape[2]
    tiles = planes // 4 + 1
    me, members = lax.axis_index("gz"), lax.axis_size("gz")
    whole = [bit for group in groups for bit in group]
    line = [bit for bit in whole if bit[0] == "gz"]

    apart = me < members
    barrier = pltpu.get_barrier_semaphore()
    for mask in range(1, 2 ** len(whole)):
        pl.semaphore_signal(barrier, inc=1, device_id=by_parts(whole, mask), device_id_type=MESH)
    loads = {
        at: pltpu.make_async_copy(inputs[at], refs[10 + at], sems_in.at[at]) for at in range(1, len(inputs))
    }
    parts = 4
    share = c1 // parts
    loads_v = [
        pltpu.make_async_copy(
            inputs[0].at[i * share : (i + 1) * share],
            volume.at[i * share : (i + 1) * share],
            sems_in.at[0],
        )
        for i in range(parts)
    ]
    for load in loads_v:
        load.start()
    for at in (5, 1, 3, 2, 4):
        loads[at].start()

    @pl.when(me == 0)
    def _():
        for inbox in inboxes:
            for box in (inbox[0], inbox[3]):
                box[...] = jnp.zeros_like(box)

    @pl.when(me == members - 1)
    def _():
        for inbox in inboxes:
            for box in (inbox[1], inbox[4]):
                box[...] = jnp.zeros_like(box)

    pltpu.make_async_copy(inputs[0], volume, sems_in.at[0]).wait()
    for g in range(2):
        for i in range(4):
            part = volume[:, 4 * g + i].astype(f32).reshape(c1 * planes, width)
            stage[:, width * i : width * (i + 1)] = part
        for z in range(planes):
            tile = stage[pl.ds(z, c1, stride=planes), :]
            own_a[:, z * 256 + g * 128 : z * 256 + (g + 1) * 128] = tile.astype(bf16)

    def read_a(z):
        return tuple(own_a[:, z * 256 + g * 128 : z * 256 + (g + 1) * 128] for g in range(2))

    edges[0][...] = gathered_edge([tile.astype(f32) for z in range(planes) for tile in read_a(z)], 32, 32).astype(bf16)
    pl.semaphore_wait(barrier, 2 ** len(whole) - 1)

    border_a = Border(own_a.at[:, :256], own_a.at[:, (planes - 1) * 256 :], edges[0], inboxes[0], sems_halo, 0)
    border_a.start()

    def exchange(sent, came, sems):
        size = sent.shape[0] // members
        for mask in range(1, members):
            begin = pl.multiple_of(own_rank(line, mask) * size, 16)
            remote(
                sent.at[pl.ds(begin, size)],
                came.at[pl.ds(pl.multiple_of(me * size, 16), size)],
                sems,
                0,
                by_parts(line, mask),
            ).start()
        here = pl.ds(pl.multiple_of(me * size, 16), size)
        came[here] = sent[here]
        most = (members - 1) * size
        return remote(sent.at[:most], came.at[:most], sems, 0, by_parts(line, 1))

    for at in range(1, 5):
        loads[at].wait()

    high = lax.axis_index("gx") == 0
    eye = ones_where(rows_of((c2, c2)) == lanes_of((c2, c2)))
    eye_b = ones_where(rows_of((c3, c3)) == lanes_of((c3, c3)))
    for kz in range(3):
        block = w_a[:].reshape(9, 3, c1, c2)[:, kz].reshape(3, 3 * c1, c2)
        block = jnp.concatenate([block[1], *[jnp.where(high, a, b) for a, b in ((block[0], block[2]), (block[2], block[0]))]], axis=0)
        mat_a[kz * c2 : (kz + 1) * c2] = dot_rows(eye, block).astype(bf16)
        block = w_b[:].reshape(9, 3, c2, c3)[:, kz].reshape(9 * c2, c3)
        mat_b[kz * c3 : (kz + 1) * c3] = dot_rows(eye_b, block).astype(bf16)
        for ky in range(3):
            for kx in range(3):
                tap = ((2 - kx) * 3 + 2 - ky) * 3 + 2 - kz
                at = kz * 3 + ky
                mat_ga[at * c1 : (at + 1) * c1, kx * c2 : (kx + 1) * c2] = w_a[tap]
                mat_gb[at * c2 : (at + 1) * c2, kx * c3 : (kx + 1) * c3] = w_b[tap]
    col_a, col_b = column(b_a[...], c2), column(b_b[...], c3)
    r, l = rows_of(far.shape), lanes_of(far.shape)
    far[...] = ones_where(((r >> 3) & 3 == l >> 7) & (((r >> 5) << 3) + (r & 7) == l & 127))
    loads[5].wait()
    half_rows = rows // 2
    stage[...] = cot[...].astype(f32)
    spaced = [stage[pl.ds(y, c3, stride=half_rows), :].astype(bf16) for y in range(half_rows)]
    cot_sent[...] = dot_rows(far[...], jnp.concatenate(spaced, axis=1)).astype(bf16)
    cot_flying = exchange(cot_sent, cot_came, sems_cot)
    deep = 3 * c1
    lane = lanes_of((c1, 128)) & 31

    @pl.when(apart)
    def _():
        for p in range(1, planes + 1):
            pair = read_a(p - 1)
            zero = jnp.zeros_like(pair[0])
            before = [jnp.where(lane == 0, zero, rolled(tile, 1)) for tile in pair]
            after = [jnp.where(lane == 31, zero, rolled(tile, -1)) for tile in pair]
            plain = [jnp.where(high, a, b) for a, b in zip(before, after)]
            met = [jnp.where(high, b, a) for a, b in zip(before, after)]
            put_rows(windows_a, pair, 0, p, c1)
            put_rows(windows_a, plain, deep, p, c1)
            for g in range(2):
                windows_a[2 * deep + c1 : 2 * deep + 2 * c1, p * 256 + g * 128 : p * 256 + (g + 1) * 128] = met[g]
            if p % 2 == 0:
                here = slice((p - 1) * 256, (p + 1) * 256)
                sums_a[:, here] = dot(mat_a[:, : 2 * deep], windows_a[: 2 * deep, here])

    r, l = rows_of((512, 128)), lanes_of((512, 128))
    pool = ones_where(
        (r >> 8 == l >> 6) & ((r >> 6) & 3 == (l >> 4) & 3) & ((r & 31) >> 1 == l & 15)
    )
    halves[...] = jnp.zeros_like(halves)
    for kz in range(3):
        for p in range(planes + 2):
            if not 0 <= p + kz - 2 < planes:
                grads_a[kz * c2 : (kz + 1) * c2, p * 256 : (p + 1) * 256] = jnp.zeros((c2, 256), bf16)
    acc_a[...] = jnp.zeros_like(acc_a)
    border_a.wait()

    @pl.when(apart)
    def _():
        boxes = [ref[...] for ref in inboxes[0]]
        turned = [jnp.where(high, rolled(edge, 31), edge) for edge in boxes[2:]]
        for p in range(planes + 2):
            if 0 < p <= planes:
                edge, at = turned[0], 2 * (p - 1)
                pair = [
                    windows_a[2 * deep + c1 : 2 * deep + 2 * c1, p * 256 + g * 128 : p * 256 + (g + 1) * 128]
                    for g in range(2)
                ]
            else:
                edge, at = (turned[2], 0) if p else (turned[1], 2 * (planes - 1))
                tiles_p = [boxes[1 if p else 0][:, g * 128 : (g + 1) * 128] for g in range(2)]
                zero = jnp.zeros_like(tiles_p[0])
                before = [jnp.where(lane == 0, zero, rolled(tile, 1)) for tile in tiles_p]
                after = [jnp.where(lane == 31, zero, rolled(tile, -1)) for tile in tiles_p]
                put_rows(windows_a, tiles_p, 0, p, c1)
                put_rows(windows_a, [jnp.where(high, a, b) for a, b in zip(before, after)], deep, p, c1)
                pair = [jnp.where(high, b, a) for a, b in zip(before, after)]
            side = jnp.where(high, 31, 0)
            pair = [jnp.where(lane == side, rolled(edge, -at - g), tile) for g, tile in enumerate(pair)]
            put_rows(windows_a, pair, 2 * deep, p, c1)
            here = slice((p - 1) * 256, (p + 1) * 256)
            if p == 0 or p == planes + 1:
                here = slice(p * 256, (p + 1) * 256)
                sums_a[:, here] = dot(mat_a[...], windows_a[:, here])
            elif p % 2 == 0:
                sums_a[:, here] = sums_a[:, here] + dot(mat_a[:, 2 * deep :], windows_a[2 * deep :, here])

    for z in range(planes):
        value = (
            sums_a[:c2, z * 256 : (z + 1) * 256]
            + sums_a[c2 : 2 * c2, (z + 1) * 256 : (z + 2) * 256]
            + sums_a[2 * c2 :, (z + 2) * 256 : (z + 3) * 256]
            + col_a
        )
        sigma = jax.nn.sigmoid(value)
        active = value * sigma
        slope_a[:, z * 256 : (z + 1) * 256] = (sigma + active * (1.0 - sigma)) * 0.125
        if z % 2:
            active = active + kept
            pz = z // 2 + 1
            upper = active.astype(bf16)
            lower = (active - upper.astype(f32)).astype(bf16)
            at, lane = pz // 2 * c2, pz % 2 * 256
            halves[at : at + c2, lane : lane + 256] = upper
            halves[tiles * c2 + at : tiles * c2 + at + c2, lane : lane + 256] = lower
        else:
            kept = active
    both = dot(halves[...], pool)
    both = (both[: tiles * c2] + both[tiles * c2 :]) * 0.125
    for t in range(tiles):
        pooled[:, t * 128 : (t + 1) * 128] = both[t * c2 : (t + 1) * c2].astype(bf16)

    def coarse_border(field, edge, ends, inbox, at):
        parts = [field[:, t * 128 : (t + 1) * 128].astype(f32) for t in range(tiles)]
        edge[...] = quarters(gathered_edge(parts, 16, 4)).astype(bf16)
        ends[0][...] = halved(parts[0], False).astype(bf16)
        ends[1][...] = halved(parts[-1], True).astype(bf16)
        return Border(ends[0], ends[1], edge, inbox, sems_halo, at)

    border_b = coarse_border(pooled, edges[1], ends_b, inboxes[1], 5)
    border_b.start()
    cot_flying.wait()
    r, l = rows_of(near.shape), lanes_of(near.shape)
    near[...] = ones_where(
        ((r & 7) + 1 == l >> 6) & ((r >> 3) & 3 == (l >> 4) & 3) & (r >> 5 == l & 15)
    )
    came = jnp.transpose(cot_came[...].astype(f32)).astype(bf16)
    cot_here[...] = dot(came, near[...])
    border_b.wait()

    @pl.when(apart)
    def _():
        for t, thirds in coarse_tiles(pooled, inboxes[1], tiles):
            for kx, tile in enumerate(thirds):
                before, after = moved_half(tile, 16)
                for ky, value in enumerate((before, tile, after)):
                    at = (kx * 3 + ky) * c2
                    windows_b[at : at + c2, t * 128 : (t + 1) * 128] = value.astype(bf16)
            if t % 2 or t == tiles - 1:
                here = slice(t // 2 * 256, (t + 1) * 128)
                sums_b[:, here] = dot(mat_b[...], windows_b[:, here])

    joined = joined_thirds(lambda k, t: sums_b[k * c3 : (k + 1) * c3, t * 128 : (t + 1) * 128], tiles)
    feats = []
    for t, value in enumerate(joined):
        value = value + col_b
        sigma = jax.nn.sigmoid(value)
        active = value * sigma
        feats.append(active.astype(bf16))
        slope = sigma + active * (1.0 - sigma)
        grad = cot_here[:, t * 128 : (t + 1) * 128] * slope
        grad_b[c3 : 2 * c3, t * 128 : (t + 1) * 128] = grad.astype(bf16)
    own_gb = grad_b.at[c3 : 2 * c3]
    border_gb = coarse_border(own_gb, edges[2], ends_gb, inboxes[2], 10)
    border_gb.start()

    half = lanes_of((c3, 128)) < 64
    turned = [rolled(own_gb[:, t * 128 : (t + 1) * 128].astype(f32), 64) for t in range(tiles)]
    zero = jnp.zeros_like(turned[0])
    for t in range(tiles):
        later = turned[t + 1] if t + 1 < tiles else zero
        earlier = turned[t - 1] if t else zero
        here = slice(t * 128, (t + 1) * 128)
        grad_b[:c3, here] = jnp.where(half, turned[t], later).astype(bf16)
        grad_b[2 * c3 :, here] = jnp.where(half, earlier, turned[t]).astype(bf16)
    top = 27 * c2

    def sum_terms(first, last):
        terms = dot_rows(windows_b[first * c2 : last * c2], grad_b[...])
        for at in range(first, last):
            for kz in range(3):
                tap = at * 3 + kz
                acc_b[tap * c2 : (tap + 1) * c2] = terms[
                    (at - first) * c2 : (at - first + 1) * c2, kz * c3 : (kz + 1) * c3
                ]

    cut = cuts[0]
    early = -(-cut // (3 * c2))
    pl.when(apart)(functools.partial(sum_terms, 0, early))
    total_b = Reduction(groups, False, acc_b.at[:cut], sum_b.at[:cut], send_b, recv_b, sems_b)
    total_b.start()
    pl.when(apart)(functools.partial(sum_terms, early, 9))
    acc_b[top:] = jnp.zeros((acc_b.shape[0] - top, c3), f32)
    acc_b[top : top + 8] = dot_rows(jnp.ones((8, tiles * 128), bf16), own_gb[...])
    total_c = Reduction(groups, False, acc_b.at[cut:], sum_b.at[cut:], send_c, recv_c, sems_c)
    total_c.start()
    feat_sent[...] = dot_rows(near[...], jnp.concatenate(feats, axis=1)).astype(bf16)
    feat_flying = exchange(feat_sent, feat_came, sems_feat)
    total_b.step()
    total_c.step()
    border_gb.wait()

    @pl.when(apart)
    def _():
        for t, thirds in coarse_tiles(own_gb, inboxes[2], tiles):
            for kx, tile in enumerate(thirds):
                lines_b[kx * c3 : (kx + 1) * c3, t * 128 : (t + 1) * 128] = tile.astype(bf16)
            if t % 2 or t == tiles - 1:
                here = slice(t // 2 * 256, (t + 1) * 128)
                sums_gb[:, here] = dot(mat_gb[...], lines_b[:, here])

    by_row = [
        joined_thirds(
            lambda k, t: sums_gb[(k * 3 + ky) * c2 : (k * 3 + ky + 1) * c2, t * 128 : (t + 1) * 128], tiles
        )
        for ky in range(3)
    ]
    small = []
    for t in range(tiles):
        value = by_row[1][t] + moved_half(by_row[0][t], 16)[0] + moved_half(by_row[2][t], 16)[1]
        small.append(value.astype(bf16))
    spread = dot_rows(jnp.concatenate(small, axis=0), pool)
    for z in range(planes):
        pz = z // 2 + 1
        large = spread[pz // 2 * c2 : (pz // 2 + 1) * c2, pz % 2 * 256 : (pz % 2 + 1) * 256]
        grad = (large * slope_a[:, z * 256 : (z + 1) * 256]).astype(bf16)
        for kz in range(3):
            grads_a[kz * c2 : (kz + 1) * c2, (z + kz) * 256 : (z + kz + 1) * 256] = grad

    own_ga = grads_a.at[c2 : 2 * c2]

    def read_ga(z):
        return tuple(
            own_ga[:, (z + 1) * 256 + g * 128 : (z + 1) * 256 + (g + 1) * 128] for g in range(2)
        )

    edges[3][...] = gathered_edge([tile.astype(f32) for z in range(planes) for tile in read_ga(z)], 32, 32).astype(bf16)
    border_ga = Border(
        own_ga.at[:, 256:512], own_ga.at[:, planes * 256 : (planes + 1) * 256], edges[3], inboxes[3], sems_halo, 15
    )
    border_ga.start()

    @pl.when(apart)
    def _():
        top_a = 9 * c1 + 9 * c1 // 2
        terms = dot_rows(windows_a[...], grads_a[...])
        near_x, far_x = terms[deep : 2 * deep], terms[2 * deep :]
        terms = jnp.concatenate(
            [jnp.where(high, near_x, far_x), terms[:deep], jnp.where(high, far_x, near_x)], axis=0
        )
        full = 9 * c1
        acc_a[:full] = terms[:, : 2 * c2]
        acc_a[full:top_a, :c2] = terms[: full // 2, 2 * c2 :]
        acc_a[full:top_a, c2:] = terms[full // 2 :, 2 * c2 :]
        acc_a[top_a : top_a + 8, :c2] = dot_rows(
            jnp.ones((8, planes * 256), bf16), own_ga[:, 256 : (planes + 1) * 256]
        )

    total_a = Reduction(groups_a, True, acc_a, sum_a, send_a, recv_a, sems_a)
    total_a.start()
    total_b.step()
    total_c.step()
    border_ga.wait()

    @pl.when(apart)
    def _():
        for p, thirds in fine_planes(read_ga, inboxes[3], planes):
            for kx, pair in enumerate(thirds):
                for g, tile in enumerate(pair):
                    at = p * 256 + g * 128
                    lines_a[kx * c2 : (kx + 1) * c2, at : at + 128] = tile.astype(bf16)
            if p % 2:
                here = slice((p - 1) * 256, (p + 1) * 256)
                sums_ga[:, here] = dot(mat_ga[...], lines_a[:, here])

    total_a.step()
    total_b.step()
    total_c.step()
    feat_flying.wait()
    came = jnp.transpose(feat_came[...].astype(f32)).astype(bf16)
    ours = dot(came, far[...])
    for y in range(half_rows):
        stage[pl.ds(y, c3, stride=half_rows), :] = ours[:, y * 128 : (y + 1) * 128]
    features[...] = stage[...].astype(bf16)
    results = []
    for z in range(planes):
        by_row = []
        for ky in range(3):
            value = None
            for kz in range(3):
                at = (kz * 3 + ky) * c1
                term = sums_ga[at : at + c1, (z + kz) * 256 : (z + kz + 1) * 256]
                value = term if value is None else value + term
            by_row.append((value[:, :128], value[:, 128:]))
        before, after = moved_rows(by_row[0], 32)[0], moved_rows(by_row[2], 32)[1]
        results.append([by_row[1][g] + before[g] + after[g] for g in range(2)])
    for g in range(2):
        for z in range(planes):
            stage[pl.ds(z, c1, stride=planes), :] = results[z][g]
        for i in range(4):
            part = stage[:, width * i : width * (i + 1)].astype(bf16)
            grad_in[:, 4 * g + i] = part.reshape(c1, planes, width)

    while min(total.stage - total.stages for total in (total_a, total_b, total_c)) < 0:
        for total in (total_b, total_c, total_a):
            if total.stage < total.stages:
                total.step()


def last_kernel(scales, *refs):
    feat, grad, sum_a, sum_b, out_feat, out_grad, out_wa, out_ba, out_wb, out_bb = refs[:10]
    wa, ba, wb, bb, sems_out = refs[10:]
    f32 = jnp.float32
    scale_a, scale_b = scales
    places = ((grad, out_grad), (feat, out_feat), (wb, out_wb), (bb, out_bb), (wa, out_wa), (ba, out_ba))
    stores = [
        pltpu.make_async_copy(source, target, sems_out.at[at]) for at, (source, target) in enumerate(places)
    ]
    stores[0].start()
    stores[1].start()
    top = wb.shape[0]
    wb[...] = sum_b[:top].astype(f32) * scale_b
    stores[2].start()
    bb[...] = sum_b[top : top + 16].astype(f32)[:1] * scale_b
    stores[3].start()
    c1, c2 = wa.shape[1:]
    deep = 9 * c1
    pairs = sum_a[:deep].astype(f32) * scale_a
    tail = sum_a[deep : deep + deep // 2].astype(f32) * scale_a
    thirds = jnp.concatenate([tail[:, :c2], tail[:, c2:]], axis=0)
    for at in range(9):
        here = slice(at * c1, (at + 1) * c1)
        wa[at * 3] = pairs[here, :c2]
        wa[at * 3 + 1] = pairs[here, c2:]
        wa[at * 3 + 2] = thirds[here]
    stores[4].start()
    top_a = deep + deep // 2
    ba[...] = sum_a[top_a : top_a + 16].astype(f32)[:1, :c2] * scale_a
    stores[5].start()
    for store in stores:
        store.wait()


def all_groups():
    cut = {axis: [2**i for i in range(lax.axis_size(axis).bit_length() - 1)] for axis in ("gz", "gx")}
    line = [("gz", bit) for bit in cut["gz"]]
    return [line[:1], [("gx", bit) for bit in cut["gx"]] + line[1:2], line[2:]]


def on_blocks(volume, weight_a, bias_a, weight_b, bias_b, cotangent, scales):
    f32, bf16 = jnp.float32, jnp.bfloat16
    c1, width, rows, planes = volume.shape
    c2, c3 = weight_b.shape[3:]
    members = lax.axis_size("gz")
    groups = all_groups()
    tiles = planes // 4 + 1
    long, short = (planes + 2) * 256, tiles * 128
    cells = planes * 256
    rows_a, rows_b = 512, 27 * c2 + 64
    fewer = cells // 8

    def buffers(total, groups, exchanged):
        sends, recvs = [], []
        size = total
        for at, group in enumerate(groups):
            n = 2 ** len(group)
            if exchanged and at == len(groups) - 1:
                recvs.append(pltpu.VMEM((n, size, 128), bf16))
                continue
            sends.append(pltpu.VMEM((size, 128), bf16))
            size //= n
            recvs.append(pltpu.VMEM((n - 1, size, 128), bf16))
        return sends + recvs

    inboxes = []
    for size, plane, edge in ((c1, 256, c1), (c2 // 2, 128, c2 // 4), (c3 // 2, 128, c3 // 4), (c2, 256, c2)):
        inboxes += [pltpu.VMEM((size, plane), bf16)] * 2 + [pltpu.VMEM((edge, 128), bf16)] * 3
    groups_a = [groups[0] + groups[1], groups[2]]
    by_level = [2 ** len(group) for group in groups]
    count_a = len(groups_a) + by_level[1]
    count_b = len(groups) + by_level[2] * by_level[1]
    cuts = (1024, rows_b - 1024)
    passed = [
        ((c3 * rows // 2, 128), bf16),
        ((c1, rows, planes, width), bf16),
        ((rows_a, 128), bf16),
        ((rows_b, 128), bf16),
    ]
    operands = (
        jnp.transpose(volume, (0, 2, 3, 1)),
        weight_a.reshape(27, c1, c2),
        bias_a[None],
        weight_b.reshape(27, c2, c3),
        bias_b[None],
        cotangent.reshape(c3 * rows // 2, 128),
    )
    anywhere, inside = pl.BlockSpec(memory_space=pl.ANY), pl.BlockSpec(memory_space=pltpu.VMEM)
    middle = pl.pallas_call(
        functools.partial(block_kernel, (groups, groups_a, cuts)),
        out_shape=[pltpu.VMEM(shape, dtype) for shape, dtype in passed],
        in_specs=[anywhere] * len(operands),
        out_specs=[inside] * len(passed),
        scratch_shapes=[
            *[pltpu.VMEM(x.shape, x.dtype) for x in operands],
            pltpu.VMEM((c1 * planes, 128), f32),
            pltpu.VMEM((c1, cells), bf16),
            pltpu.VMEM((9 * c1, long), bf16),
            pltpu.VMEM((3 * c2, long), f32),
            pltpu.VMEM((c2, cells), f32),
            pltpu.VMEM((2 * tiles * c2, 512), bf16),
            pltpu.VMEM((c2, short), bf16),
            pltpu.VMEM((9 * c2, short), bf16),
            pltpu.VMEM((3 * c3, short), f32),
            pltpu.VMEM((fewer, c3), bf16),
            pltpu.VMEM((fewer, c3), bf16),
            pltpu.VMEM((c3, short), f32),
            pltpu.VMEM((3 * c3, short), bf16),
            pltpu.VMEM((3 * c3, short), bf16),
            pltpu.VMEM((9 * c2, short), f32),
            pltpu.VMEM((3 * c2, long), bf16),
            pltpu.VMEM((3 * c2, long), bf16),
            pltpu.VMEM((9 * c1, long), f32),
            pltpu.VMEM((fewer, c3), bf16),
            pltpu.VMEM((fewer, c3), bf16),
            pltpu.VMEM((3 * c2, 9 * c1), bf16),
            pltpu.VMEM((3 * c3, 9 * c2), bf16),
            pltpu.VMEM((9 * c1, 3 * c2), bf16),
            pltpu.VMEM((9 * c2, 3 * c3), bf16),
            pltpu.VMEM((fewer, short), bf16),
            pltpu.VMEM((fewer, fewer), bf16),
            pltpu.VMEM((rows_a, 128), f32),
            pltpu.VMEM((rows_b, 128), f32),
            *inboxes,
            *[pltpu.VMEM((size, 128), bf16) for size in (c1, c2 // 4, c3 // 4, c2)],
            *[pltpu.VMEM((size // 2, 128), bf16) for size in (c2, c2, c3, c3)],
            *buffers(rows_a, groups_a, True),
            *buffers(cuts[0], groups, False),
            *buffers(cuts[1], groups, False),
            *[pltpu.SemaphoreType.DMA((20,))] * 2,
            *[pltpu.SemaphoreType.DMA((1,))] * 4,
            *[pltpu.SemaphoreType.DMA((n,)) for n in (len(groups_a) + 1, count_a)],
            *[pltpu.SemaphoreType.DMA((n,)) for n in (len(groups) + 1, count_b)] * 2,
            pltpu.SemaphoreType.DMA((len(operands),)),
        ],
        compiler_params=pltpu.CompilerParams(
            collective_id=2, has_side_effects=True, vmem_limit_bytes=60 * 2**20
        ),
    )(*operands)
    outs = [
        *passed[:2],
        ((27, c1, c2), f32),
        ((1, c2), f32),
        ((27 * c2, c3), f32),
        ((1, c3), f32),
    ]
    features, grad_in, sum_wa, sum_ba, sum_wb, sum_bb = pl.pallas_call(
        functools.partial(last_kernel, scales),
        out_shape=[jax.ShapeDtypeStruct(shape, dtype) for shape, dtype in outs],
        in_specs=[inside] * len(passed),
        out_specs=[anywhere] * len(outs),
        scratch_shapes=[
            *[pltpu.VMEM(shape, dtype) for shape, dtype in outs[2:]],
            pltpu.SemaphoreType.DMA((len(outs),)),
        ],
    )(*[pltpu.with_memory_space_constraint(x, pltpu.VMEM) for x in middle])
    return (
        features.reshape(cotangent.shape),
        jnp.transpose(grad_in, (0, 3, 1, 2)),
        sum_wa.reshape(weight_a.shape),
        sum_ba.reshape(c2),
        sum_wb.reshape(weight_b.shape),
        sum_bb.reshape(c3),
    )


def fits_blocks(volume, weight_b):
    c1, width, rows, planes = volume.shape
    sizes = {axis: lax.axis_size(axis) for axis in ("gx", "gy", "gz")}
    return (
        sizes == {"gx": 2, "gy": 1, "gz": planes}
        and (width, rows, planes) == (32, 8, 16)
        and (c1, *weight_b.shape[3:]) == (32, 64, 128)
    )


def on_device(volume, weight_a, bias_a, weight_b, bias_b, cotangent):
    f32, bf16 = jnp.float32, jnp.bfloat16
    count = lax.axis_size("gz")
    devices_all = lax.axis_size("gx") * lax.axis_size("gy") * count
    c1, nx, rows, nz = volume.shape
    cells = nx * rows * nz
    scale_a = 1.0 / math.sqrt(cells * devices_all)
    scale_b = 1.0 / math.sqrt(cells * devices_all // 8)
    c2, c3 = weight_b.shape[3:]
    if fits_blocks(volume, weight_b):
        return on_blocks(volume, weight_a, bias_a, weight_b, bias_b, cotangent, (scale_a, scale_b))
    planes, depth = nx // count, nz * count
    fine = (planes, rows, depth)
    coarse = (planes // 2, rows // 2, depth // 2)
    fewer = cells // 8
    pool = (jnp.arange(depth)[:, None] // 2 == jnp.arange(depth // 2)[None]).astype(f32)
    work_a = 2 * 27 * c1 * c2 * cells
    work_b = 2 * 27 * c2 * c3 * fewer

    slab = lax.all_to_all(volume, "gz", split_axis=1, concat_axis=3, tiled=True).reshape(c1, cells)
    if lax.axis_size("gy") == 1:
        features, grad_slab, sum_wa, sum_ba, sum_wb, sum_bb = between_exchanges(
            fine,
            coarse,
            (scale_a, scale_b),
            slab,
            weight_a,
            bias_a,
            weight_b,
            bias_b,
            cotangent.reshape(c3, fewer),
            pool,
        )
    else:
        wide_a = widened(slab, *fine)
        before_a, pooled = local_kernel(
            functools.partial(forward_a_kernel, fine),
            [((c2, cells), f32), ((c2, fewer), bf16)],
            (27 * c1, cells),
            work_a,
            wide_a,
            outward(weight_a),
            bias_a[:, None],
            pool,
        )
        wide_b = widened(pooled, *coarse)
        features, grad_b, part_wb, part_bb = local_kernel(
            functools.partial(middle_kernel, coarse),
            [((c3, fewer), bf16), ((c3, fewer), bf16), ((27 * c2, c3), f32), ((8, c3), f32)],
            (27 * c2, fewer),
            2 * work_b,
            wide_b,
            outward(weight_b),
            bias_b[:, None],
            cotangent.reshape(c3, fewer),
        )
        (grad_a,) = local_kernel(
            functools.partial(backward_b_kernel, coarse, fine),
            [((c2, cells), bf16)],
            (27 * c3, fewer),
            work_b,
            widened(grad_b, *coarse),
            inward(weight_b),
            before_a,
            pool.T.astype(bf16),
        )
        part_wa, part_ba = local_kernel(
            functools.partial(weight_a_kernel, fine),
            [((27 * c1, c2), f32), ((8, c2), f32)],
            (27 * c1, cells),
            work_a,
            wide_a,
            grad_a,
        )
        (grad_slab,) = local_kernel(
            functools.partial(backward_a_kernel, fine),
            [((c1, cells), bf16)],
            (27 * c2, cells),
            work_a,
            widened(grad_a, *fine),
            inward(weight_a),
        )
        sum_wa, sum_ba, sum_wb, sum_bb = summed_grads(
            part_wa, part_ba, part_wb, part_bb, (scale_a, scale_b)
        )
    grad_input = lax.all_to_all(
        grad_slab.reshape(c1, planes, rows, depth), "gz", split_axis=3, concat_axis=1, tiled=True
    )
    return (
        features.reshape(cotangent.shape),
        grad_input,
        sum_wa.reshape(weight_a.shape),
        sum_ba.reshape(c2),
        sum_wb.reshape(weight_b.shape),
        sum_bb.reshape(c3),
    )


def solution(mesh):
    return jax.shard_map(
        on_device,
        mesh=mesh,
        in_specs=(P(None, "gx", "gy", "gz"), P(), P(), P(), P(), P(None, ("gx", "gz"), "gy", None)),
        out_specs=(
            P(None, ("gx", "gz"), "gy", None),
            P(None, "gx", "gy", "gz"),
            P(),
            P(),
            P(),
            P(),
        ),
        check_vma=False,
    )
```

```python
import functools
import math

import jax
import jax.numpy as jnp
from jax import lax
from jax.experimental import pallas as pl
from jax.experimental.pallas import tpu as pltpu
from jax.sharding import PartitionSpec as P

LINE = ("gx", "gz")
MESH = pl.DeviceIdType.MESH


def shared(block, axis, dim, width):
    count = lax.axis_size(axis)
    if count == 1:
        edge = jnp.zeros_like(lax.slice_in_dim(block, 0, width, axis=dim))
        return edge, edge
    forward = [(i, i + 1) for i in range(count - 1)]
    backward = [(target, source) for source, target in forward]
    last = block.shape[dim]
    low = lax.ppermute(lax.slice_in_dim(block, last - width, last, axis=dim), axis, forward)
    high = lax.ppermute(lax.slice_in_dim(block, 0, width, axis=dim), axis, backward)
    return low, high


def widened(flat, planes, rows, depth):
    low, high = shared(flat, LINE, 1, rows * depth)
    if lax.axis_size("gy") == 1:
        gap = jnp.zeros((flat.shape[0], depth), flat.dtype)
        pieces = [gap, low, gap]
        for plane in range(planes):
            pieces += [gap, flat[:, plane * rows * depth : (plane + 1) * rows * depth], gap]
        return jnp.concatenate(pieces + [gap, high, gap], axis=1)
    whole = jnp.concatenate([low, flat, high], axis=1)
    whole = whole.reshape(flat.shape[0], planes + 2, rows, depth)
    low, high = shared(whole, "gy", 2, 1)
    return jnp.concatenate([low, whole, high], axis=2).reshape(flat.shape[0], -1)


def slope_of(value):
    sigma = jax.nn.sigmoid(value)
    return sigma + value * sigma * (1.0 - sigma)


def put_windows(wide_ref, windows, planes, rows, depth):
    wide = wide_ref[...]
    width, extent = wide.shape
    place = lax.broadcasted_iota(jnp.int32, (width, extent), 1) % depth
    loose = wide.astype(jnp.float32)
    before = jnp.where(place == 0, 0.0, pltpu.roll(loose, 1, 1)).astype(jnp.bfloat16)
    after = jnp.where(place == depth - 1, 0.0, pltpu.roll(loose, extent - 1, 1)).astype(jnp.bfloat16)
    size = rows * depth
    for third, moved in enumerate((before, wide, after)):
        for first in range(3):
            for second in range(3):
                at = (first * 9 + second * 3 + third) * width
                for plane in range(planes):
                    begin = ((plane + first) * (rows + 2) + second) * depth
                    windows[at : at + width, plane * size : (plane + 1) * size] = moved[
                        :, begin : begin + size
                    ]


def dot_rows(left, right):
    return lax.dot_general(
        left, right, (((1,), (1,)), ((), ())), preferred_element_type=jnp.float32
    )


def forward_a_kernel(dims, wide_ref, weight_ref, bias_ref, pool_ref, before_ref, pooled_ref, windows):
    planes, rows, depth = dims
    put_windows(wide_ref, windows, *dims)
    before = jnp.dot(weight_ref[...], windows[...], preferred_element_type=jnp.float32)
    before = before + bias_ref[...]
    before_ref[...] = before
    active = before * jax.nn.sigmoid(before)
    size = rows * depth
    for row in range(rows // 2):
        parts = [
            active[:, plane * size + (2 * row + j) * depth : plane * size + (2 * row + j + 1) * depth]
            for plane in range(planes)
            for j in range(2)
        ]
        summed = sum(parts[1:], parts[0])
        paired = jnp.dot(
            summed, pool_ref[...], precision=lax.Precision.HIGHEST, preferred_element_type=jnp.float32
        )
        pooled_ref[:, row * depth // 2 : (row + 1) * depth // 2] = (paired * 0.125).astype(jnp.bfloat16)


def middle_kernel(dims, wide_ref, weight_ref, bias_ref, cot_ref, feat_ref, grad_ref, wb_ref, bb_ref, windows):
    put_windows(wide_ref, windows, *dims)
    before = jnp.dot(weight_ref[...], windows[...], preferred_element_type=jnp.float32)
    before = before + bias_ref[...]
    feat_ref[...] = (before * jax.nn.sigmoid(before)).astype(jnp.bfloat16)
    grad = (cot_ref[...].astype(jnp.float32) * slope_of(before)).astype(jnp.bfloat16)
    grad_ref[...] = grad
    wb_ref[...] = dot_rows(windows[...], grad)
    bb_ref[...] = dot_rows(jnp.ones((8, grad.shape[1]), jnp.bfloat16), grad)


def backward_b_kernel(dims, fine, wide_ref, weight_ref, before_ref, spread_ref, grad_ref, windows):
    put_windows(wide_ref, windows, *dims)
    pooled = jnp.dot(weight_ref[...], windows[...], preferred_element_type=jnp.float32)
    pooled = pooled.astype(jnp.bfloat16)
    planes, rows, depth = fine
    size = rows * depth
    for row in range(rows // 2):
        part = pooled[:, row * depth // 2 : (row + 1) * depth // 2]
        spread = jnp.dot(part, spread_ref[...], preferred_element_type=jnp.float32) * 0.125
        for plane in range(planes):
            for j in range(2):
                begin = plane * size + (2 * row + j) * depth
                slope = slope_of(before_ref[:, begin : begin + depth])
                grad_ref[:, begin : begin + depth] = (spread * slope).astype(jnp.bfloat16)


def weight_a_kernel(dims, wide_ref, grad_ref, wa_ref, ba_ref, windows):
    put_windows(wide_ref, windows, *dims)
    grad = grad_ref[...]
    wa_ref[...] = dot_rows(windows[...], grad)
    ba_ref[...] = dot_rows(jnp.ones((8, grad.shape[1]), jnp.bfloat16), grad)


def backward_a_kernel(dims, wide_ref, weight_ref, out_ref, windows):
    put_windows(wide_ref, windows, *dims)
    out = jnp.dot(weight_ref[...], windows[...], preferred_element_type=jnp.float32)
    out_ref[...] = out.astype(jnp.bfloat16)


def local_kernel(body, outs, windows, flops, *operands):
    moved = sum(x.size * x.dtype.itemsize for x in operands)
    return pl.pallas_call(
        body,
        out_shape=[jax.ShapeDtypeStruct(shape, dtype) for shape, dtype in outs],
        in_specs=[pl.BlockSpec(memory_space=pltpu.VMEM)] * len(operands),
        out_specs=[pl.BlockSpec(memory_space=pltpu.VMEM)] * len(outs),
        scratch_shapes=[pltpu.VMEM(windows, jnp.bfloat16)],
        compiler_params=pltpu.CompilerParams(vmem_limit_bytes=48 * 2**20),
        cost_estimate=pl.CostEstimate(flops=flops, bytes_accessed=moved, transcendentals=0),
    )(*operands)


def partner_of(axis, bit):
    me = lax.axis_index(axis)
    mine = (me // bit) % 2
    return me + bit * (1 - 2 * mine), mine


def sum_kernel(steps, halvings, rows, scales, wa_ref, ba_ref, wb_ref, bb_ref, *rest):
    out_wa, out_ba, out_wb, out_bb, acc, gathered, *scratch = rest
    half, width = wa_ref.shape[0] // 2, wa_ref.shape[1]
    top = wb_ref.shape[0]
    count = len(steps)
    sends = scratch[:count]
    recvs = scratch[count : 2 * count]
    sem_send, sem_recv = scratch[2 * count :]
    partners = [partner_of(axis, bit) for axis, bit in steps]
    barrier = pltpu.get_barrier_semaphore()
    for (axis, _), (partner, _) in zip(steps, partners):
        pl.semaphore_signal(barrier, inc=1, device_id={axis: partner}, device_id_type=MESH)
    acc[:top] = wb_ref[...]
    acc[top : top + half, :width] = wa_ref[:half]
    acc[top : top + half, width:] = wa_ref[half:]
    acc[top + half :] = jnp.zeros((rows - top - half, 128), jnp.float32)
    acc[top + half : top + half + 8, :width] = ba_ref[...]
    acc[top + half + 8 : top + half + 16] = bb_ref[...]
    pl.semaphore_wait(barrier, count)
    offset = 0
    size = rows
    kept = []
    for at, ((axis, _), (partner, mine)) in enumerate(zip(steps, partners)):
        source = acc
        if at < halvings:
            size = size // 2
            away = pl.multiple_of(offset + (1 - mine) * size, 16)
            offset = pl.multiple_of(offset + mine * size, 16)
        else:
            away = offset
        sends[at][...] = source[pl.ds(away, size)].astype(jnp.bfloat16)
        copy = pltpu.make_async_remote_copy(
            src_ref=sends[at],
            dst_ref=recvs[at],
            send_sem=sem_send.at[at],
            recv_sem=sem_recv.at[at],
            device_id={axis: partner},
            device_id_type=MESH,
        )
        copy.start()
        copy.wait()
        if at < halvings:
            acc[pl.ds(offset, size)] = source[pl.ds(offset, size)] + recvs[at][...].astype(jnp.float32)
            kept.append((offset, size))
        else:
            acc[pl.ds(offset, size)] = sends[at][...].astype(jnp.float32) + recvs[at][...].astype(jnp.float32)
    gathered[pl.ds(offset, size)] = acc[pl.ds(offset, size)].astype(jnp.bfloat16)
    for back in range(halvings):
        at = halvings - 1 - back
        begin, extent = kept[at]
        (axis, _), (partner, _) = steps[at], partners[at]
        here = gathered.at[pl.ds(begin, extent)]
        copy = pltpu.make_async_remote_copy(
            src_ref=here,
            dst_ref=here,
            send_sem=sem_send.at[count + back],
            recv_sem=sem_recv.at[count + back],
            device_id={axis: partner},
            device_id_type=MESH,
        )
        copy.start()
        copy.wait()
    scale_a, scale_b = scales
    total = gathered[...].astype(jnp.float32)
    out_wb[...] = total[:top] * scale_b
    out_wa[:half] = total[top : top + half, :width] * scale_a
    out_wa[half:] = total[top : top + half, width:] * scale_a
    out_ba[...] = total[top + half : top + half + 1, :width] * scale_a
    out_bb[...] = total[top + half + 8 : top + half + 9] * scale_b


def summed_grads(wa, ba, wb, bb, scales):
    used = wb.shape[0] + wa.shape[0] // 2 + 16
    rows = used + -used % 128
    cut = {
        axis: [2**i for i in range(lax.axis_size(axis).bit_length() - 1)] for axis in ("gz", "gx", "gy")
    }
    steps = [("gz", bit) for bit in cut["gz"][:1]]
    steps += [("gx", bit) for bit in cut["gx"]] + [("gy", bit) for bit in cut["gy"]]
    steps += [("gz", bit) for bit in cut["gz"][1:]]
    halvings = 0
    sizes = []
    size = rows
    for _ in steps:
        if len(sizes) == halvings and size % 32 == 0:
            size //= 2
            halvings += 1
        sizes.append(size)
    buffers = [pltpu.VMEM((s, 128), jnp.bfloat16) for s in sizes]
    total = len(steps) + halvings
    shapes = [wa.shape, (1, ba.shape[1]), wb.shape, (1, bb.shape[1])]
    return pl.pallas_call(
        functools.partial(sum_kernel, steps, halvings, rows, scales),
        out_shape=[jax.ShapeDtypeStruct(shape, jnp.float32) for shape in shapes],
        in_specs=[pl.BlockSpec(memory_space=pltpu.VMEM)] * 4,
        out_specs=[pl.BlockSpec(memory_space=pltpu.VMEM)] * 4,
        scratch_shapes=[
            pltpu.VMEM((rows, 128), jnp.float32),
            pltpu.VMEM((rows, 128), jnp.bfloat16),
            *buffers,
            *buffers,
            pltpu.SemaphoreType.DMA((total,)),
            pltpu.SemaphoreType.DMA((total,)),
        ],
        compiler_params=pltpu.CompilerParams(collective_id=0, has_side_effects=True),
    )(wa, ba, wb, bb)


def line_ends(axis_sizes):
    across, count = axis_sizes
    total = across * count
    line = lax.axis_index("gx") * count + lax.axis_index("gz")
    after, before = (line + 1) % total, (line + total - 1) % total
    ids = [{"gx": at // count, "gz": at % count} for at in (after, before)]
    return line, total, ids


class Halo:
    def __init__(self, wide, dims, where, sems, at):
        planes, rows, depth = dims
        self.line, self.total, ids = where
        size, stride = rows * depth, (rows + 2) * depth
        spot = lambda plane: wide.at[:, plane * stride + depth : plane * stride + depth + size]
        send, recv = sems
        self.up, self.down = [
            pltpu.make_async_remote_copy(
                src_ref=spot(source),
                dst_ref=spot(target),
                send_sem=send.at[at + i],
                recv_sem=recv.at[at + i],
                device_id=ids[i],
                device_id_type=MESH,
            )
            for i, (source, target) in enumerate(((planes, 0), (1, planes + 1)))
        ]

    def start(self):
        pl.when(self.line < self.total - 1)(self.up.start)
        pl.when(self.line > 0)(self.down.start)

    def wait(self):
        @pl.when(self.line < self.total - 1)
        def _():
            self.up.wait_send()
            self.down.wait_recv()

        @pl.when(self.line > 0)
        def _():
            self.down.wait_send()
            self.up.wait_recv()


class Summing:
    def __init__(self, steps, sizes, acc, gathered, sends, recvs, sems):
        self.steps, self.sizes = steps, sizes
        self.acc, self.gathered, self.sends, self.recvs = acc, gathered, sends, recvs
        self.sems = sems
        self.partners = [partner_of(axis, bit) for axis, bit in steps]
        rows = [acc.shape[0]] + list(sizes)
        self.halvings = sum(a != b for a, b in zip(rows, sizes))
        self.stages = len(steps) + self.halvings
        self.offset = 0
        self.kept = []
        self.flying = None

    def copy(self, stage, source, target, step):
        send, recv = self.sems
        self.flying = pltpu.make_async_remote_copy(
            src_ref=source,
            dst_ref=target,
            send_sem=send.at[stage],
            recv_sem=recv.at[stage],
            device_id={self.steps[step][0]: self.partners[step][0]},
            device_id_type=MESH,
        )
        self.flying.start()

    def start(self, stage):
        if stage < len(self.steps):
            size = self.sizes[stage]
            away = self.offset
            if stage < self.halvings:
                mine = self.partners[stage][1]
                away = pl.multiple_of(self.offset + (1 - mine) * size, 16)
                self.offset = pl.multiple_of(self.offset + mine * size, 16)
                self.kept.append((self.offset, size))
            self.sends[stage][...] = self.acc[pl.ds(away, size)].astype(jnp.bfloat16)
            self.copy(stage, self.sends[stage], self.recvs[stage], stage)
        else:
            step = self.halvings - 1 - (stage - len(self.steps))
            begin, size = self.kept[step]
            here = self.gathered.at[pl.ds(begin, size)]
            self.copy(stage, here, here, step)

    def finish(self, stage):
        self.flying.wait()
        if stage >= len(self.steps):
            return
        here = pl.ds(self.offset, self.sizes[stage])
        came = self.recvs[stage][...].astype(jnp.float32)
        own = self.acc[here] if stage < self.halvings else self.sends[stage][...].astype(jnp.float32)
        total = own + came
        if stage == len(self.steps) - 1:
            self.gathered[here] = total.astype(jnp.bfloat16)
        else:
            self.acc[here] = total


def place(wide, flat, dims):
    planes, rows, depth = dims
    size, stride = rows * depth, (rows + 2) * depth
    for plane in range(planes):
        begin = (plane + 1) * stride + depth
        wide[:, begin : begin + size] = flat[:, plane * size : (plane + 1) * size]


def whole_kernel(setting, *refs):
    fine, coarse, sizes_line, steps, cuts_a, cuts_b, scales = setting
    slab, w_a, b_a, pool, w_b, b_b, cot, v_b, spread, v_a = refs[:10]
    features, grad_slab, out_wa, out_ba, out_wb, out_bb = refs[10:16]
    wide_a, wide_b, wide_gb, wide_ga, win_a, win_b, win_gb, win_ga = refs[16:24]
    before_a, pooled, grad_b, grad_a, acc_a, acc_b, all_a, all_b = refs[24:32]
    count = len(steps)
    send_a, recv_a, send_b, recv_b = [refs[32 + i * count : 32 + (i + 1) * count] for i in range(4)]
    sems = refs[32 + 4 * count :]
    where = line_ends(sizes_line)
    line, total, ids = where
    barrier = pltpu.get_barrier_semaphore()
    for wide in (wide_a, wide_b, wide_gb, wide_ga):
        wide[...] = jnp.zeros_like(wide)
    place(wide_a, slab, fine)
    for axis, bit in steps:
        partner, _ = partner_of(axis, bit)
        pl.semaphore_signal(barrier, inc=1, device_id={axis: partner}, device_id_type=MESH)
    for device in ids:
        pl.semaphore_signal(barrier, inc=1, device_id=device, device_id_type=MESH)
    pl.semaphore_wait(barrier, count + 2)
    halos = [
        Halo(wide, dims, where, sems[:2], 2 * i)
        for i, (wide, dims) in enumerate(
            ((wide_a, fine), (wide_b, coarse), (wide_gb, coarse), (wide_ga, fine))
        )
    ]
    sum_a = Summing(steps, cuts_a, acc_a, all_a, send_a, recv_a, sems[2:4])
    sum_b = Summing(steps, cuts_b, acc_b, all_b, send_b, recv_b, sems[4:6])

    halos[0].start()
    halos[0].wait()
    forward_a_kernel(fine, wide_a, w_a, b_a, pool, before_a, pooled, win_a)
    place(wide_b, pooled, coarse)
    halos[1].start()
    halos[1].wait()
    top_b = out_wb.shape[0]
    middle_kernel(
        coarse, wide_b, w_b, b_b, cot, features, grad_b, acc_b.at[:top_b], acc_b.at[top_b : top_b + 8], win_b
    )
    place(wide_gb, grad_b, coarse)
    halos[2].start()
    acc_b[top_b + 8 :] = jnp.zeros((acc_b.shape[0] - top_b - 8, acc_b.shape[1]), jnp.float32)
    sum_b.start(0)
    halos[2].wait()
    backward_b_kernel(coarse, fine, wide_gb, v_b, before_a, spread, grad_a, win_gb)
    place(wide_ga, grad_a, fine)
    halos[3].start()
    sum_b.finish(0)
    sum_b.start(1)
    grad = grad_a[...]
    half, width = out_wa.shape[0] // 2, out_wa.shape[1]
    acc_a[:half, :width] = dot_rows(win_a[:half], grad)
    acc_a[:half, width:] = dot_rows(win_a[half:], grad)
    acc_a[half:] = jnp.zeros((acc_a.shape[0] - half, acc_a.shape[1]), jnp.float32)
    acc_a[half : half + 8, :width] = dot_rows(jnp.ones((8, grad.shape[1]), jnp.bfloat16), grad)
    sum_b.finish(1)
    sum_b.start(2)
    sum_a.start(0)
    halos[3].wait()
    backward_a_kernel(fine, wide_ga, v_a, grad_slab, win_ga)
    for stage in range(max(sum_a.stages, sum_b.stages - 2)):
        if stage + 2 < sum_b.stages:
            sum_b.finish(stage + 2)
            if stage + 3 < sum_b.stages:
                sum_b.start(stage + 3)
        if stage < sum_a.stages:
            sum_a.finish(stage)
            if stage + 1 < sum_a.stages:
                sum_a.start(stage + 1)
    scale_a, scale_b = scales
    out_wb[...] = all_b[:top_b].astype(jnp.float32) * scale_b
    out_bb[...] = all_b[top_b : top_b + 16].astype(jnp.float32)[:1] * scale_b
    out_wa[:half] = all_a[:half, :width].astype(jnp.float32) * scale_a
    out_wa[half:] = all_a[:half, width:].astype(jnp.float32) * scale_a
    out_ba[...] = all_a[half : half + 16, :width].astype(jnp.float32)[:1] * scale_a


def stage_sizes(rows, steps):
    sizes = []
    for _ in steps:
        halve = rows % 32 == 0 and len(sizes) < 3
        rows = rows // 2 if halve else rows
        sizes.append(rows)
    return sizes


def all_steps():
    cut = {
        axis: [2**i for i in range(lax.axis_size(axis).bit_length() - 1)] for axis in ("gz", "gx", "gy")
    }
    steps = [("gz", bit) for bit in cut["gz"][:1]]
    steps += [("gx", bit) for bit in cut["gx"]] + [("gy", bit) for bit in cut["gy"]]
    return steps + [("gz", bit) for bit in cut["gz"][1:]]


def between_exchanges(fine, coarse, scales, slab, weight_a, bias_a, weight_b, bias_b, cot, pool):
    f32, bf16 = jnp.float32, jnp.bfloat16
    c1, cells = slab.shape
    c2, c3 = weight_b.shape[3:]
    fewer = cells // 8
    steps = all_steps()
    rows_a = 27 * c1 // 2 + 16
    rows_a += -rows_a % 128
    rows_b = 27 * c2 + 16
    rows_b += -rows_b % 128
    cuts_a, cuts_b = stage_sizes(rows_a, steps), stage_sizes(rows_b, steps)
    extent = lambda dims: (dims[0] + 2) * (dims[1] + 2) * dims[2]
    setting = (fine, coarse, (lax.axis_size("gx"), lax.axis_size("gz")), steps, cuts_a, cuts_b, scales)
    buffers = [pltpu.VMEM((n, 128), bf16) for cuts in (cuts_a, cuts_a, cuts_b, cuts_b) for n in cuts]
    outs = [
        ((c3, fewer), bf16),
        ((c1, cells), bf16),
        ((27 * c1, c2), f32),
        ((1, c2), f32),
        ((27 * c2, c3), f32),
        ((1, c3), f32),
    ]
    operands = (
        slab,
        outward(weight_a),
        bias_a[:, None],
        pool,
        outward(weight_b),
        bias_b[:, None],
        cot,
        inward(weight_b),
        pool.T.astype(bf16),
        inward(weight_a),
    )
    most = 2 * len(steps)
    return pl.pallas_call(
        functools.partial(whole_kernel, setting),
        out_shape=[jax.ShapeDtypeStruct(shape, dtype) for shape, dtype in outs],
        in_specs=[pl.BlockSpec(memory_space=pltpu.VMEM)] * len(operands),
        out_specs=[pl.BlockSpec(memory_space=pltpu.VMEM)] * len(outs),
        scratch_shapes=[
            pltpu.VMEM((c1, extent(fine)), bf16),
            pltpu.VMEM((c2, extent(coarse)), bf16),
            pltpu.VMEM((c3, extent(coarse)), bf16),
            pltpu.VMEM((c2, extent(fine)), bf16),
            pltpu.VMEM((27 * c1, cells), bf16),
            pltpu.VMEM((27 * c2, fewer), bf16),
            pltpu.VMEM((27 * c3, fewer), bf16),
            pltpu.VMEM((27 * c2, cells), bf16),
            pltpu.VMEM((c2, cells), f32),
            pltpu.VMEM((c2, fewer), bf16),
            pltpu.VMEM((c3, fewer), bf16),
            pltpu.VMEM((c2, cells), bf16),
            pltpu.VMEM((rows_a, 128), f32),
            pltpu.VMEM((rows_b, 128), f32),
            pltpu.VMEM((rows_a, 128), bf16),
            pltpu.VMEM((rows_b, 128), bf16),
            *buffers,
            pltpu.SemaphoreType.DMA((8,)),
            pltpu.SemaphoreType.DMA((8,)),
            *[pltpu.SemaphoreType.DMA((most,))] * 4,
        ],
        compiler_params=pltpu.CompilerParams(
            collective_id=1, has_side_effects=True, vmem_limit_bytes=60 * 2**20
        ),
    )(*operands)


def outward(weight):
    return weight.reshape(-1, weight.shape[-1]).T


def inward(weight):
    taps = weight[::-1, ::-1, ::-1].reshape(27, *weight.shape[3:])
    return jnp.transpose(taps, (1, 0, 2)).reshape(weight.shape[3], -1)


def lanes_of(shape):
    return lax.broadcasted_iota(jnp.int32, shape, len(shape) - 1)


def rows_of(shape):
    return lax.broadcasted_iota(jnp.int32, shape, 0)


def ones_where(mask):
    return jnp.where(mask, 1.0, 0.0).astype(jnp.bfloat16)


def dot(left, right):
    return jnp.dot(left, right, preferred_element_type=jnp.float32)


def by_parts(rank_bits, mask):
    place = {}
    for at, (axis, bit) in enumerate(rank_bits):
        if mask >> at & 1:
            me = place.get(axis, lax.axis_index(axis))
            place[axis] = me + bit * (1 - 2 * ((lax.axis_index(axis) // bit) % 2))
    return place


def own_rank(rank_bits, mask=0):
    total = 0
    for at, (axis, bit) in enumerate(rank_bits):
        mine = (lax.axis_index(axis) // bit) % 2
        total = total + ((1 - mine) if mask >> at & 1 else mine) * 2**at
    return total


def remote(source, target, sems, at, device, sent_at=None):
    return pltpu.make_async_remote_copy(
        src_ref=source,
        dst_ref=target,
        send_sem=sems[0].at[at if sent_at is None else sent_at],
        recv_sem=sems[1].at[at],
        device_id=device,
        device_id_type=MESH,
    )


def flipped_bits(bits, mask):
    return tuple(bit for at, bit in enumerate(bits) if mask >> at & 1)


class Reduction:
    def __init__(self, groups, exchanged, acc, summed, sends, recvs, sems):
        self.groups, self.exchanged, self.acc, self.summed = groups, exchanged, acc, summed
        self.sends, self.recvs, self.sems = sends, recvs, sems
        self.offset, self.size = 0, acc.shape[0]
        self.parts = []
        self.all = None
        self.stage = 0
        bits = sum(groups[:-1] if exchanged else groups, [])
        self.levels = [level for level in reversed(all_groups()) if level[0] in bits]
        self.stages = len(groups) + len(self.levels)
        self.used = len(groups)
        self.places = {}
        self.sent = 0

    def fly(self, source, target, device):
        remote(source, target, self.sems, self.stage, device).start()

    def piece(self, flipped, level, mask, arrived):
        key = (flipped, level, mask) if level + 1 < len(self.levels) else level
        if key not in self.places:
            self.places[key] = self.used
            self.used += 1
        whose = flipped + flipped_bits(self.levels[level], mask) if arrived else flipped
        offset = 0
        for bits, part in self.parts:
            turned = sum(1 << at for at, bit in enumerate(bits) if bit in whose)
            offset = offset + own_rank(bits, turned) * part
        here = self.summed.at[pl.ds(pl.multiple_of(offset, 8), self.size)]
        device = by_parts(self.levels[level], mask)
        return remote(here, here, self.sems, self.places[key], device, len(self.groups))

    def pieces(self, count, at):
        here = self.summed.at[: count * self.size]
        return remote(here, here, self.sems, at, by_parts(self.levels[-1], 1), len(self.groups))

    def pass_on(self, flipped, first):
        for level in range(first, len(self.levels)):
            for mask in range(1, 2 ** len(self.levels[level])):
                self.piece(flipped, level, mask, False).start()
                self.sent += 1

    def start(self):
        at = self.stage
        count = len(self.groups)
        if at > count:
            return
        if at == count:
            self.known = [()]
            self.pass_on((), 0)
        elif self.exchanged and at == count - 1:
            bits = self.groups[at]
            recv = self.recvs[at]
            mine = own_rank(bits)
            recv[mine] = self.acc[pl.ds(self.offset, self.size)].astype(jnp.bfloat16)
            for mask in range(1, 2 ** len(bits)):
                self.fly(recv.at[mine], recv.at[mine], by_parts(bits, mask))
            rest = recv.at[: recv.shape[0] - 1]
            self.all = remote(rest, rest, self.sems, at, by_parts(bits, 1))
        else:
            bits = self.groups[at]
            members = 2 ** len(bits)
            part = self.size // members
            send, recv = self.sends[at], self.recvs[at]
            send[...] = self.acc[pl.ds(self.offset, self.size)].astype(jnp.bfloat16)
            for mask in range(1, members):
                begin = pl.multiple_of(own_rank(bits, mask) * part, 8)
                self.fly(send.at[pl.ds(begin, part)], recv.at[mask - 1], by_parts(bits, mask))
            self.all = remote(recv, recv, self.sems, at, by_parts(bits, 1))
            self.parts.append((bits, part))
            self.offset = pl.multiple_of(self.offset + own_rank(bits) * part, 8)
            self.size = part

    def finish(self):
        at = self.stage
        count = len(self.groups)
        if at >= count:
            level = at - count
            if level + 1 == len(self.levels):
                self.stage += 1
                self.pieces(len(self.known) * (2 ** len(self.levels[level]) - 1), self.places[level]).wait_recv()
                self.pieces(self.sent, 0).wait_send()
                return
            for _ in self.arrivals():
                pass
            return
        self.stage += 1
        self.all.wait()
        recv = self.recvs[at]
        here = pl.ds(self.offset, self.size)
        if self.exchanged and at == count - 1:
            total = recv[0].astype(jnp.float32)
            for i in range(1, recv.shape[0]):
                total = total + recv[i].astype(jnp.float32)
        else:
            total = self.acc[here]
            for i in range(recv.shape[0]):
                total = total + recv[i].astype(jnp.float32)
        if at == count - 1:
            self.summed[here] = total.astype(jnp.bfloat16)
        else:
            self.acc[here] = total

    def arrivals(self):
        level = self.stage - len(self.groups)
        came = []
        for flipped in self.known:
            for mask in range(1, 2 ** len(self.levels[level])):
                self.piece(flipped, level, mask, True).wait_recv()
                whose = flipped + flipped_bits(self.levels[level], mask)
                self.pass_on(whose, level + 1)
                came.append(whose)
                yield
        self.known = self.known + came
        self.stage += 1

    def step(self):
        self.finish()
        if self.stage < self.stages:
            self.start()


class Border:
    def __init__(self, first, last, edge, inbox, sems, at):
        me, count = lax.axis_index("gz"), lax.axis_size("gz")
        side = 1 - lax.axis_index("gx")
        self.inner, self.outer = me > 0, me < count - 1
        up, down = (me + 1) % count, (me + count - 1) % count
        low, high, beside, beside_low, beside_high = inbox
        self.always = remote(edge, beside, sems, at + 2, {"gx": side})
        self.up = [
            remote(last, low, sems, at, {"gz": up}),
            remote(edge, beside_low, sems, at + 3, {"gx": side, "gz": up}),
        ]
        self.down = [
            remote(first, high, sems, at + 1, {"gz": down}),
            remote(edge, beside_high, sems, at + 4, {"gx": side, "gz": down}),
        ]

    def start(self):
        @pl.when(self.outer)
        def _():
            for copy in self.up:
                copy.start()

        @pl.when(self.inner)
        def _():
            for copy in self.down:
                copy.start()

        self.always.start()

    def wait(self):
        self.always.wait()

        @pl.when(self.outer)
        def _():
            for copy in self.up:
                copy.wait_send()
            for copy in self.down:
                copy.wait_recv()

        @pl.when(self.inner)
        def _():
            for copy in self.down:
                copy.wait_send()
            for copy in self.up:
                copy.wait_recv()


def gathered_edge(tiles, extent, slots):
    shape = tiles[0].shape
    lane = lanes_of(shape)
    high = lax.axis_index("gx") == 0
    edge = jnp.where(high, extent - 1, 0)
    at_edge = lane & (extent - 1) == edge
    total = None
    for i, tile in enumerate(tiles):
        kept = rolled(jnp.where(at_edge, tile, 0.0), i % slots)
        total = kept if total is None else total + kept
    back = pltpu.roll(total, 128 - (extent - 1), 1)
    return jnp.where(high, back, total)


def rolled(value, by):
    by = by % 128
    return pltpu.roll(value, by, 1) if by else value


def quarters(edge):
    size = edge.shape[0] // 4
    return sum(rolled(edge[q * size : (q + 1) * size], 4 * q) for q in range(4))


def spread_edge(edge, by, packed):
    if not packed:
        return rolled(edge, by)
    return jnp.concatenate([rolled(edge, by - 4 * q) for q in range(4)], axis=0)


def halved(tile, low):
    size = tile.shape[0] // 2
    lane = lanes_of((size, 128))
    upper, lower = tile[:size], rolled(tile[size:], 64)
    return jnp.where(lane < 64, upper, lower) if low else jnp.where(lane < 64, lower, upper)


def beside(tile, edges, extent, packed):
    low_edge, high_edge, at = edges
    lane = lanes_of(tile.shape) & (extent - 1)
    before = jnp.where(lane == 0, spread_edge(low_edge, -at, packed), rolled(tile, 1))
    after = jnp.where(lane == extent - 1, spread_edge(high_edge, extent - 1 - at, packed), rolled(tile, -1))
    return before, after


def sided(edge):
    high = lax.axis_index("gx") == 0
    zero = jnp.zeros_like(edge)
    return jnp.where(high, zero, edge), jnp.where(high, edge, zero)


def moved_rows(pair, stride):
    lane = lanes_of(pair[0].shape)
    down = [rolled(tile, stride) for tile in pair]
    up = [rolled(tile, -stride) for tile in pair]
    low = lane < stride
    high = lane < 128 - stride
    zero = jnp.zeros_like(pair[0])
    before = (jnp.where(low, zero, down[0]), jnp.where(low, down[0], down[1]))
    after = (jnp.where(high, up[0], up[1]), jnp.where(high, up[1], zero))
    return before, after


def put_rows(windows, pair, begin, plane, size):
    before, after = moved_rows(pair, 32)
    for ky, tiles in enumerate((before, pair, after)):
        for g, tile in enumerate(tiles):
            lane = plane * 256 + g * 128
            windows[begin + ky * size : begin + (ky + 1) * size, lane : lane + 128] = tile


def moved_half(tile, stride):
    lane = lanes_of(tile.shape) & 63
    zero = jnp.zeros_like(tile)
    before = jnp.where(lane < stride, zero, rolled(tile, stride))
    after = jnp.where(lane < 64 - stride, rolled(tile, -stride), zero)
    return before, after


def inbox_values(inbox):
    low, high, across, across_low, across_high = [ref[...] for ref in inbox]
    return low, high, sided(across), sided(across_low), sided(across_high)


def fine_planes(read, inbox, planes):
    low, high, across, across_low, across_high = inbox_values(inbox)
    for p in range(planes + 2):
        if p == 0:
            pair, edge, at = (low[:, :128], low[:, 128:]), across_low, 2 * (planes - 1)
        elif p == planes + 1:
            pair, edge, at = (high[:, :128], high[:, 128:]), across_high, 0
        else:
            pair, edge, at = read(p - 1), across, 2 * (p - 1)
        sides = [beside(tile, (*edge, at + g), 32, False) for g, tile in enumerate(pair)]
        yield p, ((sides[0][0], sides[1][0]), pair, (sides[0][1], sides[1][1]))


def coarse_tiles(field, inbox, tiles):
    low, high, across, across_low, across_high = inbox_values(inbox)
    low = jnp.concatenate([low, rolled(low, 64)], axis=0)
    high = jnp.concatenate([high, rolled(high, 64)], axis=0)
    half = lanes_of(low.shape) < 64
    for t in range(tiles):
        tile = field[:, t * 128 : (t + 1) * 128]
        sides = list(beside(tile, (*across, t % 4), 16, True))
        if t == 0:
            sides_low = beside(low, (*across_low, (tiles - 1) % 4), 16, True)
            tile = jnp.where(half, low, tile)
            sides = [jnp.where(half, a, b) for a, b in zip(sides_low, sides)]
        if t == tiles - 1:
            sides_high = beside(high, (*across_high, 0), 16, True)
            tile = jnp.where(half, tile, high)
            sides = [jnp.where(half, b, a) for a, b in zip(sides_high, sides)]
        yield t, (sides[0], tile, sides[1])


def column(row, size):
    wide = jnp.broadcast_to(row, (size, size))
    eye = rows_of((size, size)) == lanes_of((size, size))
    return jnp.sum(jnp.where(eye, wide, 0.0), axis=1, keepdims=True)


def joined_thirds(terms, tiles):
    half = None
    low = [rolled(terms(0, t), 64) for t in range(tiles)]
    high = [rolled(terms(2, t), 64) for t in range(tiles)]
    out = []
    for t in range(tiles):
        if half is None:
            half = lanes_of(low[0].shape) < 64
        before, after = low[max(t - 1, 0)], high[min(t + 1, tiles - 1)]
        out.append(terms(1, t) + jnp.where(half, before + high[t], low[t] + after))
    return out


def block_kernel(setting, *refs):
    groups, groups_a, cuts = setting
    inputs = refs[:6]
    features, grad_in, sum_a, sum_b = refs[6:10]
    volume, w_a, b_a, w_b, b_b, cot = refs[10:16]
    (
        stage, own_a, windows_a, sums_a, slope_a, halves, pooled, windows_b, sums_b,
        cot_sent, cot_came, cot_here, grad_b, lines_b, sums_gb, grads_a, lines_a, sums_ga,
        feat_sent, feat_came, mat_a, mat_b, mat_ga, mat_gb, near, far, pool, acc_a, acc_b,
    ) = refs[16:45]
    rest = list(refs[45:])
    inboxes = [[rest.pop(0) for _ in range(5)] for _ in range(4)]
    edges = [rest.pop(0) for _ in range(4)]
    ends_b, ends_gb = [[rest.pop(0), rest.pop(0)] for _ in range(2)]
    count = len(groups)
    takes = lambda n: [rest.pop(0) for _ in range(n)]
    send_a, recv_a = takes(1), takes(2)
    send_b, recv_b, send_c, recv_c = [takes(count) for _ in range(4)]
    sems_halo, sems_cot, sems_feat, sems_a, sems_b, sems_c = [takes(2) for _ in range(6)]
    (sems_in,) = rest
    f32, bf16 = jnp.float32, jnp.bfloat16
    c1, rows, planes, width = volume.shape
    c2, c3 = w_a.shape[2], w_b.shape[2]
    tiles = planes // 4 + 1
    me, members = lax.axis_index("gz"), lax.axis_size("gz")
    whole = [bit for group in groups for bit in group]
    line = [bit for bit in whole if bit[0] == "gz"]

    apart = me < members
    barrier = pltpu.get_barrier_semaphore()
    for mask in range(1, 2 ** len(whole)):
        pl.semaphore_signal(barrier, inc=1, device_id=by_parts(whole, mask), device_id_type=MESH)
    loads = {
        at: pltpu.make_async_copy(inputs[at], refs[10 + at], sems_in.at[at]) for at in range(1, len(inputs))
    }
    parts = 4
    share = c1 // parts
    loads_v = [
        pltpu.make_async_copy(
            inputs[0].at[i * share : (i + 1) * share],
            volume.at[i * share : (i + 1) * share],
            sems_in.at[0],
        )
        for i in range(parts)
    ]
    for load in loads_v:
        load.start()
    for at in (5, 1, 3, 2, 4):
        loads[at].start()

    @pl.when(me == 0)
    def _():
        for inbox in inboxes:
            for box in (inbox[0], inbox[3]):
                box[...] = jnp.zeros_like(box)

    @pl.when(me == members - 1)
    def _():
        for inbox in inboxes:
            for box in (inbox[1], inbox[4]):
                box[...] = jnp.zeros_like(box)

    pltpu.make_async_copy(inputs[0], volume, sems_in.at[0]).wait()
    for g in range(2):
        for i in range(4):
            part = volume[:, 4 * g + i].astype(f32).reshape(c1 * planes, width)
            stage[:, width * i : width * (i + 1)] = part
        for z in range(planes):
            tile = stage[pl.ds(z, c1, stride=planes), :]
            own_a[:, z * 256 + g * 128 : z * 256 + (g + 1) * 128] = tile.astype(bf16)

    def read_a(z):
        return tuple(own_a[:, z * 256 + g * 128 : z * 256 + (g + 1) * 128] for g in range(2))

    edges[0][...] = gathered_edge([tile.astype(f32) for z in range(planes) for tile in read_a(z)], 32, 32).astype(bf16)
    pl.semaphore_wait(barrier, 2 ** len(whole) - 1)

    border_a = Border(own_a.at[:, :256], own_a.at[:, (planes - 1) * 256 :], edges[0], inboxes[0], sems_halo, 0)
    border_a.start()

    def exchange(sent, came, sems):
        size = sent.shape[0] // members
        for mask in range(1, members):
            begin = pl.multiple_of(own_rank(line, mask) * size, 16)
            remote(
                sent.at[pl.ds(begin, size)],
                came.at[pl.ds(pl.multiple_of(me * size, 16), size)],
                sems,
                0,
                by_parts(line, mask),
            ).start()
        here = pl.ds(pl.multiple_of(me * size, 16), size)
        came[here] = sent[here]
        most = (members - 1) * size
        return remote(sent.at[:most], came.at[:most], sems, 0, by_parts(line, 1))

    for at in range(1, 5):
        loads[at].wait()

    high = lax.axis_index("gx") == 0
    eye = ones_where(rows_of((c2, c2)) == lanes_of((c2, c2)))
    eye_b = ones_where(rows_of((c3, c3)) == lanes_of((c3, c3)))
    for kz in range(3):
        block = w_a[:].reshape(9, 3, c1, c2)[:, kz].reshape(3, 3 * c1, c2)
        block = jnp.concatenate([block[1], *[jnp.where(high, a, b) for a, b in ((block[0], block[2]), (block[2], block[0]))]], axis=0)
        mat_a[kz * c2 : (kz + 1) * c2] = dot_rows(eye, block).astype(bf16)
        block = w_b[:].reshape(9, 3, c2, c3)[:, kz].reshape(9 * c2, c3)
        mat_b[kz * c3 : (kz + 1) * c3] = dot_rows(eye_b, block).astype(bf16)
        for ky in range(3):
            for kx in range(3):
                tap = ((2 - kx) * 3 + 2 - ky) * 3 + 2 - kz
                at = kz * 3 + ky
                mat_ga[at * c1 : (at + 1) * c1, kx * c2 : (kx + 1) * c2] = w_a[tap]
                mat_gb[at * c2 : (at + 1) * c2, kx * c3 : (kx + 1) * c3] = w_b[tap]
    col_a, col_b = column(b_a[...], c2), column(b_b[...], c3)
    r, l = rows_of(far.shape), lanes_of(far.shape)
    far[...] = ones_where(((r >> 3) & 3 == l >> 7) & (((r >> 5) << 3) + (r & 7) == l & 127))
    loads[5].wait()
    half_rows = rows // 2
    stage[...] = cot[...].astype(f32)
    spaced = [stage[pl.ds(y, c3, stride=half_rows), :].astype(bf16) for y in range(half_rows)]
    cot_sent[...] = dot_rows(far[...], jnp.concatenate(spaced, axis=1)).astype(bf16)
    cot_flying = exchange(cot_sent, cot_came, sems_cot)
    deep = 3 * c1
    lane = lanes_of((c1, 128)) & 31

    @pl.when(apart)
    def _():
        for p in range(1, planes + 1):
            pair = read_a(p - 1)
            zero = jnp.zeros_like(pair[0])
            before = [jnp.where(lane == 0, zero, rolled(tile, 1)) for tile in pair]
            after = [jnp.where(lane == 31, zero, rolled(tile, -1)) for tile in pair]
            plain = [jnp.where(high, a, b) for a, b in zip(before, after)]
            met = [jnp.where(high, b, a) for a, b in zip(before, after)]
            put_rows(windows_a, pair, 0, p, c1)
            put_rows(windows_a, plain, deep, p, c1)
            for g in range(2):
                windows_a[2 * deep + c1 : 2 * deep + 2 * c1, p * 256 + g * 128 : p * 256 + (g + 1) * 128] = met[g]
            if p % 2 == 0:
                here = slice((p - 1) * 256, (p + 1) * 256)
                sums_a[:, here] = dot(mat_a[:, : 2 * deep], windows_a[: 2 * deep, here])

    r, l = rows_of((512, 128)), lanes_of((512, 128))
    pool[...] = ones_where(
        (r >> 8 == l >> 6) & ((r >> 6) & 3 == (l >> 4) & 3) & ((r & 31) >> 1 == l & 15)
    )
    halves[...] = jnp.zeros_like(halves)
    for kz in range(3):
        for p in range(planes + 2):
            if not 0 <= p + kz - 2 < planes:
                grads_a[kz * c2 : (kz + 1) * c2, p * 256 : (p + 1) * 256] = jnp.zeros((c2, 256), bf16)
    acc_a[...] = jnp.zeros_like(acc_a)
    border_a.wait()

    @pl.when(apart)
    def _():
        boxes = [ref[...] for ref in inboxes[0]]
        turned = [jnp.where(high, rolled(edge, 31), edge) for edge in boxes[2:]]
        for p in range(planes + 2):
            if 0 < p <= planes:
                edge, at = turned[0], 2 * (p - 1)
                pair = [
                    windows_a[2 * deep + c1 : 2 * deep + 2 * c1, p * 256 + g * 128 : p * 256 + (g + 1) * 128]
                    for g in range(2)
                ]
            else:
                edge, at = (turned[2], 0) if p else (turned[1], 2 * (planes - 1))
                tiles_p = [boxes[1 if p else 0][:, g * 128 : (g + 1) * 128] for g in range(2)]
                zero = jnp.zeros_like(tiles_p[0])
                before = [jnp.where(lane == 0, zero, rolled(tile, 1)) for tile in tiles_p]
                after = [jnp.where(lane == 31, zero, rolled(tile, -1)) for tile in tiles_p]
                put_rows(windows_a, tiles_p, 0, p, c1)
                put_rows(windows_a, [jnp.where(high, a, b) for a, b in zip(before, after)], deep, p, c1)
                pair = [jnp.where(high, b, a) for a, b in zip(before, after)]
            side = jnp.where(high, 31, 0)
            pair = [jnp.where(lane == side, rolled(edge, -at - g), tile) for g, tile in enumerate(pair)]
            put_rows(windows_a, pair, 2 * deep, p, c1)
            here = slice((p - 1) * 256, (p + 1) * 256)
            if p == 0 or p == planes + 1:
                here = slice(p * 256, (p + 1) * 256)
                sums_a[:, here] = dot(mat_a[...], windows_a[:, here])
            elif p % 2 == 0:
                sums_a[:, here] = sums_a[:, here] + dot(mat_a[:, 2 * deep :], windows_a[2 * deep :, here])

    @pl.when(apart)
    def _():
        for z in range(planes):
            value = (
                sums_a[:c2, z * 256 : (z + 1) * 256]
                + sums_a[c2 : 2 * c2, (z + 1) * 256 : (z + 2) * 256]
                + sums_a[2 * c2 :, (z + 2) * 256 : (z + 3) * 256]
                + col_a
            )
            sigma = jax.nn.sigmoid(value)
            active = value * sigma
            slope_a[:, z * 256 : (z + 1) * 256] = (sigma + active * (1.0 - sigma)) * 0.125
            if z % 2:
                active = active + kept
                pz = z // 2 + 1
                upper = active.astype(bf16)
                lower = (active - upper.astype(f32)).astype(bf16)
                at, lane = pz // 2 * c2, pz % 2 * 256
                halves[at : at + c2, lane : lane + 256] = upper
                halves[tiles * c2 + at : tiles * c2 + at + c2, lane : lane + 256] = lower
                if pz % 2 or z == planes - 1:
                    low_at = tiles * c2 + at
                    both = dot(halves[at : at + c2], pool[...]) + dot(halves[low_at : low_at + c2], pool[...])
                    pooled[:, pz // 2 * 128 : (pz // 2 + 1) * 128] = (both * 0.125).astype(bf16)
            else:
                kept = active

    def coarse_border(field, edge, ends, inbox, at):
        parts = [field[:, t * 128 : (t + 1) * 128].astype(f32) for t in range(tiles)]
        edge[...] = quarters(gathered_edge(parts, 16, 4)).astype(bf16)
        ends[0][...] = halved(parts[0], False).astype(bf16)
        ends[1][...] = halved(parts[-1], True).astype(bf16)
        return Border(ends[0], ends[1], edge, inbox, sems_halo, at)

    border_b = coarse_border(pooled, edges[1], ends_b, inboxes[1], 5)
    border_b.start()
    cot_flying.wait()
    r, l = rows_of(near.shape), lanes_of(near.shape)
    near[...] = ones_where(
        ((r & 7) + 1 == l >> 6) & ((r >> 3) & 3 == (l >> 4) & 3) & (r >> 5 == l & 15)
    )
    came = jnp.transpose(cot_came[...].astype(f32)).astype(bf16)
    cot_here[...] = dot(came, near[...])
    border_b.wait()

    @pl.when(apart)
    def _():
        for t, thirds in coarse_tiles(pooled, inboxes[1], tiles):
            for kx, tile in enumerate(thirds):
                before, after = moved_half(tile, 16)
                for ky, value in enumerate((before, tile, after)):
                    at = (kx * 3 + ky) * c2
                    windows_b[at : at + c2, t * 128 : (t + 1) * 128] = value.astype(bf16)
            if t % 2 or t == tiles - 1:
                here = slice(t // 2 * 256, (t + 1) * 128)
                sums_b[:, here] = dot(mat_b[...], windows_b[:, here])

    joined = joined_thirds(lambda k, t: sums_b[k * c3 : (k + 1) * c3, t * 128 : (t + 1) * 128], tiles)
    feats = []
    for t, value in enumerate(joined):
        value = value + col_b
        sigma = jax.nn.sigmoid(value)
        active = value * sigma
        feats.append(active.astype(bf16))
        slope = sigma + active * (1.0 - sigma)
        grad = cot_here[:, t * 128 : (t + 1) * 128] * slope
        grad_b[c3 : 2 * c3, t * 128 : (t + 1) * 128] = grad.astype(bf16)
    own_gb = grad_b.at[c3 : 2 * c3]
    border_gb = coarse_border(own_gb, edges[2], ends_gb, inboxes[2], 10)
    border_gb.start()

    half = lanes_of((c3, 128)) < 64
    turned = [rolled(own_gb[:, t * 128 : (t + 1) * 128].astype(f32), 64) for t in range(tiles)]
    zero = jnp.zeros_like(turned[0])
    for t in range(tiles):
        later = turned[t + 1] if t + 1 < tiles else zero
        earlier = turned[t - 1] if t else zero
        here = slice(t * 128, (t + 1) * 128)
        grad_b[:c3, here] = jnp.where(half, turned[t], later).astype(bf16)
        grad_b[2 * c3 :, here] = jnp.where(half, earlier, turned[t]).astype(bf16)
    top = 27 * c2

    def sum_terms(first, last):
        terms = dot_rows(windows_b[first * c2 : last * c2], grad_b[...])
        for at in range(first, last):
            for kz in range(3):
                tap = at * 3 + kz
                acc_b[tap * c2 : (tap + 1) * c2] = terms[
                    (at - first) * c2 : (at - first + 1) * c2, kz * c3 : (kz + 1) * c3
                ]

    cut = cuts[0]
    early = -(-cut // (3 * c2))
    pl.when(apart)(functools.partial(sum_terms, 0, early))
    total_b = Reduction(groups, False, acc_b.at[:cut], sum_b.at[:cut], send_b, recv_b, sems_b)
    total_b.start()
    pl.when(apart)(functools.partial(sum_terms, early, 9))
    acc_b[top:] = jnp.zeros((acc_b.shape[0] - top, c3), f32)
    acc_b[top : top + 8] = dot_rows(jnp.ones((8, tiles * 128), bf16), own_gb[...])
    total_c = Reduction(groups, False, acc_b.at[cut:], sum_b.at[cut:], send_c, recv_c, sems_c)
    total_c.start()
    total_b.step()
    total_c.step()
    border_gb.wait()

    @pl.when(apart)
    def _():
        for t, thirds in coarse_tiles(own_gb, inboxes[2], tiles):
            for kx, tile in enumerate(thirds):
                lines_b[kx * c3 : (kx + 1) * c3, t * 128 : (t + 1) * 128] = tile.astype(bf16)
            if t % 2 or t == tiles - 1:
                here = slice(t // 2 * 256, (t + 1) * 128)
                sums_gb[:, here] = dot(mat_gb[...], lines_b[:, here])

    by_row = [
        joined_thirds(
            lambda k, t: sums_gb[(k * 3 + ky) * c2 : (k * 3 + ky + 1) * c2, t * 128 : (t + 1) * 128], tiles
        )
        for ky in range(3)
    ]
    small = []
    for t in range(tiles):
        value = by_row[1][t] + moved_half(by_row[0][t], 16)[0] + moved_half(by_row[2][t], 16)[1]
        small.append(value.astype(bf16))
    spread = dot_rows(jnp.concatenate(small, axis=0), pool[...])
    for z in range(planes):
        pz = z // 2 + 1
        large = spread[pz // 2 * c2 : (pz // 2 + 1) * c2, pz % 2 * 256 : (pz % 2 + 1) * 256]
        grad = (large * slope_a[:, z * 256 : (z + 1) * 256]).astype(bf16)
        for kz in range(3):
            grads_a[kz * c2 : (kz + 1) * c2, (z + kz) * 256 : (z + kz + 1) * 256] = grad

    own_ga = grads_a.at[c2 : 2 * c2]

    def read_ga(z):
        return tuple(
            own_ga[:, (z + 1) * 256 + g * 128 : (z + 1) * 256 + (g + 1) * 128] for g in range(2)
        )

    edges[3][...] = gathered_edge([tile.astype(f32) for z in range(planes) for tile in read_ga(z)], 32, 32).astype(bf16)
    border_ga = Border(
        own_ga.at[:, 256:512], own_ga.at[:, planes * 256 : (planes + 1) * 256], edges[3], inboxes[3], sems_halo, 15
    )
    border_ga.start()

    @pl.when(apart)
    def _():
        top_a = 9 * c1 + 9 * c1 // 2
        terms = dot_rows(windows_a[...], grads_a[...])
        near_x, far_x = terms[deep : 2 * deep], terms[2 * deep :]
        terms = jnp.concatenate(
            [jnp.where(high, near_x, far_x), terms[:deep], jnp.where(high, far_x, near_x)], axis=0
        )
        full = 9 * c1
        acc_a[:full] = terms[:, : 2 * c2]
        acc_a[full:top_a, :c2] = terms[: full // 2, 2 * c2 :]
        acc_a[full:top_a, c2:] = terms[full // 2 :, 2 * c2 :]
        acc_a[top_a : top_a + 8, :c2] = dot_rows(
            jnp.ones((8, planes * 256), bf16), own_ga[:, 256 : (planes + 1) * 256]
        )

    total_a = Reduction(groups_a, True, acc_a, sum_a, send_a, recv_a, sems_a)
    total_a.start()
    total_b.step()
    total_c.step()
    feat_sent[...] = dot_rows(near[...], jnp.concatenate(feats, axis=1)).astype(bf16)
    feat_flying = exchange(feat_sent, feat_came, sems_feat)
    border_ga.wait()

    @pl.when(apart)
    def _():
        for p, thirds in fine_planes(read_ga, inboxes[3], planes):
            for kx, pair in enumerate(thirds):
                for g, tile in enumerate(pair):
                    at = p * 256 + g * 128
                    lines_a[kx * c2 : (kx + 1) * c2, at : at + 128] = tile.astype(bf16)
            if p % 2:
                here = slice((p - 1) * 256, (p + 1) * 256)
                sums_ga[:, here] = dot(mat_ga[...], lines_a[:, here])

    total_a.step()
    total_b.step()
    total_c.step()
    results = []
    for z in range(planes):
        by_row = []
        for ky in range(3):
            value = None
            for kz in range(3):
                at = (kz * 3 + ky) * c1
                term = sums_ga[at : at + c1, (z + kz) * 256 : (z + kz + 1) * 256]
                value = term if value is None else value + term
            by_row.append((value[:, :128], value[:, 128:]))
        before, after = moved_rows(by_row[0], 32)[0], moved_rows(by_row[2], 32)[1]
        results.append([by_row[1][g] + before[g] + after[g] for g in range(2)])
    for g in range(2):
        for z in range(planes):
            stage[pl.ds(z, c1, stride=planes), :] = results[z][g]
        for i in range(4):
            part = stage[:, width * i : width * (i + 1)].astype(bf16)
            grad_in[:, 4 * g + i] = part.reshape(c1, planes, width)

    def together(*totals):
        for _ in zip(*[total.arrivals() for total in totals], strict=True):
            pass

    together(total_b, total_c)
    total_a.step()
    feat_flying.wait()
    came = jnp.transpose(feat_came[...].astype(f32)).astype(bf16)
    ours = dot(came, far[...])
    for y in range(half_rows):
        stage[pl.ds(y, c3, stride=half_rows), :] = ours[:, y * 128 : (y + 1) * 128]
    features[...] = stage[...].astype(bf16)
    together(total_b, total_c)
    total_a.step()
    total_b.step()
    total_c.step()
    total_a.step()


def last_kernel(scales, *refs):
    feat, grad, sum_a, sum_b, out_feat, out_grad, out_wa, out_ba, out_wb, out_bb = refs[:10]
    wa, ba, wb, bb, sems_out = refs[10:]
    f32 = jnp.float32
    scale_a, scale_b = scales
    places = ((grad, out_grad), (feat, out_feat), (wb, out_wb), (bb, out_bb), (wa, out_wa), (ba, out_ba))
    stores = [
        pltpu.make_async_copy(source, target, sems_out.at[at]) for at, (source, target) in enumerate(places)
    ]
    stores[0].start()
    stores[1].start()
    top = wb.shape[0]
    wb[...] = sum_b[:top].astype(f32) * scale_b
    stores[2].start()
    bb[...] = sum_b[top : top + 16].astype(f32)[:1] * scale_b
    stores[3].start()
    c1, c2 = wa.shape[1:]
    deep = 9 * c1
    pairs = sum_a[:deep].astype(f32) * scale_a
    tail = sum_a[deep : deep + deep // 2].astype(f32) * scale_a
    thirds = jnp.concatenate([tail[:, :c2], tail[:, c2:]], axis=0)
    for at in range(9):
        here = slice(at * c1, (at + 1) * c1)
        wa[at * 3] = pairs[here, :c2]
        wa[at * 3 + 1] = pairs[here, c2:]
        wa[at * 3 + 2] = thirds[here]
    stores[4].start()
    top_a = deep + deep // 2
    ba[...] = sum_a[top_a : top_a + 16].astype(f32)[:1, :c2] * scale_a
    stores[5].start()
    for store in stores:
        store.wait()


def all_groups():
    cut = {axis: [2**i for i in range(lax.axis_size(axis).bit_length() - 1)] for axis in ("gz", "gx")}
    line = [("gz", bit) for bit in cut["gz"]]
    return [line[:1], [("gx", bit) for bit in cut["gx"]] + line[1:2], line[2:]]


def on_blocks(volume, weight_a, bias_a, weight_b, bias_b, cotangent, scales):
    f32, bf16 = jnp.float32, jnp.bfloat16
    c1, width, rows, planes = volume.shape
    c2, c3 = weight_b.shape[3:]
    members = lax.axis_size("gz")
    groups = all_groups()
    tiles = planes // 4 + 1
    long, short = (planes + 2) * 256, tiles * 128
    cells = planes * 256
    rows_a, rows_b = 512, 27 * c2 + 64
    fewer = cells // 8

    def buffers(total, groups, exchanged):
        sends, recvs = [], []
        size = total
        for at, group in enumerate(groups):
            n = 2 ** len(group)
            if exchanged and at == len(groups) - 1:
                recvs.append(pltpu.VMEM((n, size, 128), bf16))
                continue
            sends.append(pltpu.VMEM((size, 128), bf16))
            size //= n
            recvs.append(pltpu.VMEM((n - 1, size, 128), bf16))
        return sends + recvs

    inboxes = []
    for size, plane, edge in ((c1, 256, c1), (c2 // 2, 128, c2 // 4), (c3 // 2, 128, c3 // 4), (c2, 256, c2)):
        inboxes += [pltpu.VMEM((size, plane), bf16)] * 2 + [pltpu.VMEM((edge, 128), bf16)] * 3
    groups_a = [groups[0] + groups[1], groups[2]]
    by_level = [2 ** len(group) for group in groups]
    count_a = len(groups_a) + by_level[1]
    count_b = len(groups) + by_level[2] * by_level[1]
    cuts = (1024, rows_b - 1024)
    passed = [
        ((c3 * rows // 2, 128), bf16),
        ((c1, rows, planes, width), bf16),
        ((rows_a, 128), bf16),
        ((rows_b, 128), bf16),
    ]
    operands = (
        jnp.transpose(volume, (0, 2, 3, 1)),
        weight_a.reshape(27, c1, c2),
        bias_a[None],
        weight_b.reshape(27, c2, c3),
        bias_b[None],
        cotangent.reshape(c3 * rows // 2, 128),
    )
    anywhere, inside = pl.BlockSpec(memory_space=pl.ANY), pl.BlockSpec(memory_space=pltpu.VMEM)
    middle = pl.pallas_call(
        functools.partial(block_kernel, (groups, groups_a, cuts)),
        out_shape=[pltpu.VMEM(shape, dtype) for shape, dtype in passed],
        in_specs=[anywhere] * len(operands),
        out_specs=[inside] * len(passed),
        scratch_shapes=[
            *[pltpu.VMEM(x.shape, x.dtype) for x in operands],
            pltpu.VMEM((c1 * planes, 128), f32),
            pltpu.VMEM((c1, cells), bf16),
            pltpu.VMEM((9 * c1, long), bf16),
            pltpu.VMEM((3 * c2, long), f32),
            pltpu.VMEM((c2, cells), f32),
            pltpu.VMEM((2 * tiles * c2, 512), bf16),
            pltpu.VMEM((c2, short), bf16),
            pltpu.VMEM((9 * c2, short), bf16),
            pltpu.VMEM((3 * c3, short), f32),
            pltpu.VMEM((fewer, c3), bf16),
            pltpu.VMEM((fewer, c3), bf16),
            pltpu.VMEM((c3, short), f32),
            pltpu.VMEM((3 * c3, short), bf16),
            pltpu.VMEM((3 * c3, short), bf16),
            pltpu.VMEM((9 * c2, short), f32),
            pltpu.VMEM((3 * c2, long), bf16),
            pltpu.VMEM((3 * c2, long), bf16),
            pltpu.VMEM((9 * c1, long), f32),
            pltpu.VMEM((fewer, c3), bf16),
            pltpu.VMEM((fewer, c3), bf16),
            pltpu.VMEM((3 * c2, 9 * c1), bf16),
            pltpu.VMEM((3 * c3, 9 * c2), bf16),
            pltpu.VMEM((9 * c1, 3 * c2), bf16),
            pltpu.VMEM((9 * c2, 3 * c3), bf16),
            pltpu.VMEM((fewer, short), bf16),
            pltpu.VMEM((fewer, fewer), bf16),
            pltpu.VMEM((512, 128), bf16),
            pltpu.VMEM((rows_a, 128), f32),
            pltpu.VMEM((rows_b, 128), f32),
            *inboxes,
            *[pltpu.VMEM((size, 128), bf16) for size in (c1, c2 // 4, c3 // 4, c2)],
            *[pltpu.VMEM((size // 2, 128), bf16) for size in (c2, c2, c3, c3)],
            *buffers(rows_a, groups_a, True),
            *buffers(cuts[0], groups, False),
            *buffers(cuts[1], groups, False),
            *[pltpu.SemaphoreType.DMA((20,))] * 2,
            *[pltpu.SemaphoreType.DMA((1,))] * 4,
            *[pltpu.SemaphoreType.DMA((n,)) for n in (len(groups_a) + 1, count_a)],
            *[pltpu.SemaphoreType.DMA((n,)) for n in (len(groups) + 1, count_b)] * 2,
            pltpu.SemaphoreType.DMA((len(operands),)),
        ],
        compiler_params=pltpu.CompilerParams(
            collective_id=2, has_side_effects=True, vmem_limit_bytes=60 * 2**20
        ),
    )(*operands)
    outs = [
        *passed[:2],
        ((27, c1, c2), f32),
        ((1, c2), f32),
        ((27 * c2, c3), f32),
        ((1, c3), f32),
    ]
    features, grad_in, sum_wa, sum_ba, sum_wb, sum_bb = pl.pallas_call(
        functools.partial(last_kernel, scales),
        out_shape=[jax.ShapeDtypeStruct(shape, dtype) for shape, dtype in outs],
        in_specs=[inside] * len(passed),
        out_specs=[anywhere] * len(outs),
        scratch_shapes=[
            *[pltpu.VMEM(shape, dtype) for shape, dtype in outs[2:]],
            pltpu.SemaphoreType.DMA((len(outs),)),
        ],
    )(*[pltpu.with_memory_space_constraint(x, pltpu.VMEM) for x in middle])
    return (
        features.reshape(cotangent.shape),
        jnp.transpose(grad_in, (0, 3, 1, 2)),
        sum_wa.reshape(weight_a.shape),
        sum_ba.reshape(c2),
        sum_wb.reshape(weight_b.shape),
        sum_bb.reshape(c3),
    )


def fits_blocks(volume, weight_b):
    c1, width, rows, planes = volume.shape
    sizes = {axis: lax.axis_size(axis) for axis in ("gx", "gy", "gz")}
    return (
        sizes == {"gx": 2, "gy": 1, "gz": planes}
        and (width, rows, planes) == (32, 8, 16)
        and (c1, *weight_b.shape[3:]) == (32, 64, 128)
    )


def on_device(volume, weight_a, bias_a, weight_b, bias_b, cotangent):
    f32, bf16 = jnp.float32, jnp.bfloat16
    count = lax.axis_size("gz")
    devices_all = lax.axis_size("gx") * lax.axis_size("gy") * count
    c1, nx, rows, nz = volume.shape
    cells = nx * rows * nz
    scale_a = 1.0 / math.sqrt(cells * devices_all)
    scale_b = 1.0 / math.sqrt(cells * devices_all // 8)
    c2, c3 = weight_b.shape[3:]
    if fits_blocks(volume, weight_b):
        return on_blocks(volume, weight_a, bias_a, weight_b, bias_b, cotangent, (scale_a, scale_b))
    planes, depth = nx // count, nz * count
    fine = (planes, rows, depth)
    coarse = (planes // 2, rows // 2, depth // 2)
    fewer = cells // 8
    pool = (jnp.arange(depth)[:, None] // 2 == jnp.arange(depth // 2)[None]).astype(f32)
    work_a = 2 * 27 * c1 * c2 * cells
    work_b = 2 * 27 * c2 * c3 * fewer

    slab = lax.all_to_all(volume, "gz", split_axis=1, concat_axis=3, tiled=True).reshape(c1, cells)
    if lax.axis_size("gy") == 1:
        features, grad_slab, sum_wa, sum_ba, sum_wb, sum_bb = between_exchanges(
            fine,
            coarse,
            (scale_a, scale_b),
            slab,
            weight_a,
            bias_a,
            weight_b,
            bias_b,
            cotangent.reshape(c3, fewer),
            pool,
        )
    else:
        wide_a = widened(slab, *fine)
        before_a, pooled = local_kernel(
            functools.partial(forward_a_kernel, fine),
            [((c2, cells), f32), ((c2, fewer), bf16)],
            (27 * c1, cells),
            work_a,
            wide_a,
            outward(weight_a),
            bias_a[:, None],
            pool,
        )
        wide_b = widened(pooled, *coarse)
        features, grad_b, part_wb, part_bb = local_kernel(
            functools.partial(middle_kernel, coarse),
            [((c3, fewer), bf16), ((c3, fewer), bf16), ((27 * c2, c3), f32), ((8, c3), f32)],
            (27 * c2, fewer),
            2 * work_b,
            wide_b,
            outward(weight_b),
            bias_b[:, None],
            cotangent.reshape(c3, fewer),
        )
        (grad_a,) = local_kernel(
            functools.partial(backward_b_kernel, coarse, fine),
            [((c2, cells), bf16)],
            (27 * c3, fewer),
            work_b,
            widened(grad_b, *coarse),
            inward(weight_b),
            before_a,
            pool.T.astype(bf16),
        )
        part_wa, part_ba = local_kernel(
            functools.partial(weight_a_kernel, fine),
            [((27 * c1, c2), f32), ((8, c2), f32)],
            (27 * c1, cells),
            work_a,
            wide_a,
            grad_a,
        )
        (grad_slab,) = local_kernel(
            functools.partial(backward_a_kernel, fine),
            [((c1, cells), bf16)],
            (27 * c2, cells),
            work_a,
            widened(grad_a, *fine),
            inward(weight_a),
        )
        sum_wa, sum_ba, sum_wb, sum_bb = summed_grads(
            part_wa, part_ba, part_wb, part_bb, (scale_a, scale_b)
        )
    grad_input = lax.all_to_all(
        grad_slab.reshape(c1, planes, rows, depth), "gz", split_axis=3, concat_axis=1, tiled=True
    )
    return (
        features.reshape(cotangent.shape),
        grad_input,
        sum_wa.reshape(weight_a.shape),
        sum_ba.reshape(c2),
        sum_wb.reshape(weight_b.shape),
        sum_bb.reshape(c3),
    )


def solution(mesh):
    return jax.shard_map(
        on_device,
        mesh=mesh,
        in_specs=(P(None, "gx", "gy", "gz"), P(), P(), P(), P(), P(None, ("gx", "gz"), "gy", None)),
        out_specs=(
            P(None, ("gx", "gz"), "gy", None),
            P(None, "gx", "gy", "gz"),
            P(),
            P(),
            P(),
            P(),
        ),
        check_vma=False,
    )
```

```python
import functools
import math

import jax
import jax.numpy as jnp
from jax import lax
from jax.experimental import pallas as pl
from jax.experimental.pallas import tpu as pltpu
from jax.sharding import PartitionSpec as P

LINE = ("gx", "gz")
MESH = pl.DeviceIdType.MESH


def shared(block, axis, dim, width):
    count = lax.axis_size(axis)
    if count == 1:
        edge = jnp.zeros_like(lax.slice_in_dim(block, 0, width, axis=dim))
        return edge, edge
    forward = [(i, i + 1) for i in range(count - 1)]
    backward = [(target, source) for source, target in forward]
    last = block.shape[dim]
    low = lax.ppermute(lax.slice_in_dim(block, last - width, last, axis=dim), axis, forward)
    high = lax.ppermute(lax.slice_in_dim(block, 0, width, axis=dim), axis, backward)
    return low, high


def widened(flat, planes, rows, depth):
    low, high = shared(flat, LINE, 1, rows * depth)
    if lax.axis_size("gy") == 1:
        gap = jnp.zeros((flat.shape[0], depth), flat.dtype)
        pieces = [gap, low, gap]
        for plane in range(planes):
            pieces += [gap, flat[:, plane * rows * depth : (plane + 1) * rows * depth], gap]
        return jnp.concatenate(pieces + [gap, high, gap], axis=1)
    whole = jnp.concatenate([low, flat, high], axis=1)
    whole = whole.reshape(flat.shape[0], planes + 2, rows, depth)
    low, high = shared(whole, "gy", 2, 1)
    return jnp.concatenate([low, whole, high], axis=2).reshape(flat.shape[0], -1)


def slope_of(value):
    sigma = jax.nn.sigmoid(value)
    return sigma + value * sigma * (1.0 - sigma)


def put_windows(wide_ref, windows, planes, rows, depth):
    wide = wide_ref[...]
    width, extent = wide.shape
    place = lax.broadcasted_iota(jnp.int32, (width, extent), 1) % depth
    loose = wide.astype(jnp.float32)
    before = jnp.where(place == 0, 0.0, pltpu.roll(loose, 1, 1)).astype(jnp.bfloat16)
    after = jnp.where(place == depth - 1, 0.0, pltpu.roll(loose, extent - 1, 1)).astype(jnp.bfloat16)
    size = rows * depth
    for third, moved in enumerate((before, wide, after)):
        for first in range(3):
            for second in range(3):
                at = (first * 9 + second * 3 + third) * width
                for plane in range(planes):
                    begin = ((plane + first) * (rows + 2) + second) * depth
                    windows[at : at + width, plane * size : (plane + 1) * size] = moved[
                        :, begin : begin + size
                    ]


def dot_rows(left, right):
    return lax.dot_general(
        left, right, (((1,), (1,)), ((), ())), preferred_element_type=jnp.float32
    )


def forward_a_kernel(dims, wide_ref, weight_ref, bias_ref, pool_ref, before_ref, pooled_ref, windows):
    planes, rows, depth = dims
    put_windows(wide_ref, windows, *dims)
    before = jnp.dot(weight_ref[...], windows[...], preferred_element_type=jnp.float32)
    before = before + bias_ref[...]
    before_ref[...] = before
    active = before * jax.nn.sigmoid(before)
    size = rows * depth
    for row in range(rows // 2):
        parts = [
            active[:, plane * size + (2 * row + j) * depth : plane * size + (2 * row + j + 1) * depth]
            for plane in range(planes)
            for j in range(2)
        ]
        summed = sum(parts[1:], parts[0])
        paired = jnp.dot(
            summed, pool_ref[...], precision=lax.Precision.HIGHEST, preferred_element_type=jnp.float32
        )
        pooled_ref[:, row * depth // 2 : (row + 1) * depth // 2] = (paired * 0.125).astype(jnp.bfloat16)


def middle_kernel(dims, wide_ref, weight_ref, bias_ref, cot_ref, feat_ref, grad_ref, wb_ref, bb_ref, windows):
    put_windows(wide_ref, windows, *dims)
    before = jnp.dot(weight_ref[...], windows[...], preferred_element_type=jnp.float32)
    before = before + bias_ref[...]
    feat_ref[...] = (before * jax.nn.sigmoid(before)).astype(jnp.bfloat16)
    grad = (cot_ref[...].astype(jnp.float32) * slope_of(before)).astype(jnp.bfloat16)
    grad_ref[...] = grad
    wb_ref[...] = dot_rows(windows[...], grad)
    bb_ref[...] = dot_rows(jnp.ones((8, grad.shape[1]), jnp.bfloat16), grad)


def backward_b_kernel(dims, fine, wide_ref, weight_ref, before_ref, spread_ref, grad_ref, windows):
    put_windows(wide_ref, windows, *dims)
    pooled = jnp.dot(weight_ref[...], windows[...], preferred_element_type=jnp.float32)
    pooled = pooled.astype(jnp.bfloat16)
    planes, rows, depth = fine
    size = rows * depth
    for row in range(rows // 2):
        part = pooled[:, row * depth // 2 : (row + 1) * depth // 2]
        spread = jnp.dot(part, spread_ref[...], preferred_element_type=jnp.float32) * 0.125
        for plane in range(planes):
            for j in range(2):
                begin = plane * size + (2 * row + j) * depth
                slope = slope_of(before_ref[:, begin : begin + depth])
                grad_ref[:, begin : begin + depth] = (spread * slope).astype(jnp.bfloat16)


def weight_a_kernel(dims, wide_ref, grad_ref, wa_ref, ba_ref, windows):
    put_windows(wide_ref, windows, *dims)
    grad = grad_ref[...]
    wa_ref[...] = dot_rows(windows[...], grad)
    ba_ref[...] = dot_rows(jnp.ones((8, grad.shape[1]), jnp.bfloat16), grad)


def backward_a_kernel(dims, wide_ref, weight_ref, out_ref, windows):
    put_windows(wide_ref, windows, *dims)
    out = jnp.dot(weight_ref[...], windows[...], preferred_element_type=jnp.float32)
    out_ref[...] = out.astype(jnp.bfloat16)


def local_kernel(body, outs, windows, flops, *operands):
    moved = sum(x.size * x.dtype.itemsize for x in operands)
    return pl.pallas_call(
        body,
        out_shape=[jax.ShapeDtypeStruct(shape, dtype) for shape, dtype in outs],
        in_specs=[pl.BlockSpec(memory_space=pltpu.VMEM)] * len(operands),
        out_specs=[pl.BlockSpec(memory_space=pltpu.VMEM)] * len(outs),
        scratch_shapes=[pltpu.VMEM(windows, jnp.bfloat16)],
        compiler_params=pltpu.CompilerParams(vmem_limit_bytes=48 * 2**20),
        cost_estimate=pl.CostEstimate(flops=flops, bytes_accessed=moved, transcendentals=0),
    )(*operands)


def partner_of(axis, bit):
    me = lax.axis_index(axis)
    mine = (me // bit) % 2
    return me + bit * (1 - 2 * mine), mine


def sum_kernel(steps, halvings, rows, scales, wa_ref, ba_ref, wb_ref, bb_ref, *rest):
    out_wa, out_ba, out_wb, out_bb, acc, gathered, *scratch = rest
    half, width = wa_ref.shape[0] // 2, wa_ref.shape[1]
    top = wb_ref.shape[0]
    count = len(steps)
    sends = scratch[:count]
    recvs = scratch[count : 2 * count]
    sem_send, sem_recv = scratch[2 * count :]
    partners = [partner_of(axis, bit) for axis, bit in steps]
    barrier = pltpu.get_barrier_semaphore()
    for (axis, _), (partner, _) in zip(steps, partners):
        pl.semaphore_signal(barrier, inc=1, device_id={axis: partner}, device_id_type=MESH)
    acc[:top] = wb_ref[...]
    acc[top : top + half, :width] = wa_ref[:half]
    acc[top : top + half, width:] = wa_ref[half:]
    acc[top + half :] = jnp.zeros((rows - top - half, 128), jnp.float32)
    acc[top + half : top + half + 8, :width] = ba_ref[...]
    acc[top + half + 8 : top + half + 16] = bb_ref[...]
    pl.semaphore_wait(barrier, count)
    offset = 0
    size = rows
    kept = []
    for at, ((axis, _), (partner, mine)) in enumerate(zip(steps, partners)):
        source = acc
        if at < halvings:
            size = size // 2
            away = pl.multiple_of(offset + (1 - mine) * size, 16)
            offset = pl.multiple_of(offset + mine * size, 16)
        else:
            away = offset
        sends[at][...] = source[pl.ds(away, size)].astype(jnp.bfloat16)
        copy = pltpu.make_async_remote_copy(
            src_ref=sends[at],
            dst_ref=recvs[at],
            send_sem=sem_send.at[at],
            recv_sem=sem_recv.at[at],
            device_id={axis: partner},
            device_id_type=MESH,
        )
        copy.start()
        copy.wait()
        if at < halvings:
            acc[pl.ds(offset, size)] = source[pl.ds(offset, size)] + recvs[at][...].astype(jnp.float32)
            kept.append((offset, size))
        else:
            acc[pl.ds(offset, size)] = sends[at][...].astype(jnp.float32) + recvs[at][...].astype(jnp.float32)
    gathered[pl.ds(offset, size)] = acc[pl.ds(offset, size)].astype(jnp.bfloat16)
    for back in range(halvings):
        at = halvings - 1 - back
        begin, extent = kept[at]
        (axis, _), (partner, _) = steps[at], partners[at]
        here = gathered.at[pl.ds(begin, extent)]
        copy = pltpu.make_async_remote_copy(
            src_ref=here,
            dst_ref=here,
            send_sem=sem_send.at[count + back],
            recv_sem=sem_recv.at[count + back],
            device_id={axis: partner},
            device_id_type=MESH,
        )
        copy.start()
        copy.wait()
    scale_a, scale_b = scales
    total = gathered[...].astype(jnp.float32)
    out_wb[...] = total[:top] * scale_b
    out_wa[:half] = total[top : top + half, :width] * scale_a
    out_wa[half:] = total[top : top + half, width:] * scale_a
    out_ba[...] = total[top + half : top + half + 1, :width] * scale_a
    out_bb[...] = total[top + half + 8 : top + half + 9] * scale_b


def summed_grads(wa, ba, wb, bb, scales):
    used = wb.shape[0] + wa.shape[0] // 2 + 16
    rows = used + -used % 128
    cut = {
        axis: [2**i for i in range(lax.axis_size(axis).bit_length() - 1)] for axis in ("gz", "gx", "gy")
    }
    steps = [("gz", bit) for bit in cut["gz"][:1]]
    steps += [("gx", bit) for bit in cut["gx"]] + [("gy", bit) for bit in cut["gy"]]
    steps += [("gz", bit) for bit in cut["gz"][1:]]
    halvings = 0
    sizes = []
    size = rows
    for _ in steps:
        if len(sizes) == halvings and size % 32 == 0:
            size //= 2
            halvings += 1
        sizes.append(size)
    buffers = [pltpu.VMEM((s, 128), jnp.bfloat16) for s in sizes]
    total = len(steps) + halvings
    shapes = [wa.shape, (1, ba.shape[1]), wb.shape, (1, bb.shape[1])]
    return pl.pallas_call(
        functools.partial(sum_kernel, steps, halvings, rows, scales),
        out_shape=[jax.ShapeDtypeStruct(shape, jnp.float32) for shape in shapes],
        in_specs=[pl.BlockSpec(memory_space=pltpu.VMEM)] * 4,
        out_specs=[pl.BlockSpec(memory_space=pltpu.VMEM)] * 4,
        scratch_shapes=[
            pltpu.VMEM((rows, 128), jnp.float32),
            pltpu.VMEM((rows, 128), jnp.bfloat16),
            *buffers,
            *buffers,
            pltpu.SemaphoreType.DMA((total,)),
            pltpu.SemaphoreType.DMA((total,)),
        ],
        compiler_params=pltpu.CompilerParams(collective_id=0, has_side_effects=True),
    )(wa, ba, wb, bb)


def line_ends(axis_sizes):
    across, count = axis_sizes
    total = across * count
    line = lax.axis_index("gx") * count + lax.axis_index("gz")
    after, before = (line + 1) % total, (line + total - 1) % total
    ids = [{"gx": at // count, "gz": at % count} for at in (after, before)]
    return line, total, ids


class Halo:
    def __init__(self, wide, dims, where, sems, at):
        planes, rows, depth = dims
        self.line, self.total, ids = where
        size, stride = rows * depth, (rows + 2) * depth
        spot = lambda plane: wide.at[:, plane * stride + depth : plane * stride + depth + size]
        send, recv = sems
        self.up, self.down = [
            pltpu.make_async_remote_copy(
                src_ref=spot(source),
                dst_ref=spot(target),
                send_sem=send.at[at + i],
                recv_sem=recv.at[at + i],
                device_id=ids[i],
                device_id_type=MESH,
            )
            for i, (source, target) in enumerate(((planes, 0), (1, planes + 1)))
        ]

    def start(self):
        pl.when(self.line < self.total - 1)(self.up.start)
        pl.when(self.line > 0)(self.down.start)

    def wait(self):
        @pl.when(self.line < self.total - 1)
        def _():
            self.up.wait_send()
            self.down.wait_recv()

        @pl.when(self.line > 0)
        def _():
            self.down.wait_send()
            self.up.wait_recv()


class Summing:
    def __init__(self, steps, sizes, acc, gathered, sends, recvs, sems):
        self.steps, self.sizes = steps, sizes
        self.acc, self.gathered, self.sends, self.recvs = acc, gathered, sends, recvs
        self.sems = sems
        self.partners = [partner_of(axis, bit) for axis, bit in steps]
        rows = [acc.shape[0]] + list(sizes)
        self.halvings = sum(a != b for a, b in zip(rows, sizes))
        self.stages = len(steps) + self.halvings
        self.offset = 0
        self.kept = []
        self.flying = None

    def copy(self, stage, source, target, step):
        send, recv = self.sems
        self.flying = pltpu.make_async_remote_copy(
            src_ref=source,
            dst_ref=target,
            send_sem=send.at[stage],
            recv_sem=recv.at[stage],
            device_id={self.steps[step][0]: self.partners[step][0]},
            device_id_type=MESH,
        )
        self.flying.start()

    def start(self, stage):
        if stage < len(self.steps):
            size = self.sizes[stage]
            away = self.offset
            if stage < self.halvings:
                mine = self.partners[stage][1]
                away = pl.multiple_of(self.offset + (1 - mine) * size, 16)
                self.offset = pl.multiple_of(self.offset + mine * size, 16)
                self.kept.append((self.offset, size))
            self.sends[stage][...] = self.acc[pl.ds(away, size)].astype(jnp.bfloat16)
            self.copy(stage, self.sends[stage], self.recvs[stage], stage)
        else:
            step = self.halvings - 1 - (stage - len(self.steps))
            begin, size = self.kept[step]
            here = self.gathered.at[pl.ds(begin, size)]
            self.copy(stage, here, here, step)

    def finish(self, stage):
        self.flying.wait()
        if stage >= len(self.steps):
            return
        here = pl.ds(self.offset, self.sizes[stage])
        came = self.recvs[stage][...].astype(jnp.float32)
        own = self.acc[here] if stage < self.halvings else self.sends[stage][...].astype(jnp.float32)
        total = own + came
        if stage == len(self.steps) - 1:
            self.gathered[here] = total.astype(jnp.bfloat16)
        else:
            self.acc[here] = total


def place(wide, flat, dims):
    planes, rows, depth = dims
    size, stride = rows * depth, (rows + 2) * depth
    for plane in range(planes):
        begin = (plane + 1) * stride + depth
        wide[:, begin : begin + size] = flat[:, plane * size : (plane + 1) * size]


def whole_kernel(setting, *refs):
    fine, coarse, sizes_line, steps, cuts_a, cuts_b, scales = setting
    slab, w_a, b_a, pool, w_b, b_b, cot, v_b, spread, v_a = refs[:10]
    features, grad_slab, out_wa, out_ba, out_wb, out_bb = refs[10:16]
    wide_a, wide_b, wide_gb, wide_ga, win_a, win_b, win_gb, win_ga = refs[16:24]
    before_a, pooled, grad_b, grad_a, acc_a, acc_b, all_a, all_b = refs[24:32]
    count = len(steps)
    send_a, recv_a, send_b, recv_b = [refs[32 + i * count : 32 + (i + 1) * count] for i in range(4)]
    sems = refs[32 + 4 * count :]
    where = line_ends(sizes_line)
    line, total, ids = where
    barrier = pltpu.get_barrier_semaphore()
    for wide in (wide_a, wide_b, wide_gb, wide_ga):
        wide[...] = jnp.zeros_like(wide)
    place(wide_a, slab, fine)
    for axis, bit in steps:
        partner, _ = partner_of(axis, bit)
        pl.semaphore_signal(barrier, inc=1, device_id={axis: partner}, device_id_type=MESH)
    for device in ids:
        pl.semaphore_signal(barrier, inc=1, device_id=device, device_id_type=MESH)
    pl.semaphore_wait(barrier, count + 2)
    halos = [
        Halo(wide, dims, where, sems[:2], 2 * i)
        for i, (wide, dims) in enumerate(
            ((wide_a, fine), (wide_b, coarse), (wide_gb, coarse), (wide_ga, fine))
        )
    ]
    sum_a = Summing(steps, cuts_a, acc_a, all_a, send_a, recv_a, sems[2:4])
    sum_b = Summing(steps, cuts_b, acc_b, all_b, send_b, recv_b, sems[4:6])

    halos[0].start()
    halos[0].wait()
    forward_a_kernel(fine, wide_a, w_a, b_a, pool, before_a, pooled, win_a)
    place(wide_b, pooled, coarse)
    halos[1].start()
    halos[1].wait()
    top_b = out_wb.shape[0]
    middle_kernel(
        coarse, wide_b, w_b, b_b, cot, features, grad_b, acc_b.at[:top_b], acc_b.at[top_b : top_b + 8], win_b
    )
    place(wide_gb, grad_b, coarse)
    halos[2].start()
    acc_b[top_b + 8 :] = jnp.zeros((acc_b.shape[0] - top_b - 8, acc_b.shape[1]), jnp.float32)
    sum_b.start(0)
    halos[2].wait()
    backward_b_kernel(coarse, fine, wide_gb, v_b, before_a, spread, grad_a, win_gb)
    place(wide_ga, grad_a, fine)
    halos[3].start()
    sum_b.finish(0)
    sum_b.start(1)
    grad = grad_a[...]
    half, width = out_wa.shape[0] // 2, out_wa.shape[1]
    acc_a[:half, :width] = dot_rows(win_a[:half], grad)
    acc_a[:half, width:] = dot_rows(win_a[half:], grad)
    acc_a[half:] = jnp.zeros((acc_a.shape[0] - half, acc_a.shape[1]), jnp.float32)
    acc_a[half : half + 8, :width] = dot_rows(jnp.ones((8, grad.shape[1]), jnp.bfloat16), grad)
    sum_b.finish(1)
    sum_b.start(2)
    sum_a.start(0)
    halos[3].wait()
    backward_a_kernel(fine, wide_ga, v_a, grad_slab, win_ga)
    for stage in range(max(sum_a.stages, sum_b.stages - 2)):
        if stage + 2 < sum_b.stages:
            sum_b.finish(stage + 2)
            if stage + 3 < sum_b.stages:
                sum_b.start(stage + 3)
        if stage < sum_a.stages:
            sum_a.finish(stage)
            if stage + 1 < sum_a.stages:
                sum_a.start(stage + 1)
    scale_a, scale_b = scales
    out_wb[...] = all_b[:top_b].astype(jnp.float32) * scale_b
    out_bb[...] = all_b[top_b : top_b + 16].astype(jnp.float32)[:1] * scale_b
    out_wa[:half] = all_a[:half, :width].astype(jnp.float32) * scale_a
    out_wa[half:] = all_a[:half, width:].astype(jnp.float32) * scale_a
    out_ba[...] = all_a[half : half + 16, :width].astype(jnp.float32)[:1] * scale_a


def stage_sizes(rows, steps):
    sizes = []
    for _ in steps:
        halve = rows % 32 == 0 and len(sizes) < 3
        rows = rows // 2 if halve else rows
        sizes.append(rows)
    return sizes


def all_steps():
    cut = {
        axis: [2**i for i in range(lax.axis_size(axis).bit_length() - 1)] for axis in ("gz", "gx", "gy")
    }
    steps = [("gz", bit) for bit in cut["gz"][:1]]
    steps += [("gx", bit) for bit in cut["gx"]] + [("gy", bit) for bit in cut["gy"]]
    return steps + [("gz", bit) for bit in cut["gz"][1:]]


def between_exchanges(fine, coarse, scales, slab, weight_a, bias_a, weight_b, bias_b, cot, pool):
    f32, bf16 = jnp.float32, jnp.bfloat16
    c1, cells = slab.shape
    c2, c3 = weight_b.shape[3:]
    fewer = cells // 8
    steps = all_steps()
    rows_a = 27 * c1 // 2 + 16
    rows_a += -rows_a % 128
    rows_b = 27 * c2 + 16
    rows_b += -rows_b % 128
    cuts_a, cuts_b = stage_sizes(rows_a, steps), stage_sizes(rows_b, steps)
    extent = lambda dims: (dims[0] + 2) * (dims[1] + 2) * dims[2]
    setting = (fine, coarse, (lax.axis_size("gx"), lax.axis_size("gz")), steps, cuts_a, cuts_b, scales)
    buffers = [pltpu.VMEM((n, 128), bf16) for cuts in (cuts_a, cuts_a, cuts_b, cuts_b) for n in cuts]
    outs = [
        ((c3, fewer), bf16),
        ((c1, cells), bf16),
        ((27 * c1, c2), f32),
        ((1, c2), f32),
        ((27 * c2, c3), f32),
        ((1, c3), f32),
    ]
    operands = (
        slab,
        outward(weight_a),
        bias_a[:, None],
        pool,
        outward(weight_b),
        bias_b[:, None],
        cot,
        inward(weight_b),
        pool.T.astype(bf16),
        inward(weight_a),
    )
    most = 2 * len(steps)
    return pl.pallas_call(
        functools.partial(whole_kernel, setting),
        out_shape=[jax.ShapeDtypeStruct(shape, dtype) for shape, dtype in outs],
        in_specs=[pl.BlockSpec(memory_space=pltpu.VMEM)] * len(operands),
        out_specs=[pl.BlockSpec(memory_space=pltpu.VMEM)] * len(outs),
        scratch_shapes=[
            pltpu.VMEM((c1, extent(fine)), bf16),
            pltpu.VMEM((c2, extent(coarse)), bf16),
            pltpu.VMEM((c3, extent(coarse)), bf16),
            pltpu.VMEM((c2, extent(fine)), bf16),
            pltpu.VMEM((27 * c1, cells), bf16),
            pltpu.VMEM((27 * c2, fewer), bf16),
            pltpu.VMEM((27 * c3, fewer), bf16),
            pltpu.VMEM((27 * c2, cells), bf16),
            pltpu.VMEM((c2, cells), f32),
            pltpu.VMEM((c2, fewer), bf16),
            pltpu.VMEM((c3, fewer), bf16),
            pltpu.VMEM((c2, cells), bf16),
            pltpu.VMEM((rows_a, 128), f32),
            pltpu.VMEM((rows_b, 128), f32),
            pltpu.VMEM((rows_a, 128), bf16),
            pltpu.VMEM((rows_b, 128), bf16),
            *buffers,
            pltpu.SemaphoreType.DMA((8,)),
            pltpu.SemaphoreType.DMA((8,)),
            *[pltpu.SemaphoreType.DMA((most,))] * 4,
        ],
        compiler_params=pltpu.CompilerParams(
            collective_id=1, has_side_effects=True, vmem_limit_bytes=60 * 2**20
        ),
    )(*operands)


def outward(weight):
    return weight.reshape(-1, weight.shape[-1]).T


def inward(weight):
    taps = weight[::-1, ::-1, ::-1].reshape(27, *weight.shape[3:])
    return jnp.transpose(taps, (1, 0, 2)).reshape(weight.shape[3], -1)


def lanes_of(shape):
    return lax.broadcasted_iota(jnp.int32, shape, len(shape) - 1)


def rows_of(shape):
    return lax.broadcasted_iota(jnp.int32, shape, 0)


def ones_where(mask):
    return jnp.where(mask, 1.0, 0.0).astype(jnp.bfloat16)


def dot(left, right):
    return jnp.dot(left, right, preferred_element_type=jnp.float32)


def by_parts(rank_bits, mask):
    place = {}
    for at, (axis, bit) in enumerate(rank_bits):
        if mask >> at & 1:
            me = place.get(axis, lax.axis_index(axis))
            place[axis] = me + bit * (1 - 2 * ((lax.axis_index(axis) // bit) % 2))
    return place


def own_rank(rank_bits, mask=0):
    total = 0
    for at, (axis, bit) in enumerate(rank_bits):
        mine = (lax.axis_index(axis) // bit) % 2
        total = total + ((1 - mine) if mask >> at & 1 else mine) * 2**at
    return total


def remote(source, target, sems, at, device, sent_at=None):
    return pltpu.make_async_remote_copy(
        src_ref=source,
        dst_ref=target,
        send_sem=sems[0].at[at if sent_at is None else sent_at],
        recv_sem=sems[1].at[at],
        device_id=device,
        device_id_type=MESH,
    )


def flipped_bits(bits, mask):
    return tuple(bit for at, bit in enumerate(bits) if mask >> at & 1)


class Reduction:
    def __init__(self, groups, exchanged, acc, summed, sends, recvs, sems):
        self.groups, self.exchanged, self.acc, self.summed = groups, exchanged, acc, summed
        self.sends, self.recvs, self.sems = sends, recvs, sems
        self.offset, self.size = 0, acc.shape[0]
        self.parts = []
        self.all = None
        self.stage = 0
        bits = sum(groups[:-1] if exchanged else groups, [])
        self.levels = [level for level in reversed(all_groups()) if level[0] in bits]
        self.stages = len(groups) + len(self.levels)
        self.used = len(groups)
        self.places = {}
        self.sent = 0

    def fly(self, source, target, device):
        remote(source, target, self.sems, self.stage, device).start()

    def piece(self, flipped, level, mask, arrived):
        key = (flipped, level, mask if level == 0 else 0)
        if level + 1 == len(self.levels):
            key = level
        if key not in self.places:
            self.places[key] = self.used
            self.used += 1
        whose = flipped + flipped_bits(self.levels[level], mask) if arrived else flipped
        offset = 0
        for bits, part in self.parts:
            turned = sum(1 << at for at, bit in enumerate(bits) if bit in whose)
            offset = offset + own_rank(bits, turned) * part
        here = self.summed.at[pl.ds(pl.multiple_of(offset, 8), self.size)]
        device = by_parts(self.levels[level], mask)
        return remote(here, here, self.sems, self.places[key], device, len(self.groups))

    def pieces(self, count, at):
        here = self.summed.at[: count * self.size]
        return remote(here, here, self.sems, at, by_parts(self.levels[-1], 1), len(self.groups))

    def pass_on(self, flipped, first):
        for level in range(first, len(self.levels)):
            for mask in range(1, 2 ** len(self.levels[level])):
                self.piece(flipped, level, mask, False).start()
                self.sent += 1

    def start(self):
        at = self.stage
        count = len(self.groups)
        if at > count:
            return
        if at == count:
            self.known = [()]
            self.pass_on((), 0)
        elif self.exchanged and at == count - 1:
            bits = self.groups[at]
            recv = self.recvs[at]
            mine = own_rank(bits)
            recv[mine] = self.acc[pl.ds(self.offset, self.size)].astype(jnp.bfloat16)
            for mask in range(1, 2 ** len(bits)):
                self.fly(recv.at[mine], recv.at[mine], by_parts(bits, mask))
            rest = recv.at[: recv.shape[0] - 1]
            self.all = remote(rest, rest, self.sems, at, by_parts(bits, 1))
        else:
            bits = self.groups[at]
            members = 2 ** len(bits)
            part = self.size // members
            send, recv = self.sends[at], self.recvs[at]
            send[...] = self.acc[pl.ds(self.offset, self.size)].astype(jnp.bfloat16)
            for mask in range(1, members):
                begin = pl.multiple_of(own_rank(bits, mask) * part, 8)
                self.fly(send.at[pl.ds(begin, part)], recv.at[mask - 1], by_parts(bits, mask))
            self.all = remote(recv, recv, self.sems, at, by_parts(bits, 1))
            self.parts.append((bits, part))
            self.offset = pl.multiple_of(self.offset + own_rank(bits) * part, 8)
            self.size = part

    def finish(self):
        at = self.stage
        count = len(self.groups)
        if at >= count:
            level = at - count
            if level + 1 == len(self.levels):
                self.stage += 1
                self.pieces(len(self.known) * (2 ** len(self.levels[level]) - 1), self.places[level]).wait_recv()
                self.pieces(self.sent, 0).wait_send()
                return
            for _ in self.arrivals():
                pass
            return
        self.stage += 1
        self.all.wait()
        recv = self.recvs[at]
        here = pl.ds(self.offset, self.size)
        if self.exchanged and at == count - 1:
            total = recv[0].astype(jnp.float32)
            for i in range(1, recv.shape[0]):
                total = total + recv[i].astype(jnp.float32)
        else:
            total = self.acc[here]
            for i in range(recv.shape[0]):
                total = total + recv[i].astype(jnp.float32)
        if at == count - 1:
            self.summed[here] = total.astype(jnp.bfloat16)
        else:
            self.acc[here] = total

    def arrivals(self):
        level = self.stage - len(self.groups)
        came = []
        for flipped in self.known:
            members = 2 ** len(self.levels[level])
            if level:
                self.pieces(members - 1, self.places[(flipped, level, 0)]).wait_recv()
            for mask in range(1, members):
                if not level:
                    self.piece(flipped, level, mask, True).wait_recv()
                whose = flipped + flipped_bits(self.levels[level], mask)
                self.pass_on(whose, level + 1)
                came.append(whose)
                yield
        self.known = self.known + came
        self.stage += 1

    def step(self):
        self.finish()
        if self.stage < self.stages:
            self.start()


class Border:
    def __init__(self, first, last, edge, inbox, sems, at):
        me, count = lax.axis_index("gz"), lax.axis_size("gz")
        side = 1 - lax.axis_index("gx")
        self.inner, self.outer = me > 0, me < count - 1
        up, down = (me + 1) % count, (me + count - 1) % count
        low, high, beside, beside_low, beside_high = inbox
        self.always = remote(edge, beside, sems, at + 2, {"gx": side})
        self.up = [
            remote(last, low, sems, at, {"gz": up}),
            remote(edge, beside_low, sems, at + 3, {"gx": side, "gz": up}),
        ]
        self.down = [
            remote(first, high, sems, at + 1, {"gz": down}),
            remote(edge, beside_high, sems, at + 4, {"gx": side, "gz": down}),
        ]

    def start(self):
        @pl.when(self.outer)
        def _():
            self.up[1].start()

        @pl.when(self.inner)
        def _():
            self.down[1].start()

        self.always.start()

        @pl.when(self.outer)
        def _():
            self.up[0].start()

        @pl.when(self.inner)
        def _():
            self.down[0].start()

    def wait(self):
        self.always.wait()

        @pl.when(self.outer)
        def _():
            for copy in self.up:
                copy.wait_send()
            for copy in self.down:
                copy.wait_recv()

        @pl.when(self.inner)
        def _():
            for copy in self.down:
                copy.wait_send()
            for copy in self.up:
                copy.wait_recv()


def gathered_edge(tiles, extent, slots):
    shape = tiles[0].shape
    lane = lanes_of(shape)
    high = lax.axis_index("gx") == 0
    edge = jnp.where(high, extent - 1, 0)
    at_edge = lane & (extent - 1) == edge
    total = None
    for i, tile in enumerate(tiles):
        kept = rolled(jnp.where(at_edge, tile, 0.0), i % slots)
        total = kept if total is None else total + kept
    back = pltpu.roll(total, 128 - (extent - 1), 1)
    return jnp.where(high, back, total)


def rolled(value, by):
    by = by % 128
    return pltpu.roll(value, by, 1) if by else value


def quarters(edge):
    size = edge.shape[0] // 4
    return sum(rolled(edge[q * size : (q + 1) * size], 4 * q) for q in range(4))


def spread_edge(edge, by, packed):
    if not packed:
        return rolled(edge, by)
    return jnp.concatenate([rolled(edge, by - 4 * q) for q in range(4)], axis=0)


def halved(tile, low):
    size = tile.shape[0] // 2
    lane = lanes_of((size, 128))
    upper, lower = tile[:size], rolled(tile[size:], 64)
    return jnp.where(lane < 64, upper, lower) if low else jnp.where(lane < 64, lower, upper)


def beside(tile, edges, extent, packed):
    low_edge, high_edge, at = edges
    lane = lanes_of(tile.shape) & (extent - 1)
    before = jnp.where(lane == 0, spread_edge(low_edge, -at, packed), rolled(tile, 1))
    after = jnp.where(lane == extent - 1, spread_edge(high_edge, extent - 1 - at, packed), rolled(tile, -1))
    return before, after


def sided(edge):
    high = lax.axis_index("gx") == 0
    zero = jnp.zeros_like(edge)
    return jnp.where(high, zero, edge), jnp.where(high, edge, zero)


def moved_rows(pair, stride):
    lane = lanes_of(pair[0].shape)
    down = [rolled(tile, stride) for tile in pair]
    up = [rolled(tile, -stride) for tile in pair]
    low = lane < stride
    high = lane < 128 - stride
    zero = jnp.zeros_like(pair[0])
    before = (jnp.where(low, zero, down[0]), jnp.where(low, down[0], down[1]))
    after = (jnp.where(high, up[0], up[1]), jnp.where(high, up[1], zero))
    return before, after


def put_rows(windows, pair, begin, plane, size):
    before, after = moved_rows(pair, 32)
    for ky, tiles in enumerate((before, pair, after)):
        for g, tile in enumerate(tiles):
            lane = plane * 256 + g * 128
            windows[begin + ky * size : begin + (ky + 1) * size, lane : lane + 128] = tile


def moved_half(tile, stride):
    lane = lanes_of(tile.shape) & 63
    zero = jnp.zeros_like(tile)
    before = jnp.where(lane < stride, zero, rolled(tile, stride))
    after = jnp.where(lane < 64 - stride, rolled(tile, -stride), zero)
    return before, after


def inbox_values(inbox):
    low, high, across, across_low, across_high = [ref[...] for ref in inbox]
    return low, high, sided(across), sided(across_low), sided(across_high)


def fine_planes(read, inbox, planes):
    low, high, across, across_low, across_high = inbox_values(inbox)
    for p in range(planes + 2):
        if p == 0:
            pair, edge, at = (low[:, :128], low[:, 128:]), across_low, 2 * (planes - 1)
        elif p == planes + 1:
            pair, edge, at = (high[:, :128], high[:, 128:]), across_high, 0
        else:
            pair, edge, at = read(p - 1), across, 2 * (p - 1)
        sides = [beside(tile, (*edge, at + g), 32, False) for g, tile in enumerate(pair)]
        yield p, ((sides[0][0], sides[1][0]), pair, (sides[0][1], sides[1][1]))


def coarse_tiles(field, inbox, tiles):
    low, high, across, across_low, across_high = inbox_values(inbox)
    low = jnp.concatenate([low, rolled(low, 64)], axis=0)
    high = jnp.concatenate([high, rolled(high, 64)], axis=0)
    half = lanes_of(low.shape) < 64
    for t in range(tiles):
        tile = field[:, t * 128 : (t + 1) * 128]
        sides = list(beside(tile, (*across, t % 4), 16, True))
        if t == 0:
            sides_low = beside(low, (*across_low, (tiles - 1) % 4), 16, True)
            tile = jnp.where(half, low, tile)
            sides = [jnp.where(half, a, b) for a, b in zip(sides_low, sides)]
        if t == tiles - 1:
            sides_high = beside(high, (*across_high, 0), 16, True)
            tile = jnp.where(half, tile, high)
            sides = [jnp.where(half, b, a) for a, b in zip(sides_high, sides)]
        yield t, (sides[0], tile, sides[1])


def column(row, size):
    wide = jnp.broadcast_to(row, (size, size))
    eye = rows_of((size, size)) == lanes_of((size, size))
    return jnp.sum(jnp.where(eye, wide, 0.0), axis=1, keepdims=True)


def joined_thirds(terms, tiles):
    half = None
    low = [rolled(terms(0, t), 64) for t in range(tiles)]
    high = [rolled(terms(2, t), 64) for t in range(tiles)]
    out = []
    for t in range(tiles):
        if half is None:
            half = lanes_of(low[0].shape) < 64
        before, after = low[max(t - 1, 0)], high[min(t + 1, tiles - 1)]
        out.append(terms(1, t) + jnp.where(half, before + high[t], low[t] + after))
    return out


def block_kernel(setting, *refs):
    groups, groups_a, cuts = setting
    inputs = refs[:6]
    features, grad_in, sum_a, sum_b = refs[6:10]
    volume, w_a, b_a, w_b, b_b, cot = refs[10:16]
    (
        stage, own_a, windows_a, sums_a, slope_a, halves, pooled, windows_b, sums_b,
        cot_sent, cot_came, cot_here, grad_b, lines_b, sums_gb, grads_a, lines_a, sums_ga,
        feat_sent, feat_came, mat_a, mat_b, mat_ga, mat_gb, near, far, pool, acc_a, acc_b,
    ) = refs[16:45]
    rest = list(refs[45:])
    inboxes = [[rest.pop(0) for _ in range(5)] for _ in range(4)]
    edges = [rest.pop(0) for _ in range(4)]
    ends_b, ends_gb = [[rest.pop(0), rest.pop(0)] for _ in range(2)]
    count = len(groups)
    takes = lambda n: [rest.pop(0) for _ in range(n)]
    send_a, recv_a = takes(1), takes(2)
    send_b, recv_b, send_c, recv_c = [takes(count) for _ in range(4)]
    sems_halo, sems_cot, sems_feat, sems_a, sems_b, sems_c = [takes(2) for _ in range(6)]
    (sems_in,) = rest
    f32, bf16 = jnp.float32, jnp.bfloat16
    c1, rows, planes, width = volume.shape
    c2, c3 = w_a.shape[2], w_b.shape[2]
    tiles = planes // 4 + 1
    me, members = lax.axis_index("gz"), lax.axis_size("gz")
    whole = [bit for group in groups for bit in group]
    line = [bit for bit in whole if bit[0] == "gz"]

    apart = me < members
    barrier = pltpu.get_barrier_semaphore()
    for mask in range(1, 2 ** len(whole)):
        pl.semaphore_signal(barrier, inc=1, device_id=by_parts(whole, mask), device_id_type=MESH)
    loads = {
        at: pltpu.make_async_copy(inputs[at], refs[10 + at], sems_in.at[at]) for at in range(1, len(inputs))
    }
    parts = 4
    share = c1 // parts
    loads_v = [
        pltpu.make_async_copy(
            inputs[0].at[i * share : (i + 1) * share],
            volume.at[i * share : (i + 1) * share],
            sems_in.at[0],
        )
        for i in range(parts)
    ]
    for load in loads_v:
        load.start()
    for at in (5, 1, 3, 2, 4):
        loads[at].start()

    @pl.when(me == 0)
    def _():
        for inbox in inboxes:
            for box in (inbox[0], inbox[3]):
                box[...] = jnp.zeros_like(box)

    @pl.when(me == members - 1)
    def _():
        for inbox in inboxes:
            for box in (inbox[1], inbox[4]):
                box[...] = jnp.zeros_like(box)

    r, l = rows_of(far.shape), lanes_of(far.shape)
    far[...] = ones_where(((r >> 3) & 3 == l >> 7) & (((r >> 5) << 3) + (r & 7) == l & 127))
    r, l = rows_of(near.shape), lanes_of(near.shape)
    near[...] = ones_where(
        ((r & 7) + 1 == l >> 6) & ((r >> 3) & 3 == (l >> 4) & 3) & (r >> 5 == l & 15)
    )
    r, l = rows_of((512, 128)), lanes_of((512, 128))
    pool[...] = ones_where(
        (r >> 8 == l >> 6) & ((r >> 6) & 3 == (l >> 4) & 3) & ((r & 31) >> 1 == l & 15)
    )

    pltpu.make_async_copy(inputs[0], volume, sems_in.at[0]).wait()
    for g in range(2):
        for i in range(4):
            part = volume[:, 4 * g + i].astype(f32).reshape(c1 * planes, width)
            stage[:, width * i : width * (i + 1)] = part
        for z in range(planes):
            tile = stage[pl.ds(z, c1, stride=planes), :]
            own_a[:, z * 256 + g * 128 : z * 256 + (g + 1) * 128] = tile.astype(bf16)

    def read_a(z):
        return tuple(own_a[:, z * 256 + g * 128 : z * 256 + (g + 1) * 128] for g in range(2))

    edges[0][...] = gathered_edge([tile.astype(f32) for z in range(planes) for tile in read_a(z)], 32, 32).astype(bf16)
    pl.semaphore_wait(barrier, 2 ** len(whole) - 1)

    border_a = Border(own_a.at[:, :256], own_a.at[:, (planes - 1) * 256 :], edges[0], inboxes[0], sems_halo, 0)
    border_a.start()

    def exchange(sent, came, sems):
        size = sent.shape[0] // members
        for mask in range(1, members):
            begin = pl.multiple_of(own_rank(line, mask) * size, 16)
            remote(
                sent.at[pl.ds(begin, size)],
                came.at[pl.ds(pl.multiple_of(me * size, 16), size)],
                sems,
                0,
                by_parts(line, mask),
            ).start()
        here = pl.ds(pl.multiple_of(me * size, 16), size)
        came[here] = sent[here]
        most = (members - 1) * size
        return remote(sent.at[:most], came.at[:most], sems, 0, by_parts(line, 1))

    for at in range(1, 5):
        loads[at].wait()

    high = lax.axis_index("gx") == 0
    eye = ones_where(rows_of((c2, c2)) == lanes_of((c2, c2)))
    eye_b = ones_where(rows_of((c3, c3)) == lanes_of((c3, c3)))
    for kz in range(3):
        block = w_a[:].reshape(9, 3, c1, c2)[:, kz].reshape(3, 3 * c1, c2)
        block = jnp.concatenate([block[1], *[jnp.where(high, a, b) for a, b in ((block[0], block[2]), (block[2], block[0]))]], axis=0)
        mat_a[kz * c2 : (kz + 1) * c2] = dot_rows(eye, block).astype(bf16)
        block = w_b[:].reshape(9, 3, c2, c3)[:, kz].reshape(9 * c2, c3)
        mat_b[kz * c3 : (kz + 1) * c3] = dot_rows(eye_b, block).astype(bf16)
        for ky in range(3):
            for kx in range(3):
                tap = ((2 - kx) * 3 + 2 - ky) * 3 + 2 - kz
                at = kz * 3 + ky
                mat_ga[at * c1 : (at + 1) * c1, kx * c2 : (kx + 1) * c2] = w_a[tap]
                mat_gb[at * c2 : (at + 1) * c2, kx * c3 : (kx + 1) * c3] = w_b[tap]
    col_a, col_b = column(b_a[...], c2), column(b_b[...], c3)
    loads[5].wait()
    half_rows = rows // 2
    stage[...] = cot[...].astype(f32)
    spaced = [stage[pl.ds(y, c3, stride=half_rows), :].astype(bf16) for y in range(half_rows)]
    cot_sent[...] = dot_rows(far[...], jnp.concatenate(spaced, axis=1)).astype(bf16)
    cot_flying = exchange(cot_sent, cot_came, sems_cot)
    deep = 3 * c1
    lane = lanes_of((c1, 128)) & 31

    @pl.when(apart)
    def _():
        for p in range(1, planes + 1):
            pair = read_a(p - 1)
            zero = jnp.zeros_like(pair[0])
            before = [jnp.where(lane == 0, zero, rolled(tile, 1)) for tile in pair]
            after = [jnp.where(lane == 31, zero, rolled(tile, -1)) for tile in pair]
            plain = [jnp.where(high, a, b) for a, b in zip(before, after)]
            met = [jnp.where(high, b, a) for a, b in zip(before, after)]
            put_rows(windows_a, pair, 0, p, c1)
            put_rows(windows_a, plain, deep, p, c1)
            for g in range(2):
                windows_a[2 * deep + c1 : 2 * deep + 2 * c1, p * 256 + g * 128 : p * 256 + (g + 1) * 128] = met[g]
            if p % 2 == 0:
                here = slice((p - 1) * 256, (p + 1) * 256)
                sums_a[:, here] = dot(mat_a[:, : 2 * deep], windows_a[: 2 * deep, here])

    halves[...] = jnp.zeros_like(halves)
    for kz in range(3):
        for p in range(planes + 2):
            if not 0 <= p + kz - 2 < planes:
                grads_a[kz * c2 : (kz + 1) * c2, p * 256 : (p + 1) * 256] = jnp.zeros((c2, 256), bf16)
    acc_a[...] = jnp.zeros_like(acc_a)
    border_a.wait()

    @pl.when(apart)
    def _():
        boxes = [ref[...] for ref in inboxes[0]]
        turned = [jnp.where(high, rolled(edge, 31), edge) for edge in boxes[2:]]
        for p in range(planes + 2):
            if 0 < p <= planes:
                edge, at = turned[0], 2 * (p - 1)
                pair = [
                    windows_a[2 * deep + c1 : 2 * deep + 2 * c1, p * 256 + g * 128 : p * 256 + (g + 1) * 128]
                    for g in range(2)
                ]
            else:
                edge, at = (turned[2], 0) if p else (turned[1], 2 * (planes - 1))
                tiles_p = [boxes[1 if p else 0][:, g * 128 : (g + 1) * 128] for g in range(2)]
                zero = jnp.zeros_like(tiles_p[0])
                before = [jnp.where(lane == 0, zero, rolled(tile, 1)) for tile in tiles_p]
                after = [jnp.where(lane == 31, zero, rolled(tile, -1)) for tile in tiles_p]
                put_rows(windows_a, tiles_p, 0, p, c1)
                put_rows(windows_a, [jnp.where(high, a, b) for a, b in zip(before, after)], deep, p, c1)
                pair = [jnp.where(high, b, a) for a, b in zip(before, after)]
            side = jnp.where(high, 31, 0)
            pair = [jnp.where(lane == side, rolled(edge, -at - g), tile) for g, tile in enumerate(pair)]
            put_rows(windows_a, pair, 2 * deep, p, c1)
            here = slice((p - 1) * 256, (p + 1) * 256)
            if p == 0 or p == planes + 1:
                here = slice(p * 256, (p + 1) * 256)
                sums_a[:, here] = dot(mat_a[...], windows_a[:, here])
            elif p % 2 == 0:
                sums_a[:, here] = sums_a[:, here] + dot(mat_a[:, 2 * deep :], windows_a[2 * deep :, here])

    @pl.when(apart)
    def _():
        for z in range(planes):
            value = (
                sums_a[:c2, z * 256 : (z + 1) * 256]
                + sums_a[c2 : 2 * c2, (z + 1) * 256 : (z + 2) * 256]
                + sums_a[2 * c2 :, (z + 2) * 256 : (z + 3) * 256]
                + col_a
            )
            sigma = jax.nn.sigmoid(value)
            active = value * sigma
            slope_a[:, z * 256 : (z + 1) * 256] = (sigma + active * (1.0 - sigma)) * 0.125
            if z % 2:
                active = active + kept
                pz = z // 2 + 1
                upper = active.astype(bf16)
                lower = (active - upper.astype(f32)).astype(bf16)
                at, lane = pz // 2 * c2, pz % 2 * 256
                halves[at : at + c2, lane : lane + 256] = upper
                halves[tiles * c2 + at : tiles * c2 + at + c2, lane : lane + 256] = lower
                if pz % 2 or z == planes - 1:
                    low_at = tiles * c2 + at
                    both = dot(halves[at : at + c2], pool[...]) + dot(halves[low_at : low_at + c2], pool[...])
                    pooled[:, pz // 2 * 128 : (pz // 2 + 1) * 128] = (both * 0.125).astype(bf16)
            else:
                kept = active

    def coarse_border(field, edge, ends, inbox, at):
        parts = [field[:, t * 128 : (t + 1) * 128].astype(f32) for t in range(tiles)]
        edge[...] = quarters(gathered_edge(parts, 16, 4)).astype(bf16)
        ends[0][...] = halved(parts[0], False).astype(bf16)
        ends[1][...] = halved(parts[-1], True).astype(bf16)
        return Border(ends[0], ends[1], edge, inbox, sems_halo, at)

    border_b = coarse_border(pooled, edges[1], ends_b, inboxes[1], 5)
    border_b.start()
    cot_flying.wait()
    came = jnp.transpose(cot_came[...].astype(f32)).astype(bf16)
    cot_here[...] = dot(came, near[...])
    border_b.wait()

    @pl.when(apart)
    def _():
        for t, thirds in coarse_tiles(pooled, inboxes[1], tiles):
            for kx, tile in enumerate(thirds):
                before, after = moved_half(tile, 16)
                for ky, value in enumerate((before, tile, after)):
                    at = (kx * 3 + ky) * c2
                    windows_b[at : at + c2, t * 128 : (t + 1) * 128] = value.astype(bf16)
            if t % 2 or t == tiles - 1:
                here = slice(t // 2 * 256, (t + 1) * 128)
                sums_b[:, here] = dot(mat_b[...], windows_b[:, here])

    joined = joined_thirds(lambda k, t: sums_b[k * c3 : (k + 1) * c3, t * 128 : (t + 1) * 128], tiles)
    feats = []
    for t, value in enumerate(joined):
        value = value + col_b
        sigma = jax.nn.sigmoid(value)
        active = value * sigma
        feats.append(active.astype(bf16))
        slope = sigma + active * (1.0 - sigma)
        grad = cot_here[:, t * 128 : (t + 1) * 128] * slope
        grad_b[c3 : 2 * c3, t * 128 : (t + 1) * 128] = grad.astype(bf16)
    own_gb = grad_b.at[c3 : 2 * c3]
    border_gb = coarse_border(own_gb, edges[2], ends_gb, inboxes[2], 10)
    border_gb.start()

    half = lanes_of((c3, 128)) < 64
    turned = [rolled(own_gb[:, t * 128 : (t + 1) * 128].astype(f32), 64) for t in range(tiles)]
    zero = jnp.zeros_like(turned[0])
    for t in range(tiles):
        later = turned[t + 1] if t + 1 < tiles else zero
        earlier = turned[t - 1] if t else zero
        here = slice(t * 128, (t + 1) * 128)
        grad_b[:c3, here] = jnp.where(half, turned[t], later).astype(bf16)
        grad_b[2 * c3 :, here] = jnp.where(half, earlier, turned[t]).astype(bf16)
    top = 27 * c2

    def sum_terms(first, last):
        terms = dot_rows(windows_b[first * c2 : last * c2], grad_b[...])
        for at in range(first, last):
            for kz in range(3):
                tap = at * 3 + kz
                acc_b[tap * c2 : (tap + 1) * c2] = terms[
                    (at - first) * c2 : (at - first + 1) * c2, kz * c3 : (kz + 1) * c3
                ]

    cut = cuts[0]
    early = -(-cut // (3 * c2))
    pl.when(apart)(functools.partial(sum_terms, 0, early))
    total_b = Reduction(groups, False, acc_b.at[:cut], sum_b.at[:cut], send_b, recv_b, sems_b)
    total_b.start()
    pl.when(apart)(functools.partial(sum_terms, early, 9))
    acc_b[top:] = jnp.zeros((acc_b.shape[0] - top, c3), f32)
    acc_b[top : top + 8] = dot_rows(jnp.ones((8, tiles * 128), bf16), own_gb[...])
    total_c = Reduction(groups, False, acc_b.at[cut:], sum_b.at[cut:], send_c, recv_c, sems_c)
    total_c.start()
    total_b.step()
    total_c.step()
    border_gb.wait()

    @pl.when(apart)
    def _():
        for t, thirds in coarse_tiles(own_gb, inboxes[2], tiles):
            for kx, tile in enumerate(thirds):
                lines_b[kx * c3 : (kx + 1) * c3, t * 128 : (t + 1) * 128] = tile.astype(bf16)
            if t % 2 or t == tiles - 1:
                here = slice(t // 2 * 256, (t + 1) * 128)
                sums_gb[:, here] = dot(mat_gb[...], lines_b[:, here])

    by_row = [
        joined_thirds(
            lambda k, t: sums_gb[(k * 3 + ky) * c2 : (k * 3 + ky + 1) * c2, t * 128 : (t + 1) * 128], tiles
        )
        for ky in range(3)
    ]
    small = []
    for t in range(tiles):
        value = by_row[1][t] + moved_half(by_row[0][t], 16)[0] + moved_half(by_row[2][t], 16)[1]
        small.append(value.astype(bf16))
    spread = dot_rows(jnp.concatenate(small, axis=0), pool[...])
    for z in range(planes):
        pz = z // 2 + 1
        large = spread[pz // 2 * c2 : (pz // 2 + 1) * c2, pz % 2 * 256 : (pz % 2 + 1) * 256]
        grad = (large * slope_a[:, z * 256 : (z + 1) * 256]).astype(bf16)
        for kz in range(3):
            grads_a[kz * c2 : (kz + 1) * c2, (z + kz) * 256 : (z + kz + 1) * 256] = grad

    own_ga = grads_a.at[c2 : 2 * c2]

    def read_ga(z):
        return tuple(
            own_ga[:, (z + 1) * 256 + g * 128 : (z + 1) * 256 + (g + 1) * 128] for g in range(2)
        )

    edges[3][...] = gathered_edge([tile.astype(f32) for z in range(planes) for tile in read_ga(z)], 32, 32).astype(bf16)
    border_ga = Border(
        own_ga.at[:, 256:512], own_ga.at[:, planes * 256 : (planes + 1) * 256], edges[3], inboxes[3], sems_halo, 15
    )
    border_ga.start()

    @pl.when(apart)
    def _():
        top_a = 9 * c1 + 9 * c1 // 2
        terms = dot_rows(windows_a[...], grads_a[...])
        near_x, far_x = terms[deep : 2 * deep], terms[2 * deep :]
        terms = jnp.concatenate(
            [jnp.where(high, near_x, far_x), terms[:deep], jnp.where(high, far_x, near_x)], axis=0
        )
        full = 9 * c1
        acc_a[:full] = terms[:, : 2 * c2]
        acc_a[full:top_a, :c2] = terms[: full // 2, 2 * c2 :]
        acc_a[full:top_a, c2:] = terms[full // 2 :, 2 * c2 :]
        acc_a[top_a : top_a + 8, :c2] = dot_rows(
            jnp.ones((8, planes * 256), bf16), own_ga[:, 256 : (planes + 1) * 256]
        )

    total_a = Reduction(groups_a, True, acc_a, sum_a, send_a, recv_a, sems_a)
    total_a.start()
    total_b.step()
    total_c.step()
    feat_sent[...] = dot_rows(near[...], jnp.concatenate(feats, axis=1)).astype(bf16)
    feat_flying = exchange(feat_sent, feat_came, sems_feat)
    border_ga.wait()

    @pl.when(apart)
    def _():
        for p, thirds in fine_planes(read_ga, inboxes[3], planes):
            for kx, pair in enumerate(thirds):
                for g, tile in enumerate(pair):
                    at = p * 256 + g * 128
                    lines_a[kx * c2 : (kx + 1) * c2, at : at + 128] = tile.astype(bf16)
            if p % 2:
                here = slice((p - 1) * 256, (p + 1) * 256)
                sums_ga[:, here] = dot(mat_ga[...], lines_a[:, here])

    total_b.step()
    total_c.step()
    total_a.step()
    results = []
    for z in range(planes):
        by_row = []
        for ky in range(3):
            value = None
            for kz in range(3):
                at = (kz * 3 + ky) * c1
                term = sums_ga[at : at + c1, (z + kz) * 256 : (z + kz + 1) * 256]
                value = term if value is None else value + term
            by_row.append((value[:, :128], value[:, 128:]))
        before, after = moved_rows(by_row[0], 32)[0], moved_rows(by_row[2], 32)[1]
        results.append([by_row[1][g] + before[g] + after[g] for g in range(2)])
    for g in range(2):
        for z in range(planes):
            stage[pl.ds(z, c1, stride=planes), :] = results[z][g]
        for i in range(4):
            part = stage[:, width * i : width * (i + 1)].astype(bf16)
            grad_in[:, 4 * g + i] = part.reshape(c1, planes, width)

    def together(*totals):
        for _ in zip(*[total.arrivals() for total in totals], strict=True):
            pass

    together(total_b, total_c)
    total_a.step()
    feat_flying.wait()
    came = jnp.transpose(feat_came[...].astype(f32)).astype(bf16)
    ours = dot(came, far[...])
    for y in range(half_rows):
        stage[pl.ds(y, c3, stride=half_rows), :] = ours[:, y * 128 : (y + 1) * 128]
    features[...] = stage[...].astype(bf16)
    together(total_b, total_c)
    total_a.step()
    total_b.step()
    total_c.step()
    total_a.step()


def last_kernel(scales, *refs):
    feat, grad, sum_a, sum_b, out_feat, out_grad, out_wa, out_ba, out_wb, out_bb = refs[:10]
    wa, ba, wb, bb, sems_out = refs[10:]
    f32 = jnp.float32
    scale_a, scale_b = scales
    places = ((grad, out_grad), (feat, out_feat), (wb, out_wb), (bb, out_bb), (wa, out_wa), (ba, out_ba))
    stores = [
        pltpu.make_async_copy(source, target, sems_out.at[at]) for at, (source, target) in enumerate(places)
    ]
    stores[0].start()
    stores[1].start()
    top = wb.shape[0]
    wb[...] = sum_b[:top].astype(f32) * scale_b
    stores[2].start()
    bb[...] = sum_b[top : top + 16].astype(f32)[:1] * scale_b
    stores[3].start()
    c1, c2 = wa.shape[1:]
    deep = 9 * c1
    pairs = sum_a[:deep].astype(f32) * scale_a
    tail = sum_a[deep : deep + deep // 2].astype(f32) * scale_a
    thirds = jnp.concatenate([tail[:, :c2], tail[:, c2:]], axis=0)
    for at in range(9):
        here = slice(at * c1, (at + 1) * c1)
        wa[at * 3] = pairs[here, :c2]
        wa[at * 3 + 1] = pairs[here, c2:]
        wa[at * 3 + 2] = thirds[here]
    stores[4].start()
    top_a = deep + deep // 2
    ba[...] = sum_a[top_a : top_a + 16].astype(f32)[:1, :c2] * scale_a
    stores[5].start()
    for store in stores:
        store.wait()


def all_groups():
    cut = {axis: [2**i for i in range(lax.axis_size(axis).bit_length() - 1)] for axis in ("gz", "gx")}
    line = [("gz", bit) for bit in cut["gz"]]
    return [line[:1], [("gx", bit) for bit in cut["gx"]] + line[1:2], line[2:]]


def on_blocks(volume, weight_a, bias_a, weight_b, bias_b, cotangent, scales):
    f32, bf16 = jnp.float32, jnp.bfloat16
    c1, width, rows, planes = volume.shape
    c2, c3 = weight_b.shape[3:]
    members = lax.axis_size("gz")
    groups = all_groups()
    tiles = planes // 4 + 1
    long, short = (planes + 2) * 256, tiles * 128
    cells = planes * 256
    rows_a, rows_b = 512, 27 * c2 + 64
    fewer = cells // 8

    def buffers(total, groups, exchanged):
        sends, recvs = [], []
        size = total
        for at, group in enumerate(groups):
            n = 2 ** len(group)
            if exchanged and at == len(groups) - 1:
                recvs.append(pltpu.VMEM((n, size, 128), bf16))
                continue
            sends.append(pltpu.VMEM((size, 128), bf16))
            size //= n
            recvs.append(pltpu.VMEM((n - 1, size, 128), bf16))
        return sends + recvs

    inboxes = []
    for size, plane, edge in ((c1, 256, c1), (c2 // 2, 128, c2 // 4), (c3 // 2, 128, c3 // 4), (c2, 256, c2)):
        inboxes += [pltpu.VMEM((size, plane), bf16)] * 2 + [pltpu.VMEM((edge, 128), bf16)] * 3
    groups_a = [groups[0] + groups[1], groups[2]]
    by_level = [2 ** len(group) for group in groups]
    count_a = len(groups_a) + by_level[1]
    count_b = len(groups) + 2 * by_level[2]
    cuts = (1024, rows_b - 1024)
    passed = [
        ((c3 * rows // 2, 128), bf16),
        ((c1, rows, planes, width), bf16),
        ((rows_a, 128), bf16),
        ((rows_b, 128), bf16),
    ]
    operands = (
        jnp.transpose(volume, (0, 2, 3, 1)),
        weight_a.reshape(27, c1, c2),
        bias_a[None],
        weight_b.reshape(27, c2, c3),
        bias_b[None],
        cotangent.reshape(c3 * rows // 2, 128),
    )
    anywhere, inside = pl.BlockSpec(memory_space=pl.ANY), pl.BlockSpec(memory_space=pltpu.VMEM)
    middle = pl.pallas_call(
        functools.partial(block_kernel, (groups, groups_a, cuts)),
        out_shape=[pltpu.VMEM(shape, dtype) for shape, dtype in passed],
        in_specs=[anywhere] * len(operands),
        out_specs=[inside] * len(passed),
        scratch_shapes=[
            *[pltpu.VMEM(x.shape, x.dtype) for x in operands],
            pltpu.VMEM((c1 * planes, 128), f32),
            pltpu.VMEM((c1, cells), bf16),
            pltpu.VMEM((9 * c1, long), bf16),
            pltpu.VMEM((3 * c2, long), f32),
            pltpu.VMEM((c2, cells), f32),
            pltpu.VMEM((2 * tiles * c2, 512), bf16),
            pltpu.VMEM((c2, short), bf16),
            pltpu.VMEM((9 * c2, short), bf16),
            pltpu.VMEM((3 * c3, short), f32),
            pltpu.VMEM((fewer, c3), bf16),
            pltpu.VMEM((fewer, c3), bf16),
            pltpu.VMEM((c3, short), f32),
            pltpu.VMEM((3 * c3, short), bf16),
            pltpu.VMEM((3 * c3, short), bf16),
            pltpu.VMEM((9 * c2, short), f32),
            pltpu.VMEM((3 * c2, long), bf16),
            pltpu.VMEM((3 * c2, long), bf16),
            pltpu.VMEM((9 * c1, long), f32),
            pltpu.VMEM((fewer, c3), bf16),
            pltpu.VMEM((fewer, c3), bf16),
            pltpu.VMEM((3 * c2, 9 * c1), bf16),
            pltpu.VMEM((3 * c3, 9 * c2), bf16),
            pltpu.VMEM((9 * c1, 3 * c2), bf16),
            pltpu.VMEM((9 * c2, 3 * c3), bf16),
            pltpu.VMEM((fewer, short), bf16),
            pltpu.VMEM((fewer, fewer), bf16),
            pltpu.VMEM((512, 128), bf16),
            pltpu.VMEM((rows_a, 128), f32),
            pltpu.VMEM((rows_b, 128), f32),
            *inboxes,
            *[pltpu.VMEM((size, 128), bf16) for size in (c1, c2 // 4, c3 // 4, c2)],
            *[pltpu.VMEM((size // 2, 128), bf16) for size in (c2, c2, c3, c3)],
            *buffers(rows_a, groups_a, True),
            *buffers(cuts[0], groups, False),
            *buffers(cuts[1], groups, False),
            *[pltpu.SemaphoreType.DMA((20,))] * 2,
            *[pltpu.SemaphoreType.DMA((1,))] * 4,
            *[pltpu.SemaphoreType.DMA((n,)) for n in (len(groups_a) + 1, count_a)],
            *[pltpu.SemaphoreType.DMA((n,)) for n in (len(groups) + 1, count_b)] * 2,
            pltpu.SemaphoreType.DMA((len(operands),)),
        ],
        compiler_params=pltpu.CompilerParams(
            collective_id=2, has_side_effects=True, vmem_limit_bytes=60 * 2**20
        ),
    )(*operands)
    outs = [
        *passed[:2],
        ((27, c1, c2), f32),
        ((1, c2), f32),
        ((27 * c2, c3), f32),
        ((1, c3), f32),
    ]
    features, grad_in, sum_wa, sum_ba, sum_wb, sum_bb = pl.pallas_call(
        functools.partial(last_kernel, scales),
        out_shape=[jax.ShapeDtypeStruct(shape, dtype) for shape, dtype in outs],
        in_specs=[inside] * len(passed),
        out_specs=[anywhere] * len(outs),
        scratch_shapes=[
            *[pltpu.VMEM(shape, dtype) for shape, dtype in outs[2:]],
            pltpu.SemaphoreType.DMA((len(outs),)),
        ],
    )(*[pltpu.with_memory_space_constraint(x, pltpu.VMEM) for x in middle])
    return (
        features.reshape(cotangent.shape),
        jnp.transpose(grad_in, (0, 3, 1, 2)),
        sum_wa.reshape(weight_a.shape),
        sum_ba.reshape(c2),
        sum_wb.reshape(weight_b.shape),
        sum_bb.reshape(c3),
    )


def fits_blocks(volume, weight_b):
    c1, width, rows, planes = volume.shape
    sizes = {axis: lax.axis_size(axis) for axis in ("gx", "gy", "gz")}
    return (
        sizes == {"gx": 2, "gy": 1, "gz": planes}
        and (width, rows, planes) == (32, 8, 16)
        and (c1, *weight_b.shape[3:]) == (32, 64, 128)
    )


def on_device(volume, weight_a, bias_a, weight_b, bias_b, cotangent):
    f32, bf16 = jnp.float32, jnp.bfloat16
    count = lax.axis_size("gz")
    devices_all = lax.axis_size("gx") * lax.axis_size("gy") * count
    c1, nx, rows, nz = volume.shape
    cells = nx * rows * nz
    scale_a = 1.0 / math.sqrt(cells * devices_all)
    scale_b = 1.0 / math.sqrt(cells * devices_all // 8)
    c2, c3 = weight_b.shape[3:]
    if fits_blocks(volume, weight_b):
        return on_blocks(volume, weight_a, bias_a, weight_b, bias_b, cotangent, (scale_a, scale_b))
    planes, depth = nx // count, nz * count
    fine = (planes, rows, depth)
    coarse = (planes // 2, rows // 2, depth // 2)
    fewer = cells // 8
    pool = (jnp.arange(depth)[:, None] // 2 == jnp.arange(depth // 2)[None]).astype(f32)
    work_a = 2 * 27 * c1 * c2 * cells
    work_b = 2 * 27 * c2 * c3 * fewer

    slab = lax.all_to_all(volume, "gz", split_axis=1, concat_axis=3, tiled=True).reshape(c1, cells)
    if lax.axis_size("gy") == 1:
        features, grad_slab, sum_wa, sum_ba, sum_wb, sum_bb = between_exchanges(
            fine,
            coarse,
            (scale_a, scale_b),
            slab,
            weight_a,
            bias_a,
            weight_b,
            bias_b,
            cotangent.reshape(c3, fewer),
            pool,
        )
    else:
        wide_a = widened(slab, *fine)
        before_a, pooled = local_kernel(
            functools.partial(forward_a_kernel, fine),
            [((c2, cells), f32), ((c2, fewer), bf16)],
            (27 * c1, cells),
            work_a,
            wide_a,
            outward(weight_a),
            bias_a[:, None],
            pool,
        )
        wide_b = widened(pooled, *coarse)
        features, grad_b, part_wb, part_bb = local_kernel(
            functools.partial(middle_kernel, coarse),
            [((c3, fewer), bf16), ((c3, fewer), bf16), ((27 * c2, c3), f32), ((8, c3), f32)],
            (27 * c2, fewer),
            2 * work_b,
            wide_b,
            outward(weight_b),
            bias_b[:, None],
            cotangent.reshape(c3, fewer),
        )
        (grad_a,) = local_kernel(
            functools.partial(backward_b_kernel, coarse, fine),
            [((c2, cells), bf16)],
            (27 * c3, fewer),
            work_b,
            widened(grad_b, *coarse),
            inward(weight_b),
            before_a,
            pool.T.astype(bf16),
        )
        part_wa, part_ba = local_kernel(
            functools.partial(weight_a_kernel, fine),
            [((27 * c1, c2), f32), ((8, c2), f32)],
            (27 * c1, cells),
            work_a,
            wide_a,
            grad_a,
        )
        (grad_slab,) = local_kernel(
            functools.partial(backward_a_kernel, fine),
            [((c1, cells), bf16)],
            (27 * c2, cells),
            work_a,
            widened(grad_a, *fine),
            inward(weight_a),
        )
        sum_wa, sum_ba, sum_wb, sum_bb = summed_grads(
            part_wa, part_ba, part_wb, part_bb, (scale_a, scale_b)
        )
    grad_input = lax.all_to_all(
        grad_slab.reshape(c1, planes, rows, depth), "gz", split_axis=3, concat_axis=1, tiled=True
    )
    return (
        features.reshape(cotangent.shape),
        grad_input,
        sum_wa.reshape(weight_a.shape),
        sum_ba.reshape(c2),
        sum_wb.reshape(weight_b.shape),
        sum_bb.reshape(c3),
    )


def solution(mesh):
    return jax.shard_map(
        on_device,
        mesh=mesh,
        in_specs=(P(None, "gx", "gy", "gz"), P(), P(), P(), P(), P(None, ("gx", "gz"), "gy", None)),
        out_specs=(
            P(None, ("gx", "gz"), "gy", None),
            P(None, "gx", "gy", "gz"),
            P(),
            P(),
            P(),
            P(),
        ),
        check_vma=False,
    )
```
